8 devices in a mesh: tp: 4 (over z, y, x), cp: 2 (over core).
Axes of the slice: x: 2, y: 2, z: 1, core: 2. Of those that a mesh axis runs over, the one named last changes fastest.
Arguments:
- tokens: int32 [2048], P('cp')
- pos: int32 [2048], P('cp')
- doc_id: int32 [2048], P('cp')
- dy: bfloat16 [2048, 2048], P('cp')
- table: bfloat16 [92544, 2048], P('tp')
- w_q: bfloat16 [2048, 2048], P(None, 'tp')
- w_k: bfloat16 [2048, 1024], P(None, 'tp')
- w_v: bfloat16 [2048, 1024], P(None, 'tp')
- w_o: bfloat16 [2048, 2048], P('tp')
- w_gate: bfloat16 [2048, 8192], P(None, 'tp')
- w_up: bfloat16 [2048, 8192], P(None, 'tp')
- w_down: bfloat16 [8192, 2048], P('tp')
- gain_one: bfloat16 [2048], replicated
- gain_two: bfloat16 [2048], replicated
- inv_freq: float32 [64], replicated
Outputs:
- output 1: bfloat16 [2048, 2048], P('cp')
- output 2: float32 [92544, 2048], P('tp')
- output 3: float32 [2048, 2048], P(None, 'tp')
- output 4: float32 [2048, 1024], P(None, 'tp')
- output 5: float32 [2048, 1024], P(None, 'tp')
- output 6: float32 [2048, 2048], P('tp')
- output 7: float32 [2048, 8192], P(None, 'tp')
- output 8: float32 [2048, 8192], P(None, 'tp')
- output 9: float32 [8192, 2048], P('tp')
- output 10: float32 [2048], replicated
- output 11: float32 [2048], replicated
All inputs are finite; a program needn't handle non-finite values.
Results may differ from the reference program's by a relative error of at most 0.014724.
Values are sent between devices in bfloat16 or wider.
A program may use at most 1.5 GiB of HBM per device.

```python
import math
import jax
import jax.numpy as jnp
from jax import lax

VOCAB = 92544
MODEL_DIM = 2048
HEADS = 16
KV_HEADS = 8
HEAD_DIM = 128
FFN_DIM = 8192
TOK_BLOCK = 512
CP_SIZE = 2

TOKENS = 2 * CP_SIZE * TOK_BLOCK
GROUP = HEADS // KV_HEADS
HOT_COUNT = 2 ** 5
NORM_EPS = 1e-5
SCORE_SCALE = HEAD_DIM ** -0.5
NEG_BIG = -1e30


def slot_sequence():
    slot = jnp.arange(TOKENS)
    shard = slot // (2 * TOK_BLOCK)
    within = slot % (2 * TOK_BLOCK)
    block_no = jnp.where(within < TOK_BLOCK, shard, 2 * CP_SIZE - 1 - shard)
    return block_no * TOK_BLOCK + within % TOK_BLOCK


def draw_layout(key):
    keys = jax.random.split(key, 5)
    seq_pos = slot_sequence()
    cuts = jax.random.randint(keys[0], (CP_SIZE,), 1, TOKENS)
    after_cut = cuts[None, :] <= seq_pos[:, None]
    doc_id = jnp.sum(after_cut.astype(jnp.int32), axis=1)
    doc_start = jnp.max(jnp.where(after_cut, cuts[None, :], 0), axis=1)
    pos = (seq_pos - doc_start).astype(jnp.int32)
    hot_ids = jax.random.randint(keys[1], (HOT_COUNT,), 0, VOCAB // 8)
    hot_pick = jax.random.randint(keys[2], (TOKENS,), 0, HOT_COUNT)
    spread_ids = jax.random.randint(keys[3], (TOKENS,), 0, VOCAB)
    use_hot = jax.random.randint(keys[4], (TOKENS,), 0, 2)
    tokens = jnp.where(use_hot == 1, hot_ids[hot_pick], spread_ids)
    tokens = tokens.at[0].set(0).at[1].set(VOCAB - 1)
    return tokens, pos, doc_id.astype(jnp.int32)


def setup_inputs(seed: int = 0) -> dict:
    base = jax.random.key(seed)
    tokens, pos, doc_id = draw_layout(jax.random.fold_in(base, 1))
    keys = jax.random.split(jax.random.fold_in(base, 2), 14)

    def weight(which, fan_in, fan_out):
        return (jax.random.normal(keys[which], (fan_in, fan_out), jnp.float32) * fan_in ** -0.5).astype(jnp.bfloat16)

    def gain(which):
        return (1.0 + 0.25 * jax.random.normal(keys[which], (MODEL_DIM,), jnp.float32)).astype(jnp.bfloat16)

    log_theta = jax.random.uniform(keys[11], (), jnp.float32, math.log(1e4), math.log(5e5))
    exponent = jnp.arange(HEAD_DIM // 2, dtype=jnp.float32) * (2.0 / HEAD_DIM)
    jitter = jax.random.uniform(keys[12], (HEAD_DIM // 2,), jnp.float32, 0.9, 1.1)
    return {
        "tokens": tokens,
        "pos": pos,
        "doc_id": doc_id,
        "dy": jax.random.normal(keys[0], (TOKENS, MODEL_DIM), jnp.float32).astype(jnp.bfloat16),
        "table": jax.random.normal(keys[1], (VOCAB, MODEL_DIM), jnp.float32).astype(jnp.bfloat16),
        "w_q": weight(2, MODEL_DIM, HEADS * HEAD_DIM),
        "w_k": weight(3, MODEL_DIM, KV_HEADS * HEAD_DIM),
        "w_v": weight(4, MODEL_DIM, KV_HEADS * HEAD_DIM),
        "w_o": weight(5, HEADS * HEAD_DIM, MODEL_DIM),
        "w_gate": weight(6, MODEL_DIM, FFN_DIM),
        "w_up": weight(7, MODEL_DIM, FFN_DIM),
        "w_down": weight(8, FFN_DIM, MODEL_DIM),
        "gain_one": gain(9),
        "gain_two": gain(10),
        "inv_freq": jnp.exp(-log_theta * exponent) * jitter,
    }


def to_bf16(feats):
    return feats.astype(jnp.bfloat16).astype(jnp.float32)


def rms_norm(feats, gain_vec):
    return feats * lax.rsqrt(jnp.mean(feats * feats, axis=-1, keepdims=True) + NORM_EPS) * gain_vec


def rotate(tensor_in, cosine, sine):
    half = tensor_in.shape[-1] // 2
    first = tensor_in[..., :half]
    second = tensor_in[..., half:]
    return jnp.concatenate([first * cosine - second * sine, second * cosine + first * sine], axis=-1)


def forward_pass(params, tokens, pos, doc_id, inv_freq):
    table, w_q, w_k, w_v, w_o, w_gate, w_up, w_down, gain_one, gain_two = params
    embed = jnp.take(table, tokens, axis=0)
    act_one = to_bf16(rms_norm(embed, gain_one))
    angle = pos.astype(jnp.float32)[:, None, None] * inv_freq
    cosine = jnp.cos(angle)
    sine = jnp.sin(angle)
    query = jnp.dot(act_one, w_q, preferred_element_type=jnp.float32).reshape(TOKENS, HEADS, HEAD_DIM)
    query = to_bf16(rotate(query, cosine, sine)).reshape(2 * CP_SIZE, TOK_BLOCK, KV_HEADS, GROUP, HEAD_DIM)
    key_all = jnp.dot(act_one, w_k, preferred_element_type=jnp.float32).reshape(TOKENS, KV_HEADS, HEAD_DIM)
    key_all = to_bf16(rotate(key_all, cosine, sine))
    value_all = to_bf16(jnp.dot(act_one, w_v, preferred_element_type=jnp.float32)).reshape(TOKENS, KV_HEADS, HEAD_DIM)
    seq_pos = slot_sequence()

    def attend(block):
        query_blk, seq_blk, doc_blk = block
        scores = jnp.einsum("qkgd,skd->kgqs", query_blk, key_all) * SCORE_SCALE
        allowed = (doc_blk[:, None] == doc_id[None, :]) & (seq_pos[None, :] <= seq_blk[:, None])
        attn_prob = jax.nn.softmax(jnp.where(allowed, scores, NEG_BIG), axis=-1)
        return jnp.einsum("kgqs,skd->qkgd", to_bf16(attn_prob), value_all)

    blocks = (query, seq_pos.reshape(2 * CP_SIZE, TOK_BLOCK), doc_id.reshape(2 * CP_SIZE, TOK_BLOCK))
    attended = to_bf16(lax.map(jax.checkpoint(attend), blocks)).reshape(TOKENS, HEADS * HEAD_DIM)
    residual = embed + jnp.dot(attended, w_o, preferred_element_type=jnp.float32)
    act_two = to_bf16(rms_norm(residual, gain_two))
    gate = jnp.dot(act_two, w_gate, preferred_element_type=jnp.float32)
    hidden = to_bf16(jax.nn.silu(gate) * jnp.dot(act_two, w_up, preferred_element_type=jnp.float32))
    return residual + jnp.dot(hidden, w_down, preferred_element_type=jnp.float32)


def reference(tokens, pos, doc_id, dy, table, w_q, w_k, w_v, w_o, w_gate, w_up, w_down, gain_one, gain_two, inv_freq):
    params = tuple(weight.astype(jnp.float32) for weight in (table, w_q, w_k, w_v, w_o, w_gate, w_up, w_down, gain_one, gain_two))
    layer_out, pullback = jax.vjp(lambda *weights: forward_pass(weights, tokens, pos, doc_id, inv_freq), *params)
    grads = pullback(dy.astype(jnp.float32))
    return (layer_out.astype(jnp.bfloat16), grads[0], grads[1], grads[2], grads[3], grads[4], grads[5], grads[6], grads[7], grads[8], grads[9])
```

```python
import functools

import jax
import jax.numpy as jnp
from jax import lax
from jax.experimental import pallas as pl
from jax.experimental.pallas import tpu as pltpu
from jax.sharding import PartitionSpec as P

NORM_EPS = 1e-5
NEG_BIG = -1e30
F32 = jnp.float32
BF16 = jnp.bfloat16
MIB = 2**20
LOCAL_VMEM = 56 * MIB
REMOTE_VMEM = 63 * MIB
STEPS = 4
SUBLANES = 8
ROW_BLOCK = 32
WIDE_TILE = 512
MESH_ID = pl.DeviceIdType.MESH
NT = (((1,), (1,)), ((), ()))
CONTRACT_FIRST = (((0,), (0,)), ((), ()))
VMEM = pl.BlockSpec(memory_space=pltpu.VMEM)
SMEM = pl.BlockSpec(memory_space=pltpu.SMEM)
HBM = pl.BlockSpec(memory_space=pl.ANY)
DMA = pltpu.SemaphoreType.DMA


X_PAIRS, Y_PAIRS = ([(chip, chip ^ flip) for chip in range(4)] for flip in (1, 2))
C_PAIRS = X_PAIRS[:2]
CORE_PAIRS = tuple([(2 * a + core, 2 * b + core) for core, pairs in enumerate(kinds) for a, b in pairs] for kinds in ((Y_PAIRS, X_PAIRS), (X_PAIRS, Y_PAIRS)))


def swap_x(v):
    return lax.ppermute(v, "tp", X_PAIRS)


def swap_y(v):
    return lax.ppermute(v, "tp", Y_PAIRS)


def swap_c(v):
    return lax.ppermute(v, "cp", C_PAIRS)


def swap_core(v, which):
    return lax.ppermute(v, ("tp", "cp"), CORE_PAIRS[which])


def cost(gflops, mib):
    return pl.CostEstimate(flops=gflops * 10**9, bytes_accessed=mib * MIB, transcendentals=0)


def shape(rows, cols, dtype=BF16):
    return jax.ShapeDtypeStruct((rows, cols), dtype)


ZERO_ROWS = 96
ZERO_FIRST = 25
ZERO_ATTEND = (6, 18)
ZERO_BACK = (10, 20)


def zero_block(out_ref, block, count=1):
    return out_ref.at[pl.ds(pl.multiple_of(block * ZERO_ROWS, ZERO_ROWS), count * ZERO_ROWS)]


def clear(ref, value=0.0):
    ref[...] = jnp.full(ref.shape, value, F32)


def start_zeros(out_ref, zero_ref, sem, first, count):
    for i in range(count):
        pltpu.make_async_copy(zero_ref, zero_block(out_ref, first + i), sem).start()


def wait_zeros(out_ref, sem, first, count):
    whole = zero_block(out_ref, first, count)
    pltpu.make_async_copy(whole, whole, sem).wait()


def zero_scratch(width):
    return [pltpu.VMEM((ZERO_ROWS, width), F32), DMA]


def grid_zeros(grad_ref, zero_ref, sem, before, early, late):
    head, tile = pl.program_id(0), pl.program_id(1)
    heads, tiles = pl.num_programs(0), pl.num_programs(1)
    half = tiles // 2
    whole = half * (early + late)
    pl.when((head == 0) & (tile == 0))(functools.partial(clear, zero_ref))
    first = before + head * whole + tile * early + jnp.maximum(tile - half, 0) * (late - early)
    start_zeros(grad_ref, zero_ref, sem, first, early)
    pl.when(tile >= half)(functools.partial(start_zeros, grad_ref, zero_ref, sem, first + early, late - early))
    last = (head == heads - 1) & (tile == tiles - 1)
    return lambda: pl.when(last)(lambda: wait_zeros(grad_ref, sem, before, heads * whole))


GATHER_BATCH = 16
GATHER_SLOTS = 8


def pick_body(group_ref, count_ref, lane_ref, table_ref, out_ref, grad_ref, buf, sems, zero_ref, zero_sem):
    batches = out_ref.shape[0] // GATHER_BATCH

    def row_copy(group, slot, j):
        return pltpu.make_async_copy(table_ref.at[group], buf.at[slot, j], sems.at[slot])

    def start(step):
        slot = lax.rem(step, GATHER_SLOTS)
        for j in range(GATHER_BATCH):
            group = group_ref[step * GATHER_BATCH + j]
            pl.when(group >= 0)(lambda: row_copy(group, slot, j).start())

    buf[...] = jnp.zeros(buf.shape, BF16)
    clear(zero_ref)
    for step in range(GATHER_SLOTS - 1):
        start(step)
    start_zeros(grad_ref, zero_ref, zero_sem, 0, ZERO_FIRST)

    def loop(step, carry):
        slot = lax.rem(step, GATHER_SLOTS)

        @pl.when(step + GATHER_SLOTS - 1 < batches)
        def _():
            start(step + GATHER_SLOTS - 1)

        def arrived(i, carry):
            row_copy(0, slot, 0).wait()
            return carry

        lax.fori_loop(0, count_ref[step], arrived, 0)
        first = pl.multiple_of(step * GATHER_BATCH, GATHER_BATCH)
        want = lane_ref[pl.ds(first, GATHER_BATCH), :]
        lanes = lax.broadcasted_iota(jnp.int32, (GATHER_BATCH, GATHER_BATCH * SUBLANES), 1)
        choose = (lanes == want).astype(BF16)
        rows = buf[slot].reshape(GATHER_BATCH * SUBLANES, buf.shape[-1])
        out_ref[pl.ds(first, GATHER_BATCH), :] = jnp.dot(choose, rows, preferred_element_type=F32).astype(BF16)
        return carry

    lax.fori_loop(0, batches, loop, 0)
    wait_zeros(grad_ref, zero_sem, 0, ZERO_FIRST)


def pick_rows(tokens, table, base):
    span = tokens.shape[0]
    rows, width = table.shape
    local = tokens - base
    owned = (local >= 0) & (local < rows)
    slot_no = jnp.arange(span, dtype=jnp.int32)
    group = jnp.where(owned, local // SUBLANES, -1)
    count = jnp.sum(owned.reshape(-1, GATHER_BATCH).astype(jnp.int32), axis=1)
    lane = jnp.where(owned, local % SUBLANES + (slot_no % GATHER_BATCH) * SUBLANES, -1)
    return pl.pallas_call(
        pick_body,
        out_shape=[shape(span, width), shape(rows, width, F32)],
        in_specs=[SMEM, SMEM, VMEM, HBM],
        out_specs=[VMEM, HBM],
        scratch_shapes=[pltpu.VMEM((GATHER_SLOTS, GATHER_BATCH, SUBLANES, width), BF16), DMA((GATHER_SLOTS,))] + zero_scratch(width),
        compiler_params=pltpu.CompilerParams(vmem_limit_bytes=LOCAL_VMEM),
        cost_estimate=cost(20, 40),
        name="pick_rows",
    )(group, count, lane[:, None], table.reshape(rows // SUBLANES, SUBLANES, width))


SEMS = 32


def put_body(ids_ref, perm_ref, range_ref, all_ref, zero_ref, out_ref, rows_ref, load_sem, sems):
    load = pltpu.make_async_copy(all_ref, rows_ref, load_sem)
    load.start()
    low, high, base = range_ref[0], range_ref[1], range_ref[2]
    load.wait()

    def wait_slot(slot):
        pltpu.make_async_copy(rows_ref.at[pl.ds(0, 1), :], out_ref.at[pl.ds(0, 1), :], sems.at[slot]).wait()

    def loop(pos, carry):
        running, joined, count = carry
        row_id = ids_ref[pos]
        at = pl.ds(perm_ref[pos], 1)
        more = (pos + 1 < high) & (ids_ref[jnp.minimum(pos + 1, high - 1)] == row_id)
        running = rows_ref[at, :] + jnp.where(joined, running, 0.0)

        @pl.when(jnp.logical_not(more))
        def _():
            slot = lax.rem(count, SEMS)

            @pl.when(joined)
            def _():
                rows_ref[at, :] = running

            @pl.when(count >= SEMS)
            def _():
                wait_slot(slot)

            pltpu.make_async_copy(rows_ref.at[at, :], out_ref.at[pl.ds(row_id - base, 1), :], sems.at[slot]).start()

        return running, more, count + jnp.where(more, 0, 1)

    start = (jnp.zeros((1, rows_ref.shape[1]), F32), jnp.bool_(False), jnp.int32(0))
    _, _, count = lax.fori_loop(low, high, loop, start)

    def drain(slot, carry):
        @pl.when(slot < count)
        def _():
            wait_slot(slot)

        return carry

    lax.fori_loop(0, SEMS, drain, 0)


def put_rows(ids, perm, bounds, rows, zeros):
    return pl.pallas_call(
        put_body,
        out_shape=shape(*zeros.shape, F32),
        in_specs=[SMEM, SMEM, SMEM, HBM, HBM],
        out_specs=HBM,
        scratch_shapes=[pltpu.VMEM(rows.shape, F32), DMA, DMA((SEMS,))],
        input_output_aliases={4: 0},
        compiler_params=pltpu.CompilerParams(vmem_limit_bytes=LOCAL_VMEM),
        cost_estimate=cost(20, 40),
        name="put_rows",
    )(ids, perm, bounds, rows, zeros)


Q_TILE = 256
K_TILE = 512


def stack_heads(v):
    half = v.shape[1] // 2
    return jnp.concatenate([v[:, :half], v[:, half:]], axis=0)


def unstack_heads(v):
    half = v.shape[0] // 2
    return jnp.concatenate([v[:half], v[half:]], axis=1)


def for_blocks(tile, cp, visit):
    early = tile < (K_TILE // Q_TILE)
    late = jnp.logical_not(early)
    visit(0, None)
    for block, needed in ((1, late), (2, late | (cp == 1)), (3, late & (cp == 0))):
        pl.when(needed)(functools.partial(visit, block, needed))


def block_refs(block, own_ref, other_ref):
    ref = own_ref if block < 2 else other_ref
    return ref, pl.ds((block % 2) * K_TILE, K_TILE)


def masked_scores(scale, q, k, q_low, q_high, k_seq):
    scores = lax.dot_general(q, k, NT, preferred_element_type=F32) * scale
    allowed = (k_seq >= q_low) & (k_seq <= q_high)
    return jnp.where(allowed, scores, NEG_BIG)


def attend_body(scale, info_ref, q_ref, k_ref, v_ref, k2_ref, v2_ref, low_ref, high_ref, seq_ref, zeros_in, out_ref, lse_ref, grad_ref, s_ref, m_ref, l_ref, acc_ref, zero_ref, zero_sem):
    end_zeros = grid_zeros(grad_ref, zero_ref, zero_sem, ZERO_FIRST, *ZERO_ATTEND)
    tile = pl.program_id(1)
    cp = info_ref[0]
    q = stack_heads(q_ref[...])
    q_low = jnp.concatenate([low_ref[...], low_ref[...]], axis=0)
    q_high = jnp.concatenate([high_ref[...], high_ref[...]], axis=0)
    clear(m_ref, NEG_BIG)
    clear(l_ref)
    clear(acc_ref)

    def score(block, needed):
        ref, rows = block_refs(block, k_ref, k2_ref)
        s = masked_scores(scale, q, ref[rows, :], q_low, q_high, seq_ref[:, block * K_TILE : (block + 1) * K_TILE])
        s_ref[block] = s
        m_ref[...] = jnp.maximum(m_ref[...], jnp.max(s, axis=1, keepdims=True))

    for_blocks(tile, cp, score)

    def exponent(block, needed):
        e = jnp.exp(s_ref[block] - m_ref[...])
        s_ref[block] = e
        l_ref[...] += jnp.sum(e, axis=1, keepdims=True)

    for_blocks(tile, cp, exponent)
    inverse = 1.0 / l_ref[...]

    def mix(block, needed):
        ref, rows = block_refs(block, v_ref, v2_ref)
        prob = (s_ref[block] * inverse).astype(BF16)
        acc_ref[...] += jnp.dot(prob, ref[rows, :], preferred_element_type=F32)

    for_blocks(tile, cp, mix)
    out_ref[...] = unstack_heads(acc_ref[...].astype(BF16))
    lse_ref[...] = (m_ref[...] + jnp.log(l_ref[...])).reshape(lse_ref.shape)
    end_zeros()


def attention_specs(span, head_dim):
    tile = pl.BlockSpec((Q_TILE, 2 * head_dim), lambda h, t: (t, h))
    keys = pl.BlockSpec((span, head_dim), lambda h, t: (0, h))
    bound = pl.BlockSpec((Q_TILE, 1), lambda h, t: (t, 0))
    seq = pl.BlockSpec((1, 2 * span), lambda h, t: (0, 0))
    lse = pl.BlockSpec((1, 1, 2 * Q_TILE, 1), lambda h, t: (h, t, 0, 0))
    return tile, keys, bound, seq, lse


def attend(scale, info, q, k, v, k2, v2, low, high, seq, grad):
    span = q.shape[0]
    head_dim = k.shape[1] // 2
    tile, keys, bound, seq_spec, lse = attention_specs(span, head_dim)
    stacked = 2 * Q_TILE
    return pl.pallas_call(
        functools.partial(attend_body, scale),
        grid=(2, span // Q_TILE),
        out_shape=[shape(*q.shape), jax.ShapeDtypeStruct((2, span // Q_TILE, stacked, 1), F32), shape(*grad.shape, F32)],
        in_specs=[SMEM, tile, keys, keys, keys, keys, bound, bound, seq_spec, HBM],
        out_specs=[tile, lse, HBM],
        scratch_shapes=[pltpu.VMEM((4, stacked, K_TILE), F32), pltpu.VMEM((stacked, 1), F32), pltpu.VMEM((stacked, 1), F32), pltpu.VMEM((stacked, head_dim), F32)] + zero_scratch(grad.shape[1]),
        input_output_aliases={9: 2},
        compiler_params=pltpu.CompilerParams(vmem_limit_bytes=LOCAL_VMEM),
        cost_estimate=cost(14, 4),
        name="attend",
    )(info, q, k, v, k2, v2, low, high, seq, grad)


def attend_back_body(scale, info_ref, q_ref, do_ref, lse_ref, k_ref, v_ref, k2_ref, v2_ref, low_ref, high_ref, seq_ref, zeros_in, dq_ref, dk_ref, dv_ref, dk2_ref, dv2_ref, grad_ref, p_ref, dp_ref, d_ref, acc_ref, zero_ref, zero_sem):
    steps = pl.num_programs(0) * pl.num_programs(1)
    end_zeros = grid_zeros(grad_ref, zero_ref, zero_sem, ZERO_FIRST + steps // 2 * sum(ZERO_ATTEND), *ZERO_BACK)
    tile = pl.program_id(1)
    cp = info_ref[0]
    q = stack_heads(q_ref[...])
    d_out = stack_heads(do_ref[...])
    q_low = jnp.concatenate([low_ref[...], low_ref[...]], axis=0)
    q_high = jnp.concatenate([high_ref[...], high_ref[...]], axis=0)
    lse = lse_ref[...].reshape(q.shape[0], 1)
    clear(d_ref)
    clear(acc_ref)

    @pl.when(tile == 0)
    def _():
        for ref in (dk_ref, dv_ref, dk2_ref, dv2_ref):
            clear(ref)

    def first(block, needed):
        k_block, rows = block_refs(block, k_ref, k2_ref)
        v_block, _ = block_refs(block, v_ref, v2_ref)
        s = masked_scores(scale, q, k_block[rows, :], q_low, q_high, seq_ref[:, block * K_TILE : (block + 1) * K_TILE])
        p = jnp.exp(s - lse)
        dp = lax.dot_general(d_out, v_block[rows, :], NT, preferred_element_type=F32).astype(BF16)
        p_ref[block] = p
        dp_ref[block] = dp
        d_ref[...] += jnp.sum(p * dp.astype(F32), axis=1, keepdims=True)

    for_blocks(tile, cp, first)

    def second(block, needed):
        k_block, rows = block_refs(block, k_ref, k2_ref)
        dk_block, _ = block_refs(block, dk_ref, dk2_ref)
        dv_block, _ = block_refs(block, dv_ref, dv2_ref)
        p = p_ref[block]
        ds = (p * (dp_ref[block].astype(F32) - d_ref[...]) * scale).astype(BF16)
        acc_ref[...] += jnp.dot(ds, k_block[rows, :], preferred_element_type=F32)
        dk_block[rows, :] += lax.dot_general(ds, q, CONTRACT_FIRST, preferred_element_type=F32)
        dv_block[rows, :] += lax.dot_general(p.astype(BF16), d_out, CONTRACT_FIRST, preferred_element_type=F32)

    for_blocks(tile, cp, second)
    dq_ref[...] = unstack_heads(acc_ref[...].astype(BF16))
    end_zeros()


def attend_back(scale, info, q, d_out, lse, k, v, k2, v2, low, high, seq, grad):
    span = q.shape[0]
    head_dim = k.shape[1] // 2
    tile, keys, bound, seq_spec, lse_spec = attention_specs(span, head_dim)
    stacked = 2 * Q_TILE
    return pl.pallas_call(
        functools.partial(attend_back_body, scale),
        grid=(2, span // Q_TILE),
        out_shape=[shape(*q.shape)] + [shape(*k.shape, F32)] * 4 + [shape(*grad.shape, F32)],
        in_specs=[SMEM, tile, tile, lse_spec, keys, keys, keys, keys, bound, bound, seq_spec, HBM],
        out_specs=[tile, keys, keys, keys, keys, HBM],
        scratch_shapes=[pltpu.VMEM((4, stacked, K_TILE), F32), pltpu.VMEM((4, stacked, K_TILE), BF16), pltpu.VMEM((stacked, 1), F32), pltpu.VMEM((stacked, head_dim), F32)] + zero_scratch(grad.shape[1]),
        input_output_aliases={11: 5},
        compiler_params=pltpu.CompilerParams(vmem_limit_bytes=LOCAL_VMEM),
        cost_estimate=cost(30, 8),
        name="attend_back",
    )(info, q, d_out, lse, k, v, k2, v2, low, high, seq, grad)


def rows_at(start, size, step=32):
    return pl.ds(pl.multiple_of(start, step), size)


def remote(src, dst, send, recv, device):
    return pltpu.make_async_remote_copy(src_ref=src, dst_ref=dst, send_sem=send, recv_sem=recv, device_id=device, device_id_type=MESH_ID)


def flipped(bit, flip):
    return bit + flip - 2 * bit * flip


class Place:
    def __init__(self):
        self.tp = lax.axis_index("tp")
        self.cp = lax.axis_index("cp")
        self.x = lax.rem(self.tp, 2)
        self.y = lax.div(self.tp, 2)
        self.over_x = (self.chip(1, 0), self.cp)
        self.over_y = (self.chip(0, 1), self.cp)
        self.twin = (self.tp, 1 - self.cp)

    def chip(self, dx, dy):
        return 2 * flipped(self.y, dy) + flipped(self.x, dx)

    def meet(self):
        barrier = pltpu.get_barrier_semaphore()
        peers = (self.over_x, self.over_y, self.twin)
        for device in peers:
            pl.semaphore_signal(barrier, inc=1, device_id=device, device_id_type=MESH_ID)
        pl.semaphore_wait(barrier, len(peers))


class Total:
    def __init__(self, place, part, wide, mid, narrow, out, send, recv):
        self.part, self.wide, self.mid, self.narrow, self.out = part, wide, mid, narrow, out
        self.send, self.recv = send, recv
        self.rows = out.shape[0] // STEPS
        self.half, self.quarter, self.eighth = (self.rows // n for n in (2, 4, 8))
        self.kinds = [(place.x, place.y, place.over_x, place.over_y), (place.y, place.x, place.over_y, place.over_x)]

    def _rows(self, step, kind):
        first, second = self.kinds[kind][:2]
        side = step * self.rows + kind * self.half + first * self.quarter
        return rows_at(side, self.quarter), rows_at(side + second * self.eighth, self.eighth)

    def _kept(self, kind, flip=0):
        return rows_at(kind * self.half + flipped(self.kinds[kind][0], flip) * self.quarter, self.quarter)

    def _eighth(self, kind, flip=0):
        return rows_at(flipped(self.kinds[kind][1], flip) * self.eighth, self.eighth)

    def _copy(self, step, kind, stage):
        side, mine = self._rows(step, kind)
        _, _, peer_first, peer_second = self.kinds[kind]
        src, dst, peer = (
            lambda: (self.part(step).at[self._kept(kind, 1)], self.wide.at[step, kind], peer_first),
            lambda: (self.mid.at[step, kind, self._eighth(kind, 1)], self.narrow.at[step, kind], peer_second),
            lambda: (self.out.at[mine], self.out.at[mine], peer_second),
            lambda: (self.out.at[side], self.out.at[side], peer_first),
        )[stage]()
        return remote(src, dst, self.send.at[step, kind, stage], self.recv.at[step, kind, stage], peer)

    def begin(self, step):
        for kind in range(2):
            self._copy(step, kind, 0).start()

    def fold_wide(self, step):
        for kind in range(2):
            self._copy(step, kind, 0).wait_recv()
            self.mid[step, kind] = self.part(step)[self._kept(kind), :] + self.wide[step, kind]
            self._copy(step, kind, 1).start()

    def fold_narrow(self, step):
        for kind in range(2):
            self._copy(step, kind, 1).wait_recv()
            total = self.mid[step, kind, self._eighth(kind), :] + self.narrow[step, kind]
            self.out[self._rows(step, kind)[1], :] = total.astype(BF16)
            self._copy(step, kind, 2).start()

    def widen(self, step):
        for kind in range(2):
            self._copy(step, kind, 2).wait_recv()
            self._copy(step, kind, 3).start()

    def finish(self, step):
        for kind in range(2):
            self._copy(step, kind, 3).wait_recv()

    def sent(self, step, stages):
        for kind in range(2):
            for stage in stages:
                self._copy(step, kind, stage).wait_send()

    def advance(self, tick):
        for lag, stage in enumerate((self.fold_wide, self.fold_narrow, self.widen)):
            if 0 <= tick - lag < STEPS:
                stage(tick - lag)


def total_scratch(width, dtype, rows):
    sems = DMA((STEPS, 2, 4))
    part = lambda n: pltpu.VMEM((STEPS, 2, rows // n, width), dtype)
    return [part(4), part(4), part(8), sems, sems]


class Share:
    def __init__(self, place, sems, span):
        self.place, self.sems, self.first, self.open = place, sems, place.cp * span, []

    def start(self, src, dst, start):
        here_sem, send, recv = (self.sems.at[len(self.open), i] for i in range(3))
        at = dst.at[rows_at(self.first + start, src.shape[0])]
        pair = (pltpu.make_async_copy(src, at, here_sem), remote(src, at, send, recv, self.place.twin))
        for copy in pair:
            copy.start()
        self.open.append(pair)
        return lambda: (pair[0].wait(), pair[1].wait_send())

    def arrived(self):
        for _, there in self.open:
            there.wait_recv()


class Loads:
    def __init__(self, sems):
        self.sems, self.names = sems, []

    def start(self, **moves):
        self.names += [name for name in moves if name not in self.names]
        copies = [pltpu.make_async_copy(src, dst, self.sems.at[self.names.index(name)]) for name, (src, dst) in moves.items()]
        for copy in copies:
            copy.start()
        return lambda: [copy.wait() for copy in copies]

    def wait(self, name, src, dst):
        pltpu.make_async_copy(src, dst, self.sems.at[self.names.index(name)]).wait()


def rope(v, cosine, sine):
    wide = cosine.shape[1]
    heads = []
    for h in range(v.shape[1] // wide):
        part = v[:, h * wide : (h + 1) * wide]
        turned = jnp.concatenate([part[:, wide // 2 :], part[:, : wide // 2]], axis=1)
        heads.append(part * cosine + turned * sine)
    return jnp.concatenate(heads, axis=1)


def each(count, size, visit):
    def body(i, carry):
        visit(pl.multiple_of(i * size, size))
        return carry

    lax.fori_loop(0, count // size, body, 0)


def col_loop(cols, tile, visit):
    each(cols, tile, lambda start: visit(pl.ds(start, tile)))


def dot_nt(a, b):
    return lax.dot_general(a, b, NT, preferred_element_type=F32)


def dot(a, b):
    return jnp.dot(a, b, preferred_element_type=F32)


def norm_block(feats):
    inverse = lax.rsqrt(jnp.mean(feats * feats, axis=-1, keepdims=True) + NORM_EPS)
    return feats * inverse, inverse


def norm_back(d_act, gain, normed, inverse):
    d_normed = d_act * gain
    return inverse * (d_normed - normed * jnp.mean(d_normed * normed, axis=-1, keepdims=True))


def remote_call(body, collective_id, name, out_shape, in_specs, out_specs, scratch, gflops):
    return pl.pallas_call(
        body,
        out_shape=out_shape,
        in_specs=in_specs,
        out_specs=out_specs,
        scratch_shapes=scratch,
        compiler_params=pltpu.CompilerParams(collective_id=collective_id, has_side_effects=True, vmem_limit_bytes=REMOTE_VMEM),
        cost_estimate=cost(gflops, 60),
        name=name,
    )


def join_columns(parts, whole):
    start, moves = 0, {}
    for i, part in enumerate(parts):
        moves[f"join{i}"] = (part, whole.at[:, pl.ds(start, part.shape[1])])
        start += part.shape[1]
    return moves


def enter_body(picked, wq_in, wk_in, wv_in, gain, cosine_in, sine_in, dy_in, wd_in, x_out, q_out, k_out, v_out, dh_out, k2_out, v2_out, act_all, wide, mid, narrow, send, recv, act, dy, wd, dh, w_all, cosine, sine, pair_sems, share_sems, load_sems):
    place = Place()
    place.meet()
    span = x_out.shape[0]
    rows = span // STEPS
    total = Total(place, lambda step: picked.at[pl.ds(step * rows, rows)], wide, mid, narrow, x_out, send, recv)
    share = Share(place, share_sems, span)
    loads = Loads(load_sems)
    for step in range(STEPS):
        total.begin(step)
    loaded = loads.start(dy=(dy_in, dy), wd=(wd_in, wd))
    projection = loads.start(cosine=(cosine_in, cosine), sine=(sine_in, sine), **join_columns((wq_in, wk_in, wv_in), w_all))
    stores = []
    kw = k_out.shape[1]
    qw = q_out.shape[1]

    def back(step):
        here = pl.ds(step * rows, rows)

        def tile(cols):
            dh[here, cols] = dot_nt(dy[here, :], wd[cols, :]).astype(BF16)

        col_loop(wd.shape[0], WIDE_TILE, tile)
        stores.append(loads.start(**{f"dh{step}": (dh.at[here], dh_out.at[here])}))

    pairs = []

    def project(step):
        here = pl.ds(step * rows, rows)

        def norm(start):
            at = pl.ds(step * rows + start, ROW_BLOCK)
            normed, _ = norm_block(x_out[at, :].astype(F32))
            act[at, :] = (normed * gain[...]).astype(BF16)

        each(rows, ROW_BLOCK, norm)
        stores.append(share.start(act.at[here], act_all, step * rows))
        c, s = cosine[here, :], sine[here, :]
        out = dot(act[here, :], w_all[...])
        q_out[here, :] = rope(out[:, :qw], c, s).astype(BF16)
        k_out[here, :] = rope(out[:, qw : qw + kw], c, s).astype(BF16)
        v_out[here, :] = out[:, qw + kw :].astype(BF16)
        for i, (src, dst) in enumerate(((k_out, k2_out), (v_out, v2_out))):
            pairs.append(remote(src.at[here], dst.at[here], pair_sems.at[step, i, 0], pair_sems.at[step, i, 1], place.twin))
            pairs[-1].start()

    loaded()
    for tick in range(2 * STEPS):
        if tick < STEPS:
            back(tick)
        total.advance(tick)
        if tick == STEPS:
            projection()
        if tick >= STEPS:
            total.finish(tick - STEPS)
            project(tick - STEPS)
    for step in range(STEPS):
        total.sent(step, range(4))
    for copy in pairs:
        copy.wait()
    for done in stores:
        done()
    share.arrived()


def enter(picked, wq, wk, wv, gain, cosine, sine, dy, wd):
    span, width = picked.shape
    key = shape(span, wk.shape[1])
    big = pltpu.VMEM((span, width), BF16)
    out_shape = [shape(span, width), shape(span, wq.shape[1]), key, key, shape(span, wd.shape[0]), key, key, shape(2 * span, width)]
    angles = pltpu.VMEM(cosine.shape, F32)
    scratch = total_scratch(width, BF16, span // STEPS) + [big, big, pltpu.VMEM(wd.shape, BF16), pltpu.VMEM((span, wd.shape[0]), BF16), pltpu.VMEM((width, wq.shape[1] + 2 * wk.shape[1]), BF16), angles, angles]
    scratch += [DMA((STEPS, 2, 2)), DMA((STEPS, 3)), DMA((7 + STEPS,))]
    return remote_call(enter_body, 1, "enter", out_shape, [VMEM] + [HBM] * 3 + [VMEM] + [HBM] * 4, [VMEM] * 4 + [HBM] * 4, scratch, 80)(picked, wq, wk, wv, gain, cosine, sine, dy, wd)


def middle_body(att, wo_own, wo_1, wo_2, wo_3, x_in, wg_in, wu_in, wd_in, dh_in, dy_in, gain, h_out, keep_x, send_x, keep_y, send_y, b_all, hidden_all, dgate_all, dup_all, att_all, drb_all, dr_out, datt_out, dgain_out,
                wide, mid, narrow, send, recv, wo, wg, wu, att_full, part_buf, d_b, h, row_in, dh, b, hid, dgt, dup, att_send, att_recv, wo_sems, load_sems, share_sems):
    place = Place()
    span, width = x_in.shape
    rows = span // STEPS
    half = rows // 2
    cols = att.shape[1]
    ffn = wg.shape[1]
    loads = Loads(load_sems)
    chunk = lambda step: pl.ds(step * rows, rows)
    by_chip = lambda tp: rows_at(tp * cols, cols, 128)

    mine = loads.start(att=(att, att_full.at[:, by_chip(place.tp)]), wo=(wo_own, wo.at[by_chip(place.tp)]))
    place.meet()

    x_tp, y_tp = place.over_x[0], place.over_y[0]

    def att_copy(step, i):
        kind = i % 2
        at = pl.ds(step * rows + kind * half, half)
        first, second = ((place.over_y, place.over_x), (place.over_x, place.over_y))[kind]
        dst = att_full.at[at, by_chip(place.tp if i < 4 else first[0])]
        return remote(att.at[at] if i < 4 else dst, dst, att_send.at[step, i], att_recv.at[step, i], first if i < 2 else second)

    def att_begin(step):
        for i in range(4):
            att_copy(step, i).start()

    def att_forward(step):
        for i in range(2):
            att_copy(step, i).wait_recv()
            att_copy(step, 4 + i).start()

    att_begin(0)
    part = wo_1.shape[0]
    arrivals = []
    for i, src in enumerate((wo_1, wo_2, wo_3)):
        flip_y, flip_x = ((1, 0), (0, 1), (1, 1))[i]
        swap = place.cp if i < 2 else 0
        chip = 2 * flipped(place.y, flipped(flip_y, swap)) + flipped(place.x, flipped(flip_x, swap))
        at = wo.at[rows_at((2 * chip + place.cp) * part, part, 128)]
        here = pltpu.make_async_copy(src, at, wo_sems.at[i, 0])
        there = remote(src, at, wo_sems.at[i, 1], wo_sems.at[i, 2], place.twin)
        here.start()
        there.start()
        arrivals += [here, there]
    att_begin(1)
    weights = loads.start(wg=(wg_in, wg), wu=(wu_in, wu))

    share = Share(place, share_sems, span)
    open_shares = [share.start(att, att_all, 0)]
    total = Total(place, lambda step: part_buf.at[step % 2], wide, mid, narrow, d_b, send, recv)

    def fetch(step):
        return loads.start(rows=(x_in.at[chunk(step)], row_in), dh=(dh_in.at[chunk(step)], dh))

    def close():
        while open_shares:
            open_shares.pop()()

    def residual_step(step):
        for i in range(2, 6):
            att_copy(step, i).wait_recv()

        def tile(c):
            h[:, c] = row_in[:, c].astype(F32) + dot(att_full[chunk(step), :], wo[:, c])

        col_loop(width, 2 * WIDE_TILE, tile)
        open_shares.append(loads.start(h_out=(h, h_out.at[chunk(step)])))

        def norm(start):
            at = pl.ds(start, ROW_BLOCK)
            normed, _ = norm_block(h[at, :])
            b[at, :] = (normed * gain[...]).astype(BF16)

        each(rows, ROW_BLOCK, norm)
        open_shares.append(share.start(b, b_all, step * rows))

    def ffn_step(step):
        def tile(c):
            gate = dot(b[...], wg[:, c])
            up = dot(b[...], wu[:, c])
            sig = 1.0 / (1.0 + jnp.exp(-gate))
            d_hid = dh[:, c].astype(F32)
            act = gate * sig
            hid[:, c] = (act * up).astype(BF16)
            dgt[:, c] = (d_hid * up * sig * (1.0 + gate * (1.0 - sig))).astype(BF16)
            dup[:, c] = (d_hid * act).astype(BF16)

        col_loop(ffn, WIDE_TILE, tile)
        for src, dst in ((hid, hidden_all), (dgt, dgate_all), (dup, dup_all)):
            open_shares.append(share.start(src, dst, step * rows))

    def back_step(step):
        def tile(c):
            part_buf[step % 2, :, c] = dot_nt(dgt[...], wg[c, :]) + dot_nt(dup[...], wu[c, :])

        col_loop(width, WIDE_TILE, tile)
        total.begin(step)

    fetched = fetch(0)
    att_forward(0)
    for step in range(2, STEPS):
        att_begin(step)
    mine()
    for copy in arrivals:
        copy.wait()
    for step in range(STEPS):
        if step >= 1:
            close()
        fetched()
        residual_step(step)
        if step + 1 < STEPS:
            att_forward(step + 1)
        if step == 0:
            weights()
        if step >= 1:
            total.fold_wide(step - 1)
        if step >= 2:
            total.fold_narrow(step - 2)
        ffn_step(step)
        if step + 1 < STEPS:
            fetched = fetch(step + 1)
        if step >= 3:
            total.widen(step - 3)
        if step >= 2:
            total.sent(step - 2, (0,))
        back_step(step)

    clear(dgain_out)
    close()
    wd = wg
    weights = loads.start(wg=(wd_in, wd))
    d_r, y_buf = part_buf.at[0], part_buf.at[1]

    def reload(step):
        at = pl.ds(pl.multiple_of(place.cp * span + step * rows, rows), rows)
        return loads.start(h_in=(h_out.at[chunk(step)], h), rows=(dy_in.at[chunk(step)], row_in), hid=(hidden_all.at[at], hid))

    def resid_grad(step):
        def grad(start):
            at = pl.ds(start, ROW_BLOCK)
            normed, inverse = norm_block(h[at, :])
            d_act = d_b[pl.ds(step * rows + start, ROW_BLOCK), :].astype(F32)
            dgain_out[...] += jnp.sum(d_act * normed, axis=0, keepdims=True)
            out = row_in[at, :].astype(F32) + norm_back(d_act, gain[...], normed, inverse)
            d_r[at, :] = out
            b[at, :] = out.astype(BF16)

        each(rows, ROW_BLOCK, grad)
        open_shares.append(loads.start(dr=(d_r, dr_out.at[chunk(step)])))
        open_shares.append(share.start(b, drb_all, step * rows))
        datt_out[chunk(step), :] = dot_nt(b[...], wo[by_chip(place.tp), :]).astype(BF16)

    def output_step(step):
        kind = step // 2
        first, second = ((place.x, place.y), (place.y, place.x))[kind]
        kept = first == step % 2
        row = lax.broadcasted_iota(jnp.int32, (rows, 1), 0)
        owner = kept & (lax.div(row, half) == second)

        def tile(c):
            y_buf[:, c] = dot(hid[...], wd[:, c]) + jnp.where(owner, h[:, c], 0.0)

        col_loop(width, 2 * WIDE_TILE, tile)
        keep, send = ((keep_x, send_x), (keep_y, send_y))[kind]
        for chosen, dst in ((kept, keep), (jnp.logical_not(kept), send)):

            @pl.when(chosen)
            def _():
                loads.start(y=(y_buf, dst))

        open_shares.append(functools.partial(loads.wait, "y", y_buf, keep))

    fetched = reload(0)
    for tick in range(STEPS, 2 * STEPS):
        step = tick - STEPS
        for lag, stage in enumerate((total.fold_wide, total.fold_narrow, total.widen)):
            if tick - 1 - lag < STEPS:
                stage(tick - 1 - lag)
        if step == 0:
            for done in (STEPS - 2, STEPS - 1):
                total.sent(done, (0,))
            weights()
        fetched()
        output_step(step)
        total.finish(step)
        resid_grad(step)
        close()
        if step + 1 < STEPS:
            fetched = reload(step + 1)
    for copy_step in range(STEPS):
        total.sent(copy_step, range(1, 4))
        for i in range(6):
            att_copy(copy_step, i).wait_send()
    share.arrived()


def middle(att, wo_pieces, x, wg, wu, wd, d_hidden, dy, gain):
    span, width = x.shape
    rows = span // STEPS
    ffn = wg.shape[1]
    cols = att.shape[1]
    full = shape(span, width, F32)
    both = shape(2 * span, ffn)
    out_shape = [full] + [shape(rows, width, F32)] * 4 + [shape(2 * span, width), both, both, both, shape(2 * span, cols), shape(2 * span, width), full, shape(span, cols), shape(1, width, F32)]
    buf = lambda r, c, dtype=BF16: pltpu.VMEM((r, c), dtype)
    scratch = total_scratch(width, F32, rows)
    scratch += [buf(width, width), buf(width, ffn), buf(width, ffn), buf(span, width), pltpu.VMEM((2, rows, width), F32), buf(span, width), buf(rows, width, F32)]
    scratch += [buf(rows, c) for c in (width, ffn, width, ffn, ffn, ffn)]
    scratch += [DMA((STEPS, 6)), DMA((STEPS, 6)), DMA((3, 3)), DMA((11,)), DMA((1 + 5 * STEPS, 3))]
    call = remote_call(middle_body, 2, "middle", out_shape, [VMEM] + [HBM] * 10 + [VMEM], [HBM] * 12 + [VMEM] * 2, scratch, 120)
    return call(att, *wo_pieces, x, wg, wu, wd, d_hidden, dy, gain)


def leave_body(dq_in, dk_in, dv_in, dk2_in, dv2_in, cosine, sine, wq_in, wk_in, wv_in, x_in, dr_in, gain, dgain_b, d_all, dx_all, gains_out,
               wide, mid, narrow, send, recv, part_buf, d_a, dk_got, dv_got, d_qkv, w_all, xs, drs, dxs, gain_got, pair_sems, load_sems, share_sems):
    place = Place()
    place.meet()
    span, width = x_in.shape
    rows = span // STEPS
    chunk = lambda step: pl.ds(step * rows, rows)
    swap = lambda i, src, dst: remote(src, dst, pair_sems.at[i, 0], pair_sems.at[i, 1], place.twin)
    pairs = [[swap(2 * step + i, src.at[chunk(step)], dst.at[chunk(step)]) for i, (src, dst) in enumerate(((dk2_in, dk_got), (dv2_in, dv_got)))] for step in range(STEPS)]
    for copy in sum(pairs, []):
        copy.start()
    qw = dq_in.shape[1]
    kw = dk_in.shape[1]
    share = Share(place, share_sems, span)
    loads = Loads(load_sems)
    total = Total(place, lambda step: part_buf.at[step], wide, mid, narrow, d_a, send, recv)

    def partial(step):
        here = chunk(step)
        c, s = cosine[here, :], -sine[here, :]
        for copy in pairs[step]:
            copy.wait()
        d_qkv[here, :qw] = rope(dq_in[here, :].astype(F32), c, s).astype(BF16)
        dk_sum = (dk_in[here, :] + dk_got[here, :]).astype(BF16).astype(F32)
        d_qkv[here, qw : qw + kw] = rope(dk_sum, c, s).astype(BF16)
        d_qkv[here, qw + kw :] = (dv_in[here, :] + dv_got[here, :]).astype(BF16)
        if step == 0:
            weights()

        def tile(n):
            part_buf[step, :, n] = dot_nt(d_qkv[here, :], w_all[n, :])

        col_loop(width, 2 * WIDE_TILE, tile)
        total.begin(step)

    def load(step):
        return loads.start(x=(x_in.at[chunk(step)], xs), dr=(dr_in.at[chunk(step)], drs))

    gain_a = pl.ds(0, 1)
    clear(gains_out.at[gain_a])
    gains_out[pl.ds(1, 1), :] = dgain_b[...]
    open_shares = []

    def grad_x(step):
        def grad(start):
            at = pl.ds(start, ROW_BLOCK)
            normed, inverse = norm_block(xs[at, :].astype(F32))
            d_act = d_a[pl.ds(step * rows + start, ROW_BLOCK), :].astype(F32)
            gains_out[gain_a, :] += jnp.sum(d_act * normed, axis=0, keepdims=True)
            dxs[at, :] = drs[at, :] + norm_back(d_act, gain[...], normed, inverse)

        each(rows, ROW_BLOCK, grad)
        open_shares.append(share.start(dxs, dx_all, step * rows))

    weights = loads.start(**join_columns((wq_in, wk_in, wv_in), w_all))
    loaded = load(0)
    for step in range(STEPS):
        partial(step)
    first = [share.start(d_qkv, d_all, 0)]
    for tick in range(2 * STEPS):
        total.advance(tick)
        if tick >= STEPS:
            step = tick - STEPS
            loaded()
            total.finish(step)
            while open_shares:
                open_shares.pop()()
            grad_x(step)
            if step + 1 < STEPS:
                loaded = load(step + 1)
    last = swap(2 * STEPS, gains_out, gain_got)
    last.start()
    last.wait()
    gains_out[...] = gains_out[...] + gain_got[...]
    for done in open_shares + first:
        done()
    for step in range(STEPS):
        total.sent(step, range(4))
    share.arrived()


def leave(dq, dk, dv, dk2, dv2, cosine, sine, wq, wk, wv, x, d_resid, gain, dgain_b):
    span, width = x.shape
    rows = span // STEPS
    kw = wk.shape[1]
    qw = wq.shape[1]
    cols = qw + 2 * kw
    buf = lambda r, c, dtype=F32: pltpu.VMEM((r, c), dtype)
    out_shape = [shape(2 * span, cols), shape(2 * span, width, F32), shape(2, width, F32)]
    scratch = total_scratch(width, F32, rows) + [pltpu.VMEM((STEPS, rows, width), F32), buf(span, width, BF16), buf(span, kw), buf(span, kw), buf(span, cols, BF16), buf(width, cols, BF16)]
    scratch += [buf(rows, width, BF16), buf(rows, width), buf(rows, width), buf(2, width)]
    scratch += [DMA((2 * STEPS + 1, 2)), DMA((5,)), DMA((1 + STEPS, 3))]
    call = remote_call(leave_body, 3, "leave", out_shape, [VMEM] * 3 + [HBM] * 2 + [VMEM] * 2 + [HBM] * 5 + [VMEM] * 2, [HBM] * 2 + [VMEM], scratch, 90)
    return call(dq, dk, dv, dk2, dv2, cosine, sine, wq, wk, wv, x, d_resid, gain, dgain_b)


def slot_sequence(slot, block_len, cp_count):
    shard = slot // (2 * block_len)
    within = slot % (2 * block_len)
    block_no = jnp.where(within < block_len, shard, 2 * cp_count - 1 - shard)
    return block_no * block_len + within % block_len


def side(v, bit):
    half = v.shape[0] // 2
    return lax.dynamic_slice_in_dim(v, bit * half, half, 0)


def join(own, other, bit):
    return jnp.where(bit == 0, jnp.concatenate([own, other]), jnp.concatenate([other, own]))


def solution(mesh):
    cp_count = mesh.shape["cp"]

    def device_step(tokens, pos, doc_id, dy, table, w_q, w_k, w_v, w_o, w_gate, w_up, w_down, gain_one, gain_two, inv_freq):
        span = tokens.shape[0]
        rows, width = table.shape
        head_dim = 2 * inv_freq.shape[0]
        scale = head_dim ** -0.5
        tp = lax.axis_index("tp")
        cp = lax.axis_index("cp")
        gain_a = gain_one.astype(F32)[None, :]
        gain_b = gain_two.astype(F32)[None, :]
        base = tp * rows

        wo_half = side(w_o, cp)
        wo_1 = swap_core(wo_half, 0)
        picked, grad = pick_rows(tokens, table, base)

        other_ids = swap_c(tokens)
        all_ids = join(tokens, other_ids, cp)
        packed = lax.sort(all_ids * (2 * span) + jnp.arange(2 * span, dtype=jnp.int32))
        sorted_ids, perm = packed // (2 * span), packed % (2 * span)
        lowest = jnp.sum((all_ids < base).astype(jnp.int32))
        highest = jnp.sum((all_ids < base + rows).astype(jnp.int32))
        bounds = jnp.stack([lowest, highest, base.astype(jnp.int32)])

        angle = pos.astype(F32)[:, None] * inv_freq
        cosine = jnp.cos(angle)
        sine = jnp.sin(angle)
        cosine = jnp.concatenate([cosine, cosine], axis=1)
        sine = jnp.concatenate([-sine, sine], axis=1)
        x, query, key, value, d_hidden, key2, value2, act_a_all = enter(picked, w_q, w_k, w_v, gain_a, cosine, sine, dy, w_down)

        wo_1, wo_half, query = lax.optimization_barrier((wo_1, wo_half, query))
        wo_pieces = (w_o, wo_1, swap_core(wo_half, 1), swap_core(wo_1, 1))
        slots = jnp.arange(span, dtype=jnp.int32)
        q_seq = slot_sequence(cp * span + slots, span // 2, cp_count)
        k_seq2 = slot_sequence((1 - cp) * span + slots, span // 2, cp_count)
        q_low = (q_seq - pos)[:, None]
        q_high = q_seq[:, None]
        seq_row = jnp.concatenate([q_seq, k_seq2])[None, :]
        info = jnp.stack([cp.astype(jnp.int32)])
        att, lse, grad = attend(scale, info, query, key, value, key2, value2, q_low, q_high, seq_row, grad)

        _, keep_x, send_x, keep_y, send_y, act_b_all, hidden_all, d_gate_all, d_up_all, att_all, d_resid_all, d_resid, d_att, d_gain_b = middle(att, wo_pieces, x, w_gate, w_up, w_down, d_hidden, dy, gain_b)

        x_bit, y_bit = tp % 2, tp // 2
        ways = ((keep_x, swap_x, x_bit, swap_y, y_bit), (keep_y, swap_y, y_bit, swap_x, x_bit))
        y_wide = [swap_x(send_x), swap_y(send_y)]

        d_query, d_key, d_value, d_key2, d_value2, grad = attend_back(scale, info, query, d_att, lse, key, value, key2, value2, q_low, q_high, seq_row, grad)
        d_qkv_all, d_x_all, gains = leave(d_query, d_key, d_value, d_key2, d_value2, cosine, sine, w_q, w_k, w_v, x, d_resid, gain_a, d_gain_b)

        def over_tokens(left, right):
            return jnp.einsum("ta,tb->ab", left, right, preferred_element_type=F32)

        y_wide, d_x_all = lax.optimization_barrier((y_wide, d_x_all))
        y_mid = [keep + wide for (keep, _, _, _, _), wide in zip(ways, y_wide)]
        y_narrow = [swap_2(side(mid, 1 - bit_2)) for (_, _, _, swap_2, bit_2), mid in zip(ways, y_mid)]
        y_mid, d_x_all = lax.optimization_barrier((y_mid, d_x_all))
        grad_table = put_rows(sorted_ids, perm, bounds, d_x_all, grad)
        y_narrow, grad_table = lax.optimization_barrier((y_narrow, grad_table))
        y_own = [(side(mid, bit_2) + narrow).astype(BF16) for (_, _, _, _, bit_2), mid, narrow in zip(ways, y_mid, y_narrow)]
        y_pair = [join(own, swap_2(own), bit_2) for (_, _, _, swap_2, bit_2), own in zip(ways, y_own)]
        y_own, hidden_all = lax.optimization_barrier((y_own, hidden_all))
        dy_all = join(dy, swap_c(dy), cp)
        grad_down = over_tokens(hidden_all, dy_all)
        y_pair, grad_down = lax.optimization_barrier((y_pair, grad_down))
        y_full = [join(pair, swap_1(pair), bit_1) for (_, swap_1, bit_1, _, _), pair in zip(ways, y_pair)]
        y_pair, act_b_all = lax.optimization_barrier((y_pair, act_b_all))
        grad_gate = over_tokens(act_b_all, d_gate_all)
        grad_up = over_tokens(act_b_all, d_up_all)
        grad_out = over_tokens(att_all, d_resid_all)
        qw, kw = query.shape[1], key.shape[1]
        grad_q, grad_k, grad_v = (over_tokens(act_a_all, d) for d in jnp.split(d_qkv_all, (qw, qw + kw), axis=1))
        return (jnp.concatenate(y_full), grad_table, grad_q, grad_k, grad_v, grad_out, grad_gate, grad_up, grad_down, gains[0], gains[1])

    col_spec = P(None, "tp")
    row_spec = P("tp", None)
    tok_spec = P("cp")
    rep_spec = P(None)
    in_specs = (tok_spec, tok_spec, tok_spec, P("cp", None), row_spec, col_spec, col_spec, col_spec, row_spec, col_spec, col_spec, row_spec, rep_spec, rep_spec, rep_spec)
    out_specs = (P("cp", None), row_spec, col_spec, col_spec, col_spec, row_spec, col_spec, col_spec, row_spec, rep_spec, rep_spec)
    return jax.shard_map(device_step, mesh=mesh, in_specs=in_specs, out_specs=out_specs, check_vma=False)
```

```python
import functools

import jax
import jax.numpy as jnp
from jax import lax
from jax.experimental import pallas as pl
from jax.experimental.pallas import tpu as pltpu
from jax.sharding import PartitionSpec as P

NORM_EPS = 1e-5
NEG_BIG = -1e30
F32 = jnp.float32
BF16 = jnp.bfloat16
MIB = 2**20
LOCAL_VMEM = 56 * MIB
REMOTE_VMEM = 63 * MIB
STEPS = 4
SUBLANES = 8
ROW_BLOCK = 32
WIDE_TILE = 512
TILE = 256
MESH_ID = pl.DeviceIdType.MESH
NT = (((1,), (1,)), ((), ()))
CONTRACT_FIRST = (((0,), (0,)), ((), ()))
VMEM = pl.BlockSpec(memory_space=pltpu.VMEM)
SMEM = pl.BlockSpec(memory_space=pltpu.SMEM)
HBM = pl.BlockSpec(memory_space=pl.ANY)
DMA = pltpu.SemaphoreType.DMA


X_PAIRS, Y_PAIRS = ([(chip, chip ^ flip) for chip in range(4)] for flip in (1, 2))
C_PAIRS = X_PAIRS[:2]
CORE_PAIRS = tuple([(2 * a + core, 2 * b + core) for core, pairs in enumerate(kinds) for a, b in pairs] for kinds in ((Y_PAIRS, X_PAIRS), (X_PAIRS, Y_PAIRS)))


def swap_x(v):
    return lax.ppermute(v, "tp", X_PAIRS)


def swap_y(v):
    return lax.ppermute(v, "tp", Y_PAIRS)


def swap_c(v):
    return lax.ppermute(v, "cp", C_PAIRS)


def swap_core(v, which):
    return lax.ppermute(v, ("tp", "cp"), CORE_PAIRS[which])


def over_row(reduce, v):
    return reduce(v, axis=-1, keepdims=True)


def over_column(v):
    return jnp.sum(v, axis=0, keepdims=True)


def specs(places):
    return [{"v": VMEM, "h": HBM, "s": SMEM}[place] for place in places]


def cost(gflops, mib):
    return pl.CostEstimate(flops=gflops * 10**9, bytes_accessed=mib * MIB, transcendentals=0)


def shape(rows, cols, dtype=BF16):
    return jax.ShapeDtypeStruct((rows, cols), dtype)


def local_call(body, name, out_shape, in_specs, out_specs, scratch, gflops, aliases={}, **grid):
    return pl.pallas_call(
        body,
        out_shape=out_shape,
        in_specs=in_specs,
        out_specs=out_specs,
        scratch_shapes=scratch,
        input_output_aliases=aliases,
        compiler_params=pltpu.CompilerParams(vmem_limit_bytes=LOCAL_VMEM),
        cost_estimate=cost(gflops, 60),
        name=name,
        **grid,
    )


def rows_at(start, size, step=32):
    return pl.ds(pl.multiple_of(start, step), size)


class Ring:
    def __init__(self, buf, sems, inward):
        self.buf, self.sems, self.inward = buf, sems, inward

    def slot(self, count):
        return lax.rem(count, self.buf.shape[0])

    def _copy(self, count, view):
        pair = (view, self.buf.at[self.slot(count)])
        return pltpu.make_async_copy(*(pair if self.inward else pair[::-1]), self.sems.at[self.slot(count)])

    def start(self, count, kind, views):
        for k, view in enumerate(views):
            pl.when(kind == k)(lambda: self._copy(count, view).start())

    def wait(self, count, view):
        self._copy(count, view).wait()


ZERO_ROWS = 96
ZERO_FIRST = 25
ZERO_ATTEND = (6, 18)
ZERO_BACK = (10, 20)


def zero_block(out_ref, block, count=1):
    return out_ref.at[pl.ds(pl.multiple_of(block * ZERO_ROWS, ZERO_ROWS), count * ZERO_ROWS)]


def clear(ref, value=0.0):
    ref[()] = jnp.full(ref.shape, value, F32)


def start_zeros(out_ref, zero_ref, sem, first, count):
    for i in range(count):
        pltpu.make_async_copy(zero_ref, zero_block(out_ref, first + i), sem).start()


def wait_zeros(out_ref, sem, first, count):
    whole = zero_block(out_ref, first, count)
    pltpu.make_async_copy(whole, whole, sem).wait()


def zero_scratch(width):
    return [pltpu.VMEM((ZERO_ROWS, width), F32), DMA]


def grid_zeros(grad_ref, zero_ref, sem, before, early, late):
    head, tile = pl.program_id(0), pl.program_id(1)
    heads, tiles = pl.num_programs(0), pl.num_programs(1)
    half = tiles // 2
    whole = half * (early + late)
    pl.when((head == 0) & (tile == 0))(functools.partial(clear, zero_ref))
    first = before + head * whole + tile * early + jnp.maximum(tile - half, 0) * (late - early)
    start_zeros(grad_ref, zero_ref, sem, first, early)
    pl.when(tile >= half)(functools.partial(start_zeros, grad_ref, zero_ref, sem, first + early, late - early))
    last = (head == heads - 1) & (tile == tiles - 1)
    return lambda: pl.when(last)(lambda: wait_zeros(grad_ref, sem, before, heads * whole))


GATHER_BATCH = 16
GATHER_SLOTS = 8


def pick_body(group_ref, lane_ref, count_ref, table_ref, out_ref, grad_ref, buf, sems, zero_ref, zero_sem):
    batches = out_ref.shape[0] // GATHER_BATCH
    width = out_ref.shape[1]

    def row_copy(group, slot, j):
        return pltpu.make_async_copy(table_ref.at[group], buf.at[slot, j], sems.at[slot])

    def start(step):
        slot = lax.rem(step, GATHER_SLOTS)
        for j in range(GATHER_BATCH):
            group = group_ref[step * GATHER_BATCH + j]
            pl.when(group >= 0)(lambda: row_copy(group, slot, j).start())

    for step in range(GATHER_SLOTS - 1):
        start(step)
    clear(zero_ref)
    start_zeros(grad_ref, zero_ref, zero_sem, 0, ZERO_FIRST)
    row = lax.broadcasted_iota(jnp.int32, (SUBLANES, width), 0)

    def loop(step, carry):
        slot = lax.rem(step, GATHER_SLOTS)

        @pl.when(step + GATHER_SLOTS - 1 < batches)
        def _():
            start(step + GATHER_SLOTS - 1)

        def arrived(i, carry):
            row_copy(0, slot, 0).wait()
            return carry

        lax.fori_loop(0, count_ref[step], arrived, 0)
        first = pl.multiple_of(step * GATHER_BATCH, GATHER_BATCH)
        parts = []
        for j in range(GATHER_BATCH):
            lane = lane_ref[first + j]
            goal = j % SUBLANES
            if goal == 0:
                parts.append(jnp.zeros((SUBLANES, width), F32))
            turned = pltpu.roll(buf[slot, j].astype(F32), lax.rem(goal + SUBLANES - lane, SUBLANES), 0)
            parts[-1] = jnp.where(row == jnp.where(lane < SUBLANES, goal, SUBLANES), turned, parts[-1])
        out_ref[pl.ds(first, GATHER_BATCH), :] = jnp.concatenate(parts, axis=0).astype(BF16)
        return carry

    lax.fori_loop(0, batches, loop, 0)
    wait_zeros(grad_ref, zero_sem, 0, ZERO_FIRST)


def pick_rows(tokens, table, base):
    span = tokens.shape[0]
    rows, width = table.shape
    local = tokens - base
    owned = (local >= 0) & (local < rows)
    group = jnp.where(owned, local // SUBLANES, -1)
    lane = jnp.where(owned, local % SUBLANES, SUBLANES)
    count = jnp.sum(owned.reshape(-1, GATHER_BATCH).astype(jnp.int32), axis=1)
    return local_call(pick_body, "pick_rows", [shape(span, width), shape(rows, width, F32)], [SMEM, SMEM, SMEM, HBM], [VMEM, HBM],
                      [pltpu.VMEM((GATHER_SLOTS, GATHER_BATCH, SUBLANES, width), BF16), DMA((GATHER_SLOTS,))] + zero_scratch(width), 20)(group, lane, count, table.reshape(rows // SUBLANES, SUBLANES, width))


SEMS = 32
AHEAD = 4
MOVE_SLOTS = 8
MOVE_ROWS = 128


def put_body(ids_ref, perm_ref, range_ref, all_ref, zero_ref, *refs):
    kinds = len(refs) // 2 - 4
    sources, out_ref, rest = refs[:kinds], refs[kinds], refs[kinds + 1 :]
    targets, (rows_ref, load_sem, sems, moved, read_sems, write_sems, place, sent) = rest[:kinds], rest[kinds:]
    load = pltpu.make_async_copy(all_ref, rows_ref, load_sem)
    load.start()
    low, high, base = (range_ref[i] for i in range(3))
    pieces = sources[0].shape[0] // MOVE_ROWS
    moves = kinds * pieces
    lag = MOVE_SLOTS // 2
    steps = moves + MOVE_SLOTS

    reads, writes = Ring(moved, read_sems, True), Ring(moved, write_sems, False)

    def views(arrays, step):
        return [ref.at[rows_at(lax.rem(step, pieces) * MOVE_ROWS, MOVE_ROWS)] for ref in arrays]

    def move(step):
        @pl.when(step >= MOVE_SLOTS)
        def _():
            writes.wait(step, views(targets, step)[0])

        @pl.when(step < moves)
        def _():
            reads.start(step, lax.div(step, pieces), views(sources, step))

        ready = step - lag

        @pl.when((ready >= 0) & (ready < moves))
        def _():
            reads.wait(ready, views(sources, ready)[0])
            writes.start(ready, lax.div(ready, pieces), views(targets, ready))

    def row(pos):
        return pl.ds(pos, 1)

    def wait_slot(slot):
        pltpu.make_async_copy(rows_ref.at[row(0), :], out_ref.at[row(0), :], sems.at[slot]).wait()

    def token(pos):
        return rows_ref[row(perm_ref[pos]), :]

    def one_id(carry):
        pos, count = carry
        row_id = ids_ref[pos]
        first = row(perm_ref[pos])

        def more(carry):
            return ids_ref[carry[0]] == row_id

        def add(carry):
            start, total = carry
            end = start
            for k in range(AHEAD):
                same = ids_ref[start + k] == row_id
                total = total + jnp.where(same, token(start + k), 0.0)
                end = end + same.astype(jnp.int32)
            return end, total

        after, total = lax.while_loop(more, add, (pos + 1, token(pos)))

        @pl.when(after > pos + 1)
        def _():
            rows_ref[first, :] = total

        slot = lax.rem(count, SEMS)
        pl.when(count >= SEMS)(lambda: wait_slot(slot))
        pltpu.make_async_copy(rows_ref.at[first, :], out_ref.at[row(row_id - base), :], sems.at[slot]).start()
        return after, count + 1

    place[0] = low
    sent[0] = 0

    def step_body(step, carry):
        move(step)
        pl.when(step == 0)(load.wait)
        limit = low + lax.div((high - low) * (step + 1), steps)
        pos, count = lax.while_loop(lambda c: c[0] < limit, one_id, (place[0], sent[0]))
        place[0] = pos
        sent[0] = count
        return carry

    lax.fori_loop(0, steps, step_body, 0)
    count = sent[0]

    def drain(slot, carry):
        pl.when(slot < count)(lambda: wait_slot(slot))
        return carry

    lax.fori_loop(0, SEMS, drain, 0)


def move_body(*refs):
    half = len(refs) // 2
    for src, dst in zip(refs[:half], refs[half:]):
        dst[()] = src[()]


def move(*arrays):
    steps = SUBLANES
    specs = [pl.BlockSpec((v.shape[0] // steps, v.shape[1]), lambda i: (i, 0)) for v in arrays]
    return local_call(move_body, "move", [shape(*v.shape, F32) for v in arrays], specs, specs, [], 20, grid=(steps,))(*arrays)


def put_rows(ids, perm, bounds, rows, zeros, results):
    ids = jnp.concatenate([ids, jnp.full((AHEAD,), -1, jnp.int32)])
    perm = jnp.concatenate([perm, jnp.zeros((AHEAD,), jnp.int32)])
    slots = DMA((MOVE_SLOTS,))
    counter = pltpu.SMEM((1,), jnp.int32)
    scratch = [pltpu.VMEM(rows.shape, F32), DMA, DMA((SEMS,)), pltpu.VMEM((MOVE_SLOTS, MOVE_ROWS, rows.shape[1]), F32), slots, slots, counter, counter]
    out_shape = [shape(*v.shape, F32) for v in (zeros, *results)]
    return local_call(put_body, "put_rows", out_shape, specs("ssshh") + [HBM] * len(results), [HBM] * len(out_shape), scratch, 20, {4: 0})(ids, perm, bounds, rows, zeros, *results)


Q_TILE = 256
K_TILE = 512


def stack_heads(v):
    half = v.shape[1] // 2
    return jnp.concatenate([v[:, :half], v[:, half:]], axis=0)


def unstack_heads(v):
    half = v.shape[0] // 2
    return jnp.concatenate([v[:half], v[half:]], axis=1)


def sequence_chunks(cp):
    return [chunk * K_TILE for chunk in (cp, 3 - cp, 1 - cp, 2 + cp)]


class Tile:
    def __init__(self, q_ref, pos_ref):
        tile = pl.program_id(1)
        per_chunk = K_TILE // Q_TILE
        self.cp = lax.axis_index("cp")
        self.late = tile >= per_chunk
        self.chunks = sequence_chunks(self.cp)
        first = jnp.where(self.late, self.chunks[1], self.chunks[0]) + lax.rem(tile, per_chunk) * Q_TILE
        high = first + lax.broadcasted_iota(jnp.int32, pos_ref.shape, 0)
        twice = lambda v: jnp.concatenate([v, v], axis=0)
        self.low, self.high = twice(high - pos_ref[()]), twice(high)
        self.q = stack_heads(q_ref[()])

    def visit(self, visit):
        needed = (True, self.late, self.late | (self.cp == 1), self.late & (self.cp == 0))
        for block, when in enumerate(needed):
            pl.when(when)(functools.partial(visit, block))

    def scores(self, scale, k, block):
        scores = lax.dot_general(self.q, k, NT, preferred_element_type=F32) * scale
        at = self.chunks[block] + lax.broadcasted_iota(jnp.int32, (1, K_TILE), 1)
        return jnp.where((at >= self.low) & (at <= self.high), scores, NEG_BIG)


def block_refs(block, *pairs):
    rows = pl.ds((block % 2) * K_TILE, K_TILE)
    return [pair[block // 2].at[rows] for pair in pairs]


def attend_body(scale, q_ref, k_ref, v_ref, k2_ref, v2_ref, pos_ref, zeros_in, out_ref, lse_ref, grad_ref, s_ref, m_ref, l_ref, acc_ref, zero_ref, zero_sem):
    end_zeros = grid_zeros(grad_ref, zero_ref, zero_sem, ZERO_FIRST, *ZERO_ATTEND)
    tile = Tile(q_ref, pos_ref)
    clear(m_ref, NEG_BIG)
    clear(l_ref)
    clear(acc_ref)

    def score(block):
        (k,) = block_refs(block, (k_ref, k2_ref))
        s = tile.scores(scale, k[()], block)
        s_ref[block] = s
        m_ref[()] = jnp.maximum(m_ref[()], over_row(jnp.max, s))

    def exponent(block):
        e = jnp.exp(s_ref[block] - m_ref[()])
        s_ref[block] = e
        l_ref[()] += over_row(jnp.sum, e)

    tile.visit(score)
    tile.visit(exponent)
    inverse = 1.0 / l_ref[()]

    def mix(block):
        (v,) = block_refs(block, (v_ref, v2_ref))
        prob = (s_ref[block] * inverse).astype(BF16)
        acc_ref[()] += jnp.dot(prob, v[()], preferred_element_type=F32)

    tile.visit(mix)
    out_ref[()] = unstack_heads(acc_ref[()].astype(BF16))
    lse_ref[()] = (m_ref[()] + jnp.log(l_ref[()])).reshape(lse_ref.shape)
    end_zeros()


def attention_specs(span, head_dim):
    tile = pl.BlockSpec((Q_TILE, 2 * head_dim), lambda h, t: (t, h))
    keys = pl.BlockSpec((span, head_dim), lambda h, t: (0, h))
    pos = pl.BlockSpec((Q_TILE, 1), lambda h, t: (t, 0))
    lse = pl.BlockSpec((1, 1, 2 * Q_TILE, 1), lambda h, t: (h, t, 0, 0))
    return tile, keys, pos, lse


def attention_call(body, name, heads, span, out_shape, in_specs, out_specs, scratch, gflops):
    alias = {len(in_specs) - 1: len(out_specs) - 1}
    scratch = scratch + zero_scratch(out_shape[-1].shape[1])
    return local_call(body, name, out_shape, in_specs, out_specs, scratch, gflops, alias, grid=(heads, span // Q_TILE))


def attend(scale, q, k, v, k2, v2, pos, grad):
    span = q.shape[0]
    heads = 2
    head_dim = k.shape[1] // heads
    tile, keys, pos_spec, lse = attention_specs(span, head_dim)
    stacked = heads * Q_TILE
    buf = lambda c: pltpu.VMEM((stacked, c), F32)
    out_shape = [shape(*q.shape), jax.ShapeDtypeStruct((heads, span // Q_TILE, stacked, 1), F32), shape(*grad.shape, F32)]
    scratch = [pltpu.VMEM((4, stacked, K_TILE), F32), buf(1), buf(1), buf(head_dim)]
    call = attention_call(functools.partial(attend_body, scale), "attend", heads, span, out_shape, [tile] + [keys] * 4 + [pos_spec, HBM], [tile, lse, HBM], scratch, 14)
    return call(q, k, v, k2, v2, pos, grad)


def attend_back_body(scale, q_ref, do_ref, lse_ref, k_ref, v_ref, k2_ref, v2_ref, pos_ref, zeros_in, dq_ref, dk_ref, dv_ref, dk2_ref, dv2_ref, grad_ref, p_ref, dp_ref, d_ref, acc_ref, zero_ref, zero_sem):
    steps = pl.num_programs(0) * pl.num_programs(1)
    end_zeros = grid_zeros(grad_ref, zero_ref, zero_sem, ZERO_FIRST + steps // 2 * sum(ZERO_ATTEND), *ZERO_BACK)
    tile = Tile(q_ref, pos_ref)
    d_out = stack_heads(do_ref[()])
    lse = lse_ref[()].reshape(d_out.shape[0], 1)
    clear(d_ref)
    clear(acc_ref)

    @pl.when(pl.program_id(1) == 0)
    def _():
        for ref in (dk_ref, dv_ref, dk2_ref, dv2_ref):
            clear(ref)

    def first(block):
        k, v = block_refs(block, (k_ref, k2_ref), (v_ref, v2_ref))
        p = jnp.exp(tile.scores(scale, k[()], block) - lse)
        dp = lax.dot_general(d_out, v[()], NT, preferred_element_type=F32).astype(BF16)
        p_ref[block] = p
        dp_ref[block] = dp
        d_ref[()] += over_row(jnp.sum, p * dp.astype(F32))

    def second(block):
        k, dk, dv = block_refs(block, (k_ref, k2_ref), (dk_ref, dk2_ref), (dv_ref, dv2_ref))
        p = p_ref[block]
        ds = (p * (dp_ref[block].astype(F32) - d_ref[()]) * scale).astype(BF16)
        acc_ref[()] += jnp.dot(ds, k[()], preferred_element_type=F32)
        dk[()] += lax.dot_general(ds, tile.q, CONTRACT_FIRST, preferred_element_type=F32)
        dv[()] += lax.dot_general(p.astype(BF16), d_out, CONTRACT_FIRST, preferred_element_type=F32)

    tile.visit(first)
    tile.visit(second)
    dq_ref[()] = unstack_heads(acc_ref[()].astype(BF16))
    end_zeros()


def attend_back(scale, q, d_out, lse, k, v, k2, v2, pos, grad):
    span = q.shape[0]
    heads = 2
    head_dim = k.shape[1] // heads
    tile, keys, pos_spec, lse_spec = attention_specs(span, head_dim)
    stacked = heads * Q_TILE
    buf = lambda c: pltpu.VMEM((stacked, c), F32)
    probs = lambda dtype: pltpu.VMEM((4, stacked, K_TILE), dtype)
    out_shape = [shape(*q.shape)] + [shape(*k.shape, F32)] * 4 + [shape(*grad.shape, F32)]
    in_specs = [tile, tile, lse_spec] + [keys] * 4 + [pos_spec, HBM]
    call = attention_call(functools.partial(attend_back_body, scale), "attend_back", heads, span, out_shape, in_specs, [tile] + [keys] * 4 + [HBM], [probs(F32), probs(BF16), buf(1), buf(head_dim)], 30)
    return call(q, d_out, lse, k, v, k2, v2, pos, grad)


def remote(src, dst, send, recv, device):
    return pltpu.make_async_remote_copy(src_ref=src, dst_ref=dst, send_sem=send, recv_sem=recv, device_id=device, device_id_type=MESH_ID)


def flipped(bit, flip):
    return bit + flip - 2 * bit * flip


class Place:
    def __init__(self):
        self.tp = lax.axis_index("tp")
        self.cp = lax.axis_index("cp")
        self.x = lax.rem(self.tp, 2)
        self.y = lax.div(self.tp, 2)
        self.over_x = (self.chip(1, 0), self.cp)
        self.over_y = (self.chip(0, 1), self.cp)
        self.twin = (self.tp, 1 - self.cp)

    def chip(self, dx, dy):
        return 2 * flipped(self.y, dy) + flipped(self.x, dx)

    def meet(self):
        barrier = pltpu.get_barrier_semaphore()
        peers = (self.over_x, self.over_y, self.twin)
        for device in peers:
            pl.semaphore_signal(barrier, inc=1, device_id=device, device_id_type=MESH_ID)
        pl.semaphore_wait(barrier, len(peers))


class Total:
    def __init__(self, place, part, wide, mid, narrow, out, send, recv):
        self.part, self.wide, self.mid, self.narrow, self.out = part, wide, mid, narrow, out
        self.send, self.recv = send, recv
        self.rows = out.shape[0] // STEPS
        self.half, self.quarter, self.eighth = (self.rows // n for n in (2, 4, 8))
        self.kinds = [(place.x, place.y, place.over_x, place.over_y), (place.y, place.x, place.over_y, place.over_x)]

    def _rows(self, step, kind):
        first, second = self.kinds[kind][:2]
        side = step * self.rows + kind * self.half + first * self.quarter
        return rows_at(side, self.quarter), rows_at(side + second * self.eighth, self.eighth)

    def _kept(self, kind, flip=0):
        return rows_at(kind * self.half + flipped(self.kinds[kind][0], flip) * self.quarter, self.quarter)

    def _eighth(self, kind, flip=0):
        return rows_at(flipped(self.kinds[kind][1], flip) * self.eighth, self.eighth)

    def _copy(self, step, kind, stage):
        side, mine = self._rows(step, kind)
        _, _, peer_first, peer_second = self.kinds[kind]
        src, dst, peer = (
            lambda: (self.part(step).at[self._kept(kind, 1)], self.wide.at[step, kind], peer_first),
            lambda: (self.mid.at[step, kind, self._eighth(kind, 1)], self.narrow.at[step, kind], peer_second),
            lambda: (self.out.at[mine], self.out.at[mine], peer_second),
            lambda: (self.out.at[side], self.out.at[side], peer_first),
        )[stage]()
        return remote(src, dst, self.send.at[step, kind, stage], self.recv.at[step, kind, stage], peer)

    def begin(self, step):
        for kind in range(2):
            self._copy(step, kind, 0).start()

    def fold_wide(self, step):
        for kind in range(2):
            self._copy(step, kind, 0).wait_recv()
            self.mid[step, kind] = self.part(step)[self._kept(kind), :] + self.wide[step, kind]
            self._copy(step, kind, 1).start()

    def fold_narrow(self, step):
        for kind in range(2):
            self._copy(step, kind, 1).wait_recv()
            total = self.mid[step, kind, self._eighth(kind), :] + self.narrow[step, kind]
            self.out[self._rows(step, kind)[1], :] = total.astype(BF16)
            self._copy(step, kind, 2).start()

    def widen(self, step):
        for kind in range(2):
            self._copy(step, kind, 2).wait_recv()
            self._copy(step, kind, 3).start()

    def finish(self, step):
        for kind in range(2):
            self._copy(step, kind, 3).wait_recv()

    def sent(self, step, stages):
        for kind in range(2):
            for stage in stages:
                self._copy(step, kind, stage).wait_send()


def sems(*dims):
    return DMA((*dims, 3))


def total_scratch(width, dtype, rows):
    stages = DMA((STEPS, 2, 4))
    part = lambda n: pltpu.VMEM((STEPS, 2, rows // n, width), dtype)
    return [part(4), part(4), part(8), stages, stages]


class Share:
    def __init__(self, place, sems, span):
        self.place, self.sems, self.first, self.open, self.count = place, sems, place.cp * span, [], 0

    def start(self, src, dst, start):
        here_sem, send, recv = (self.sems.at[self.count, i] for i in range(3))
        self.count += 1
        at = dst.at[rows_at(self.first + start, src.shape[0])]
        pair = (pltpu.make_async_copy(src, at, here_sem), remote(src, at, send, recv, self.place.twin))
        for copy in pair:
            copy.start()
        self.open.append(pair)
        return lambda: (pair[0].wait(), pair[1].wait_send())

    def apart(self, src, dst):
        self.start(src, dst, 0)
        here, there = self.open.pop()
        return there.wait_send, lambda: (here.wait(), there.wait_recv())

    def arrived(self):
        for _, there in self.open:
            there.wait_recv()


class Loads:
    def __init__(self, sems):
        self.sems, self.names = sems, []

    def start(self, **moves):
        self.names += [name for name in moves if name not in self.names]
        copies = [pltpu.make_async_copy(src, dst, self.sems.at[self.names.index(name)]) for name, (src, dst) in moves.items()]
        for copy in copies:
            copy.start()
        return lambda: [copy.wait() for copy in copies]

    def wait(self, name, src, dst):
        pltpu.make_async_copy(src, dst, self.sems.at[self.names.index(name)]).wait()


def rope(v, cosine, sine):
    wide = cosine.shape[1]
    heads = []
    for h in range(v.shape[1] // wide):
        part = v[:, h * wide : (h + 1) * wide]
        turned = jnp.concatenate([part[:, wide // 2 :], part[:, : wide // 2]], axis=1)
        heads.append(part * cosine + turned * sine)
    return jnp.concatenate(heads, axis=1)


def each(count, size, visit):
    def body(i, carry):
        visit(pl.multiple_of(i * size, size))
        return carry

    lax.fori_loop(0, count // size, body, 0)


def col_loop(cols, tile, visit):
    each(cols, tile, lambda start: visit(pl.ds(start, tile)))


def dot_nt(a, b):
    return lax.dot_general(a, b, NT, preferred_element_type=F32)


def dot(a, b):
    return jnp.dot(a, b, preferred_element_type=F32)


def norm_block(feats):
    inverse = lax.rsqrt(over_row(jnp.mean, feats * feats) + NORM_EPS)
    return feats * inverse, inverse


def norm_back(d_act, gain, normed, inverse):
    d_normed = d_act * gain
    return inverse * (d_normed - normed * over_row(jnp.mean, d_normed * normed))


def remote_call(body, collective_id, name, out_shape, in_places, out_places, scratch, gflops):
    return pl.pallas_call(
        body,
        out_shape=out_shape,
        in_specs=specs(in_places),
        out_specs=specs(out_places),
        scratch_shapes=scratch,
        compiler_params=pltpu.CompilerParams(collective_id=collective_id, has_side_effects=True, vmem_limit_bytes=REMOTE_VMEM),
        cost_estimate=cost(gflops, 60),
        name=name,
    )


def join_columns(parts, whole):
    start, moves = 0, {}
    for i, part in enumerate(parts):
        moves[f"join{i}"] = (part, whole.at[:, pl.ds(start, part.shape[1])])
        start += part.shape[1]
    return moves


def enter_body(picked, wq_in, wk_in, wv_in, gain, pos, inv_freq, dy_in, wd_in, x_out, q_out, k_out, v_out, cosine, sine, dh_out, k2_out, v2_out, act_all, dy_all, wide, mid, narrow, send, recv, act, dy, wd, dh, w_all, pair_sems, share_sems, load_sems):
    place = Place()
    place.meet()
    span = x_out.shape[0]
    rows = span // STEPS
    total = Total(place, lambda step: picked.at[pl.ds(step * rows, rows)], wide, mid, narrow, x_out, send, recv)
    share = Share(place, share_sems, span)
    loads = Loads(load_sems)
    for step in range(STEPS):
        total.begin(step)
    loaded = loads.start(dy=(dy_in, dy), wd=(wd_in, wd))
    projection = loads.start(**join_columns((wq_in, wk_in, wv_in), w_all))
    stores = []
    kw = k_out.shape[1]
    qw = q_out.shape[1]

    def back(step):
        here = pl.ds(step * rows, rows)

        def tile(cols):
            dh[here, cols] = dot_nt(dy[here, :], wd[cols, :]).astype(BF16)

        col_loop(wd.shape[0], WIDE_TILE, tile)
        stores.append(loads.start(**{f"dh{step}": (dh.at[here], dh_out.at[here])}))

    pairs = []

    def project(step):
        here = pl.ds(step * rows, rows)

        def norm(start):
            at = pl.ds(step * rows + start, ROW_BLOCK)
            normed, _ = norm_block(x_out[at, :].astype(F32))
            act[at, :] = (normed * gain[()].astype(F32)).astype(BF16)

        each(rows, ROW_BLOCK, norm)
        stores.append(share.start(act.at[here], act_all, step * rows))
        c, s = cosine[here, :], sine[here, :]
        out = dot(act[here, :], w_all[()])
        q_out[here, :] = rope(out[:, :qw], c, s).astype(BF16)
        k_out[here, :] = rope(out[:, qw : qw + kw], c, s).astype(BF16)
        v_out[here, :] = out[:, qw + kw :].astype(BF16)
        for i, (src, dst) in enumerate(((k_out, k2_out), (v_out, v2_out))):
            pairs.append(remote(src.at[here], dst.at[here], *(pair_sems.at[step, i, end] for end in range(2)), place.twin))
            pairs[-1].start()

    def angles(start):
        at = pl.ds(start, ROW_BLOCK)
        angle = pos[at, :].astype(F32) * inv_freq[()]
        c, s = jnp.cos(angle), jnp.sin(angle)
        cosine[at, :] = jnp.concatenate([c, c], axis=1)
        sine[at, :] = jnp.concatenate([-s, s], axis=1)

    loaded()
    stores.append(share.start(dy, dy_all, 0))
    each(span, ROW_BLOCK, angles)
    for step in range(STEPS):
        back(step)
        total.fold_wide(step)
    for stage in (total.fold_narrow, total.widen):
        for step in range(STEPS):
            stage(step)
    projection()
    for step in range(STEPS):
        total.finish(step)
        project(step)
    for step in range(STEPS):
        total.sent(step, range(4))
    for copy in pairs:
        copy.wait()
    for done in stores:
        done()
    share.arrived()


def enter(picked, wq, wk, wv, gain, pos, inv_freq, dy, wd):
    span, width = picked.shape
    key = shape(span, wk.shape[1])
    angles = shape(span, 2 * inv_freq.shape[1], F32)
    all_rows = shape(2 * span, width)
    big = pltpu.VMEM((span, width), BF16)
    out_shape = [shape(span, width), shape(span, wq.shape[1]), key, key, angles, angles, shape(span, wd.shape[0]), key, key, all_rows, all_rows]
    scratch = total_scratch(width, BF16, span // STEPS) + [big, big, pltpu.VMEM(wd.shape, BF16), pltpu.VMEM((span, wd.shape[0]), BF16), pltpu.VMEM((width, wq.shape[1] + 2 * wk.shape[1]), BF16)]
    scratch += [DMA((STEPS, 2, 2)), sems(STEPS + 1), DMA((5 + STEPS,))]
    call = remote_call(enter_body, 1, "enter", out_shape, "vhhhvvvhh", "vvvvvvhhhhh", scratch, 80)
    return call(picked, wq, wk, wv, gain, pos, inv_freq, dy, wd)


def middle_body(att, wo_own, wo_1, wo_2, wo_3, x_in, wg_in, wu_in, wd_in, dh_in, dy_in, gain, h_out, keep_x, send_x, keep_y, send_y, b_all, hidden_all, dgate_all, dup_all, att_all, drb_all, dr_out, datt_out, dgain_out,
                wide, mid, narrow, send, recv, wo, wg, wu, att_full, part_buf, d_b, h, row_in, dh, b, hid, dgt, dup, att_send, att_recv, wo_sems, load_sems, share_sems):
    place = Place()
    span, width = x_in.shape
    rows = span // STEPS
    half = rows // 2
    cols = att.shape[1]
    ffn = wg.shape[1]
    loads = Loads(load_sems)
    chunk = lambda step: pl.ds(step * rows, rows)
    by_chip = lambda tp: rows_at(tp * cols, cols, 128)

    mine = loads.start(att=(att, att_full.at[:, by_chip(place.tp)]), wo=(wo_own, wo.at[by_chip(place.tp)]))
    place.meet()

    x_tp, y_tp = place.over_x[0], place.over_y[0]

    def att_copy(step, kind, hop):
        at = pl.ds(step * rows + kind * half, half)
        first, second = ((place.over_y, place.over_x), (place.over_x, place.over_y))[kind]
        relay = hop == 2
        dst = att_full.at[at, by_chip(first[0] if relay else place.tp)]
        return remote(dst if relay else att.at[at], dst, att_send.at[step, kind, hop], att_recv.at[step, kind, hop], second if hop else first)

    def att_begin(step):
        for hop in range(2):
            for kind in range(2):
                att_copy(step, kind, hop).start()

    def att_forward(step):
        for kind in range(2):
            att_copy(step, kind, 0).wait_recv()
            att_copy(step, kind, 2).start()

    att_begin(0)
    part = wo_1.shape[0]
    arrivals = []
    near = jnp.where(place.cp == 0, y_tp, x_tp)
    chips = (near, x_tp + y_tp - near, place.chip(1, 1))
    for i, (src, chip) in enumerate(zip((wo_1, wo_2, wo_3), chips)):
        at = wo.at[rows_at((2 * chip + place.cp) * part, part, 128)]
        here_sem, send_sem, recv_sem = (wo_sems.at[i, end] for end in range(3))
        for copy in (pltpu.make_async_copy(src, at, here_sem), remote(src, at, send_sem, recv_sem, place.twin)):
            copy.start()
            arrivals.append(copy)
    att_begin(1)
    weights = loads.start(wg=(wg_in, wg), wu=(wu_in, wu))

    share = Share(place, share_sems, span)
    open_shares = [share.start(att, att_all, 0)]
    total = Total(place, lambda step: part_buf.at[step], wide, mid, narrow, d_b, send, recv)

    def fetch(step):
        return loads.start(rows=(x_in.at[chunk(step)], row_in), dh=(dh_in.at[chunk(step)], dh))

    def close():
        while open_shares:
            open_shares.pop()()

    def residual_step(step):
        for kind in range(2):
            for hop in (1, 2):
                att_copy(step, kind, hop).wait_recv()

        def tile(c):
            h[:, c] = row_in[:, c].astype(F32) + dot(att_full[chunk(step), :], wo[:, c])

        col_loop(width, 2 * WIDE_TILE, tile)
        open_shares.append(loads.start(h_out=(h, h_out.at[chunk(step)])))

        def norm(start):
            at = pl.ds(start, ROW_BLOCK)
            normed, _ = norm_block(h[at, :])
            b[at, :] = (normed * gain[()].astype(F32)).astype(BF16)

        each(rows, ROW_BLOCK, norm)
        open_shares.append(share.start(b, b_all, step * rows))

    def ffn_step(step):
        def tile(c):
            gate = dot(b[()], wg[:, c])
            up = dot(b[()], wu[:, c])
            sig = 1.0 / (1.0 + jnp.exp(-gate))
            d_hid = dh[:, c].astype(F32)
            act = gate * sig
            hid[:, c] = (act * up).astype(BF16)
            dgt[:, c] = (d_hid * up * sig * (1.0 + gate * (1.0 - sig))).astype(BF16)
            dup[:, c] = (d_hid * act).astype(BF16)

        col_loop(ffn, WIDE_TILE, tile)
        for src, dst in ((hid, hidden_all), (dgt, dgate_all), (dup, dup_all)):
            open_shares.append(share.start(src, dst, step * rows))

    def back_step(step):
        def tile(c):
            part_buf[step, :, c] = dot_nt(dgt[()], wg[c, :]) + dot_nt(dup[()], wu[c, :])

        col_loop(width, WIDE_TILE, tile)
        total.begin(step)

    fetched = fetch(0)
    att_forward(0)
    for step in range(2, STEPS):
        att_begin(step)
    mine()
    for copy in arrivals:
        copy.wait()
    att_forward(1)
    for step in range(STEPS):
        if step >= 1:
            close()
        fetched()
        residual_step(step)
        if step == 0:
            weights()
        ffn_step(step)
        if step == 0:
            att_forward(2)
        if step + 1 < STEPS:
            fetched = fetch(step + 1)
        back_step(step)
        if step == 0:
            att_forward(3)
        if step >= 2:
            total.fold_wide(step - 2)

    clear(dgain_out)
    close()
    wd = wg
    weights = loads.start(wg=(wd_in, wd))
    d_r, y_buf = part_buf.at[0], part_buf.at[1]

    def reload(step):
        to_output = step < STEPS
        step = step % STEPS
        at = pl.ds(pl.multiple_of(place.cp * span + step * rows, rows), rows)
        return loads.start(h_in=(h_out.at[chunk(step)], h), **(dict(hid=(hidden_all.at[at], hid)) if to_output else dict(rows=(dy_in.at[chunk(step)], row_in))))

    def resid_grad(step):
        def grad(start):
            at = pl.ds(start, ROW_BLOCK)
            normed, inverse = norm_block(h[at, :])
            d_act = d_b[pl.ds(step * rows + start, ROW_BLOCK), :].astype(F32)
            dgain_out[()] += over_column(d_act * normed)
            out = row_in[at, :].astype(F32) + norm_back(d_act, gain[()].astype(F32), normed, inverse)
            d_r[at, :] = out
            b[at, :] = out.astype(BF16)

        each(rows, ROW_BLOCK, grad)
        open_shares.append(loads.start(dr=(d_r, dr_out.at[chunk(step)])))
        open_shares.append(share.start(b, drb_all, step * rows))
        datt_out[chunk(step), :] = dot_nt(b[()], wo[by_chip(place.tp), :]).astype(BF16)

    def output_step(step):
        kind = step // 2
        first, second = ((place.x, place.y), (place.y, place.x))[kind]
        kept = first == step % 2
        row = lax.broadcasted_iota(jnp.int32, (rows, 1), 0)
        owner = kept & (lax.div(row, half) == second)

        def tile(c):
            y_buf[:, c] = dot(hid[()], wd[:, c]) + jnp.where(owner, h[:, c], 0.0)

        col_loop(width, 2 * WIDE_TILE, tile)
        keep, send = ((keep_x, send_x), (keep_y, send_y))[kind]
        for chosen, dst in ((kept, keep), (jnp.logical_not(kept), send)):

            @pl.when(chosen)
            def _():
                loads.start(y=(y_buf, dst))

        open_shares.append(functools.partial(loads.wait, "y", y_buf, keep))

    for step in range(2):
        total.sent(step, (0,))
    item = [0, reload(0)]

    def next_item():
        step, fetched = item
        fetched()
        if step == 0:
            weights()
        close()
        if step < STEPS:
            output_step(step)
        else:
            resid_grad(step - STEPS)
        step += 1
        item[:] = [step, reload(step) if step < 2 * STEPS else None]

    for tick in range(STEPS):
        for stage, step in ((total.fold_wide, tick + 2), (total.fold_narrow, tick), (total.widen, tick - 2)):
            if 0 <= step < STEPS:
                stage(step)
            if stage == total.fold_wide:
                next_item()
    for step in range(STEPS):
        if step + 2 < STEPS:
            total.widen(step + 2)
        total.finish(step)
        next_item()
    close()
    for step in range(2, STEPS):
        total.sent(step, (0,))
    for copy_step in range(STEPS):
        total.sent(copy_step, range(1, 4))
        for kind in range(2):
            for hop in range(3):
                att_copy(copy_step, kind, hop).wait_send()
    share.arrived()


def middle(att, wo_pieces, x, wg, wu, wd, d_hidden, dy, gain):
    span, width = x.shape
    rows = span // STEPS
    ffn = wg.shape[1]
    cols = att.shape[1]
    full = shape(span, width, F32)
    both = shape(2 * span, ffn)
    out_shape = [full] + [shape(rows, width, F32)] * 4 + [shape(2 * span, width), both, both, both, shape(2 * span, cols), shape(2 * span, width), full, shape(span, cols), shape(1, width, F32)]
    buf = lambda r, c, dtype=BF16: pltpu.VMEM((r, c), dtype)
    scratch = total_scratch(width, F32, rows)
    scratch += [buf(width, width), buf(width, ffn), buf(width, ffn), buf(span, width), pltpu.VMEM((STEPS, rows, width), F32), buf(span, width), buf(rows, width, F32)]
    scratch += [buf(rows, c) for c in (width, ffn, width, ffn, ffn, ffn)]
    scratch += [sems(STEPS, 2), sems(STEPS, 2), sems(3), DMA((11,)), sems(1 + 5 * STEPS)]
    call = remote_call(middle_body, 2, "middle", out_shape, "vhhhhhhhhhhv", "hhhhhhhhhhhhvv", scratch, 120)
    return call(att, *wo_pieces, x, wg, wu, wd, d_hidden, dy, gain)


def leave_body(dq_in, dk_in, dv_in, dk2_in, dv2_in, cosine, sine, wq_in, wk_in, wv_in, x_in, dr_in, gain, dgain_b, b_all, hidden_all, dgate_all, dup_all, dy_all, act_all, att_all, drb_all, d_all, dx_all, gains_out, grad_gate, grad_up, grad_down, grad_q, grad_k, grad_v, grad_out,
               wide, mid, narrow, send, recv, part_buf, d_a, dk_got, dv_got, d_qkv, w_all, xs, drs, dxs, gain_got, left, right, result, pair_sems, load_sems, share_sems, left_sems, right_sems, result_sems):
    place = Place()
    place.meet()
    span, width = x_in.shape
    rows = span // STEPS
    chunk = lambda step: pl.ds(step * rows, rows)
    swap = lambda i, src, dst: remote(src, dst, *(pair_sems.at[i, end] for end in range(2)), place.twin)
    pairs = [[swap(2 * step + i, src.at[chunk(step)], dst.at[chunk(step)]) for i, (src, dst) in enumerate(((dk2_in, dk_got), (dv2_in, dv_got)))] for step in range(STEPS)]
    for copy in sum(pairs, []):
        copy.start()
    qw = dq_in.shape[1]
    kw = dk_in.shape[1]
    share = Share(place, share_sems, span)
    loads = Loads(load_sems)
    total = Total(place, lambda step: part_buf.at[step], wide, mid, narrow, d_a, send, recv)

    def partial(step):
        here = chunk(step)
        c, s = cosine[here, :], -sine[here, :]
        for copy in pairs[step]:
            copy.wait()
        d_qkv[here, :qw] = rope(dq_in[here, :].astype(F32), c, s).astype(BF16)
        dk_sum = (dk_in[here, :] + dk_got[here, :]).astype(BF16).astype(F32)
        d_qkv[here, qw : qw + kw] = rope(dk_sum, c, s).astype(BF16)
        d_qkv[here, qw + kw :] = (dv_in[here, :] + dv_got[here, :]).astype(BF16)
        if step == 0:
            weights()

        def tile(n):
            part_buf[step, :, n] = dot_nt(d_qkv[here, :], w_all[n, :])

        col_loop(width, 2 * WIDE_TILE, tile)
        total.begin(step)

    def load(step):
        return loads.start(x=(x_in.at[chunk(step)], xs), dr=(dr_in.at[chunk(step)], drs))

    gain_a = pl.ds(0, 1)
    clear(gains_out.at[gain_a])
    gains_out[pl.ds(1, 1), :] = dgain_b[()]
    open_shares = []

    def grad_x(step):
        def grad(start):
            at = pl.ds(start, ROW_BLOCK)
            normed, inverse = norm_block(xs[at, :].astype(F32))
            d_act = d_a[pl.ds(step * rows + start, ROW_BLOCK), :].astype(F32)
            gains_out[gain_a, :] += over_column(d_act * normed)
            dxs[at, :] = drs[at, :] + norm_back(d_act, gain[()].astype(F32), normed, inverse)

        each(rows, ROW_BLOCK, grad)
        open_shares.append(share.start(dxs, dx_all, step * rows))

    _, _, narrow_cols = left.shape
    _, _, wide_cols = right.shape
    lefts, rights = Ring(left, left_sems, True), Ring(right, right_sems, True)
    sides = width // wide_cols
    columns = lambda n: pl.ds(n * wide_cols, wide_cols)
    blocks = []
    for left_ref, right_ref, out in ((b_all, dgate_all, grad_gate), (b_all, dup_all, grad_up), (hidden_all, dy_all, grad_down), (att_all, drb_all, grad_out)):
        for n in range(sides):
            blocks.append((left_ref, right_ref.at[:, columns(n)], [(columns(0), out.at[:, columns(n)])]))
    start = 0
    outs = []
    for ref in (grad_q, grad_k, grad_v):
        outs.append((pl.ds(start, ref.shape[1]), ref))
        start += ref.shape[1]
    blocks.append((act_all, d_all, outs))

    pieces = 2
    work = [(block, piece, pieces) for block in range(3 * sides) for piece in range(pieces)]
    work += [(block, 0, 1) for block in range(3 * sides, len(blocks))]
    at = lambda i: rows_at(i * narrow_cols, narrow_cols, TILE)

    def span_of(k):
        block, piece, pieces = work[k]
        count = blocks[block][0].shape[1] // narrow_cols // pieces
        return piece * count, (piece + 1) * count

    def left_start(k, i):
        lefts.start(i, 0, [blocks[work[k][0]][0].at[:, at(i)]])

    def right_start(block):
        rights.start(block, 0, [blocks[block][1]])

    def stored(i):
        done = result.at[lefts.slot(i)]
        pltpu.make_async_copy(done, done, result_sems.at[lefts.slot(i)]).wait()

    def product(k):
        block, piece, _ = work[k]
        left_ref, right_view, outs = blocks[block]
        first, last = span_of(k)
        if piece == 0:
            if block + 2 < len(blocks):
                right_start(block + 1)
            rights.wait(block, right_view)
        more = k + 1 < len(work)
        early = more and (last - span_of(k + 1)[0]) % 2 == 0

        def step(i, carry):
            pl.when(i + 1 < last)(lambda: left_start(k, i + 1))
            if early:
                pl.when(i + 1 == last)(lambda: left_start(k + 1, span_of(k + 1)[0]))
            lefts.wait(i, left_ref.at[:, at(i)])
            if k:
                stored(i)
            slot = lefts.slot(i)
            result[slot] = lax.dot_general(left[slot], right[block % 2], CONTRACT_FIRST, preferred_element_type=F32)
            for cols, out in outs:
                pltpu.make_async_copy(result.at[slot, :, cols], out.at[at(i)], result_sems.at[slot]).start()
            return carry

        lax.fori_loop(first, last, step, 0)
        if more and not early:
            left_start(k + 1, span_of(k + 1)[0])

    left_start(0, 0)
    right_start(0)
    weights = loads.start(**join_columns((wq_in, wk_in, wv_in), w_all))
    loaded = load(0)
    for step in range(STEPS):
        partial(step)
    first = share.apart(d_qkv, d_all)
    for step in range(STEPS):
        for k in range(3 * step, 3 * step + 3):
            product(k)
        total.fold_wide(step)
    d_sent, d_arrived = first
    for stage in (total.fold_narrow, total.widen):
        for step in range(STEPS - 1):
            stage(step)
        if stage == total.fold_narrow:
            for k in range(3 * STEPS, len(work) - 1):
                product(k)
        else:
            d_arrived()
            right_start(len(blocks) - 1)
            product(len(work) - 1)
            for i in range(2):
                stored(i)
        stage(STEPS - 1)
    for step in range(STEPS):
        loaded()
        total.finish(step)
        while open_shares:
            open_shares.pop()()
        grad_x(step)
        if step + 1 < STEPS:
            loaded = load(step + 1)
    last = swap(2 * STEPS, gains_out, gain_got)
    last.start()
    last.wait()
    gains_out[()] = gains_out[()] + gain_got[()]
    for sent in open_shares + [d_sent]:
        sent()
    for step in range(STEPS):
        total.sent(step, range(4))
    share.arrived()


def leave(dq, dk, dv, dk2, dv2, cosine, sine, wq, wk, wv, x, d_resid, gain, dgain_b, *products):
    span, width = x.shape
    rows = span // STEPS
    kw = wk.shape[1]
    qw = wq.shape[1]
    cols = qw + 2 * kw
    buf = lambda r, c, dtype=F32: pltpu.VMEM((r, c), dtype)
    ffn = products[1].shape[1]
    out_shape = [shape(2 * span, cols), shape(2 * span, width, F32), shape(2, width, F32)]
    out_shape += [shape(*dims, F32) for dims in ((width, ffn), (width, ffn), (ffn, width), wq.shape, wk.shape, wv.shape, (qw, width))]
    twice = lambda r, c, dtype: pltpu.VMEM((2, r, c), dtype)
    scratch = total_scratch(width, F32, rows) + [pltpu.VMEM((STEPS, rows, width), F32), buf(span, width, BF16), buf(span, kw), buf(span, kw), buf(span, cols, BF16), buf(width, cols, BF16)]
    scratch += [buf(rows, width, BF16), buf(rows, width), buf(rows, width), buf(2, width)]
    scratch += [twice(2 * span, WIDE_TILE, BF16), twice(2 * span, 2 * WIDE_TILE, BF16), twice(WIDE_TILE, 2 * WIDE_TILE, F32)]
    scratch += [DMA((2 * STEPS + 1, 2)), DMA((5,)), sems(1 + STEPS)] + [DMA((2,))] * 3
    call = remote_call(leave_body, 3, "leave", out_shape, "vvvhhvvhhhhhvvhhhhhhhh", "hhvhhhhhhh", scratch, 1)
    return call(dq, dk, dv, dk2, dv2, cosine, sine, wq, wk, wv, x, d_resid, gain, dgain_b, *products)


def side(v, bit):
    half = v.shape[0] // 2
    return lax.dynamic_slice_in_dim(v, bit * half, half, 0)


def join(own, other, bit):
    return jnp.where(bit == 0, jnp.concatenate([own, other]), jnp.concatenate([other, own]))


def solution(mesh):
    def device_step(tokens, pos, doc_id, dy, table, w_q, w_k, w_v, w_o, w_gate, w_up, w_down, gain_one, gain_two, inv_freq):
        span = tokens.shape[0]
        rows, width = table.shape
        scale = (2 * inv_freq.shape[0]) ** -0.5
        tp = lax.axis_index("tp")
        cp = lax.axis_index("cp")
        gain_a, gain_b, inv_freq = (v[None, :] for v in (gain_one, gain_two, inv_freq))
        pos = pos[:, None]
        base = tp * rows

        wo_half = side(w_o, cp)
        wo_1 = swap_core(wo_half, 0)
        picked, grad = pick_rows(tokens, table, base)
        x, query, key, value, cosine, sine, d_hidden, key2, value2, act_a_all, dy_all = enter(picked, w_q, w_k, w_v, gain_a, pos, inv_freq, dy, w_down)
        wo_1, wo_half, query = lax.optimization_barrier((wo_1, wo_half, query))
        wo_pieces = (w_o, wo_1, swap_core(wo_half, 1), swap_core(wo_1, 1))
        att, lse, grad = attend(scale, query, key, value, key2, value2, pos, grad)
        keep_x, send_x, keep_y, send_y, act_b_all, hidden_all, d_gate_all, d_up_all, att_all, d_resid_all, d_resid, d_att, d_gain_b = middle(att, wo_pieces, x, w_gate, w_up, w_down, d_hidden, dy, gain_b)[1:]

        x_bit, y_bit = tp % 2, tp // 2
        ways = ((keep_x, swap_x, x_bit, swap_y, y_bit), (keep_y, swap_y, y_bit, swap_x, x_bit))
        y_wide = [swap_x(send_x), swap_y(send_y)]
        d_query, d_key, d_value, d_key2, d_value2, grad = attend_back(scale, query, d_att, lse, key, value, key2, value2, pos, grad)

        tokens, d_query = lax.optimization_barrier((tokens, d_query))
        all_ids = join(tokens, swap_c(tokens), cp)
        packed = lax.sort(all_ids * (2 * span) + jnp.arange(2 * span, dtype=jnp.int32))
        sorted_ids, perm = packed // (2 * span), packed % (2 * span)
        lowest, highest = (jnp.sum((all_ids < bound).astype(jnp.int32)) for bound in (base, base + rows))
        bounds = jnp.stack([lowest, highest, base.astype(jnp.int32)])

        d_query, bounds, perm = lax.optimization_barrier((d_query, bounds, perm))
        d_x_all, gains, grad_gate, grad_up, grad_down, *grads = leave(d_query, d_key, d_value, d_key2, d_value2, cosine, sine, w_q, w_k, w_v, x, d_resid, gain_a, d_gain_b, act_b_all, hidden_all, d_gate_all, d_up_all, dy_all, act_a_all, att_all, d_resid_all)[1:]
        y_wide, d_x_all = lax.optimization_barrier((y_wide, d_x_all))
        y_mid = [keep + wide for (keep, _, _, _, _), wide in zip(ways, y_wide)]
        y_narrow = [swap_2(side(mid, 1 - bit_2)) for (_, _, _, swap_2, bit_2), mid in zip(ways, y_mid)]
        y_mid, grad_gate = lax.optimization_barrier((y_mid, grad_gate))
        grad_gate, *grads = move(grad_gate, *grads)
        y_narrow, grad_gate = lax.optimization_barrier((y_narrow, grad_gate))
        y_own = [(side(mid, bit_2) + narrow).astype(BF16) for (_, _, _, _, bit_2), mid, narrow in zip(ways, y_mid, y_narrow)]
        y_pair = [join(own, swap_2(own), bit_2) for (_, _, _, swap_2, bit_2), own in zip(ways, y_own)]
        y_own, grad_down = lax.optimization_barrier((y_own, grad_down))
        (grad_down,) = move(grad_down)
        y_pair, grad_down = lax.optimization_barrier((y_pair, grad_down))
        y_far = [swap_1(pair) for (_, swap_1, _, _, _), pair in zip(ways, y_pair)]
        y_pair, d_x_all = lax.optimization_barrier((y_pair, d_x_all))
        grad_table, grad_up = put_rows(sorted_ids, perm, bounds, d_x_all, grad, (grad_up,))
        y_rows = [jnp.where(bit_1 == k, pair, far) for (_, _, bit_1, _, _), pair, far in zip(ways, y_pair, y_far) for k in range(2)]
        return (jnp.concatenate(y_rows), grad_table, *grads, grad_gate, grad_up, grad_down, *gains)

    col_spec = P(None, "tp")
    row_spec = P("tp", None)
    tok_spec = P("cp")
    rep_spec = P(None)
    in_specs = (tok_spec, tok_spec, tok_spec, P("cp", None), row_spec, col_spec, col_spec, col_spec, row_spec, col_spec, col_spec, row_spec, rep_spec, rep_spec, rep_spec)
    out_specs = (P("cp", None), row_spec, col_spec, col_spec, col_spec, row_spec, col_spec, col_spec, row_spec, rep_spec, rep_spec)
    return jax.shard_map(device_step, mesh=mesh, in_specs=in_specs, out_specs=out_specs, check_vma=False)
```

```python
import functools

import jax
import jax.numpy as jnp
from jax import lax
from jax.experimental import pallas as pl
from jax.experimental.pallas import tpu as pltpu
from jax.sharding import PartitionSpec as P

NORM_EPS = 1e-5
NEG_BIG = -1e30
F32 = jnp.float32
BF16 = jnp.bfloat16
MIB = 2**20
LOCAL_VMEM = 56 * MIB
REMOTE_VMEM = 63 * MIB
STEPS = 4
SUBLANES = 8
ROW_BLOCK = 32
WIDE_TILE = 512
BIG_TILE = 1024
TILE = 256
MESH_ID = pl.DeviceIdType.MESH
NT = (((1,), (1,)), ((), ()))
CONTRACT_FIRST = (((0,), (0,)), ((), ()))
VMEM = pl.BlockSpec(memory_space=pltpu.VMEM)
SMEM = pl.BlockSpec(memory_space=pltpu.SMEM)
HBM = pl.BlockSpec(memory_space=pl.ANY)
DMA = pltpu.SemaphoreType.DMA


X_PAIRS, Y_PAIRS = ([(chip, chip ^ flip) for chip in range(4)] for flip in (1, 2))
C_PAIRS = X_PAIRS[:2]
CORE_PAIRS = tuple([(2 * a + core, 2 * b + core) for core, pairs in enumerate(kinds) for a, b in pairs] for kinds in ((Y_PAIRS, X_PAIRS), (X_PAIRS, Y_PAIRS)))


def swap_x(v):
    return lax.ppermute(v, "tp", X_PAIRS)


def swap_y(v):
    return lax.ppermute(v, "tp", Y_PAIRS)


def swap_c(v):
    return lax.ppermute(v, "cp", C_PAIRS)


def swap_core(v, which):
    return lax.ppermute(v, ("tp", "cp"), CORE_PAIRS[which])


def over_row(reduce, v):
    return reduce(v, axis=-1, keepdims=True)


def over_column(v):
    return jnp.sum(v, axis=0, keepdims=True)


def specs(places):
    return [{"v": VMEM, "h": HBM, "s": SMEM}[place] for place in places]


def cost(gflops, mib):
    return pl.CostEstimate(flops=gflops * 10**9, bytes_accessed=mib * MIB, transcendentals=0)


def shape(rows, cols, dtype=BF16):
    return jax.ShapeDtypeStruct((rows, cols), dtype)


def local_call(body, name, out_shape, in_specs, out_specs, scratch, gflops, aliases={}, **grid):
    return pl.pallas_call(
        body,
        out_shape=out_shape,
        in_specs=in_specs,
        out_specs=out_specs,
        scratch_shapes=scratch,
        input_output_aliases=aliases,
        compiler_params=pltpu.CompilerParams(vmem_limit_bytes=LOCAL_VMEM),
        cost_estimate=cost(gflops, 60),
        name=name,
        **grid,
    )


def rows_at(start, size, step=32):
    return pl.ds(pl.multiple_of(start, step), size)


class Ring:
    def __init__(self, buf, sems, inward):
        self.buf, self.sems, self.inward = buf, sems, inward

    def slot(self, count):
        return lax.rem(count, self.buf.shape[0])

    def _copy(self, count, view):
        pair = (view, self.buf.at[self.slot(count)])
        return pltpu.make_async_copy(*(pair if self.inward else pair[::-1]), self.sems.at[self.slot(count)])

    def start(self, count, kind, views):
        for k, view in enumerate(views):
            pl.when(kind == k)(lambda: self._copy(count, view).start())

    def wait(self, count, view):
        self._copy(count, view).wait()


ZERO_ROWS = 24
ZEROS = {"attend": (24, 68), "attend_back": (39, 78)}
ZERO_PICK = 2


def zero_block(out_ref, block, count=1):
    return out_ref.at[pl.ds(pl.multiple_of(block * ZERO_ROWS, ZERO_ROWS), count * ZERO_ROWS)]


def clear(ref, value=0.0):
    ref[()] = jnp.full(ref.shape, value, F32)


def start_zeros(out_ref, zero_ref, sem, first, count):
    def start(i, carry):
        pltpu.make_async_copy(zero_ref, zero_block(out_ref, first + i), sem).start()
        return carry

    lax.fori_loop(0, count, start, 0)


def wait_zeros(out_ref, sem, first, count):
    whole = zero_block(out_ref, first, count)
    pltpu.make_async_copy(whole, whole, sem).wait()


def zero_scratch(width):
    return [pltpu.VMEM((ZERO_ROWS, width), F32), DMA]


def grid_zeros(grad_ref, zero_ref, sem, name):
    head, tile = pl.program_id(0), pl.program_id(1)
    heads, tiles = pl.num_programs(0), pl.num_programs(1)
    half = tiles // 2
    early, late = ZEROS[name]
    whole = half * (early + late)
    before = grad_ref.shape[0] // ZERO_ROWS - heads * whole
    if name == "attend":
        before -= heads * half * sum(ZEROS["attend_back"])
    pl.when((head == 0) & (tile == 0))(functools.partial(clear, zero_ref))
    first = before + head * whole + tile * early + jnp.maximum(tile - half, 0) * (late - early)
    start_zeros(grad_ref, zero_ref, sem, first, early)
    pl.when(tile >= half)(functools.partial(start_zeros, grad_ref, zero_ref, sem, first + early, late - early))
    last = (head == heads - 1) & (tile == tiles - 1)
    return lambda: pl.when(last)(lambda: wait_zeros(grad_ref, sem, before, heads * whole))


GATHER_BATCH = 16
GATHER_SLOTS = 8


def pick_body(group_ref, lane_ref, count_ref, table_ref, out_ref, grad_ref, buf, sems, zero_ref, zero_sem):
    batches = out_ref.shape[0] // GATHER_BATCH
    width = out_ref.shape[1]

    def row_copy(group, slot, j):
        return pltpu.make_async_copy(table_ref.at[group], buf.at[slot, j], sems.at[slot])

    def start(step):
        slot = lax.rem(step, GATHER_SLOTS)
        for j in range(GATHER_BATCH):
            group = group_ref[step * GATHER_BATCH + j]
            pl.when(group >= 0)(lambda: row_copy(group, slot, j).start())

    for step in range(GATHER_SLOTS - 1):
        start(step)
    clear(zero_ref)
    row = lax.broadcasted_iota(jnp.int32, (SUBLANES, width), 0)

    def loop(step, carry):
        slot = lax.rem(step, GATHER_SLOTS)

        @pl.when(step + GATHER_SLOTS - 1 < batches)
        def _():
            start(step + GATHER_SLOTS - 1)

        start_zeros(grad_ref, zero_ref, zero_sem, step * ZERO_PICK, ZERO_PICK)

        def arrived(i, carry):
            row_copy(0, slot, 0).wait()
            return carry

        lax.fori_loop(0, count_ref[step], arrived, 0)
        first = pl.multiple_of(step * GATHER_BATCH, GATHER_BATCH)
        parts = []
        for j in range(GATHER_BATCH):
            lane = lane_ref[first + j]
            goal = j % SUBLANES
            if goal == 0:
                parts.append(jnp.zeros((SUBLANES, width), F32))
            turned = pltpu.roll(buf[slot, j].astype(F32), lax.rem(goal + SUBLANES - lane, SUBLANES), 0)
            parts[-1] = jnp.where(row == jnp.where(lane < SUBLANES, goal, SUBLANES), turned, parts[-1])
        out_ref[pl.ds(first, GATHER_BATCH), :] = jnp.concatenate(parts, axis=0).astype(BF16)
        return carry

    lax.fori_loop(0, batches, loop, 0)
    wait_zeros(grad_ref, zero_sem, 0, batches * ZERO_PICK)


def pick_rows(tokens, table, base):
    span = tokens.shape[0]
    rows, width = table.shape
    local = tokens - base
    owned = (local >= 0) & (local < rows)
    group = jnp.where(owned, local // SUBLANES, -1)
    lane = jnp.where(owned, local % SUBLANES, SUBLANES)
    count = jnp.sum(owned.reshape(-1, GATHER_BATCH).astype(jnp.int32), axis=1)
    scratch = [pltpu.VMEM((GATHER_SLOTS, GATHER_BATCH, SUBLANES, width), BF16), DMA((GATHER_SLOTS,))] + zero_scratch(width)
    return local_call(pick_body, "pick_rows", [shape(span, width), shape(rows, width, F32)], specs("sssh"), specs("vh"), scratch, 20)(group, lane, count, table.reshape(rows // SUBLANES, SUBLANES, width))


SEMS = 32
AHEAD = 4
MOVE_SLOTS = 8
MOVE_ROWS = 128


LANES = 128
KEY_BITS = 11


def put_body(keys_ref, all_ref, zero_ref, *refs):
    kinds = len(refs) // 2 - 4
    sources, out_ref, rest = refs[:kinds], refs[kinds], refs[kinds + 1 :]
    targets, (rows_ref, load_sem, sems, moved, read_sems, write_sems, place, sent) = rest[:kinds], rest[kinds:]
    load = pltpu.make_async_copy(all_ref, rows_ref, load_sem)
    load.start()
    tokens = rows_ref.shape[0]
    base = lax.axis_index("tp") * out_ref.shape[0]

    def id_at(pos):
        return lax.shift_right_arithmetic(keys_ref[pos], KEY_BITS)

    def first_at(bound):
        def narrow(_, ends):
            low, high = ends
            middle = lax.div(low + high, 2)
            below = id_at(middle) < bound
            return jnp.where(below, middle + 1, low), jnp.where(below, high, middle)

        return lax.fori_loop(0, KEY_BITS + 1, narrow, (jnp.int32(0), jnp.int32(tokens)))[0]

    low, high = first_at(base), first_at(base + out_ref.shape[0])
    pieces = sources[0].shape[0] // MOVE_ROWS
    moves = kinds * pieces
    lag = MOVE_SLOTS // 2
    steps = moves + MOVE_SLOTS

    reads, writes = Ring(moved, read_sems, True), Ring(moved, write_sems, False)

    def views(arrays, step):
        return [ref.at[rows_at(lax.rem(step, pieces) * MOVE_ROWS, MOVE_ROWS)] for ref in arrays]

    def move(step):
        @pl.when(step >= MOVE_SLOTS)
        def _():
            writes.wait(step, views(targets, step)[0])

        @pl.when(step < moves)
        def _():
            reads.start(step, lax.div(step, pieces), views(sources, step))

        ready = step - lag

        @pl.when((ready >= 0) & (ready < moves))
        def _():
            reads.wait(ready, views(sources, ready)[0])
            writes.start(ready, lax.div(ready, pieces), views(targets, ready))

    def row(pos):
        return pl.ds(pos, 1)

    def wait_slot(slot):
        pltpu.make_async_copy(rows_ref.at[row(0), :], out_ref.at[row(0), :], sems.at[slot]).wait()

    def row_of(pos):
        return row(lax.bitwise_and(keys_ref[pos], tokens - 1))

    def token(pos):
        return rows_ref[row_of(pos), :]

    def one_id(carry):
        pos, count = carry
        row_id = id_at(pos)
        first = row_of(pos)

        def more(carry):
            return id_at(carry[0]) == row_id

        def add(carry):
            start, total = carry
            end = start
            for k in range(AHEAD):
                same = id_at(start + k) == row_id
                total = total + jnp.where(same, token(start + k), 0.0)
                end = end + same.astype(jnp.int32)
            return end, total

        after, total = lax.while_loop(more, add, (pos + 1, token(pos)))

        @pl.when(after > pos + 1)
        def _():
            rows_ref[first, :] = total

        slot = lax.rem(count, SEMS)
        pl.when(count >= SEMS)(lambda: wait_slot(slot))
        pltpu.make_async_copy(rows_ref.at[first, :], out_ref.at[row(row_id - base), :], sems.at[slot]).start()
        return after, count + 1

    place[0] = low
    sent[0] = 0

    def step_body(step, carry):
        move(step)
        pl.when(step == 0)(load.wait)
        limit = low + lax.div((high - low) * (step + 1), steps)
        pos, count = lax.while_loop(lambda c: c[0] < limit, one_id, (place[0], sent[0]))
        place[0] = pos
        sent[0] = count
        return carry

    lax.fori_loop(0, steps, step_body, 0)
    count = sent[0]

    def drain(slot, carry):
        pl.when(slot < count)(lambda: wait_slot(slot))
        return carry

    lax.fori_loop(0, SEMS, drain, 0)


def put_rows(keys, rows, zeros, results):
    slots = DMA((MOVE_SLOTS,))
    counter = pltpu.SMEM((1,), jnp.int32)
    scratch = [pltpu.VMEM(rows.shape, F32), DMA, DMA((SEMS,)), pltpu.VMEM((MOVE_SLOTS, MOVE_ROWS, rows.shape[1]), F32), slots, slots, counter, counter]
    out_shape = [shape(*v.shape, F32) for v in (zeros, *results)]
    return local_call(put_body, "put_rows", out_shape, specs("shh") + [HBM] * len(results), [HBM] * len(out_shape), scratch, 20, {2: 0})(keys, rows, zeros, *results)


def move_body(*refs):
    half = len(refs) // 2
    for src, dst in zip(refs[:half], refs[half:]):
        dst[()] = src[()]


def move(*arrays):
    steps = SUBLANES
    blocks = [pl.BlockSpec((v.shape[0] // steps, v.shape[1]), lambda i: (i, 0)) for v in arrays]
    return local_call(move_body, "move", [shape(*v.shape, F32) for v in arrays], blocks, blocks, [], 20, grid=(steps,))(*arrays)


Q_TILE = 256
K_TILE = 512


def as_column(row):
    return jnp.broadcast_to(row, (LANES, LANES)).T


def stack_heads(v):
    half = v.shape[1] // 2
    return jnp.concatenate([v[:, :half], v[:, half:]], axis=0)


def unstack_heads(v):
    half = v.shape[0] // 2
    return jnp.concatenate([v[:half], v[half:]], axis=1)


def sequence_chunks(cp):
    return [chunk * K_TILE for chunk in (cp, 3 - cp, 1 - cp, 2 + cp)]


class Tile:
    def __init__(self, q_ref, pos_ref):
        tile = pl.program_id(1)
        per_chunk = K_TILE // Q_TILE
        self.cp = lax.axis_index("cp")
        self.late = tile >= per_chunk
        self.chunks = sequence_chunks(self.cp)
        first = jnp.where(self.late, self.chunks[1], self.chunks[0]) + lax.rem(tile, per_chunk) * Q_TILE
        pos = jnp.concatenate([as_column(pos_ref[:, i : i + LANES])[:, :1] for i in range(0, Q_TILE, LANES)], axis=0)
        high = first + lax.broadcasted_iota(jnp.int32, pos.shape, 0)
        twice = lambda v: jnp.concatenate([v, v], axis=0)
        self.low, self.high = twice(high - pos), twice(high)
        self.q = stack_heads(q_ref[()])

    def visit(self, visit):
        needed = (True, self.late, self.late | (self.cp == 1), self.late & (self.cp == 0))
        for block, when in enumerate(needed):
            pl.when(when)(functools.partial(visit, block))

    def scores(self, scale, k, block):
        scores = lax.dot_general(self.q, k, NT, preferred_element_type=F32) * scale
        at = self.chunks[block] + lax.broadcasted_iota(jnp.int32, (1, K_TILE), 1)
        return jnp.where((at >= self.low) & (at <= self.high), scores, NEG_BIG)


def block_refs(block, *pairs):
    rows = pl.ds((block % 2) * K_TILE, K_TILE)
    return [pair[block // 2].at[rows] for pair in pairs]


def attend_body(scale, q_ref, k_ref, v_ref, k2_ref, v2_ref, pos_ref, zeros_in, out_ref, lse_ref, grad_ref, s_ref, m_ref, l_ref, acc_ref, zero_ref, zero_sem):
    end_zeros = grid_zeros(grad_ref, zero_ref, zero_sem, "attend")
    tile = Tile(q_ref, pos_ref)
    clear(m_ref, NEG_BIG)
    clear(l_ref)
    clear(acc_ref)

    def score(block):
        (k,) = block_refs(block, (k_ref, k2_ref))
        s = tile.scores(scale, k[()], block)
        s_ref[block] = s
        m_ref[()] = jnp.maximum(m_ref[()], over_row(jnp.max, s))

    def exponent(block):
        e = jnp.exp(s_ref[block] - m_ref[()])
        s_ref[block] = e
        l_ref[()] += over_row(jnp.sum, e)

    tile.visit(score)
    tile.visit(exponent)
    inverse = 1.0 / l_ref[()]

    def mix(block):
        (v,) = block_refs(block, (v_ref, v2_ref))
        prob = (s_ref[block] * inverse).astype(BF16)
        acc_ref[()] += jnp.dot(prob, v[()], preferred_element_type=F32)

    tile.visit(mix)
    out_ref[()] = unstack_heads(acc_ref[()].astype(BF16))
    lse_ref[()] = (m_ref[()] + jnp.log(l_ref[()])).reshape(lse_ref.shape)
    end_zeros()


def attention_specs(span, head_dim):
    tile = pl.BlockSpec((Q_TILE, 2 * head_dim), lambda h, t: (t, h))
    keys = pl.BlockSpec((span, head_dim), lambda h, t: (0, h))
    pos = pl.BlockSpec((1, Q_TILE), lambda h, t: (0, t))
    lse = pl.BlockSpec((1, 1, 2 * Q_TILE, 1), lambda h, t: (h, t, 0, 0))
    return tile, keys, pos, lse


def attention_buffers(heads):
    stacked = heads * Q_TILE
    return lambda c: pltpu.VMEM((stacked, c), F32), lambda dtype: pltpu.VMEM((4, stacked, K_TILE), dtype)


def attention_call(body, name, out_shape, in_specs, out_specs, scratch, gflops):
    aliases = {len(in_specs) - 1: len(out_specs) - 1}
    scratch = scratch + zero_scratch(out_shape[-1].shape[1])
    return local_call(body, name, out_shape, in_specs, out_specs, scratch, gflops, aliases, grid=(2, 4))


def attend(scale, q, k, v, k2, v2, pos, grad):
    span = q.shape[0]
    heads = 2
    head_dim = k.shape[1] // heads
    tile, keys, pos_spec, lse = attention_specs(span, head_dim)
    stacked = heads * Q_TILE
    buf, probs = attention_buffers(heads)
    out_shape = [shape(*q.shape), jax.ShapeDtypeStruct((heads, span // Q_TILE, stacked, 1), F32), shape(*grad.shape, F32)]
    column = buf(1)
    scratch = [probs(F32), column, column, buf(head_dim)]
    call = attention_call(functools.partial(attend_body, scale), "attend", out_shape, [tile] + [keys] * 4 + [pos_spec, HBM], [tile, lse, HBM], scratch, 14)
    return call(q, k, v, k2, v2, pos, grad)


def attend_back_body(scale, q_ref, do_ref, lse_ref, k_ref, v_ref, k2_ref, v2_ref, pos_ref, zeros_in, dq_ref, dk_ref, dv_ref, dk2_ref, dv2_ref, grad_ref, p_ref, dp_ref, d_ref, acc_ref, zero_ref, zero_sem):
    end_zeros = grid_zeros(grad_ref, zero_ref, zero_sem, "attend_back")
    tile = Tile(q_ref, pos_ref)
    d_out = stack_heads(do_ref[()])
    lse = lse_ref[()].reshape(d_out.shape[0], 1)
    clear(d_ref)
    clear(acc_ref)

    @pl.when(pl.program_id(1) == 0)
    def _():
        for ref in (dk_ref, dv_ref, dk2_ref, dv2_ref):
            clear(ref)

    def first(block):
        k, v = block_refs(block, (k_ref, k2_ref), (v_ref, v2_ref))
        p = jnp.exp(tile.scores(scale, k[()], block) - lse)
        dp = lax.dot_general(d_out, v[()], NT, preferred_element_type=F32).astype(BF16)
        p_ref[block] = p
        dp_ref[block] = dp
        d_ref[()] += over_row(jnp.sum, p * dp.astype(F32))

    def second(block):
        k, dk, dv = block_refs(block, (k_ref, k2_ref), (dk_ref, dk2_ref), (dv_ref, dv2_ref))
        p = p_ref[block]
        ds = (p * (dp_ref[block].astype(F32) - d_ref[()]) * scale).astype(BF16)
        acc_ref[()] += jnp.dot(ds, k[()], preferred_element_type=F32)
        dk[()] += lax.dot_general(ds, tile.q, CONTRACT_FIRST, preferred_element_type=F32)
        dv[()] += lax.dot_general(p.astype(BF16), d_out, CONTRACT_FIRST, preferred_element_type=F32)

    tile.visit(first)
    tile.visit(second)
    dq_ref[()] = unstack_heads(acc_ref[()].astype(BF16))
    end_zeros()


def attend_back(scale, q, d_out, lse, k, v, k2, v2, pos, grad):
    span = q.shape[0]
    heads = 2
    head_dim = k.shape[1] // heads
    tile, keys, pos_spec, lse_spec = attention_specs(span, head_dim)
    buf, probs = attention_buffers(heads)
    out_shape = [shape(*q.shape)] + [shape(*k.shape, F32)] * 4 + [shape(*grad.shape, F32)]
    in_specs = [tile, tile, lse_spec] + [keys] * 4 + [pos_spec, HBM]
    call = attention_call(functools.partial(attend_back_body, scale), "attend_back", out_shape, in_specs, [tile] + [keys] * 4 + [HBM], [probs(F32), probs(BF16), buf(1), buf(head_dim)], 30)
    return call(q, d_out, lse, k, v, k2, v2, pos, grad)


def remote(src, dst, send, recv, device):
    return pltpu.make_async_remote_copy(src_ref=src, dst_ref=dst, send_sem=send, recv_sem=recv, device_id=device, device_id_type=MESH_ID)


def flipped(bit, flip):
    return bit + flip - 2 * bit * flip


class Place:
    def __init__(self):
        self.tp = lax.axis_index("tp")
        self.cp = lax.axis_index("cp")
        self.x = lax.rem(self.tp, 2)
        self.y = lax.div(self.tp, 2)
        self.over_x = (self.chip(1, 0), self.cp)
        self.over_y = (self.chip(0, 1), self.cp)
        self.twin = (self.tp, 1 - self.cp)

    def chip(self, dx, dy):
        return 2 * flipped(self.y, dy) + flipped(self.x, dx)

    def meet(self):
        barrier = pltpu.get_barrier_semaphore()
        peers = (self.over_x, self.over_y, self.twin)
        for device in peers:
            pl.semaphore_signal(barrier, inc=1, device_id=device, device_id_type=MESH_ID)
        pl.semaphore_wait(barrier, len(peers))


class Total:
    def __init__(self, place, part, wide, mid, narrow, out, send, recv):
        self.part, self.wide, self.mid, self.narrow, self.out = part, wide, mid, narrow, out
        self.send, self.recv = send, recv
        self.rows = out.shape[0] // STEPS
        self.half, self.quarter, self.eighth = (self.rows // n for n in (2, 4, 8))
        self.kinds = [(place.x, place.y, place.over_x, place.over_y), (place.y, place.x, place.over_y, place.over_x)]

    def _rows(self, step, kind):
        first, second = self.kinds[kind][:2]
        side = step * self.rows + kind * self.half + first * self.quarter
        return rows_at(side, self.quarter), rows_at(side + second * self.eighth, self.eighth)

    def _kept(self, kind, flip=0):
        return rows_at(kind * self.half + flipped(self.kinds[kind][0], flip) * self.quarter, self.quarter)

    def _eighth(self, kind, flip=0):
        return rows_at(flipped(self.kinds[kind][1], flip) * self.eighth, self.eighth)

    def _copy(self, step, kind, stage):
        side, mine = self._rows(step, kind)
        _, _, peer_first, peer_second = self.kinds[kind]
        src, dst, peer = (
            lambda: (self.part(step).at[self._kept(kind, 1)], self.wide.at[step, kind], peer_first),
            lambda: (self.mid.at[step, kind, self._eighth(kind, 1)], self.narrow.at[step, kind], peer_second),
            lambda: (self.out.at[mine], self.out.at[mine], peer_second),
            lambda: (self.out.at[side], self.out.at[side], peer_first),
        )[stage]()
        return remote(src, dst, self.send.at[step, kind, stage], self.recv.at[step, kind, stage], peer)

    def begin(self, step):
        for kind in range(2):
            self._copy(step, kind, 0).start()

    def fold_wide(self, step):
        for kind in range(2):
            self._copy(step, kind, 0).wait_recv()
            self.mid[step, kind] = self.part(step)[self._kept(kind), :] + self.wide[step, kind]
            self._copy(step, kind, 1).start()

    def fold_narrow(self, step):
        for kind in range(2):
            self._copy(step, kind, 1).wait_recv()
            total = self.mid[step, kind, self._eighth(kind), :] + self.narrow[step, kind]
            self.out[self._rows(step, kind)[1], :] = total.astype(BF16)
            self._copy(step, kind, 2).start()

    def widen(self, step):
        for kind in range(2):
            self._copy(step, kind, 2).wait_recv()
            self._copy(step, kind, 3).start()

    def finish(self, step):
        for kind in range(2):
            self._copy(step, kind, 3).wait_recv()

    def sent(self, step, stages):
        for kind in range(2):
            for stage in stages:
                self._copy(step, kind, stage).wait_send()


def sems(*dims):
    return DMA((*dims, 3))


def total_scratch(width, dtype, rows):
    stages = DMA((STEPS, 2, 4))
    part = lambda n: pltpu.VMEM((STEPS, 2, rows // n, width), dtype)
    return [part(4), part(4), part(8), stages, stages]


class Share:
    def __init__(self, place, sems, span):
        self.place, self.sems, self.first = place, sems, place.cp * span

    def pair(self, k, src, dst, start):
        here_sem, send, recv = (self.sems.at[k, i] for i in range(3))
        at = dst.at[rows_at(self.first + start, src.shape[0])]
        return pltpu.make_async_copy(src, at, here_sem), remote(src, at, send, recv, self.place.twin)

    def begin(self, *numbered):
        for copy in self.pair(*numbered):
            copy.start()

    def sent(self, *numbered):
        here, there = self.pair(*numbered)
        here.wait()
        there.wait_send()

    def got(self, k, src, dst, start):
        at = dst.at[rows_at(self.first + start, src.shape[0])]
        remote(src, at, *(self.sems.at[k, i] for i in (1, 2)), self.place.twin).wait_recv()


class Loads:
    def __init__(self, sems, *names):
        self.sems, self.names = sems, list(names)

    def _copies(self, moves):
        self.names += [name for name in moves if name not in self.names]
        return [pltpu.make_async_copy(src, dst, self.sems.at[self.names.index(name)]) for name, (src, dst) in moves.items()]

    def start(self, **moves):
        for copy in self._copies(moves):
            copy.start()
        return lambda: self.wait(**moves)

    def wait(self, **moves):
        for copy in self._copies(moves):
            copy.wait()


def steps(visit):
    def body(step, carry):
        visit(step)
        return carry

    lax.fori_loop(0, STEPS, body, 0)


def rope(v, cosine, sine):
    wide = cosine.shape[1]
    heads = []
    for h in range(v.shape[1] // wide):
        part = v[:, h * wide : (h + 1) * wide]
        turned = jnp.concatenate([part[:, wide // 2 :], part[:, : wide // 2]], axis=1)
        heads.append(part * cosine + turned * sine)
    return jnp.concatenate(heads, axis=1)


def each(count, size, visit):
    def body(i, carry):
        visit(pl.multiple_of(i * size, size))
        return carry

    lax.fori_loop(0, count // size, body, 0)


def col_loop(cols, tile, visit):
    each(cols, tile, lambda start: visit(pl.ds(start, tile)))


def dot_nt(a, b):
    return lax.dot_general(a, b, NT, preferred_element_type=F32)


def dot(a, b):
    return jnp.dot(a, b, preferred_element_type=F32)


def norm_block(feats):
    inverse = lax.rsqrt(over_row(jnp.mean, feats * feats) + NORM_EPS)
    return feats * inverse, inverse


def norm_back(d_act, gain, normed, inverse):
    d_normed = d_act * gain
    return inverse * (d_normed - normed * over_row(jnp.mean, d_normed * normed))


def remote_call(body, collective_id, name, out_shape, in_places, out_places, scratch, gflops):
    return pl.pallas_call(
        body,
        out_shape=out_shape,
        in_specs=specs(in_places),
        out_specs=specs(out_places),
        scratch_shapes=scratch,
        compiler_params=pltpu.CompilerParams(collective_id=collective_id, has_side_effects=True, vmem_limit_bytes=REMOTE_VMEM),
        cost_estimate=cost(gflops, 60),
        name=name,
    )


def join_columns(parts, whole):
    start, moves = 0, {}
    for i, part in enumerate(parts):
        moves[f"join{i}"] = (part, whole.at[:, pl.ds(start, part.shape[1])])
        start += part.shape[1]
    return moves


def order_ids(cp, ids, ids_got, keys, tall, rank, keys_out):
    span = ids.shape[1]
    chunks = keys.shape[0]
    lane = lax.broadcasted_iota(jnp.int32, (1, LANES), 1)
    for core, src in ((cp, ids), (1 - cp, ids_got)):
        for c in range(span // LANES):
            start = c * LANES
            token = core * span + start + lane
            keys[core * (chunks // 2) + c] = lax.shift_left(src[:, start : start + LANES], KEY_BITS) + token

    def count(a, carry):
        mine = as_column(keys[a])
        tall[a] = mine
        rank[a] = over_row(jnp.sum, sum((keys[b] < mine).astype(F32) for b in range(chunks)))
        return carry

    def place(c, carry):
        goal = (c * LANES + lane).astype(F32)
        keys_out[pl.ds(c, 1), :] = over_column(sum(jnp.where(rank[a] == goal, tall[a], 0) for a in range(chunks)))
        return carry

    lax.fori_loop(0, chunks, count, 0)
    lax.fori_loop(0, chunks, place, 0)
    keys_out[pl.ds(chunks, 1), :] = jnp.full((1, LANES), jnp.iinfo(jnp.int32).max, jnp.int32)


def enter_body(picked, wq_in, wk_in, wv_in, gain, pos, inv_freq, ids, dy_in, wd_in, x_out, q_out, k_out, v_out, cosine, sine, keys_out, dh_out, k2_out, v2_out, act_all, dy_all, wide, mid, narrow, send, recv, act, dy, wd, dh, w_all, ids_got, keys, tall, rank, pair_sems, share_sems, load_sems, ids_sems):
    place = Place()
    place.meet()
    span = x_out.shape[0]
    rows = span // STEPS
    chunk = lambda step: rows_at(step * rows, rows)
    total = Total(place, lambda step: picked.at[chunk(step)], wide, mid, narrow, x_out, send, recv)
    share = Share(place, share_sems, span)
    loads = Loads(load_sems)
    steps(total.begin)
    ids_swap = remote(ids, ids_got, *(ids_sems.at[end] for end in range(2)), place.twin)
    ids_swap.start()
    loaded = loads.start(dy=(dy_in, dy), wd=(wd_in, wd))
    projection = loads.start(**join_columns((wq_in, wk_in, wv_in), w_all))
    kw = k_out.shape[1]
    qw = q_out.shape[1]

    def back(step):
        here = chunk(step)

        def tile(cols):
            dh[here, cols] = dot_nt(dy[here, :], wd[cols, :]).astype(BF16)

        col_loop(wd.shape[0], WIDE_TILE, tile)
        total.fold_wide(step)

    def pairs(step):
        return [remote(src.at[chunk(step)], dst.at[chunk(step)], *(pair_sems.at[step, i, end] for end in range(2)), place.twin) for i, (src, dst) in enumerate(((k_out, k2_out), (v_out, v2_out)))]

    act_share = lambda step: (1 + step, act.at[chunk(step)], act_all, step * rows)

    def project(step):
        total.finish(step)
        here = chunk(step)

        def norm(start):
            at = rows_at(step * rows + start, ROW_BLOCK)
            normed, _ = norm_block(x_out[at, :].astype(F32))
            act[at, :] = (normed * gain[()].astype(F32)).astype(BF16)

        each(rows, ROW_BLOCK, norm)
        share.begin(*act_share(step))
        c, s = cosine[here, :], sine[here, :]
        out = dot(act[here, :], w_all[()])
        q_out[here, :] = rope(out[:, :qw], c, s).astype(BF16)
        k_out[here, :] = rope(out[:, qw : qw + kw], c, s).astype(BF16)
        v_out[here, :] = out[:, qw + kw :].astype(BF16)
        for copy in pairs(step):
            copy.start()

    def angles(start):
        at = pl.ds(start, LANES)
        angle = as_column(pos[:, at])[:, : inv_freq.shape[1]].astype(F32) * inv_freq[()]
        c, s = jnp.cos(angle), jnp.sin(angle)
        cosine[at, :] = jnp.concatenate([c, c], axis=1)
        sine[at, :] = jnp.concatenate([-s, s], axis=1)

    loaded()
    dy_share = (0, dy, dy_all, 0)
    share.begin(*dy_share)
    each(span, LANES, angles)
    steps(back)
    stored = loads.start(dh=(dh, dh_out))
    ids_swap.wait()
    order_ids(place.cp, ids, ids_got, keys, tall, rank, keys_out)
    steps(total.fold_narrow)
    steps(total.widen)
    projection()
    steps(project)

    def close(step):
        total.sent(step, range(4))
        share.sent(*act_share(step))
        share.got(*act_share(step))
        for copy in pairs(step):
            copy.wait()

    steps(close)
    share.sent(*dy_share)
    share.got(*dy_share)
    stored()


def enter(picked, wq, wk, wv, gain, pos, inv_freq, ids, dy, wd):
    span, width = picked.shape
    key = shape(span, wk.shape[1])
    angles = shape(span, 2 * inv_freq.shape[1], F32)
    all_rows = shape(2 * span, width)
    chunks = 2 * span // LANES
    int_buf = lambda *dims: pltpu.VMEM(dims, jnp.int32)
    big = pltpu.VMEM((span, width), BF16)
    out_shape = [shape(span, width), shape(span, wq.shape[1]), key, key, angles, angles, shape(chunks + SUBLANES, LANES, jnp.int32), shape(span, wd.shape[0]), key, key, all_rows, all_rows]
    scratch = total_scratch(width, BF16, span // STEPS) + [big, big, pltpu.VMEM(wd.shape, BF16), pltpu.VMEM((span, wd.shape[0]), BF16), pltpu.VMEM((width, wq.shape[1] + 2 * wk.shape[1]), BF16)]
    scratch += [int_buf(1, span), int_buf(chunks, 1, LANES), int_buf(chunks, LANES, LANES), pltpu.VMEM((chunks, LANES, 1), F32)]
    scratch += [DMA((STEPS, 2, 2)), sems(STEPS + 1), DMA((6,)), DMA((2,))]
    call = remote_call(enter_body, 1, "enter", out_shape, "vhhhvvvvhh", "vvvvvvvhhhhh", scratch, 80)
    return call(picked, wq, wk, wv, gain, pos, inv_freq, ids, dy, wd)


def middle_body(att, wo_own, wo_1, wo_2, wo_3, x_in, wg_in, wu_in, wd_in, dh_in, dy_in, gain, h_out, keep_x, send_x, keep_y, send_y, b_all, hidden_all, dgate_all, dup_all, att_all, drb_all, dr_out, datt_out, dgain_out,
                wide, mid, narrow, send, recv, wo, wg, wu, att_full, part_buf, d_b, h, row_in, dh, b, hid, dgt, dup, att_send, att_recv, wo_sems, load_sems, share_sems):
    place = Place()
    span, width = x_in.shape
    rows = span // STEPS
    half = rows // 2
    cols = att.shape[1]
    ffn = wg.shape[1]
    loads = Loads(load_sems, "att", "wo", "wg", "wu", "rows", "dh", "h_out", "h_in", "hid", "dr", "y")
    chunk = lambda step: rows_at(step * rows, rows)
    by_chip = lambda tp: rows_at(tp * cols, cols, 128)

    mine = loads.start(att=(att, att_full.at[:, by_chip(place.tp)]), wo=(wo_own, wo.at[by_chip(place.tp)]))
    place.meet()

    x_tp, y_tp = place.over_x[0], place.over_y[0]

    def att_copy(step, kind, hop):
        at = rows_at(step * rows + kind * half, half)
        first, second = ((place.over_y, place.over_x), (place.over_x, place.over_y))[kind]
        relay = hop == 2
        dst = att_full.at[at, by_chip(first[0] if relay else place.tp)]
        return remote(dst if relay else att.at[at], dst, att_send.at[step, kind, hop], att_recv.at[step, kind, hop], second if hop else first)

    def att_begin(step):
        for hop in range(2):
            for kind in range(2):
                att_copy(step, kind, hop).start()

    def att_forward(step):
        for kind in range(2):
            att_copy(step, kind, 0).wait_recv()
            att_copy(step, kind, 2).start()

    att_begin(0)
    part = wo_1.shape[0]
    arrivals = []
    near = jnp.where(place.cp == 0, y_tp, x_tp)
    chips = (near, x_tp + y_tp - near, place.chip(1, 1))
    for i, (src, chip) in enumerate(zip((wo_1, wo_2, wo_3), chips)):
        at = wo.at[rows_at((2 * chip + place.cp) * part, part, 128)]
        here_sem, send_sem, recv_sem = (wo_sems.at[i, end] for end in range(3))
        for copy in (pltpu.make_async_copy(src, at, here_sem), remote(src, at, send_sem, recv_sem, place.twin)):
            copy.start()
            arrivals.append(copy)
    att_begin(1)
    weights = loads.start(wg=(wg_in, wg), wu=(wu_in, wu))

    share = Share(place, share_sems, span)
    att_share = (0, att, att_all, 0)
    share.begin(*att_share)
    total = Total(place, lambda step: part_buf.at[step], wide, mid, narrow, d_b, send, recv)

    def numbered(i, src, dst, step):
        return 1 + len(shares) * step + i, src, dst, step * rows

    shares = ((b, b_all), (hid, hidden_all), (dgt, dgate_all), (dup, dup_all), (b, drb_all))
    forward_shares = list(enumerate(shares))[:-1]
    fetched = lambda step: dict(rows=(x_in.at[chunk(step)], row_in), dh=(dh_in.at[chunk(step)], dh))
    h_kept = lambda step: dict(h_out=(h, h_out.at[chunk(step)]))

    def close(step):
        loads.wait(**h_kept(step))
        for i, pair in forward_shares:
            share.sent(*numbered(i, *pair, step))

    def forward(step):
        pl.when(step >= 1)(lambda: close(step - 1))
        loads.wait(**fetched(step))
        for kind in range(2):
            for hop in (1, 2):
                att_copy(step, kind, hop).wait_recv()

        def residual(c):
            h[:, c] = row_in[:, c].astype(F32) + dot(att_full[chunk(step), :], wo[:, c])

        col_loop(width, BIG_TILE, residual)
        loads.start(**h_kept(step))

        def norm(start):
            at = pl.ds(start, ROW_BLOCK)
            normed, _ = norm_block(h[at, :])
            b[at, :] = (normed * gain[()].astype(F32)).astype(BF16)

        each(rows, ROW_BLOCK, norm)
        share.begin(*numbered(0, b, b_all, step))
        pl.when(step == 0)(weights)

        def hidden(c):
            gate = dot(b[()], wg[:, c])
            up = dot(b[()], wu[:, c])
            sig = 1.0 / (1.0 + jnp.exp(-gate))
            d_hid = dh[:, c].astype(F32)
            act = gate * sig
            hid[:, c] = (act * up).astype(BF16)
            dgt[:, c] = (d_hid * up * sig * (1.0 + gate * (1.0 - sig))).astype(BF16)
            dup[:, c] = (d_hid * act).astype(BF16)

        col_loop(ffn, WIDE_TILE, hidden)
        for i, pair in forward_shares[1:]:
            share.begin(*numbered(i, *pair, step))
        pl.when(step == 0)(lambda: att_forward(2))

        @pl.when(step + 1 < STEPS)
        def _():
            loads.start(**fetched(step + 1))

        def back(c):
            part_buf[step, :, c] = dot_nt(dgt[()], wg[c, :]) + dot_nt(dup[()], wu[c, :])

        col_loop(width, WIDE_TILE, back)
        total.begin(step)
        pl.when(step == 0)(lambda: att_forward(3))
        pl.when(step >= 2)(lambda: total.fold_wide(step - 2))

    loads.start(**fetched(0))
    att_forward(0)
    for step in range(2, STEPS):
        att_begin(step)
    mine()
    for copy in arrivals:
        copy.wait()
    att_forward(1)
    steps(forward)
    clear(dgain_out)
    close(STEPS - 1)
    wd = wg
    weights = loads.start(wg=(wd_in, wd))
    d_r, y_buf = part_buf.at[0], part_buf.at[1]

    h_back = lambda step: dict(h_in=(h_out.at[chunk(step)], h))
    hidden_back = lambda step: dict(hid=(hidden_all.at[rows_at(place.cp * span + step * rows, rows)], hid))
    dy_back = lambda step: dict(rows=(dy_in.at[chunk(step)], row_in))
    y_kept = dict(y=(y_buf, keep_x))
    for step in range(2):
        total.sent(step, (0,))
    loads.start(**h_back(0), **hidden_back(0))

    def output(step):
        pl.when(step < 2)(lambda: total.fold_wide(step + 2))
        loads.wait(**h_back(step), **hidden_back(step))
        pl.when(step == 0)(weights)
        pl.when(step >= 1)(lambda: loads.wait(**y_kept))
        over_x_first = step < 2
        first = jnp.where(over_x_first, place.x, place.y)
        second = place.x + place.y - first
        kept = first == lax.rem(step, 2)
        row = lax.broadcasted_iota(jnp.int32, (rows, 1), 0)
        owner = kept & (lax.div(row, half) == second)

        def tile(c):
            y_buf[:, c] = dot(hid[()], wd[:, c]) + jnp.where(owner, h[:, c], 0.0)

        col_loop(width, BIG_TILE, tile)
        for side_first, keep, send_to in ((over_x_first, keep_x, send_x), (jnp.logical_not(over_x_first), keep_y, send_y)):
            for chosen, dst in ((kept, keep), (jnp.logical_not(kept), send_to)):

                @pl.when(side_first & chosen)
                def _():
                    loads.start(y=(y_buf, dst))

        @pl.when(step + 1 < STEPS)
        def _():
            loads.start(**h_back(step + 1), **hidden_back(step + 1))

        total.fold_narrow(step)
        pl.when(step >= 2)(lambda: total.widen(step - 2))

    steps(output)
    loads.start(**h_back(0), **dy_back(0))
    kept_rows = lambda step: dict(dr=(d_r, dr_out.at[chunk(step)]))
    resid_share = lambda step: numbered(len(shares) - 1, b, drb_all, step)

    def resid_sent(step):
        loads.wait(**kept_rows(step))
        share.sent(*resid_share(step))

    def resid(step):
        pl.when(step < 2)(lambda: total.widen(step + 2))
        total.finish(step)
        loads.wait(**h_back(step), **dy_back(step))
        pl.when(step >= 1)(lambda: resid_sent(step - 1))

        def grad(start):
            at = pl.ds(start, ROW_BLOCK)
            normed, inverse = norm_block(h[at, :])
            d_act = d_b[rows_at(step * rows + start, ROW_BLOCK), :].astype(F32)
            dgain_out[()] += over_column(d_act * normed)
            out = row_in[at, :].astype(F32) + norm_back(d_act, gain[()].astype(F32), normed, inverse)
            d_r[at, :] = out
            b[at, :] = out.astype(BF16)

        each(rows, ROW_BLOCK, grad)

        @pl.when(step + 1 < STEPS)
        def _():
            loads.start(**h_back(step + 1), **dy_back(step + 1))

        loads.start(**kept_rows(step))
        share.begin(*resid_share(step))
        datt_out[chunk(step), :] = dot_nt(b[()], wo[by_chip(place.tp), :]).astype(BF16)

    steps(resid)
    loads.wait(**y_kept)
    resid_sent(STEPS - 1)
    share.sent(*att_share)
    share.got(*att_share)

    def finish(step):
        total.sent(step, range(1, 4))
        pl.when(step >= 2)(lambda: total.sent(step, (0,)))
        for kind in range(2):
            for hop in range(3):
                att_copy(step, kind, hop).wait_send()
        for i, pair in enumerate(shares):
            share.got(*numbered(i, *pair, step))

    steps(finish)


def middle(att, wo_pieces, x, wg, wu, wd, d_hidden, dy, gain):
    span, width = x.shape
    rows = span // STEPS
    ffn = wg.shape[1]
    cols = att.shape[1]
    full = shape(span, width, F32)
    both = shape(2 * span, ffn)
    out_shape = [full] + [shape(rows, width, F32)] * 4 + [shape(2 * span, width), both, both, both, shape(2 * span, cols), shape(2 * span, width), full, shape(span, cols), shape(*gain.shape, F32)]
    buf = lambda r, c, dtype=BF16: pltpu.VMEM((r, c), dtype)
    scratch = total_scratch(width, F32, rows)
    scratch += [buf(width, width), buf(width, ffn), buf(width, ffn), buf(span, width), pltpu.VMEM((STEPS, rows, width), F32), buf(span, width), buf(rows, width, F32)]
    scratch += [buf(rows, c) for c in (width, ffn, width, ffn, ffn, ffn)]
    scratch += [sems(STEPS, 2), sems(STEPS, 2), sems(3), DMA((11,)), sems(1 + 5 * STEPS)]
    call = remote_call(middle_body, 2, "middle", out_shape, "vhhhhhhhhhhv", "hhhhhhhhhhhhvv", scratch, 120)
    return call(att, *wo_pieces, x, wg, wu, wd, d_hidden, dy, gain)


def leave_body(dq_in, dk_in, dv_in, dk2_in, dv2_in, cosine, sine, wq_in, wk_in, wv_in, x_in, dr_in, gain, dgain_b, b_all, dgate_all, dup_all, hidden_all, dy_all, att_all, drb_all, act_all, d_all, dx_all, gain_a_out, gain_b_out, grad_gate, grad_up, grad_down, grad_out, grad_q, grad_k, grad_v,
               wide, mid, narrow, send, recv, part_buf, d_a, dk_got, dv_got, d_qkv, w_all, xs, drs, dxs, gain_got, left, right, result, pair_sems, load_sems, share_sems, left_sems, right_sems, result_sems):
    place = Place()
    place.meet()
    span, width = x_in.shape
    rows = span // STEPS
    chunk = lambda step: rows_at(step * rows, rows)
    swap = lambda i, src, dst: remote(src, dst, *(pair_sems.at[i, end] for end in range(2)), place.twin)
    pairs = lambda step: [swap(2 * step + i, src.at[chunk(step)], dst.at[chunk(step)]) for i, (src, dst) in enumerate(((dk2_in, dk_got), (dv2_in, dv_got)))]
    for step in range(STEPS):
        for copy in pairs(step):
            copy.start()
    qw = dq_in.shape[1]
    kw = dk_in.shape[1]
    share = Share(place, share_sems, span)
    loads = Loads(load_sems)
    total = Total(place, lambda step: part_buf.at[step], wide, mid, narrow, d_a, send, recv)

    def partial(step):
        here = chunk(step)
        c, s = cosine[here, :], -sine[here, :]
        for copy in pairs(step):
            copy.wait()
        d_qkv[here, :qw] = rope(dq_in[here, :].astype(F32), c, s).astype(BF16)
        dk_sum = (dk_in[here, :] + dk_got[here, :]).astype(BF16).astype(F32)
        d_qkv[here, qw : qw + kw] = rope(dk_sum, c, s).astype(BF16)
        d_qkv[here, qw + kw :] = (dv_in[here, :] + dv_got[here, :]).astype(BF16)

        def tile(n):
            part_buf[step, :, n] = dot_nt(d_qkv[here, :], w_all[n, :])

        col_loop(width, BIG_TILE, tile)
        total.begin(step)

    rows_back = lambda step: dict(x=(x_in.at[chunk(step)], xs), dr=(dr_in.at[chunk(step)], drs))

    clear(gain_a_out)

    def grad_x(step):
        def grad(start):
            at = pl.ds(start, ROW_BLOCK)
            normed, inverse = norm_block(xs[at, :].astype(F32))
            d_act = d_a[rows_at(step * rows + start, ROW_BLOCK), :].astype(F32)
            gain_a_out[()] += over_column(d_act * normed)
            dxs[at, :] = drs[at, :] + norm_back(d_act, gain[()].astype(F32), normed, inverse)

        each(rows, ROW_BLOCK, grad)

    _, _, narrow_cols = left.shape
    _, _, wide_cols = right.shape
    lefts, rights = Ring(left, left_sems, True), Ring(right, right_sems, True)
    sides, per_side = width // wide_cols, width // narrow_cols
    whole = (grad_gate, grad_up, grad_down, grad_out)
    ffn_blocks = (len(whole) - 1) * sides
    all_blocks = len(whole) * sides
    ffn_tiles = ffn_blocks * per_side
    out_tiles = ffn_tiles + sides
    tiles = out_tiles + per_side
    block_of = lambda t: jnp.where(t < ffn_tiles, lax.div(t, per_side), jnp.where(t < out_tiles, ffn_blocks + t - ffn_tiles, all_blocks))
    at_left = lambda t: rows_at(jnp.where(t < ffn_tiles, lax.rem(t, per_side), jnp.maximum(t - out_tiles, 0)) * narrow_cols, narrow_cols, TILE)
    at_right = lambda j: rows_at(lax.rem(j, sides) * wide_cols, wide_cols, TILE)
    kind_of = lambda j: lax.div(j, sides)
    left_start = lambda t: lefts.start(t, kind_of(block_of(t)), [ref.at[:, at_left(t)] for ref in (b_all, b_all, hidden_all)] + [att_all, act_all.at[:, at_left(t)]])
    right_start = lambda j: rights.start(j, kind_of(j), [ref.at[:, at_right(j)] for ref in (dgate_all, dup_all, dy_all, drb_all)] + [d_all])

    def stored(t):
        done = result.at[lefts.slot(t)]
        pltpu.make_async_copy(done, done, result_sems.at[lefts.slot(t)]).wait()

    def store(t):
        slot = lefts.slot(t)
        j = block_of(t)

        def put(cols, dst):
            pltpu.make_async_copy(result.at[slot, :, cols], dst, result_sems.at[slot]).start()

        everything = pl.ds(0, wide_cols)
        for k, ref in enumerate(whole):
            at = at_left(t) if ref is not grad_out else pl.ds(0, narrow_cols)
            pl.when(kind_of(j) == k)(lambda: put(everything, ref.at[at, at_right(j)]))

        @pl.when(j == all_blocks)
        def _():
            put(pl.ds(0, qw), grad_q.at[at_left(t)])
            put(pl.ds(qw, kw), grad_k.at[at_left(t)])
            put(pl.ds(qw + kw, kw), grad_v.at[at_left(t)])

    def tile_step(t, carry):
        j = block_of(t)
        last = t + 1 >= tiles
        pl.when(jnp.logical_not(last))(lambda: left_start(t + 1))

        @pl.when(jnp.where(t < ffn_tiles, lax.rem(t, per_side) == 0, t <= out_tiles))
        def _():
            pl.when(j + 1 < all_blocks)(lambda: right_start(j + 1))
            rights.wait(j, d_all)

        lefts.wait(t, att_all)
        pl.when(t >= 2)(lambda: stored(t))
        slot = lefts.slot(t)
        result[slot] = lax.dot_general(left[slot], right[rights.slot(j)], CONTRACT_FIRST, preferred_element_type=F32)
        store(t)
        return carry

    left_start(jnp.int32(0))
    right_start(jnp.int32(0))
    weights = loads.start(**join_columns((wq_in, wk_in, wv_in), w_all))
    loads.start(**rows_back(0))
    weights()
    steps(partial)
    d_here, d_there = share.pair(0, d_qkv, d_all, 0)
    d_here.start()
    d_there.start()

    stages = (total.fold_wide, total.fold_narrow, total.widen)
    waits = len(stages) * STEPS
    portion = ffn_tiles // STEPS
    tiles_until = lambda p: jnp.where(p < STEPS, portion * (p + 1), jnp.where(p < 2 * STEPS - 1, ffn_tiles, jnp.where(p < waits - 1, out_tiles, tiles)))

    def wait_step(p, carry):
        @pl.when(p == waits - 1)
        def _():
            d_here.wait()
            d_there.wait_recv()
            right_start(jnp.int32(all_blocks))

        lax.fori_loop(jnp.where(p == 0, 0, tiles_until(p - 1)), tiles_until(p), tile_step, 0)
        for k, stage in enumerate(stages):
            pl.when(lax.div(p, STEPS) == k)(lambda: stage(lax.rem(p, STEPS)))
        return carry

    lax.fori_loop(0, waits, wait_step, 0)
    dx_share = lambda step: (1 + step, dxs, dx_all, step * rows)

    def last_stage(step):
        loads.wait(**rows_back(step))
        total.finish(step)
        pl.when(step >= 1)(lambda: share.sent(*dx_share(step - 1)))
        grad_x(step)
        share.begin(*dx_share(step))

        @pl.when(step + 1 < STEPS)
        def _():
            loads.start(**rows_back(step + 1))

    steps(last_stage)
    gains = ((gain_a_out, gain_a_out), (dgain_b, gain_b_out))
    swaps = [swap(2 * STEPS + i, mine, gain_got.at[i]) for i, (mine, _) in enumerate(gains)]
    for copy in swaps:
        copy.start()
    for copy in swaps:
        copy.wait()
    for i, (mine, out) in enumerate(gains):
        out[()] = mine[()] + gain_got[i]
    share.sent(*dx_share(STEPS - 1))
    d_there.wait_send()
    for t in range(2):
        stored(t)

    def close(step):
        total.sent(step, range(4))
        share.got(*dx_share(step))

    steps(close)


def leave(dq, dk, dv, dk2, dv2, cosine, sine, wq, wk, wv, x, d_resid, gain, dgain_b, *products):
    span, width = x.shape
    rows = span // STEPS
    kw = wk.shape[1]
    qw = wq.shape[1]
    cols = qw + 2 * kw
    ffn = products[1].shape[1]
    buf = lambda r, c, dtype=F32: pltpu.VMEM((r, c), dtype)
    gain_grad = shape(*gain.shape, F32)
    out_shape = [shape(2 * span, cols), shape(2 * span, width, F32), gain_grad, gain_grad]
    out_shape += [shape(*dims, F32) for dims in ((width, ffn), (width, ffn), (ffn, width), (qw, width), wq.shape, wk.shape, wv.shape)]
    twice = lambda r, c, dtype: pltpu.VMEM((2, r, c), dtype)
    scratch = total_scratch(width, F32, rows) + [pltpu.VMEM((STEPS, rows, width), F32), buf(span, width, BF16), buf(span, kw), buf(span, kw), buf(span, cols, BF16), buf(width, cols, BF16)]
    scratch += [buf(rows, width, BF16), buf(rows, width), buf(rows, width), pltpu.VMEM((2, 1, width), F32)]
    scratch += [twice(2 * span, WIDE_TILE, BF16), twice(2 * span, BIG_TILE, BF16), twice(WIDE_TILE, BIG_TILE, F32)]
    ring = DMA((2,))
    scratch += [DMA((2 * STEPS + 2, 2)), DMA((5,)), sems(1 + STEPS), ring, ring, ring]
    call = remote_call(leave_body, 3, "leave", out_shape, "vvvhhvvhhhhhvvhhhhhhhh", "hhvvhhhhhhh", scratch, 1)
    return call(dq, dk, dv, dk2, dv2, cosine, sine, wq, wk, wv, x, d_resid, gain, dgain_b, *products)


def side(v, bit):
    half = v.shape[0] // 2
    return lax.dynamic_slice_in_dim(v, bit * half, half, 0)


def join(own, other, bit):
    return jnp.where(bit == 0, jnp.concatenate([own, other]), jnp.concatenate([other, own]))


def solution(mesh):
    def device_step(tokens, pos, doc_id, dy, table, w_q, w_k, w_v, w_o, w_gate, w_up, w_down, gain_one, gain_two, inv_freq):
        span = tokens.shape[0]
        rows, width = table.shape
        scale = (2 * inv_freq.shape[0]) ** -0.5
        tp = lax.axis_index("tp")
        cp = lax.axis_index("cp")
        gain_a, gain_b, inv_freq, pos, ids = (v[None, :] for v in (gain_one, gain_two, inv_freq, pos, tokens))
        base = tp * rows

        wo_half = side(w_o, cp)
        wo_1 = swap_core(wo_half, 0)
        picked, grad = pick_rows(tokens, table, base)
        x, query, key, value, cosine, sine, keys, d_hidden, key2, value2, act_a_all, dy_all = enter(picked, w_q, w_k, w_v, gain_a, pos, inv_freq, ids, dy, w_down)
        wo_1, wo_half, query = lax.optimization_barrier((wo_1, wo_half, query))
        wo_pieces = (w_o, wo_1, swap_core(wo_half, 1), swap_core(wo_1, 1))
        att, lse, grad = attend(scale, query, key, value, key2, value2, pos, grad)
        keep_x, send_x, keep_y, send_y, act_b_all, hidden_all, d_gate_all, d_up_all, att_all, d_resid_all, d_resid, d_att, d_gain_b = middle(att, wo_pieces, x, w_gate, w_up, w_down, d_hidden, dy, gain_b)[1:]

        x_bit, y_bit = tp % 2, tp // 2
        ways = ((keep_x, swap_x, x_bit, swap_y, y_bit), (keep_y, swap_y, y_bit, swap_x, x_bit))
        y_wide = [swap_x(send_x), swap_y(send_y)]
        d_query, d_key, d_value, d_key2, d_value2, grad = attend_back(scale, query, d_att, lse, key, value, key2, value2, pos, grad)

        d_x_all, gain_1, gain_2, grad_gate, grad_up, grad_down, *grads = leave(d_query, d_key, d_value, d_key2, d_value2, cosine, sine, w_q, w_k, w_v, x, d_resid, gain_a, d_gain_b, act_b_all, d_gate_all, d_up_all, hidden_all, dy_all, att_all, d_resid_all, act_a_all)[1:]
        y_wide, d_x_all = lax.optimization_barrier((y_wide, d_x_all))
        halves = lambda bit_2, keep, wide, flip: side(keep, flipped(bit_2, flip)) + side(wide, flipped(bit_2, flip))
        y_narrow = [swap_2(halves(bit_2, keep, wide, 1)) for (keep, _, _, swap_2, bit_2), wide in zip(ways, y_wide)]
        y_wide, grad_gate = lax.optimization_barrier((y_wide, grad_gate))
        grad_gate, grad_out, *grads = move(grad_gate, *grads)
        y_narrow, grad_gate = lax.optimization_barrier((y_narrow, grad_gate))
        y_own = [(halves(bit_2, keep, wide, 0) + narrow).astype(BF16) for (keep, _, _, _, bit_2), wide, narrow in zip(ways, y_wide, y_narrow)]
        y_pair = [join(own, swap_2(own), bit_2) for (_, _, _, swap_2, bit_2), own in zip(ways, y_own)]
        y_own, grad_down = lax.optimization_barrier((y_own, grad_down))
        (grad_down,) = move(grad_down)
        y_pair, grad_down = lax.optimization_barrier((y_pair, grad_down))
        y_far = [swap_1(pair) for (_, swap_1, _, _, _), pair in zip(ways, y_pair)]
        y_pair, d_x_all = lax.optimization_barrier((y_pair, d_x_all))
        grad_table, grad_up = put_rows(keys.reshape(-1), d_x_all, grad, (grad_up,))
        y_rows = [jnp.where(bit_1 == k, pair, far) for (_, _, bit_1, _, _), pair, far in zip(ways, y_pair, y_far) for k in range(2)]
        return (jnp.concatenate(y_rows), grad_table, *grads, grad_out, grad_gate, grad_up, grad_down, gain_1[0], gain_2[0])

    col_spec = P(None, "tp")
    row_spec = P("tp", None)
    tok_spec = P("cp")
    rep_spec = P(None)
    in_specs = (tok_spec, tok_spec, tok_spec, P("cp", None), row_spec, col_spec, col_spec, col_spec, row_spec, col_spec, col_spec, row_spec, rep_spec, rep_spec, rep_spec)
    out_specs = (P("cp", None), row_spec, col_spec, col_spec, col_spec, row_spec, col_spec, col_spec, row_spec, rep_spec, rep_spec)
    return jax.shard_map(device_step, mesh=mesh, in_specs=in_specs, out_specs=out_specs, check_vma=False)
```

```python
import functools

import jax
import jax.numpy as jnp
from jax import lax
from jax.experimental import pallas as pl
from jax.experimental.pallas import tpu as pltpu
from jax.sharding import PartitionSpec as P

NORM_EPS = 1e-5
NEG_BIG = -1e30
F32 = jnp.float32
BF16 = jnp.bfloat16
MIB = 2**20
LOCAL_VMEM = 56 * MIB
REMOTE_VMEM = 63 * MIB
STEPS = 4
LOG2_E = 1.4426950408889634
SUBLANES = 8
BOTH = (0, 1)
ROW_BLOCK = 32
WIDE_TILE = 512
BIG_TILE = 1024
TILE = 256
MESH_ID = pl.DeviceIdType.MESH
NT = (((1,), (1,)), ((), ()))
CONTRACT_FIRST = (((0,), (0,)), ((), ()))
VMEM = pl.BlockSpec(memory_space=pltpu.VMEM)
SMEM = pl.BlockSpec(memory_space=pltpu.SMEM)
HBM = pl.BlockSpec(memory_space=pl.ANY)
DMA = pltpu.SemaphoreType.DMA


X_PAIRS, Y_PAIRS = ([(chip, chip ^ flip) for chip in range(4)] for flip in (1, 2))
C_PAIRS = X_PAIRS[:2]
CORE_PAIRS = tuple([(2 * a + core, 2 * b + core) for core, pairs in enumerate(kinds) for a, b in pairs] for kinds in ((Y_PAIRS, X_PAIRS), (X_PAIRS, Y_PAIRS)))


def swap_x(v):
    return lax.ppermute(v, "tp", X_PAIRS)


def swap_y(v):
    return lax.ppermute(v, "tp", Y_PAIRS)


def swap_c(v):
    return lax.ppermute(v, "cp", C_PAIRS)


def swap_core(v, which):
    return lax.ppermute(v, ("tp", "cp"), CORE_PAIRS[which])


def rows_in(v):
    return v.shape[0]


def cols_of(v):
    return v.shape[1]


def over_row(reduce, v):
    return reduce(v, axis=-1, keepdims=True)


def over_column(v):
    return jnp.sum(v, axis=0, keepdims=True)


def specs(places):
    return [{"v": VMEM, "h": HBM, "s": SMEM}[place] for place in places]


def cost(gflops, mib):
    return pl.CostEstimate(flops=gflops * 10**9, bytes_accessed=mib * MIB, transcendentals=0)


def shape(rows, cols, dtype=BF16):
    return jax.ShapeDtypeStruct((rows, cols), dtype)


def local_call(body, name, out_shape, in_specs, out_specs, scratch, gflops, aliases={}, **grid):
    return pl.pallas_call(
        body,
        out_shape=out_shape,
        in_specs=in_specs,
        out_specs=out_specs,
        scratch_shapes=scratch,
        input_output_aliases=aliases,
        compiler_params=pltpu.CompilerParams(vmem_limit_bytes=LOCAL_VMEM),
        cost_estimate=cost(gflops, 60),
        name=name,
        **grid,
    )


def rows_at(start, size, step=32):
    return pl.ds(pl.multiple_of(start, step), size)


class Ring:
    def __init__(self, buf, sems, inward):
        self.buf, self.sems, self.inward = buf, sems, inward

    def slot(self, count):
        return lax.rem(count, rows_in(self.buf))

    def _copy(self, count, view):
        pair = (view, self.buf.at[self.slot(count)])
        return pltpu.make_async_copy(*(pair if self.inward else pair[::-1]), self.sems.at[self.slot(count)])

    def start(self, count, kind, views):
        for k, view in enumerate(views):
            pl.when(kind == k)(lambda: self._copy(count, view).start())

    def wait(self, count, view):
        self._copy(count, view).wait()


ZERO_ROWS = 24
ZEROS = {"attend": (24, 68), "attend_back": (39, 78)}
ZERO_PICK = 2


def zero_block(out_ref, block, count=1):
    return out_ref.at[pl.ds(pl.multiple_of(block * ZERO_ROWS, ZERO_ROWS), count * ZERO_ROWS)]


def clear(ref, value=0.0):
    ref[()] = jnp.full(ref.shape, value, F32)


def start_zeros(out_ref, zero_ref, sem, first, count):
    def start(i, carry):
        pltpu.make_async_copy(zero_ref, zero_block(out_ref, first + i), sem).start()
        return carry

    lax.fori_loop(0, count, start, 0)


def wait_zeros(out_ref, sem, first, count):
    whole = zero_block(out_ref, first, count)
    pltpu.make_async_copy(whole, whole, sem).wait()


def zero_scratch(width):
    return [pltpu.VMEM((ZERO_ROWS, width), F32), DMA]


def grid_zeros(grad_ref, zero_ref, sem, name):
    head, tile = pl.program_id(0), pl.program_id(1)
    heads, tiles = pl.num_programs(0), pl.num_programs(1)
    half = tiles // 2
    early, late = ZEROS[name]
    whole = half * (early + late)
    before = rows_in(grad_ref) // ZERO_ROWS - heads * whole
    if name == "attend":
        before -= heads * half * sum(ZEROS["attend_back"])
    pl.when((head == 0) & (tile == 0))(functools.partial(clear, zero_ref))
    first = before + head * whole + tile * early + jnp.maximum(tile - half, 0) * (late - early)
    start_zeros(grad_ref, zero_ref, sem, first, early)
    pl.when(tile >= half)(functools.partial(start_zeros, grad_ref, zero_ref, sem, first + early, late - early))
    last = (head == heads - 1) & (tile == tiles - 1)
    return lambda: pl.when(last)(lambda: wait_zeros(grad_ref, sem, before, heads * whole))


GATHER_BATCH = 16
GATHER_SLOTS = 8


def pick_body(group_ref, lane_ref, count_ref, table_ref, out_ref, grad_ref, buf, sems, zero_ref, zero_sem):
    batches = rows_in(out_ref) // GATHER_BATCH
    width = cols_of(out_ref)

    def row_copy(group, slot, j):
        return pltpu.make_async_copy(table_ref.at[group], buf.at[slot, j], sems.at[slot])

    def start(step):
        slot = lax.rem(step, GATHER_SLOTS)
        for j in range(GATHER_BATCH):
            group = group_ref[step * GATHER_BATCH + j]
            pl.when(group >= 0)(lambda: row_copy(group, slot, j).start())

    for step in range(GATHER_SLOTS - 1):
        start(step)
    clear(zero_ref)
    row = lax.broadcasted_iota(jnp.int32, (SUBLANES, width), 0)

    def loop(step, carry):
        slot = lax.rem(step, GATHER_SLOTS)

        @pl.when(step + GATHER_SLOTS - 1 < batches)
        def _():
            start(step + GATHER_SLOTS - 1)

        start_zeros(grad_ref, zero_ref, zero_sem, step * ZERO_PICK, ZERO_PICK)

        def arrived(i, carry):
            row_copy(0, slot, 0).wait()
            return carry

        lax.fori_loop(0, count_ref[step], arrived, 0)
        first = pl.multiple_of(step * GATHER_BATCH, GATHER_BATCH)
        parts = []
        for j in range(GATHER_BATCH):
            lane = lane_ref[first + j]
            goal = j % SUBLANES
            if goal == 0:
                parts.append(jnp.zeros((SUBLANES, width), F32))
            turned = pltpu.roll(buf[slot, j].astype(F32), lax.rem(goal + SUBLANES - lane, SUBLANES), 0)
            parts[-1] = jnp.where(row == jnp.where(lane < SUBLANES, goal, SUBLANES), turned, parts[-1])
        out_ref[pl.ds(first, GATHER_BATCH), :] = jnp.concatenate(parts, axis=0).astype(BF16)
        return carry

    lax.fori_loop(0, batches, loop, 0)
    wait_zeros(grad_ref, zero_sem, 0, batches * ZERO_PICK)


def pick_rows(tokens, table, base):
    span = rows_in(tokens)
    rows, width = table.shape
    local = tokens - base
    owned = (local >= 0) & (local < rows)
    group = jnp.where(owned, local // SUBLANES, -1)
    lane = jnp.where(owned, local % SUBLANES, SUBLANES)
    count = jnp.sum(owned.reshape(-1, GATHER_BATCH).astype(jnp.int32), axis=1)
    scratch = [pltpu.VMEM((GATHER_SLOTS, GATHER_BATCH, SUBLANES, width), BF16), DMA((GATHER_SLOTS,))] + zero_scratch(width)
    return local_call(pick_body, "pick_rows", [shape(span, width), shape(rows, width, F32)], specs("sssh"), specs("vh"), scratch, 20)(group, lane, count, table.reshape(rows // SUBLANES, SUBLANES, width))


SEMS = 32
AHEAD = 4
MOVE_SLOTS = 8
MOVE_ROWS = 128
MAX_TILES = 16


LANES = 128
KEY_BITS = 11


def put_body(keys_ref, all_ref, zero_ref, *refs):
    kinds = len(refs) // 2 - 4
    sources, out_ref, rest = refs[:kinds], refs[kinds], refs[kinds + 1 :]
    targets, (rows_ref, load_sem, sems, moved, read_sems, write_sems, place, sent) = rest[:kinds], rest[kinds:]
    load = pltpu.make_async_copy(all_ref, rows_ref, load_sem)
    load.start()
    tokens = rows_in(rows_ref)
    base = lax.axis_index("tp") * rows_in(out_ref)

    def id_at(pos):
        return lax.shift_right_arithmetic(keys_ref[pos], KEY_BITS)

    def first_at(bound):
        def narrow(_, ends):
            low, high = ends
            middle = lax.div(low + high, 2)
            below = id_at(middle) < bound
            return jnp.where(below, middle + 1, low), jnp.where(below, high, middle)

        return lax.fori_loop(0, KEY_BITS + 1, narrow, (jnp.int32(0), jnp.int32(tokens)))[0]

    low, high = first_at(base), first_at(base + rows_in(out_ref))
    pieces = sources[0].shape[0] // MOVE_ROWS
    moves = kinds * pieces
    lag = MOVE_SLOTS // 2
    steps = moves + MOVE_SLOTS

    reads, writes = Ring(moved, read_sems, True), Ring(moved, write_sems, False)

    def views(arrays, step):
        return [ref.at[rows_at(lax.rem(step, pieces) * MOVE_ROWS, MOVE_ROWS)] for ref in arrays]

    def move(step):
        @pl.when(step >= MOVE_SLOTS)
        def _():
            writes.wait(step, views(targets, step)[0])

        @pl.when(step < moves)
        def _():
            reads.start(step, lax.div(step, pieces), views(sources, step))

        ready = step - lag

        @pl.when((ready >= 0) & (ready < moves))
        def _():
            reads.wait(ready, views(sources, ready)[0])
            writes.start(ready, lax.div(ready, pieces), views(targets, ready))

    def row(pos):
        return pl.ds(pos, 1)

    def wait_slot(slot):
        pltpu.make_async_copy(rows_ref.at[row(0), :], out_ref.at[row(0), :], sems.at[slot]).wait()

    def row_of(pos):
        return row(lax.bitwise_and(keys_ref[pos], tokens - 1))

    def token(pos):
        return rows_ref[row_of(pos), :]

    def one_id(carry):
        pos, count = carry
        row_id = id_at(pos)
        first = row_of(pos)

        def more(carry):
            return id_at(carry[0]) == row_id

        def add(carry):
            start, total = carry
            end = start
            for k in range(AHEAD):
                same = id_at(start + k) == row_id
                total = total + jnp.where(same, token(start + k), 0.0)
                end = end + same.astype(jnp.int32)
            return end, total

        after, total = lax.while_loop(more, add, (pos + 1, token(pos)))

        @pl.when(after > pos + 1)
        def _():
            rows_ref[first, :] = total

        slot = lax.rem(count, SEMS)
        pl.when(count >= SEMS)(lambda: wait_slot(slot))
        pltpu.make_async_copy(rows_ref.at[first, :], out_ref.at[row(row_id - base), :], sems.at[slot]).start()
        return after, count + 1

    place[0] = low
    sent[0] = 0

    def step_body(step, carry):
        move(step)
        pl.when(step == 0)(load.wait)
        limit = low + lax.div((high - low) * (step + 1), steps)
        pos, count = lax.while_loop(lambda c: c[0] < limit, one_id, (place[0], sent[0]))
        place[0] = pos
        sent[0] = count
        return carry

    lax.fori_loop(0, steps, step_body, 0)
    count = sent[0]

    def drain(slot, carry):
        pl.when(slot < count)(lambda: wait_slot(slot))
        return carry

    lax.fori_loop(0, SEMS, drain, 0)


def put_rows(keys, rows, zeros, results):
    slots = DMA((MOVE_SLOTS,))
    counter = pltpu.SMEM((1,), jnp.int32)
    scratch = [pltpu.VMEM(rows.shape, F32), DMA, DMA((SEMS,)), pltpu.VMEM((MOVE_SLOTS, MOVE_ROWS, cols_of(rows)), F32), slots, slots, counter, counter]
    out_shape = [shape(*v.shape, F32) for v in (zeros, *results)]
    return local_call(put_body, "put_rows", out_shape, specs("shh") + [HBM] * len(results), [HBM] * len(out_shape), scratch, 20, {2: 0})(keys, rows, zeros, *results)


def move_body(*refs):
    half = len(refs) // 2
    for src, dst in zip(refs[:half], refs[half:]):
        dst[()] = src[()]


def move(*arrays):
    steps = SUBLANES
    blocks = [pl.BlockSpec((rows_in(v) // steps, cols_of(v)), lambda i: (i, 0)) for v in arrays]
    return local_call(move_body, "move", [shape(*v.shape, F32) for v in arrays], blocks, blocks, [], 20, grid=(steps,))(*arrays)


Q_TILE = 256
K_TILE = 512


def as_column(row):
    return jnp.broadcast_to(row, (LANES, LANES)).T


def stack_heads(v):
    half = cols_of(v) // 2
    return jnp.concatenate([v[:, :half], v[:, half:]], axis=0)


def unstack_heads(v):
    half = rows_in(v) // 2
    return jnp.concatenate([v[:half], v[half:]], axis=1)


def sequence_chunks(cp):
    return [chunk * K_TILE for chunk in (cp, 3 - cp, 1 - cp, 2 + cp)]


class Tile:
    def __init__(self, q_ref, pos_ref, starts_ref):
        tile = pl.program_id(1)
        per_chunk = K_TILE // Q_TILE
        cp = lax.axis_index("cp")
        late = tile >= per_chunk
        self.chunks = sequence_chunks(cp)
        first = jnp.where(late, self.chunks[1], self.chunks[0]) + lax.rem(tile, per_chunk) * Q_TILE
        pos = jnp.concatenate([as_column(pos_ref[:, i : i + LANES])[:, :1] for i in range(0, Q_TILE, LANES)], axis=0)
        high = first + lax.broadcasted_iota(jnp.int32, pos.shape, 0)
        twice = lambda v: jnp.concatenate([v, v], axis=0)
        self.low, self.high = twice(high - pos), twice(high)
        self.q = stack_heads(q_ref[()])
        at = tile * Q_TILE
        ends = at + Q_TILE - 1
        lowest, highest = first - starts_ref[at], first + Q_TILE - 1 - starts_ref[ends]
        causal = (True, late, late | (cp == 1), late & (cp == 0))
        self.needed = [when & (chunk + K_TILE > lowest) for when, chunk in zip(causal, self.chunks)]
        self.free = [(chunk + K_TILE <= first + 1) & (highest <= chunk) for chunk in self.chunks]

    def visit(self, visit):
        for block, when in enumerate(self.needed):
            pl.when(when)(functools.partial(visit, block))

    def visit_scores(self, k_refs, visit):
        for block, (when, free) in enumerate(zip(self.needed, self.free)):
            (k,) = block_refs(block, k_refs)
            scores = lambda: lax.dot_general(self.q, k[()], NT, preferred_element_type=F32)
            pl.when(when & free)(lambda: visit(block, scores()))
            pl.when(when & jnp.logical_not(free))(lambda: visit(block, self.mask(scores(), block)))

    def mask(self, scores, block):
        at = self.chunks[block] + lax.broadcasted_iota(jnp.int32, (1, K_TILE), 1)
        return jnp.where((at >= self.low) & (at <= self.high), scores, NEG_BIG)


def block_refs(block, *pairs):
    rows = pl.ds((block % 2) * K_TILE, K_TILE)
    return [pair[block // 2].at[rows] for pair in pairs]


def attend_body(scale, starts_ref, q_ref, k_ref, v_ref, k2_ref, v2_ref, pos_ref, zeros_in, out_ref, lse_ref, grad_ref, s_ref, m_ref, l_ref, acc_ref, zero_ref, zero_sem):
    end_zeros = grid_zeros(grad_ref, zero_ref, zero_sem, "attend")
    tile = Tile(q_ref, pos_ref, starts_ref)
    power = scale * LOG2_E
    clear(m_ref, NEG_BIG)
    clear(l_ref)
    clear(acc_ref)

    def score(block, s):
        s_ref[block] = s
        m_ref[()] = jnp.maximum(m_ref[()], over_row(jnp.max, s))

    def exponent(block):
        e = jnp.exp2((s_ref[block] - m_ref[()]) * power)
        s_ref[block] = e
        l_ref[()] += over_row(jnp.sum, e)

    tile.visit_scores((k_ref, k2_ref), score)
    tile.visit(exponent)
    inverse = 1.0 / l_ref[()]

    def mix(block):
        (v,) = block_refs(block, (v_ref, v2_ref))
        prob = (s_ref[block] * inverse).astype(BF16)
        acc_ref[()] += jnp.dot(prob, v[()], preferred_element_type=F32)

    tile.visit(mix)
    out_ref[()] = unstack_heads(acc_ref[()].astype(BF16))
    lse_ref[()] = (m_ref[()] * power + jnp.log(l_ref[()]) * LOG2_E).reshape(lse_ref.shape)
    end_zeros()


def attention_specs(span, head_dim):
    tile = pl.BlockSpec((Q_TILE, 2 * head_dim), lambda h, t: (t, h))
    keys = pl.BlockSpec((span, head_dim), lambda h, t: (0, h))
    pos = pl.BlockSpec((1, Q_TILE), lambda h, t: (0, t))
    lse = pl.BlockSpec((1, 1, 2 * Q_TILE, 1), lambda h, t: (h, t, 0, 0))
    return tile, keys, pos, lse


def attention_buffers(heads):
    stacked = heads * Q_TILE
    return lambda c: pltpu.VMEM((stacked, c), F32), lambda dtype: pltpu.VMEM((4, stacked, K_TILE), dtype)


def attention_call(body, name, out_shape, in_specs, out_specs, scratch, gflops):
    aliases = {len(in_specs) - 1: len(out_specs) - 1}
    scratch = scratch + zero_scratch(out_shape[-1].shape[1])
    return local_call(body, name, out_shape, in_specs, out_specs, scratch, gflops, aliases, grid=(2, 4))


def attend(scale, starts, q, k, v, k2, v2, pos, grad):
    span = rows_in(q)
    heads = 2
    head_dim = cols_of(k) // heads
    tile, keys, pos_spec, lse = attention_specs(span, head_dim)
    stacked = heads * Q_TILE
    buf, probs = attention_buffers(heads)
    out_shape = [shape(*q.shape), jax.ShapeDtypeStruct((heads, span // Q_TILE, stacked, 1), F32), shape(*grad.shape, F32)]
    column = buf(1)
    scratch = [probs(F32), column, column, buf(head_dim)]
    call = attention_call(functools.partial(attend_body, scale), "attend", out_shape, [SMEM, tile] + [keys] * 4 + [pos_spec, HBM], [tile, lse, HBM], scratch, 14)
    return call(starts, q, k, v, k2, v2, pos, grad)


def attend_back_body(scale, starts_ref, q_ref, do_ref, lse_ref, k_ref, v_ref, k2_ref, v2_ref, pos_ref, zeros_in, dq_ref, dk_ref, dv_ref, dk2_ref, dv2_ref, grad_ref, p_ref, dp_ref, d_ref, acc_ref, zero_ref, zero_sem):
    end_zeros = grid_zeros(grad_ref, zero_ref, zero_sem, "attend_back")
    tile = Tile(q_ref, pos_ref, starts_ref)
    d_out = stack_heads(do_ref[()])
    lse = lse_ref[()].reshape(rows_in(d_out), 1)
    clear(d_ref)
    clear(acc_ref)

    @pl.when(pl.program_id(1) == 0)
    def _():
        for ref in (dk_ref, dv_ref, dk2_ref, dv2_ref):
            clear(ref)

    def first(block, s):
        (v,) = block_refs(block, (v_ref, v2_ref))
        p = jnp.exp2(s * (scale * LOG2_E) - lse)
        dp = lax.dot_general(d_out, v[()], NT, preferred_element_type=F32).astype(BF16)
        p_ref[block] = p
        dp_ref[block] = dp
        d_ref[()] += over_row(jnp.sum, p * dp.astype(F32))

    def second(block):
        k, dk, dv = block_refs(block, (k_ref, k2_ref), (dk_ref, dk2_ref), (dv_ref, dv2_ref))
        p = p_ref[block]
        ds = (p * (dp_ref[block].astype(F32) - d_ref[()]) * scale).astype(BF16)
        acc_ref[()] += jnp.dot(ds, k[()], preferred_element_type=F32)
        dk[()] += lax.dot_general(ds, tile.q, CONTRACT_FIRST, preferred_element_type=F32)
        dv[()] += lax.dot_general(p.astype(BF16), d_out, CONTRACT_FIRST, preferred_element_type=F32)

    tile.visit_scores((k_ref, k2_ref), first)
    tile.visit(second)
    dq_ref[()] = unstack_heads(acc_ref[()].astype(BF16))
    end_zeros()


def attend_back(scale, starts, q, d_out, lse, k, v, k2, v2, pos, grad):
    span = rows_in(q)
    heads = 2
    head_dim = cols_of(k) // heads
    tile, keys, pos_spec, lse_spec = attention_specs(span, head_dim)
    buf, probs = attention_buffers(heads)
    out_shape = [shape(*q.shape)] + [shape(*k.shape, F32)] * 4 + [shape(*grad.shape, F32)]
    in_specs = [SMEM, tile, tile, lse_spec] + [keys] * 4 + [pos_spec, HBM]
    call = attention_call(functools.partial(attend_back_body, scale), "attend_back", out_shape, in_specs, [tile] + [keys] * 4 + [HBM], [probs(F32), probs(BF16), buf(1), buf(head_dim)], 30)
    return call(starts, q, d_out, lse, k, v, k2, v2, pos, grad)


def remote(src, dst, send, recv, device):
    return pltpu.make_async_remote_copy(src_ref=src, dst_ref=dst, send_sem=send, recv_sem=recv, device_id=device, device_id_type=MESH_ID)


def flipped(bit, flip):
    return bit + flip - 2 * bit * flip


class Place:
    def __init__(self):
        self.tp = lax.axis_index("tp")
        self.cp = lax.axis_index("cp")
        self.x = lax.rem(self.tp, 2)
        self.y = lax.div(self.tp, 2)
        self.over_x = (self.chip(1, 0), self.cp)
        self.over_y = (self.chip(0, 1), self.cp)
        self.twin = (self.tp, 1 - self.cp)

    def chip(self, dx, dy):
        return 2 * flipped(self.y, dy) + flipped(self.x, dx)

    def meet(self):
        barrier = pltpu.get_barrier_semaphore()
        peers = (self.over_x, self.over_y, self.twin)
        for device in peers:
            pl.semaphore_signal(barrier, inc=1, device_id=device, device_id_type=MESH_ID)
        pl.semaphore_wait(barrier, len(peers))


class Total:
    def __init__(self, place, part, wide, mid, narrow, out, send, recv):
        self.part, self.wide, self.mid, self.narrow, self.out = part, wide, mid, narrow, out
        self.send, self.recv = send, recv
        self.rows = rows_in(out) // STEPS
        self.half, self.quarter, self.eighth = (self.rows // n for n in (2, 4, 8))
        self.kinds = [(place.x, place.y, place.over_x, place.over_y), (place.y, place.x, place.over_y, place.over_x)]

    def _rows(self, step, kind):
        first, second = self.kinds[kind][:2]
        side = step * self.rows + kind * self.half + first * self.quarter
        return rows_at(side, self.quarter), rows_at(side + second * self.eighth, self.eighth)

    def _kept(self, kind, flip=0):
        return rows_at(kind * self.half + flipped(self.kinds[kind][0], flip) * self.quarter, self.quarter)

    def _eighth(self, kind, flip=0):
        return rows_at(flipped(self.kinds[kind][1], flip) * self.eighth, self.eighth)

    def _copy(self, step, kind, stage):
        side, mine = self._rows(step, kind)
        _, _, peer_first, peer_second = self.kinds[kind]
        src, dst, peer = (
            lambda: (self.part(step).at[self._kept(kind, 1)], self.wide.at[step, kind], peer_first),
            lambda: (self.mid.at[step, kind, self._eighth(kind, 1)], self.narrow.at[step, kind], peer_second),
            lambda: (self.out.at[mine], self.out.at[mine], peer_second),
            lambda: (self.out.at[side], self.out.at[side], peer_first),
        )[stage]()
        return remote(src, dst, self.send.at[step, kind, stage], self.recv.at[step, kind, stage], peer)

    def begin(self, step):
        for kind in BOTH:
            self._copy(step, kind, 0).start()

    def fold_wide(self, step):
        for kind in BOTH:
            self._copy(step, kind, 0).wait_recv()
            self.mid[step, kind] = self.part(step)[self._kept(kind), :] + self.wide[step, kind]
            self._copy(step, kind, 1).start()

    def fold_narrow(self, step):
        for kind in BOTH:
            self._copy(step, kind, 1).wait_recv()
            total = self.mid[step, kind, self._eighth(kind), :] + self.narrow[step, kind]
            self.out[self._rows(step, kind)[1], :] = total.astype(BF16)
            self._copy(step, kind, 2).start()

    def widen(self, step):
        for kind in BOTH:
            self._copy(step, kind, 2).wait_recv()
            self._copy(step, kind, 3).start()

    def finish(self, step):
        for kind in BOTH:
            self._copy(step, kind, 3).wait_recv()

    def sent(self, step, stages):
        for kind in BOTH:
            for stage in stages:
                self._copy(step, kind, stage).wait_send()


def sems(*dims):
    return DMA((*dims, 3))


def total_scratch(width, dtype, rows):
    stages = DMA((STEPS, 2, 4))
    part = lambda n: pltpu.VMEM((STEPS, 2, rows // n, width), dtype)
    return [part(4), part(4), part(8), stages, stages]


class Share:
    def __init__(self, place, sems, span):
        self.place, self.sems, self.first = place, sems, place.cp * span

    def pair(self, k, src, dst, start):
        here_sem, send, recv = (self.sems.at[k, i] for i in range(3))
        at = dst.at[rows_at(self.first + start, rows_in(src))]
        return pltpu.make_async_copy(src, at, here_sem), remote(src, at, send, recv, self.place.twin)

    def begin(self, *numbered):
        for copy in self.pair(*numbered):
            copy.start()

    def sent(self, *numbered):
        here, there = self.pair(*numbered)
        here.wait()
        there.wait_send()

    def got(self, k, src, dst, start):
        at = dst.at[rows_at(self.first + start, rows_in(src))]
        remote(src, at, *(self.sems.at[k, i] for i in (1, 2)), self.place.twin).wait_recv()


class Loads:
    def __init__(self, sems, *names):
        self.sems, self.names = sems, list(names)

    def _copies(self, moves):
        self.names += [name for name in moves if name not in self.names]
        return [pltpu.make_async_copy(src, dst, self.sems.at[self.names.index(name)]) for name, (src, dst) in moves.items()]

    def start(self, **moves):
        for copy in self._copies(moves):
            copy.start()
        return lambda: self.wait(**moves)

    def wait(self, **moves):
        for copy in self._copies(moves):
            copy.wait()


def steps(visit):
    def body(step, carry):
        visit(step)
        return carry

    lax.fori_loop(0, STEPS, body, 0)


def rope(v, cosine, sine):
    wide = cols_of(cosine)
    heads = []
    for h in range(cols_of(v) // wide):
        part = v[:, h * wide : (h + 1) * wide]
        turned = jnp.concatenate([part[:, wide // 2 :], part[:, : wide // 2]], axis=1)
        heads.append(part * cosine + turned * sine)
    return jnp.concatenate(heads, axis=1)


def each(count, size, visit):
    def body(i, carry):
        visit(pl.multiple_of(i * size, size))
        return carry

    lax.fori_loop(0, count // size, body, 0)


def col_loop(cols, tile, visit):
    each(cols, tile, lambda start: visit(pl.ds(start, tile)))


def dot_nt(a, b):
    return lax.dot_general(a, b, NT, preferred_element_type=F32)


def dot(a, b):
    return jnp.dot(a, b, preferred_element_type=F32)


def norm_block(feats):
    inverse = lax.rsqrt(over_row(jnp.mean, feats * feats) + NORM_EPS)
    return feats * inverse, inverse


def norm_back(d_act, gain, normed, inverse):
    d_normed = d_act * gain
    return inverse * (d_normed - normed * over_row(jnp.mean, d_normed * normed))


def remote_call(body, collective_id, name, out_shape, in_places, out_places, scratch, gflops):
    return pl.pallas_call(
        body,
        out_shape=out_shape,
        in_specs=specs(in_places),
        out_specs=specs(out_places),
        scratch_shapes=scratch,
        compiler_params=pltpu.CompilerParams(collective_id=collective_id, has_side_effects=True, vmem_limit_bytes=REMOTE_VMEM),
        cost_estimate=cost(gflops, 60),
        name=name,
    )


def join_columns(parts, whole):
    start, moves = 0, {}
    for i, part in enumerate(parts):
        moves[f"join{i}"] = (part, whole.at[:, pl.ds(start, cols_of(part))])
        start += cols_of(part)
    return moves


def order_ids(cp, ids, ids_got, keys, tall, rank, keys_out):
    span = cols_of(ids)
    chunks = rows_in(keys)
    lane = lax.broadcasted_iota(jnp.int32, (1, LANES), 1)
    for core, src in ((cp, ids), (1 - cp, ids_got)):
        for c in range(span // LANES):
            start = c * LANES
            token = core * span + start + lane
            keys[core * (chunks // 2) + c] = lax.shift_left(src[:, start : start + LANES], KEY_BITS) + token

    def count(a, carry):
        mine = as_column(keys[a])
        tall[a] = mine
        rank[a] = over_row(jnp.sum, sum((keys[b] < mine).astype(F32) for b in range(chunks)))
        return carry

    def place(c, carry):
        goal = (c * LANES + lane).astype(F32)
        keys_out[pl.ds(c, 1), :] = over_column(sum(jnp.where(rank[a] == goal, tall[a], 0) for a in range(chunks)))
        return carry

    lax.fori_loop(0, chunks, count, 0)
    lax.fori_loop(0, chunks, place, 0)
    keys_out[pl.ds(chunks, 1), :] = jnp.full((1, LANES), jnp.iinfo(jnp.int32).max, jnp.int32)


def enter_body(picked, wq_in, wk_in, wv_in, gain, pos, inv_freq, ids, dy_in, wd_in, x_rows, q_out, k_out, v_out, cosine, sine, keys_out, dh_out, k2_out, v2_out, act_all, dy_all, wide, mid, narrow, send, recv, x_out, act, dy, wd, dh, w_all, ids_got, keys, tall, rank, pair_sems, share_sems, load_sems, ids_sems):
    place = Place()
    place.meet()
    span = rows_in(x_out)
    rows = span // STEPS
    chunk = lambda step: rows_at(step * rows, rows)
    total = Total(place, lambda step: picked.at[chunk(step)], wide, mid, narrow, x_out, send, recv)
    share = Share(place, share_sems, span)
    loads = Loads(load_sems)
    steps(total.begin)
    ids_swap = remote(ids, ids_got, *(ids_sems.at[end] for end in BOTH), place.twin)
    ids_swap.start()
    loaded = loads.start(dy=(dy_in, dy), wd=(wd_in, wd))
    projection = loads.start(**join_columns((wq_in, wk_in, wv_in), w_all))
    kw = cols_of(k_out)
    qw = cols_of(q_out)

    def back(step):
        here = chunk(step)

        def tile(cols):
            dh[here, cols] = dot_nt(dy[here, :], wd[cols, :]).astype(BF16)

        col_loop(rows_in(wd), WIDE_TILE, tile)
        total.fold_wide(step)

    def pairs(step):
        return [remote(src.at[chunk(step)], dst.at[chunk(step)], *(pair_sems.at[step, i, end] for end in BOTH), place.twin) for i, (src, dst) in enumerate(((k_out, k2_out), (v_out, v2_out)))]

    x_kept = lambda step: dict(x=(x_out.at[chunk(step)], x_rows.at[chunk(step)]))
    act_share = lambda step: (1 + step, act.at[chunk(step)], act_all, step * rows)

    def project(step):
        total.finish(step)
        here = chunk(step)
        pl.when(step >= 1)(lambda: loads.wait(**x_kept(step - 1)))
        loads.start(**x_kept(step))

        def norm(start):
            at = rows_at(step * rows + start, ROW_BLOCK)
            normed, _ = norm_block(x_out[at, :].astype(F32))
            act[at, :] = (normed * gain[()].astype(F32)).astype(BF16)

        each(rows, ROW_BLOCK, norm)
        share.begin(*act_share(step))
        c, s = cosine[here, :], sine[here, :]
        out = dot(act[here, :], w_all[()])
        q_out[here, :] = rope(out[:, :qw], c, s).astype(BF16)
        k_out[here, :] = rope(out[:, qw : qw + kw], c, s).astype(BF16)
        v_out[here, :] = out[:, qw + kw :].astype(BF16)
        for copy in pairs(step):
            copy.start()

    def angles(start):
        at = pl.ds(start, LANES)
        angle = as_column(pos[:, at])[:, : cols_of(inv_freq)].astype(F32) * inv_freq[()]
        c, s = jnp.cos(angle), jnp.sin(angle)
        cosine[at, :] = jnp.concatenate([c, c], axis=1)
        sine[at, :] = jnp.concatenate([-s, s], axis=1)

    loaded()
    dy_share = (0, dy, dy_all, 0)
    share.begin(*dy_share)
    each(span, LANES, angles)
    steps(back)
    stored = loads.start(dh=(dh, dh_out))
    ids_swap.wait()
    order_ids(place.cp, ids, ids_got, keys, tall, rank, keys_out)
    steps(total.fold_narrow)
    steps(total.widen)
    projection()
    steps(project)

    def close(step):
        total.sent(step, range(4))
        share.sent(*act_share(step))
        share.got(*act_share(step))
        for copy in pairs(step):
            copy.wait()

    steps(close)
    share.sent(*dy_share)
    share.got(*dy_share)
    loads.wait(**x_kept(STEPS - 1))
    stored()


def enter(picked, wq, wk, wv, gain, pos, inv_freq, ids, dy, wd):
    span, width = picked.shape
    key = shape(span, cols_of(wk))
    angles = shape(span, 2 * cols_of(inv_freq), F32)
    all_rows = shape(2 * span, width)
    chunks = 2 * span // LANES
    int_buf = lambda *dims: pltpu.VMEM(dims, jnp.int32)
    big = pltpu.VMEM((span, width), BF16)
    out_shape = [shape(span, width), shape(span, cols_of(wq)), key, key, angles, angles, shape(chunks + SUBLANES, LANES, jnp.int32), shape(span, rows_in(wd)), key, key, all_rows, all_rows]
    scratch = total_scratch(width, BF16, span // STEPS) + [big, big, big, pltpu.VMEM(wd.shape, BF16), pltpu.VMEM((span, rows_in(wd)), BF16), pltpu.VMEM((width, cols_of(wq) + 2 * cols_of(wk)), BF16)]
    scratch += [int_buf(1, span), int_buf(chunks, 1, LANES), int_buf(chunks, LANES, LANES), pltpu.VMEM((chunks, LANES, 1), F32)]
    scratch += [DMA((STEPS, 2, 2)), sems(STEPS + 1), DMA((7,)), DMA((2,))]
    call = remote_call(enter_body, 1, "enter", out_shape, "vhhhvvvvhh", "hvvvvvvhhhhh", scratch, 80)
    return call(picked, wq, wk, wv, gain, pos, inv_freq, ids, dy, wd)


def middle_body(att, wo_own, wo_1, wo_2, wo_3, x_in, wg_in, wu_in, wd_in, dh_in, dy_in, gain, h_out, keep_x, send_x, keep_y, send_y, b_all, hidden_all, dgate_all, dup_all, att_all, drb_all, dr_out, datt_out, dgain_out,
                wide, mid, narrow, send, recv, wo, wg, wu, att_full, part_buf, d_b, h, row_in, dh, b, hid, dgt, dup, att_send, att_recv, wo_sems, load_sems, share_sems):
    place = Place()
    span, width = x_in.shape
    rows = span // STEPS
    half = rows // 2
    cols = cols_of(att)
    ffn = cols_of(wg)
    loads = Loads(load_sems, "att", "wo", "wg", "wu", "rows", "dh", "h_out", "h_in", "hid", "dr", "y")
    chunk = lambda step: rows_at(step * rows, rows)
    by_chip = lambda tp: rows_at(tp * cols, cols, 128)

    mine = loads.start(att=(att, att_full.at[:, by_chip(place.tp)]), wo=(wo_own, wo.at[by_chip(place.tp)]))
    place.meet()

    x_tp, y_tp = place.over_x[0], place.over_y[0]

    def att_copy(step, kind, hop):
        at = rows_at(step * rows + kind * half, half)
        first, second = ((place.over_y, place.over_x), (place.over_x, place.over_y))[kind]
        relay = hop == 2
        dst = att_full.at[at, by_chip(first[0] if relay else place.tp)]
        return remote(dst if relay else att.at[at], dst, att_send.at[step, kind, hop], att_recv.at[step, kind, hop], second if hop else first)

    def att_begin(step):
        for hop in BOTH:
            for kind in BOTH:
                att_copy(step, kind, hop).start()

    def att_forward(step):
        for kind in BOTH:
            att_copy(step, kind, 0).wait_recv()
            att_copy(step, kind, 2).start()

    att_begin(0)
    part = rows_in(wo_1)
    arrivals = []
    near = jnp.where(place.cp == 0, y_tp, x_tp)
    chips = (near, x_tp + y_tp - near, place.chip(1, 1))
    for i, (src, chip) in enumerate(zip((wo_1, wo_2, wo_3), chips)):
        at = wo.at[rows_at((2 * chip + place.cp) * part, part, 128)]
        here_sem, send_sem, recv_sem = (wo_sems.at[i, end] for end in range(3))
        for copy in (pltpu.make_async_copy(src, at, here_sem), remote(src, at, send_sem, recv_sem, place.twin)):
            copy.start()
            arrivals.append(copy)
    att_begin(1)
    weights = loads.start(wg=(wg_in, wg), wu=(wu_in, wu))

    share = Share(place, share_sems, span)
    att_share = (0, att, att_all, 0)
    share.begin(*att_share)
    total = Total(place, lambda step: part_buf.at[step], wide, mid, narrow, d_b, send, recv)

    def numbered(i, src, dst, step):
        return 1 + len(shares) * step + i, src, dst, step * rows

    shares = ((b, b_all), (hid, hidden_all), (dgt, dgate_all), (dup, dup_all), (b, drb_all))
    forward_shares = list(enumerate(shares))[:-1]
    fetched = lambda step: dict(rows=(x_in.at[chunk(step)], row_in), dh=(dh_in.at[chunk(step)], dh))
    h_kept = lambda step: dict(h_out=(h, h_out.at[chunk(step)]))

    def close(step):
        loads.wait(**h_kept(step))
        for i, pair in forward_shares:
            share.sent(*numbered(i, *pair, step))

    def forward(step):
        pl.when(step >= 1)(lambda: close(step - 1))
        loads.wait(**fetched(step))
        for kind in BOTH:
            for hop in (1, 2):
                att_copy(step, kind, hop).wait_recv()

        def residual(c):
            h[:, c] = row_in[:, c].astype(F32) + dot(att_full[chunk(step), :], wo[:, c])

        col_loop(width, BIG_TILE, residual)
        loads.start(**h_kept(step))

        def norm(start):
            at = pl.ds(start, ROW_BLOCK)
            normed, _ = norm_block(h[at, :])
            b[at, :] = (normed * gain[()].astype(F32)).astype(BF16)

        each(rows, ROW_BLOCK, norm)
        share.begin(*numbered(0, b, b_all, step))
        pl.when(step == 0)(weights)

        def hidden(c):
            gate = dot(b[()], wg[:, c])
            up = dot(b[()], wu[:, c])
            sig = 1.0 / (1.0 + jnp.exp(-gate))
            d_hid = dh[:, c].astype(F32)
            act = gate * sig
            hid[:, c] = (act * up).astype(BF16)
            dgt[:, c] = (d_hid * up * sig * (1.0 + gate * (1.0 - sig))).astype(BF16)
            dup[:, c] = (d_hid * act).astype(BF16)

        col_loop(ffn, WIDE_TILE, hidden)
        for i, pair in forward_shares[1:]:
            share.begin(*numbered(i, *pair, step))
        pl.when(step == 0)(lambda: att_forward(2))

        @pl.when(step + 1 < STEPS)
        def _():
            loads.start(**fetched(step + 1))

        def back(c):
            part_buf[step, :, c] = dot_nt(dgt[()], wg[c, :]) + dot_nt(dup[()], wu[c, :])

        col_loop(width, WIDE_TILE, back)
        total.begin(step)
        pl.when(step == 0)(lambda: att_forward(3))
        pl.when(step >= 2)(lambda: total.fold_wide(step - 2))

    loads.start(**fetched(0))
    att_forward(0)
    for step in range(2, STEPS):
        att_begin(step)
    mine()
    for copy in arrivals:
        copy.wait()
    att_forward(1)
    steps(forward)
    clear(dgain_out)
    close(STEPS - 1)
    wd = wg
    weights = loads.start(wg=(wd_in, wd))
    d_r, y_buf = part_buf.at[0], part_buf.at[1]

    h_back = lambda step: dict(h_in=(h_out.at[chunk(step)], h))
    hidden_back = lambda step: dict(hid=(hidden_all.at[rows_at(place.cp * span + step * rows, rows)], hid))
    dy_back = lambda step: dict(rows=(dy_in.at[chunk(step)], row_in))
    y_kept = dict(y=(y_buf, keep_x))
    for step in BOTH:
        total.sent(step, (0,))
    loads.start(**h_back(0), **hidden_back(0))

    def output(step):
        pl.when(step < 2)(lambda: total.fold_wide(step + 2))
        loads.wait(**h_back(step), **hidden_back(step))
        pl.when(step == 0)(weights)
        pl.when(step >= 1)(lambda: loads.wait(**y_kept))
        over_x_first = step < 2
        first = jnp.where(over_x_first, place.x, place.y)
        second = place.x + place.y - first
        kept = first == lax.rem(step, 2)
        row = lax.broadcasted_iota(jnp.int32, (rows, 1), 0)
        owner = kept & (lax.div(row, half) == second)

        def tile(c):
            y_buf[:, c] = dot(hid[()], wd[:, c]) + jnp.where(owner, h[:, c], 0.0)

        col_loop(width, BIG_TILE, tile)
        for side_first, keep, send_to in ((over_x_first, keep_x, send_x), (jnp.logical_not(over_x_first), keep_y, send_y)):
            for chosen, dst in ((kept, keep), (jnp.logical_not(kept), send_to)):

                @pl.when(side_first & chosen)
                def _():
                    loads.start(y=(y_buf, dst))

        @pl.when(step + 1 < STEPS)
        def _():
            loads.start(**h_back(step + 1), **hidden_back(step + 1))

        total.fold_narrow(step)
        pl.when(step >= 2)(lambda: total.widen(step - 2))

    steps(output)
    loads.start(**h_back(0), **dy_back(0))
    kept_rows = lambda step: dict(dr=(d_r, dr_out.at[chunk(step)]))
    resid_share = lambda step: numbered(len(shares) - 1, b, drb_all, step)

    def resid_sent(step):
        loads.wait(**kept_rows(step))
        share.sent(*resid_share(step))

    def resid(step):
        pl.when(step < 2)(lambda: total.widen(step + 2))
        total.finish(step)
        loads.wait(**h_back(step), **dy_back(step))
        pl.when(step >= 1)(lambda: resid_sent(step - 1))

        def grad(start):
            at = pl.ds(start, ROW_BLOCK)
            normed, inverse = norm_block(h[at, :])
            d_act = d_b[rows_at(step * rows + start, ROW_BLOCK), :].astype(F32)
            dgain_out[()] += over_column(d_act * normed)
            out = row_in[at, :].astype(F32) + norm_back(d_act, gain[()].astype(F32), normed, inverse)
            d_r[at, :] = out
            b[at, :] = out.astype(BF16)

        each(rows, ROW_BLOCK, grad)

        @pl.when(step + 1 < STEPS)
        def _():
            loads.start(**h_back(step + 1), **dy_back(step + 1))

        loads.start(**kept_rows(step))
        share.begin(*resid_share(step))
        datt_out[chunk(step), :] = dot_nt(b[()], wo[by_chip(place.tp), :]).astype(BF16)

    steps(resid)
    loads.wait(**y_kept)
    resid_sent(STEPS - 1)
    share.sent(*att_share)
    share.got(*att_share)

    def finish(step):
        total.sent(step, range(1, 4))
        pl.when(step >= 2)(lambda: total.sent(step, (0,)))
        for kind in BOTH:
            for hop in range(3):
                att_copy(step, kind, hop).wait_send()
        for i, pair in enumerate(shares):
            share.got(*numbered(i, *pair, step))

    steps(finish)


def middle(att, wo_pieces, x, wg, wu, wd, d_hidden, dy, gain):
    span, width = x.shape
    rows = span // STEPS
    ffn = cols_of(wg)
    cols = cols_of(att)
    full = shape(span, width, F32)
    both = shape(2 * span, ffn)
    out_shape = [full] + [shape(rows, width, F32)] * 4 + [shape(2 * span, width), both, both, both, shape(2 * span, cols), shape(2 * span, width), full, shape(span, cols), shape(*gain.shape, F32)]
    buf = lambda r, c, dtype=BF16: pltpu.VMEM((r, c), dtype)
    scratch = total_scratch(width, F32, rows)
    scratch += [buf(width, width), buf(width, ffn), buf(width, ffn), buf(span, width), pltpu.VMEM((STEPS, rows, width), F32), buf(span, width), buf(rows, width, F32)]
    scratch += [buf(rows, c) for c in (width, ffn, width, ffn, ffn, ffn)]
    scratch += [sems(STEPS, 2), sems(STEPS, 2), sems(3), DMA((11,)), sems(1 + 5 * STEPS)]
    call = remote_call(middle_body, 2, "middle", out_shape, "vhhhhhhhhhhv", "hhhhhhhhhhhhvv", scratch, 120)
    return call(att, *wo_pieces, x, wg, wu, wd, d_hidden, dy, gain)


def leave_body(dq_in, dk_in, dv_in, dk2_in, dv2_in, cosine, sine, wq_in, wk_in, wv_in, x_in, dr_in, gain, dgain_b, b_all, dgate_all, dup_all, hidden_all, dy_all, att_all, drb_all, act_all, d_all, dx_all, gain_a_out, gain_b_out, grad_gate, grad_up, grad_down, grad_out, grad_q, grad_k, grad_v,
               wide, mid, narrow, send, recv, part_buf, d_a, dk_got, dv_got, d_qkv, w_all, xs, drs, dxs, gain_got, left, right, result, pair_sems, load_sems, share_sems, left_sems, right_sems, result_sems, result_arrivals):
    place = Place()
    place.meet()
    span, width = x_in.shape
    rows = span // STEPS
    chunk = lambda step: rows_at(step * rows, rows)
    swap = lambda i, src, dst: remote(src, dst, *(pair_sems.at[i, end] for end in BOTH), place.twin)
    pairs = lambda step: [swap(2 * step + i, src.at[chunk(step)], dst.at[chunk(step)]) for i, (src, dst) in enumerate(((dk2_in, dk_got), (dv2_in, dv_got)))]
    for step in range(STEPS):
        for copy in pairs(step):
            copy.start()
    qw = cols_of(dq_in)
    kw = cols_of(dk_in)
    share = Share(place, share_sems, span)
    loads = Loads(load_sems)
    total = Total(place, lambda step: part_buf.at[step], wide, mid, narrow, d_a, send, recv)

    def partial(step):
        here = chunk(step)
        c, s = cosine[here, :], -sine[here, :]
        for copy in pairs(step):
            copy.wait()
        d_qkv[here, :qw] = rope(dq_in[here, :].astype(F32), c, s).astype(BF16)
        dk_sum = (dk_in[here, :] + dk_got[here, :]).astype(BF16).astype(F32)
        d_qkv[here, qw : qw + kw] = rope(dk_sum, c, s).astype(BF16)
        d_qkv[here, qw + kw :] = (dv_in[here, :] + dv_got[here, :]).astype(BF16)

        def tile(n):
            part_buf[step, :, n] = dot_nt(d_qkv[here, :], w_all[n, :])

        col_loop(width, BIG_TILE, tile)
        total.begin(step)

    rows_back = lambda step: dict(x=(x_in.at[chunk(step)], xs), dr=(dr_in.at[chunk(step)], drs))

    clear(gain_a_out)

    def dx_share(step, part):
        start = part * part_rows
        return 1 + 2 * step + part, dxs.at[rows_at(start, part_rows)], dx_all, step * rows + start

    part_rows = rows // 2

    def grad_x(step):
        for part in BOTH:

            def grad(start):
                start = part * part_rows + start
                at = rows_at(start, ROW_BLOCK)
                normed, inverse = norm_block(xs[at, :].astype(F32))
                d_act = d_a[rows_at(step * rows + start, ROW_BLOCK), :].astype(F32)
                gain_a_out[()] += over_column(d_act * normed)
                dxs[at, :] = drs[at, :] + norm_back(d_act, gain[()].astype(F32), normed, inverse)

            pl.when(step >= 1)(lambda: share.sent(*dx_share(step - 1, part)))
            each(part_rows, ROW_BLOCK, grad)
            share.begin(*dx_share(step, part))

    _, _, narrow_cols = left.shape
    _, _, wide_cols = right.shape
    lefts, rights = Ring(left, left_sems, True), Ring(right, right_sems, True)
    sides, per_core = width // wide_cols, width // narrow_cols // 2
    whole = (grad_gate, grad_up, grad_down, grad_out)
    ffn_blocks = (len(whole) - 1) * sides
    ffn_tiles = ffn_blocks * per_core
    tiles = ffn_tiles + 1 + per_core
    block_of = lambda t: jnp.where(t < ffn_tiles, lax.div(t, per_core), jnp.minimum(t - ffn_tiles, 1) + ffn_blocks)
    row_of = lambda t: place.cp * per_core + jnp.where(t < ffn_tiles, lax.rem(t, per_core), jnp.maximum(t - ffn_tiles - 1, 0))
    at_left = lambda t: rows_at(row_of(t) * narrow_cols, narrow_cols, TILE)
    at_right = lambda j: rows_at(jnp.where(j < ffn_blocks, lax.rem(j, sides), place.cp) * wide_cols, wide_cols, TILE)
    kind_of = lambda j: jnp.where(j < ffn_blocks, lax.div(j, sides), len(whole) - 1 + j - ffn_blocks)
    left_start = lambda t: lefts.start(t, kind_of(block_of(t)), [ref.at[:, at_left(t)] for ref in (b_all, b_all, hidden_all)] + [att_all, act_all.at[:, at_left(t)]])
    right_start = lambda j: rights.start(j, kind_of(j), [ref.at[:, at_right(j)] for ref in (dgate_all, dup_all, dy_all, drb_all)] + [d_all])

    def to_twin(t, src, dst):
        return remote(src, dst, result_sems.at[lefts.slot(t), 1], result_arrivals.at[t], place.twin)

    def stored(t):
        done = result.at[lefts.slot(t)]
        pltpu.make_async_copy(done, done, result_sems.at[lefts.slot(t), 0]).wait()
        to_twin(t, done, done).wait_send()

    def store(t):
        slot = lefts.slot(t)
        j = block_of(t)

        def put(cols, dst):
            src = result.at[slot, :, cols]
            pltpu.make_async_copy(src, dst, result_sems.at[slot, 0]).start()
            to_twin(t, src, dst).start()

        everything = pl.ds(0, wide_cols)
        for k, ref in enumerate(whole):
            at = at_left(t) if ref is not grad_out else pl.ds(0, narrow_cols)
            pl.when(kind_of(j) == k)(lambda: put(everything, ref.at[at, at_right(j)]))

        @pl.when(j == ffn_blocks + 1)
        def _():
            put(pl.ds(0, qw), grad_q.at[at_left(t)])
            put(pl.ds(qw, kw), grad_k.at[at_left(t)])
            put(pl.ds(qw + kw, kw), grad_v.at[at_left(t)])

    def tile_step(t, carry):
        j = block_of(t)
        pl.when(t + 1 < tiles)(lambda: left_start(t + 1))

        @pl.when(jnp.where(t < ffn_tiles, lax.rem(t, per_core) == 0, t <= ffn_tiles + 1))
        def _():
            pl.when(j < ffn_blocks)(lambda: right_start(j + 1))
            rights.wait(j, d_all)

        lefts.wait(t, att_all)
        pl.when(t >= 2)(lambda: stored(t))
        slot = lefts.slot(t)
        result[slot] = lax.dot_general(left[slot], right[rights.slot(j)], CONTRACT_FIRST, preferred_element_type=F32)
        store(t)
        return carry

    left_start(jnp.int32(0))
    right_start(jnp.int32(0))
    weights = loads.start(**join_columns((wq_in, wk_in, wv_in), w_all))
    loads.start(**rows_back(0))
    weights()
    steps(partial)
    d_here, d_there = share.pair(0, d_qkv, d_all, 0)
    d_here.start()
    d_there.start()

    stages = (total.fold_wide, total.fold_narrow, total.widen)
    waits = len(stages) * STEPS
    portion = ffn_tiles // STEPS
    tiles_until = lambda p: jnp.where(p < STEPS, portion * (p + 1), jnp.where(p < 2 * STEPS - 1, ffn_tiles, jnp.where(p < waits - 1, ffn_tiles + 1, tiles)))

    def wait_step(p, carry):
        @pl.when(p == waits - 1)
        def _():
            d_here.wait()
            d_there.wait_recv()
            right_start(jnp.int32(ffn_blocks + 1))

        lax.fori_loop(jnp.where(p == 0, 0, tiles_until(p - 1)), tiles_until(p), tile_step, 0)
        for k, stage in enumerate(stages):
            pl.when(lax.div(p, STEPS) == k)(lambda: stage(lax.rem(p, STEPS)))
        return carry

    lax.fori_loop(0, waits, wait_step, 0)
    def last_stage(step):
        loads.wait(**rows_back(step))
        total.finish(step)
        grad_x(step)

        @pl.when(step + 1 < STEPS)
        def _():
            loads.start(**rows_back(step + 1))

    steps(last_stage)
    gains = ((gain_a_out, gain_a_out), (dgain_b, gain_b_out))
    swaps = [swap(2 * STEPS + i, mine, gain_got.at[i]) for i, (mine, _) in enumerate(gains)]
    for copy in swaps:
        copy.start()
    for copy in swaps:
        copy.wait()
    for i, (mine, out) in enumerate(gains):
        out[()] = mine[()] + gain_got[i]
    for part in BOTH:
        share.sent(*dx_share(STEPS - 1, part))
    d_there.wait_send()
    for t in range(tiles - 2, tiles):
        stored(t)
    done = result.at[0]
    for t in range(tiles):
        to_twin(t, done, done).wait_recv()

    def close(step):
        total.sent(step, range(4))
        for part in BOTH:
            share.got(*dx_share(step, part))

    steps(close)


def leave(dq, dk, dv, dk2, dv2, cosine, sine, wq, wk, wv, x, d_resid, gain, dgain_b, *products):
    span, width = x.shape
    rows = span // STEPS
    kw = cols_of(wk)
    qw = cols_of(wq)
    cols = qw + 2 * kw
    ffn = products[1].shape[1]
    buf = lambda r, c, dtype=F32: pltpu.VMEM((r, c), dtype)
    gain_grad = shape(*gain.shape, F32)
    out_shape = [shape(2 * span, cols), shape(2 * span, width, F32), gain_grad, gain_grad]
    out_shape += [shape(*dims, F32) for dims in ((width, ffn), (width, ffn), (ffn, width), (qw, width), wq.shape, wk.shape, wv.shape)]
    twice = lambda r, c, dtype: pltpu.VMEM((2, r, c), dtype)
    scratch = total_scratch(width, F32, rows) + [pltpu.VMEM((STEPS, rows, width), F32), buf(span, width, BF16), buf(span, kw), buf(span, kw), buf(span, cols, BF16), buf(width, cols, BF16)]
    scratch += [buf(rows, width, BF16), buf(rows, width), buf(rows, width), pltpu.VMEM((2, 1, width), F32)]
    scratch += [twice(2 * span, WIDE_TILE, BF16), twice(2 * span, BIG_TILE, BF16), twice(WIDE_TILE, BIG_TILE, F32)]
    ring = DMA((2,))
    scratch += [DMA((2 * STEPS + 2, 2)), DMA((5,)), sems(1 + 2 * STEPS), ring, ring, DMA((2, 2)), DMA((MAX_TILES,))]
    call = remote_call(leave_body, 3, "leave", out_shape, "vvvhhvvhhhhhvvhhhhhhhh", "hhvvhhhhhhh", scratch, 1)
    return call(dq, dk, dv, dk2, dv2, cosine, sine, wq, wk, wv, x, d_resid, gain, dgain_b, *products)


def side(v, bit):
    half = rows_in(v) // 2
    return lax.dynamic_slice_in_dim(v, bit * half, half, 0)


def join(own, other, bit):
    return jnp.where(bit == 0, jnp.concatenate([own, other]), jnp.concatenate([other, own]))


def solution(mesh):
    def device_step(tokens, pos, doc_id, dy, table, w_q, w_k, w_v, w_o, w_gate, w_up, w_down, gain_one, gain_two, inv_freq):
        span = rows_in(tokens)
        rows, width = table.shape
        scale = (2 * rows_in(inv_freq)) ** -0.5
        tp = lax.axis_index("tp")
        cp = lax.axis_index("cp")
        starts = pos
        gain_a, gain_b, inv_freq, pos, ids = (v[None, :] for v in (gain_one, gain_two, inv_freq, pos, tokens))
        base = tp * rows

        wo_half = side(w_o, cp)
        wo_1 = swap_core(wo_half, 0)
        picked, grad = pick_rows(tokens, table, base)
        x, query, key, value, cosine, sine, keys, d_hidden, key2, value2, act_a_all, dy_all = enter(picked, w_q, w_k, w_v, gain_a, pos, inv_freq, ids, dy, w_down)
        wo_1, wo_half, query = lax.optimization_barrier((wo_1, wo_half, query))
        wo_pieces = (w_o, wo_1, swap_core(wo_half, 1), swap_core(wo_1, 1))
        att, lse, grad = attend(scale, starts, query, key, value, key2, value2, pos, grad)
        keep_x, send_x, keep_y, send_y, act_b_all, hidden_all, d_gate_all, d_up_all, att_all, d_resid_all, d_resid, d_att, d_gain_b = middle(att, wo_pieces, x, w_gate, w_up, w_down, d_hidden, dy, gain_b)[1:]

        x_bit, y_bit = tp % 2, tp // 2
        ways = ((keep_x, swap_x, x_bit, swap_y, y_bit), (keep_y, swap_y, y_bit, swap_x, x_bit))
        y_wide = [swap_x(send_x), swap_y(send_y)]
        d_query, d_key, d_value, d_key2, d_value2, grad = attend_back(scale, starts, query, d_att, lse, key, value, key2, value2, pos, grad)

        d_x_all, gain_1, gain_2, grad_gate, grad_up, grad_down, *grads = leave(d_query, d_key, d_value, d_key2, d_value2, cosine, sine, w_q, w_k, w_v, x, d_resid, gain_a, d_gain_b, act_b_all, d_gate_all, d_up_all, hidden_all, dy_all, att_all, d_resid_all, act_a_all)[1:]
        y_wide, d_x_all = lax.optimization_barrier((y_wide, d_x_all))
        halves = lambda bit_2, keep, wide, flip: side(keep, flipped(bit_2, flip)) + side(wide, flipped(bit_2, flip))
        y_narrow = [swap_2(halves(bit_2, keep, wide, 1)) for (keep, _, _, swap_2, bit_2), wide in zip(ways, y_wide)]
        y_wide, grad_gate = lax.optimization_barrier((y_wide, grad_gate))
        grad_gate, grad_out, *grads = move(grad_gate, *grads)
        y_narrow, grad_gate = lax.optimization_barrier((y_narrow, grad_gate))
        y_own = [(halves(bit_2, keep, wide, 0) + narrow).astype(BF16) for (keep, _, _, _, bit_2), wide, narrow in zip(ways, y_wide, y_narrow)]
        y_pair = [join(own, swap_2(own), bit_2) for (_, _, _, swap_2, bit_2), own in zip(ways, y_own)]
        y_own, grad_down = lax.optimization_barrier((y_own, grad_down))
        (grad_down,) = move(grad_down)
        y_pair, grad_down = lax.optimization_barrier((y_pair, grad_down))
        y_far = [swap_1(pair) for (_, swap_1, _, _, _), pair in zip(ways, y_pair)]
        y_pair, d_x_all = lax.optimization_barrier((y_pair, d_x_all))
        grad_table, grad_up = put_rows(keys.reshape(-1), d_x_all, grad, (grad_up,))
        y_rows = [jnp.where(bit_1 == k, pair, far) for (_, _, bit_1, _, _), pair, far in zip(ways, y_pair, y_far) for k in BOTH]
        return (jnp.concatenate(y_rows), grad_table, *grads, grad_out, grad_gate, grad_up, grad_down, gain_1[0], gain_2[0])

    col_spec = P(None, "tp")
    row_spec = P("tp", None)
    tok_spec = P("cp")
    rep_spec = P(None)
    in_specs = (tok_spec, tok_spec, tok_spec, P("cp", None), row_spec, col_spec, col_spec, col_spec, row_spec, col_spec, col_spec, row_spec, rep_spec, rep_spec, rep_spec)
    out_specs = (P("cp", None), row_spec, col_spec, col_spec, col_spec, row_spec, col_spec, col_spec, row_spec, rep_spec, rep_spec)
    return jax.shard_map(device_step, mesh=mesh, in_specs=in_specs, out_specs=out_specs, check_vma=False)
```

```python
import functools

import jax
import jax.numpy as jnp
from jax import lax
from jax.experimental import pallas as pl
from jax.experimental.pallas import tpu as pltpu
from jax.sharding import PartitionSpec as P

NORM_EPS = 1e-5
NEG_BIG = -1e30
F32 = jnp.float32
BF16 = jnp.bfloat16
MIB = 2**20
LOCAL_VMEM = 56 * MIB
REMOTE_VMEM = 63 * MIB
STEPS = 4
LOG2_E = 1.4426950408889634
SUBLANES = 8
BOTH = (0, 1)
ROW_BLOCK = 32
WIDE_TILE = 512
BIG_TILE = 1024
TILE = 256
MESH_ID = pl.DeviceIdType.MESH
NT = (((1,), (1,)), ((), ()))
CONTRACT_FIRST = (((0,), (0,)), ((), ()))
VMEM = pl.BlockSpec(memory_space=pltpu.VMEM)
SMEM = pl.BlockSpec(memory_space=pltpu.SMEM)
HBM = pl.BlockSpec(memory_space=pl.ANY)
DMA = pltpu.SemaphoreType.DMA


X_PAIRS, Y_PAIRS = ([(chip, chip ^ flip) for chip in range(4)] for flip in (1, 2))
C_PAIRS = X_PAIRS[:2]
CORE_PAIRS = tuple([(2 * a + core, 2 * b + core) for core, pairs in enumerate(kinds) for a, b in pairs] for kinds in ((Y_PAIRS, X_PAIRS), (X_PAIRS, Y_PAIRS)))


def swap_x(v):
    return lax.ppermute(v, "tp", X_PAIRS)


def swap_y(v):
    return lax.ppermute(v, "tp", Y_PAIRS)


def swap_c(v):
    return lax.ppermute(v, "cp", C_PAIRS)


def swap_core(v, which):
    return lax.ppermute(v, ("tp", "cp"), CORE_PAIRS[which])


def rows_in(v):
    return v.shape[0]


def cols_of(v):
    return v.shape[1]


def over_row(reduce, v):
    return reduce(v, axis=-1, keepdims=True)


def over_column(v):
    return jnp.sum(v, axis=0, keepdims=True)


def specs(places):
    return [{"v": VMEM, "h": HBM, "s": SMEM}[place] for place in places]


def cost(gflops, mib):
    return pl.CostEstimate(flops=gflops * 10**9, bytes_accessed=mib * MIB, transcendentals=0)


def shape(rows, cols, dtype=BF16):
    return jax.ShapeDtypeStruct((rows, cols), dtype)


def local_call(body, name, out_shape, in_specs, out_specs, scratch, gflops, aliases={}, **grid):
    return pl.pallas_call(
        body,
        out_shape=out_shape,
        in_specs=in_specs,
        out_specs=out_specs,
        scratch_shapes=scratch,
        input_output_aliases=aliases,
        compiler_params=pltpu.CompilerParams(vmem_limit_bytes=LOCAL_VMEM),
        cost_estimate=cost(gflops, 60),
        name=name,
        **grid,
    )


def rows_at(start, size, step=32):
    return pl.ds(pl.multiple_of(start, step), size)


class Ring:
    def __init__(self, buf, sems, inward):
        self.buf, self.sems, self.inward = buf, sems, inward

    def slot(self, count):
        return lax.rem(count, rows_in(self.buf))

    def _copy(self, count, view):
        pair = (view, self.buf.at[self.slot(count)])
        return pltpu.make_async_copy(*(pair if self.inward else pair[::-1]), self.sems.at[self.slot(count)])

    def start(self, count, kind, views):
        for k, view in enumerate(views):
            pl.when(kind == k)(lambda: self._copy(count, view).start())

    def wait(self, count, view):
        self._copy(count, view).wait()


ZERO_ROWS = 24
ZEROS = {"attend": (21, 58), "attend_back": (43, 87)}
ZERO_PICK = 2


def zero_block(out_ref, block, count=1):
    return out_ref.at[pl.ds(pl.multiple_of(block * ZERO_ROWS, ZERO_ROWS), count * ZERO_ROWS)]


def clear(ref, value=0.0):
    ref[()] = jnp.full(ref.shape, value, F32)


def start_zeros(out_ref, zero_ref, sem, first, count):
    def start(i, carry):
        pltpu.make_async_copy(zero_ref, zero_block(out_ref, first + i), sem).start()
        return carry

    lax.fori_loop(0, count, start, 0)


def wait_zeros(out_ref, sem, first, count):
    whole = zero_block(out_ref, first, count)
    pltpu.make_async_copy(whole, whole, sem).wait()


def zero_scratch(width):
    return [pltpu.VMEM((ZERO_ROWS, width), F32), DMA]


def grid_zeros(grad_ref, zero_ref, sem, name):
    head, tile = pl.program_id(0), pl.program_id(1)
    heads, tiles = pl.num_programs(0), pl.num_programs(1)
    half = tiles // 2
    early, late = ZEROS[name]
    whole = half * (early + late)
    before = rows_in(grad_ref) // ZERO_ROWS - heads * whole
    if name == "attend":
        before -= heads * half * sum(ZEROS["attend_back"])
    pl.when((head == 0) & (tile == 0))(functools.partial(clear, zero_ref))
    first = before + head * whole + tile * early + jnp.maximum(tile - half, 0) * (late - early)
    start_zeros(grad_ref, zero_ref, sem, first, early)
    pl.when(tile >= half)(functools.partial(start_zeros, grad_ref, zero_ref, sem, first + early, late - early))
    last = (head == heads - 1) & (tile == tiles - 1)
    return lambda: pl.when(last)(lambda: wait_zeros(grad_ref, sem, before, heads * whole))


GATHER_BATCH = 16
GATHER_SLOTS = 8


def pick_body(group_ref, lane_ref, count_ref, table_ref, out_ref, grad_ref, buf, sems, zero_ref, zero_sem):
    batches = rows_in(out_ref) // GATHER_BATCH
    width = cols_of(out_ref)

    def row_copy(group, slot, j):
        return pltpu.make_async_copy(table_ref.at[group], buf.at[slot, j], sems.at[slot])

    def start(step):
        slot = lax.rem(step, GATHER_SLOTS)
        for j in range(GATHER_BATCH):
            group = group_ref[step * GATHER_BATCH + j]
            pl.when(group >= 0)(lambda: row_copy(group, slot, j).start())

    for step in range(GATHER_SLOTS - 1):
        start(step)
    clear(zero_ref)
    row = lax.broadcasted_iota(jnp.int32, (SUBLANES, width), 0)

    def loop(step, carry):
        slot = lax.rem(step, GATHER_SLOTS)

        @pl.when(step + GATHER_SLOTS - 1 < batches)
        def _():
            start(step + GATHER_SLOTS - 1)

        start_zeros(grad_ref, zero_ref, zero_sem, step * ZERO_PICK, ZERO_PICK)

        def arrived(i, carry):
            row_copy(0, slot, 0).wait()
            return carry

        lax.fori_loop(0, count_ref[step], arrived, 0)
        first = pl.multiple_of(step * GATHER_BATCH, GATHER_BATCH)
        parts = []
        for j in range(GATHER_BATCH):
            lane = lane_ref[first + j]
            goal = j % SUBLANES
            if goal == 0:
                parts.append(jnp.zeros((SUBLANES, width), F32))
            turned = pltpu.roll(buf[slot, j].astype(F32), lax.rem(goal + SUBLANES - lane, SUBLANES), 0)
            parts[-1] = jnp.where(row == jnp.where(lane < SUBLANES, goal, SUBLANES), turned, parts[-1])
        out_ref[pl.ds(first, GATHER_BATCH), :] = jnp.concatenate(parts, axis=0).astype(BF16)
        return carry

    lax.fori_loop(0, batches, loop, 0)
    wait_zeros(grad_ref, zero_sem, 0, batches * ZERO_PICK)


def pick_rows(tokens, table, base):
    span = rows_in(tokens)
    rows, width = table.shape
    local = tokens - base
    owned = (local >= 0) & (local < rows)
    group = jnp.where(owned, local // SUBLANES, -1)
    lane = jnp.where(owned, local % SUBLANES, SUBLANES)
    count = jnp.sum(owned.reshape(-1, GATHER_BATCH).astype(jnp.int32), axis=1)
    scratch = [pltpu.VMEM((GATHER_SLOTS, GATHER_BATCH, SUBLANES, width), BF16), DMA((GATHER_SLOTS,))] + zero_scratch(width)
    return local_call(pick_body, "pick_rows", [shape(span, width), shape(rows, width, F32)], specs("sssh"), specs("vh"), scratch, 20)(group, lane, count, table.reshape(rows // SUBLANES, SUBLANES, width))


SEMS = 32
AHEAD = 4
MOVE_SLOTS = 8
MOVE_ROWS = 128
MAX_TILES = 16


LANES = 128
KEY_BITS = 11


def put_body(keys_ref, all_ref, zero_ref, *refs):
    kinds = len(refs) // 2 - 4
    sources, out_ref, rest = refs[:kinds], refs[kinds], refs[kinds + 1 :]
    targets, (rows_ref, load_sem, sems, moved, read_sems, write_sems, place, sent) = rest[:kinds], rest[kinds:]
    load = pltpu.make_async_copy(all_ref, rows_ref, load_sem)
    load.start()
    tokens = rows_in(rows_ref)
    base = lax.axis_index("tp") * rows_in(out_ref)

    def id_at(pos):
        return lax.shift_right_arithmetic(keys_ref[pos], KEY_BITS)

    def first_at(bound):
        def narrow(_, ends):
            low, high = ends
            middle = lax.div(low + high, 2)
            below = id_at(middle) < bound
            return jnp.where(below, middle + 1, low), jnp.where(below, high, middle)

        return lax.fori_loop(0, KEY_BITS + 1, narrow, (jnp.int32(0), jnp.int32(tokens)))[0]

    low, high = first_at(base), first_at(base + rows_in(out_ref))
    pieces = sources[0].shape[0] // MOVE_ROWS
    moves = kinds * pieces
    lag = MOVE_SLOTS // 2
    steps = moves + MOVE_SLOTS

    reads, writes = Ring(moved, read_sems, True), Ring(moved, write_sems, False)

    def views(arrays, step):
        return [ref.at[rows_at(lax.rem(step, pieces) * MOVE_ROWS, MOVE_ROWS)] for ref in arrays]

    def move(step):
        @pl.when(step >= MOVE_SLOTS)
        def _():
            writes.wait(step, views(targets, step)[0])

        @pl.when(step < moves)
        def _():
            reads.start(step, lax.div(step, pieces), views(sources, step))

        ready = step - lag

        @pl.when((ready >= 0) & (ready < moves))
        def _():
            reads.wait(ready, views(sources, ready)[0])
            writes.start(ready, lax.div(ready, pieces), views(targets, ready))

    def row(pos):
        return pl.ds(pos, 1)

    def wait_slot(slot):
        pltpu.make_async_copy(rows_ref.at[row(0), :], out_ref.at[row(0), :], sems.at[slot]).wait()

    def row_of(pos):
        return row(lax.bitwise_and(keys_ref[pos], tokens - 1))

    def token(pos):
        return rows_ref[row_of(pos), :]

    def one_id(carry):
        pos, count = carry
        row_id = id_at(pos)
        first = row_of(pos)

        def more(carry):
            return id_at(carry[0]) == row_id

        def add(carry):
            start, total = carry
            end = start
            for k in range(AHEAD):
                same = id_at(start + k) == row_id
                total = total + jnp.where(same, token(start + k), 0.0)
                end = end + same.astype(jnp.int32)
            return end, total

        after, total = lax.while_loop(more, add, (pos + 1, token(pos)))

        @pl.when(after > pos + 1)
        def _():
            rows_ref[first, :] = total

        slot = lax.rem(count, SEMS)
        pl.when(count >= SEMS)(lambda: wait_slot(slot))
        pltpu.make_async_copy(rows_ref.at[first, :], out_ref.at[row(row_id - base), :], sems.at[slot]).start()
        return after, count + 1

    place[0] = low
    sent[0] = 0

    def step_body(step, carry):
        move(step)
        pl.when(step == 0)(load.wait)
        limit = low + lax.div((high - low) * (step + 1), steps)
        pos, count = lax.while_loop(lambda c: c[0] < limit, one_id, (place[0], sent[0]))
        place[0] = pos
        sent[0] = count
        return carry

    lax.fori_loop(0, steps, step_body, 0)
    count = sent[0]

    def drain(slot, carry):
        pl.when(slot < count)(lambda: wait_slot(slot))
        return carry

    lax.fori_loop(0, SEMS, drain, 0)


def put_rows(keys, rows, zeros, results):
    slots = DMA((MOVE_SLOTS,))
    counter = pltpu.SMEM((1,), jnp.int32)
    scratch = [pltpu.VMEM(rows.shape, F32), DMA, DMA((SEMS,)), pltpu.VMEM((MOVE_SLOTS, MOVE_ROWS, cols_of(rows)), F32), slots, slots, counter, counter]
    out_shape = [shape(*v.shape, F32) for v in (zeros, *results)]
    return local_call(put_body, "put_rows", out_shape, specs("shh") + [HBM] * len(results), [HBM] * len(out_shape), scratch, 20, {2: 0})(keys, rows, zeros, *results)


def move_body(*refs):
    half = len(refs) // 2
    for src, dst in zip(refs[:half], refs[half:]):
        dst[()] = src[()]


def move(*arrays):
    steps = SUBLANES
    blocks = [pl.BlockSpec((rows_in(v) // steps, cols_of(v)), lambda i: (i, 0)) for v in arrays]
    return local_call(move_body, "move", [shape(*v.shape, F32) for v in arrays], blocks, blocks, [], 20, grid=(steps,))(*arrays)


Q_TILE = 256
K_TILE = 512


def as_column(row):
    return jnp.broadcast_to(row, (LANES, LANES)).T


def stack_heads(v):
    half = cols_of(v) // 2
    return jnp.concatenate([v[:, :half], v[:, half:]], axis=0)


def unstack_heads(v):
    half = rows_in(v) // 2
    return jnp.concatenate([v[:half], v[half:]], axis=1)


def sequence_chunks(cp):
    return [chunk * K_TILE for chunk in (cp, 3 - cp, 1 - cp, 2 + cp)]


class Tile:
    def __init__(self, q_ref, pos_ref, starts_ref):
        tile = pl.program_id(1)
        per_chunk = K_TILE // Q_TILE
        cp = lax.axis_index("cp")
        late = tile >= per_chunk
        self.chunks = sequence_chunks(cp)
        first = jnp.where(late, self.chunks[1], self.chunks[0]) + lax.rem(tile, per_chunk) * Q_TILE
        pos = jnp.concatenate([as_column(pos_ref[:, i : i + LANES])[:, :1] for i in range(0, Q_TILE, LANES)], axis=0)
        high = first + lax.broadcasted_iota(jnp.int32, pos.shape, 0)
        twice = lambda v: jnp.concatenate([v, v], axis=0)
        self.low, self.high = twice(high - pos), twice(high)
        self.q = stack_heads(q_ref[()])
        at = tile * Q_TILE
        ends = at + Q_TILE - 1
        lowest, highest = first - starts_ref[at], first + Q_TILE - 1 - starts_ref[ends]
        causal = (True, late, late | (cp == 1), late & (cp == 0))
        self.needed = [when & (chunk + K_TILE > lowest) for when, chunk in zip(causal, self.chunks)]
        self.free = [(chunk + K_TILE <= first + 1) & (highest <= chunk) for chunk in self.chunks]

    def visit(self, visit):
        for block, when in enumerate(self.needed):
            pl.when(when)(functools.partial(visit, block))

    def visit_scores(self, k_refs, visit):
        for block, (when, free) in enumerate(zip(self.needed, self.free)):
            (k,) = block_refs(block, k_refs)
            scores = lambda: lax.dot_general(self.q, k[()], NT, preferred_element_type=F32)
            pl.when(when & free)(lambda: visit(block, scores()))
            pl.when(when & jnp.logical_not(free))(lambda: visit(block, self.mask(scores(), block)))

    def mask(self, scores, block):
        at = self.chunks[block] + lax.broadcasted_iota(jnp.int32, (1, K_TILE), 1)
        return jnp.where((at >= self.low) & (at <= self.high), scores, NEG_BIG)


def block_refs(block, *pairs):
    rows = pl.ds((block % 2) * K_TILE, K_TILE)
    return [pair[block // 2].at[rows] for pair in pairs]


def attend_body(scale, starts_ref, q_ref, k_ref, v_ref, k2_ref, v2_ref, pos_ref, zeros_in, out_ref, lse_ref, grad_ref, s_ref, m_ref, l_ref, acc_ref, zero_ref, zero_sem):
    end_zeros = grid_zeros(grad_ref, zero_ref, zero_sem, "attend")
    tile = Tile(q_ref, pos_ref, starts_ref)
    power = scale * LOG2_E
    clear(m_ref, NEG_BIG)
    clear(l_ref)
    clear(acc_ref)

    def score(block, s):
        s_ref[block] = s
        m_ref[()] = jnp.maximum(m_ref[()], over_row(jnp.max, s))

    def exponent(block):
        e = jnp.exp2((s_ref[block] - m_ref[()]) * power)
        s_ref[block] = e
        l_ref[()] += over_row(jnp.sum, e)

    tile.visit_scores((k_ref, k2_ref), score)
    tile.visit(exponent)
    inverse = 1.0 / l_ref[()]

    def mix(block):
        (v,) = block_refs(block, (v_ref, v2_ref))
        prob = (s_ref[block] * inverse).astype(BF16)
        acc_ref[()] += jnp.dot(prob, v[()], preferred_element_type=F32)

    tile.visit(mix)
    out_ref[()] = unstack_heads(acc_ref[()].astype(BF16))
    lse_ref[()] = (m_ref[()] * power + jnp.log(l_ref[()]) * LOG2_E).reshape(lse_ref.shape)
    end_zeros()


def attention_specs(span, head_dim):
    tile = pl.BlockSpec((Q_TILE, 2 * head_dim), lambda h, t: (t, h))
    keys = pl.BlockSpec((span, head_dim), lambda h, t: (0, h))
    pos = pl.BlockSpec((1, Q_TILE), lambda h, t: (0, t))
    lse = pl.BlockSpec((1, 1, 2 * Q_TILE, 1), lambda h, t: (h, t, 0, 0))
    return tile, keys, pos, lse


def attention_buffers(heads):
    stacked = heads * Q_TILE
    return lambda c: pltpu.VMEM((stacked, c), F32), lambda dtype: pltpu.VMEM((4, stacked, K_TILE), dtype)


def attention_call(body, name, out_shape, in_specs, out_specs, scratch, gflops):
    aliases = {len(in_specs) - 1: len(out_specs) - 1}
    scratch = scratch + zero_scratch(out_shape[-1].shape[1])
    return local_call(body, name, out_shape, in_specs, out_specs, scratch, gflops, aliases, grid=(2, 4))


def attend(scale, starts, q, k, v, k2, v2, pos, grad):
    span = rows_in(q)
    heads = 2
    head_dim = cols_of(k) // heads
    tile, keys, pos_spec, lse = attention_specs(span, head_dim)
    stacked = heads * Q_TILE
    buf, probs = attention_buffers(heads)
    out_shape = [shape(*q.shape), jax.ShapeDtypeStruct((heads, span // Q_TILE, stacked, 1), F32), shape(*grad.shape, F32)]
    column = buf(1)
    scratch = [probs(F32), column, column, buf(head_dim)]
    call = attention_call(functools.partial(attend_body, scale), "attend", out_shape, [SMEM, tile] + [keys] * 4 + [pos_spec, HBM], [tile, lse, HBM], scratch, 14)
    return call(starts, q, k, v, k2, v2, pos, grad)


def attend_back_body(scale, starts_ref, q_ref, do_ref, lse_ref, k_ref, v_ref, k2_ref, v2_ref, pos_ref, zeros_in, dq_ref, dk_ref, dv_ref, dk2_ref, dv2_ref, grad_ref, p_ref, dp_ref, d_ref, acc_ref, zero_ref, zero_sem):
    end_zeros = grid_zeros(grad_ref, zero_ref, zero_sem, "attend_back")
    tile = Tile(q_ref, pos_ref, starts_ref)
    d_out = stack_heads(do_ref[()])
    lse = lse_ref[()].reshape(rows_in(d_out), 1)
    clear(d_ref)
    clear(acc_ref)

    @pl.when(pl.program_id(1) == 0)
    def _():
        for ref in (dk_ref, dv_ref, dk2_ref, dv2_ref):
            clear(ref)

    def first(block, s):
        (v,) = block_refs(block, (v_ref, v2_ref))
        p = jnp.exp2(s * (scale * LOG2_E) - lse)
        dp = lax.dot_general(d_out, v[()], NT, preferred_element_type=F32).astype(BF16)
        p_ref[block] = p
        dp_ref[block] = dp
        d_ref[()] += over_row(jnp.sum, p * dp.astype(F32))

    def second(block):
        k, dk, dv = block_refs(block, (k_ref, k2_ref), (dk_ref, dk2_ref), (dv_ref, dv2_ref))
        p = p_ref[block]
        ds = (p * (dp_ref[block].astype(F32) - d_ref[()]) * scale).astype(BF16)
        acc_ref[()] += jnp.dot(ds, k[()], preferred_element_type=F32)
        dk[()] += lax.dot_general(ds, tile.q, CONTRACT_FIRST, preferred_element_type=F32)
        dv[()] += lax.dot_general(p.astype(BF16), d_out, CONTRACT_FIRST, preferred_element_type=F32)

    tile.visit_scores((k_ref, k2_ref), first)
    tile.visit(second)
    dq_ref[()] = unstack_heads(acc_ref[()].astype(BF16))
    end_zeros()


def attend_back(scale, starts, q, d_out, lse, k, v, k2, v2, pos, grad):
    span = rows_in(q)
    heads = 2
    head_dim = cols_of(k) // heads
    tile, keys, pos_spec, lse_spec = attention_specs(span, head_dim)
    buf, probs = attention_buffers(heads)
    out_shape = [shape(*q.shape)] + [shape(*k.shape, F32)] * 4 + [shape(*grad.shape, F32)]
    in_specs = [SMEM, tile, tile, lse_spec] + [keys] * 4 + [pos_spec, HBM]
    call = attention_call(functools.partial(attend_back_body, scale), "attend_back", out_shape, in_specs, [tile] + [keys] * 4 + [HBM], [probs(F32), probs(BF16), buf(1), buf(head_dim)], 30)
    return call(starts, q, d_out, lse, k, v, k2, v2, pos, grad)


def remote(src, dst, send, recv, device):
    return pltpu.make_async_remote_copy(src_ref=src, dst_ref=dst, send_sem=send, recv_sem=recv, device_id=device, device_id_type=MESH_ID)


def flipped(bit, flip):
    return bit + flip - 2 * bit * flip


class Place:
    def __init__(self):
        self.tp = lax.axis_index("tp")
        self.cp = lax.axis_index("cp")
        self.x = lax.rem(self.tp, 2)
        self.y = lax.div(self.tp, 2)
        self.over_x = (self.chip(1, 0), self.cp)
        self.over_y = (self.chip(0, 1), self.cp)
        self.twin = (self.tp, 1 - self.cp)

    def chip(self, dx, dy):
        return 2 * flipped(self.y, dy) + flipped(self.x, dx)

    def meet(self):
        barrier = pltpu.get_barrier_semaphore()
        peers = (self.over_x, self.over_y, self.twin)
        for device in peers:
            pl.semaphore_signal(barrier, inc=1, device_id=device, device_id_type=MESH_ID)
        pl.semaphore_wait(barrier, len(peers))


class Total:
    def __init__(self, place, part, wide, mid, narrow, out, send, recv, source=None):
        self.source = source or part
        self.part, self.wide, self.mid, self.narrow, self.out = part, wide, mid, narrow, out
        self.send, self.recv = send, recv
        self.rows = rows_in(out) // STEPS
        self.half, self.quarter, self.eighth = (self.rows // n for n in (2, 4, 8))
        self.kinds = [(place.x, place.y, place.over_x, place.over_y), (place.y, place.x, place.over_y, place.over_x)]

    def _rows(self, step, kind):
        first, second = self.kinds[kind][:2]
        side = step * self.rows + kind * self.half + first * self.quarter
        return rows_at(side, self.quarter), rows_at(side + second * self.eighth, self.eighth)

    def _kept(self, kind, flip=0):
        return rows_at(kind * self.half + flipped(self.kinds[kind][0], flip) * self.quarter, self.quarter)

    def _eighth(self, kind, flip=0):
        return rows_at(flipped(self.kinds[kind][1], flip) * self.eighth, self.eighth)

    def _copy(self, step, kind, stage):
        side, mine = self._rows(step, kind)
        _, _, peer_first, peer_second = self.kinds[kind]
        src, dst, peer = (
            lambda: (self.source(step).at[self._kept(kind, 1)], self.wide.at[step, kind], peer_first),
            lambda: (self.mid.at[step, kind, self._eighth(kind, 1)], self.narrow.at[step, kind], peer_second),
            lambda: (self.out.at[mine], self.out.at[mine], peer_second),
            lambda: (self.out.at[side], self.out.at[side], peer_first),
        )[stage]()
        return remote(src, dst, self.send.at[step, kind, stage], self.recv.at[step, kind, stage], peer)

    def begin(self, step):
        for kind in BOTH:
            self._copy(step, kind, 0).start()

    def fold_wide(self, step):
        for kind in BOTH:
            self._copy(step, kind, 0).wait_recv()
            self.mid[step, kind] = self.part(step)[self._kept(kind), :] + self.wide[step, kind]
            self._copy(step, kind, 1).start()

    def fold_narrow(self, step):
        for kind in BOTH:
            self._copy(step, kind, 1).wait_recv()
            total = self.mid[step, kind, self._eighth(kind), :] + self.narrow[step, kind]
            self.out[self._rows(step, kind)[1], :] = total.astype(BF16)
            self._copy(step, kind, 2).start()

    def widen(self, step):
        for kind in BOTH:
            self._copy(step, kind, 2).wait_recv()
            self._copy(step, kind, 3).start()

    def finish(self, step):
        for kind in BOTH:
            self._copy(step, kind, 3).wait_recv()

    def sent(self, step, stages):
        for kind in BOTH:
            for stage in stages:
                self._copy(step, kind, stage).wait_send()


def sems(*dims):
    return DMA((*dims, 3))


def total_scratch(width, dtype, rows):
    stages = DMA((STEPS, 2, 4))
    part = lambda n: pltpu.VMEM((STEPS, 2, rows // n, width), dtype)
    return [part(4), part(4), part(8), stages, stages]


class Share:
    def __init__(self, place, sems, span):
        self.place, self.sems, self.first = place, sems, place.cp * span

    def pair(self, k, src, dst, start):
        here_sem, send, recv = (self.sems.at[k, i] for i in range(3))
        at = dst.at[rows_at(self.first + start, rows_in(src))]
        return pltpu.make_async_copy(src, at, here_sem), remote(src, at, send, recv, self.place.twin)

    def begin(self, *numbered):
        for copy in self.pair(*numbered):
            copy.start()

    def sent(self, *numbered):
        here, there = self.pair(*numbered)
        here.wait()
        there.wait_send()

    def got(self, k, src, dst, start):
        at = dst.at[rows_at(self.first + start, rows_in(src))]
        remote(src, at, *(self.sems.at[k, i] for i in (1, 2)), self.place.twin).wait_recv()


class Loads:
    def __init__(self, sems, *names):
        self.sems, self.names = sems, list(names)

    def _copies(self, moves):
        self.names += [name for name in moves if name not in self.names]
        return [pltpu.make_async_copy(src, dst, self.sems.at[self.names.index(name)]) for name, (src, dst) in moves.items()]

    def start(self, **moves):
        for copy in self._copies(moves):
            copy.start()
        return lambda: self.wait(**moves)

    def wait(self, **moves):
        for copy in self._copies(moves):
            copy.wait()


def steps(visit):
    def body(step, carry):
        visit(step)
        return carry

    lax.fori_loop(0, STEPS, body, 0)


def rope(v, cosine, sine):
    wide = cols_of(cosine)
    heads = []
    for h in range(cols_of(v) // wide):
        part = v[:, h * wide : (h + 1) * wide]
        turned = jnp.concatenate([part[:, wide // 2 :], part[:, : wide // 2]], axis=1)
        heads.append(part * cosine + turned * sine)
    return jnp.concatenate(heads, axis=1)


def each(count, size, visit):
    def body(i, carry):
        visit(pl.multiple_of(i * size, size))
        return carry

    lax.fori_loop(0, count // size, body, 0)


def col_loop(cols, tile, visit):
    each(cols, tile, lambda start: visit(pl.ds(start, tile)))


def dot_nt(a, b):
    return lax.dot_general(a, b, NT, preferred_element_type=F32)


def dot(a, b):
    return jnp.dot(a, b, preferred_element_type=F32)


def as_row(gain):
    return gain[()].astype(F32)[None, :]


def norm_block(feats):
    inverse = lax.rsqrt(over_row(jnp.mean, feats * feats) + NORM_EPS)
    return feats * inverse, inverse


def norm_back(d_act, gain, normed, inverse):
    d_normed = d_act * gain
    return inverse * (d_normed - normed * over_row(jnp.mean, d_normed * normed))


def remote_call(body, collective_id, name, out_shape, in_places, out_places, scratch, gflops):
    return pl.pallas_call(
        body,
        out_shape=out_shape,
        in_specs=specs(in_places),
        out_specs=specs(out_places),
        scratch_shapes=scratch,
        compiler_params=pltpu.CompilerParams(collective_id=collective_id, has_side_effects=True, vmem_limit_bytes=REMOTE_VMEM),
        cost_estimate=cost(gflops, 60),
        name=name,
    )


def join_columns(parts, whole):
    start, moves = 0, {}
    for i, part in enumerate(parts):
        moves[f"join{i}"] = (part, whole.at[:, pl.ds(start, cols_of(part))])
        start += cols_of(part)
    return moves


def order_ids(cp, ids, ids_got, keys, tall, rank, keys_out):
    span = cols_of(ids)
    chunks = rows_in(keys)
    lane = lax.broadcasted_iota(jnp.int32, (1, LANES), 1)
    for core, src in ((cp, ids), (1 - cp, ids_got)):
        for c in range(span // LANES):
            start = c * LANES
            token = core * span + start + lane
            keys[core * (chunks // 2) + c] = lax.shift_left(src[:, start : start + LANES], KEY_BITS) + token

    def count(a, carry):
        mine = as_column(keys[a])
        tall[a] = mine
        rank[a] = over_row(jnp.sum, sum((keys[b] < mine).astype(F32) for b in range(chunks)))
        return carry

    def place(c, carry):
        goal = (c * LANES + lane).astype(F32)
        keys_out[rows_at(c * LANES, LANES, LANES)] = over_column(sum(jnp.where(rank[a] == goal, tall[a], 0) for a in range(chunks)))[0]
        return carry

    lax.fori_loop(0, chunks, count, 0)
    lax.fori_loop(0, chunks, place, 0)
    keys_out[pl.ds(chunks * LANES, LANES)] = jnp.full((LANES,), jnp.iinfo(jnp.int32).max, jnp.int32)


def enter_body(picked_in, wq_in, wk_in, wv_in, gain, pos, inv_freq, ids, dy_in, wd_in, x_rows, q_out, k_out, v_out, cosine, sine, keys_out, dh_out, k2_out, v2_out, act_all, dy_all, wide, mid, narrow, send, recv, picked, x_out, act, dy, wd, dh, w_all, ids_got, keys, tall, rank, pair_sems, share_sems, load_sems, ids_sems):
    place = Place()
    place.meet()
    span = rows_in(x_out)
    rows = span // STEPS
    chunk = lambda step: rows_at(step * rows, rows)
    total = Total(place, lambda step: picked.at[chunk(step)], wide, mid, narrow, x_out, send, recv, lambda step: picked_in.at[chunk(step)])
    share = Share(place, share_sems, span)
    loads = Loads(load_sems)
    steps(total.begin)
    ids_swap = remote(ids, ids_got, *(ids_sems.at[end] for end in BOTH), place.twin)
    ids_swap.start()
    loaded = loads.start(picked=(picked_in, picked), dy=(dy_in, dy), wd=(wd_in, wd))
    projection = loads.start(**join_columns((wq_in, wk_in, wv_in), w_all))
    kw = cols_of(k_out)
    qw = cols_of(q_out)

    def back(step):
        here = chunk(step)

        def tile(cols):
            dh[here, cols] = dot_nt(dy[here, :], wd[cols, :]).astype(BF16)

        col_loop(rows_in(wd), WIDE_TILE, tile)
        total.fold_wide(step)

    def pairs(step):
        return [remote(src.at[chunk(step)], dst.at[chunk(step)], *(pair_sems.at[step, i, end] for end in BOTH), place.twin) for i, (src, dst) in enumerate(((k_out, k2_out), (v_out, v2_out)))]

    x_kept = lambda step: dict(x=(x_out.at[chunk(step)], x_rows.at[chunk(step)]))
    act_share = lambda step: (1 + step, act.at[chunk(step)], act_all, step * rows)

    def project(step):
        total.finish(step)
        here = chunk(step)
        pl.when(step >= 1)(lambda: loads.wait(**x_kept(step - 1)))
        loads.start(**x_kept(step))

        def norm(start):
            at = rows_at(step * rows + start, ROW_BLOCK)
            normed, _ = norm_block(x_out[at, :].astype(F32))
            act[at, :] = (normed * as_row(gain)).astype(BF16)

        each(rows, ROW_BLOCK, norm)
        share.begin(*act_share(step))
        c, s = cosine[here, :], sine[here, :]
        out = dot(act[here, :], w_all[()])
        q_out[here, :] = rope(out[:, :qw], c, s).astype(BF16)
        k_out[here, :] = rope(out[:, qw : qw + kw], c, s).astype(BF16)
        v_out[here, :] = out[:, qw + kw :].astype(BF16)
        for copy in pairs(step):
            copy.start()

    def angles(start):
        at = pl.ds(start, LANES)
        angle = as_column(pos[:, at])[:, : cols_of(inv_freq)].astype(F32) * inv_freq[()]
        c, s = jnp.cos(angle), jnp.sin(angle)
        cosine[at, :] = jnp.concatenate([c, c], axis=1)
        sine[at, :] = jnp.concatenate([-s, s], axis=1)

    loaded()
    dy_share = (0, dy, dy_all, 0)
    share.begin(*dy_share)
    each(span, LANES, angles)
    steps(back)
    stored = loads.start(dh=(dh, dh_out))
    ids_swap.wait()
    order_ids(place.cp, ids, ids_got, keys, tall, rank, keys_out)
    steps(total.fold_narrow)
    steps(total.widen)
    projection()
    steps(project)

    def close(step):
        total.sent(step, range(4))
        share.sent(*act_share(step))
        share.got(*act_share(step))
        for copy in pairs(step):
            copy.wait()

    steps(close)
    share.sent(*dy_share)
    share.got(*dy_share)
    loads.wait(**x_kept(STEPS - 1))
    stored()


def enter(picked, wq, wk, wv, gain, pos, inv_freq, ids, dy, wd):
    span, width = picked.shape
    key = shape(span, cols_of(wk))
    angles = shape(span, 2 * cols_of(inv_freq), F32)
    all_rows = shape(2 * span, width)
    chunks = 2 * span // LANES
    int_buf = lambda *dims: pltpu.VMEM(dims, jnp.int32)
    big = pltpu.VMEM((span, width), BF16)
    out_shape = [shape(span, width), shape(span, cols_of(wq)), key, key, angles, angles, jax.ShapeDtypeStruct(((chunks + SUBLANES) * LANES,), jnp.int32), shape(span, rows_in(wd)), key, key, all_rows, all_rows]
    scratch = total_scratch(width, BF16, span // STEPS) + [big, big, big, big, pltpu.VMEM(wd.shape, BF16), pltpu.VMEM((span, rows_in(wd)), BF16), pltpu.VMEM((width, cols_of(wq) + 2 * cols_of(wk)), BF16)]
    scratch += [int_buf(1, span), int_buf(chunks, 1, LANES), int_buf(chunks, LANES, LANES), pltpu.VMEM((chunks, LANES, 1), F32)]
    scratch += [DMA((STEPS, 2, 2)), sems(STEPS + 1), DMA((8,)), DMA((2,))]
    call = remote_call(enter_body, 1, "enter", out_shape, "hhhhvvvvhh", "hvvvvvvhhhhh", scratch, 80)
    return call(picked, wq, wk, wv, gain, pos, inv_freq, ids, dy, wd)


def middle_body(att, wo_own, wo_1, wo_2, wo_3, x_in, wg_in, wu_in, wd_in, dh_in, dy_in, gain, h_out, keep_x, send_x, keep_y, send_y, b_all, hidden_all, dgate_all, dup_all, att_all, drb_all, dr_out, datt_out, dgain_out,
                wide, mid, narrow, send, recv, wo, wg, wu, att_full, part_buf, d_b, h, row_in, dh, b, hid, dgt, dup, att_send, att_recv, wo_sems, load_sems, share_sems):
    place = Place()
    span, width = x_in.shape
    rows = span // STEPS
    half = rows // 2
    cols = cols_of(att)
    ffn = cols_of(wg)
    loads = Loads(load_sems, "att", "wo", "wg", "wu", "rows", "dh", "h_out", "h_in", "hid", "dr", "y")
    chunk = lambda step: rows_at(step * rows, rows)
    by_chip = lambda tp: rows_at(tp * cols, cols, 128)

    mine = loads.start(att=(att, att_full.at[:, by_chip(place.tp)]), wo=(wo_own, wo.at[by_chip(place.tp)]))
    place.meet()

    x_tp, y_tp = place.over_x[0], place.over_y[0]

    def att_copy(step, kind, hop):
        at = rows_at(step * rows + kind * half, half)
        first, second = ((place.over_y, place.over_x), (place.over_x, place.over_y))[kind]
        relay = hop == 2
        dst = att_full.at[at, by_chip(first[0] if relay else place.tp)]
        return remote(dst if relay else att.at[at], dst, att_send.at[step, kind, hop], att_recv.at[step, kind, hop], second if hop else first)

    def att_begin(step):
        for hop in BOTH:
            for kind in BOTH:
                att_copy(step, kind, hop).start()

    def att_forward(step):
        for kind in BOTH:
            att_copy(step, kind, 0).wait_recv()
            att_copy(step, kind, 2).start()

    att_begin(0)
    part = rows_in(wo_1)
    arrivals = []
    near = jnp.where(place.cp == 0, y_tp, x_tp)
    chips = (near, x_tp + y_tp - near, place.chip(1, 1))
    for i, (src, chip) in enumerate(zip((wo_1, wo_2, wo_3), chips)):
        at = wo.at[rows_at((2 * chip + place.cp) * part, part, 128)]
        here_sem, send_sem, recv_sem = (wo_sems.at[i, end] for end in range(3))
        for copy in (pltpu.make_async_copy(src, at, here_sem), remote(src, at, send_sem, recv_sem, place.twin)):
            copy.start()
            arrivals.append(copy)
    att_begin(1)
    weights = loads.start(wg=(wg_in, wg), wu=(wu_in, wu))

    share = Share(place, share_sems, span)
    att_share = (0, att, att_all, 0)
    share.begin(*att_share)
    total = Total(place, lambda step: part_buf.at[step], wide, mid, narrow, d_b, send, recv)

    def numbered(i, src, dst, step):
        return 1 + len(shares) * step + i, src, dst, step * rows

    shares = ((b, b_all), (hid, hidden_all), (dgt, dgate_all), (dup, dup_all))
    forward_shares = list(enumerate(shares))
    fetched = lambda step: dict(rows=(x_in.at[chunk(step)], row_in), dh=(dh_in.at[chunk(step)], dh))
    h_kept = lambda step: dict(h_out=(h, h_out.at[chunk(step)]))

    def close(step):
        loads.wait(**h_kept(step))
        for i, pair in forward_shares:
            share.sent(*numbered(i, *pair, step))

    def forward(step):
        pl.when(step >= 1)(lambda: close(step - 1))
        loads.wait(**fetched(step))
        for kind in BOTH:
            for hop in (1, 2):
                att_copy(step, kind, hop).wait_recv()

        def residual(c):
            h[:, c] = row_in[:, c].astype(F32) + dot(att_full[chunk(step), :], wo[:, c])

        col_loop(width, BIG_TILE, residual)
        loads.start(**h_kept(step))

        def norm(start):
            at = pl.ds(start, ROW_BLOCK)
            normed, _ = norm_block(h[at, :])
            b[at, :] = (normed * as_row(gain)).astype(BF16)

        each(rows, ROW_BLOCK, norm)
        share.begin(*numbered(0, b, b_all, step))
        pl.when(step == 0)(weights)

        def hidden(c):
            gate = dot(b[()], wg[:, c])
            up = dot(b[()], wu[:, c])
            sig = 1.0 / (1.0 + jnp.exp(-gate))
            d_hid = dh[:, c].astype(F32)
            act = gate * sig
            hid[:, c] = (act * up).astype(BF16)
            dgt[:, c] = (d_hid * up * sig * (1.0 + gate * (1.0 - sig))).astype(BF16)
            dup[:, c] = (d_hid * act).astype(BF16)

        col_loop(ffn, WIDE_TILE, hidden)
        for i, pair in forward_shares[1:]:
            share.begin(*numbered(i, *pair, step))
        pl.when(step == 0)(lambda: att_forward(2))

        @pl.when(step + 1 < STEPS)
        def _():
            loads.start(**fetched(step + 1))

        def back(c):
            part_buf[step, :, c] = dot_nt(dgt[()], wg[c, :]) + dot_nt(dup[()], wu[c, :])

        col_loop(width, WIDE_TILE, back)
        total.begin(step)
        pl.when(step == 0)(lambda: att_forward(3))
        pl.when(step >= 2)(lambda: total.fold_wide(step - 2))

    loads.start(**fetched(0))
    att_forward(0)
    for step in range(2, STEPS):
        att_begin(step)
    mine()
    for copy in arrivals:
        copy.wait()
    att_forward(1)
    steps(forward)
    clear(dgain_out)
    close(STEPS - 1)
    wd = wg
    weights = loads.start(wg=(wd_in, wd))
    d_r, y_buf = part_buf.at[0], part_buf.at[1]

    h_back = lambda step: dict(h_in=(h_out.at[chunk(step)], h))
    hidden_back = lambda step: dict(hid=(hidden_all.at[rows_at(place.cp * span + step * rows, rows)], hid))
    dy_back = lambda step: dict(rows=(dy_in.at[chunk(step)], row_in))
    y_kept = dict(y=(y_buf, keep_x))
    for step in BOTH:
        total.sent(step, (0,))
    loads.start(**h_back(0), **hidden_back(0))

    def output(step):
        pl.when(step < 2)(lambda: total.fold_wide(step + 2))
        loads.wait(**h_back(step), **hidden_back(step))
        pl.when(step == 0)(weights)
        pl.when(step >= 1)(lambda: loads.wait(**y_kept))
        over_x_first = step < 2
        first = jnp.where(over_x_first, place.x, place.y)
        second = place.x + place.y - first
        kept = first == lax.rem(step, 2)
        row = lax.broadcasted_iota(jnp.int32, (rows, 1), 0)
        owner = kept & (lax.div(row, half) == second)

        def tile(c):
            y_buf[:, c] = dot(hid[()], wd[:, c]) + jnp.where(owner, h[:, c], 0.0)

        col_loop(width, BIG_TILE, tile)
        for side_first, keep, send_to in ((over_x_first, keep_x, send_x), (jnp.logical_not(over_x_first), keep_y, send_y)):
            for chosen, dst in ((kept, keep), (jnp.logical_not(kept), send_to)):

                @pl.when(side_first & chosen)
                def _():
                    loads.start(y=(y_buf, dst))

        @pl.when(step + 1 < STEPS)
        def _():
            loads.start(**h_back(step + 1), **hidden_back(step + 1))

        total.fold_narrow(step)
        pl.when(step >= 2)(lambda: total.widen(step - 2))

    steps(output)
    loads.start(**h_back(0), **dy_back(0))
    kept_rows = lambda step: dict(dr=(d_r, dr_out.at[chunk(step)]))

    def resid_share(step, part):
        return 1 + len(shares) * STEPS + 2 * step + part, b.at[rows_at(part * half, half)], drb_all, step * rows + part * half

    def resid_sent(step):
        loads.wait(**kept_rows(step))
        for part in BOTH:
            share.sent(*resid_share(step, part))

    def resid(step):
        pl.when(step < 2)(lambda: total.widen(step + 2))
        total.finish(step)
        loads.wait(**h_back(step), **dy_back(step))
        pl.when(step >= 1)(lambda: resid_sent(step - 1))

        for part in BOTH:

            def grad(start):
                start = part * half + start
                at = rows_at(start, ROW_BLOCK)
                normed, inverse = norm_block(h[at, :])
                d_act = d_b[rows_at(step * rows + start, ROW_BLOCK), :].astype(F32)
                dgain_out[()] += over_column(d_act * normed)
                out = row_in[at, :].astype(F32) + norm_back(d_act, as_row(gain), normed, inverse)
                d_r[at, :] = out
                b[at, :] = out.astype(BF16)

            each(half, ROW_BLOCK, grad)
            share.begin(*resid_share(step, part))

        @pl.when(step + 1 < STEPS)
        def _():
            loads.start(**h_back(step + 1), **dy_back(step + 1))

        loads.start(**kept_rows(step))
        datt_out[chunk(step), :] = dot_nt(b[()], wo[by_chip(place.tp), :]).astype(BF16)

    steps(resid)
    loads.wait(**y_kept)
    resid_sent(STEPS - 1)
    share.sent(*att_share)
    share.got(*att_share)

    def finish(step):
        total.sent(step, range(1, 4))
        pl.when(step >= 2)(lambda: total.sent(step, (0,)))
        for kind in BOTH:
            for hop in range(3):
                att_copy(step, kind, hop).wait_send()
        for i, pair in forward_shares:
            share.got(*numbered(i, *pair, step))
        for part in BOTH:
            share.got(*resid_share(step, part))

    steps(finish)


def middle(att, wo_pieces, x, wg, wu, wd, d_hidden, dy, gain):
    span, width = x.shape
    rows = span // STEPS
    ffn = cols_of(wg)
    cols = cols_of(att)
    full = shape(span, width, F32)
    both = shape(2 * span, ffn)
    out_shape = [full] + [shape(rows, width, F32)] * 4 + [shape(2 * span, width), both, both, both, shape(2 * span, cols), shape(2 * span, width), full, shape(span, cols), shape(1, width, F32)]
    buf = lambda r, c, dtype=BF16: pltpu.VMEM((r, c), dtype)
    scratch = total_scratch(width, F32, rows)
    scratch += [buf(width, width), buf(width, ffn), buf(width, ffn), buf(span, width), pltpu.VMEM((STEPS, rows, width), F32), buf(span, width), buf(rows, width, F32)]
    scratch += [buf(rows, c) for c in (width, ffn, width, ffn, ffn, ffn)]
    scratch += [sems(STEPS, 2), sems(STEPS, 2), sems(3), DMA((11,)), sems(1 + 6 * STEPS)]
    call = remote_call(middle_body, 2, "middle", out_shape, "vhhhhhhhhhhv", "hhhhhhhhhhhhvv", scratch, 120)
    return call(att, *wo_pieces, x, wg, wu, wd, d_hidden, dy, gain)


def leave_body(dq_in, dk_in, dv_in, dk2_in, dv2_in, cosine, sine, wq_in, wk_in, wv_in, x_in, dr_in, gain, dgain_b, b_all, dgate_all, dup_all, hidden_all, dy_all, att_all, drb_all, act_all, d_all, dx_all, gain_a_out, gain_b_out, grad_gate, grad_up, grad_down, grad_out, grad_q, grad_k, grad_v,
               wide, mid, narrow, send, recv, part_buf, d_a, dk_got, dv_got, d_qkv, w_all, xs, drs, dxs, gain_got, left, right, result, pair_sems, load_sems, share_sems, left_sems, right_sems, result_sems, result_arrivals):
    place = Place()
    place.meet()
    span, width = x_in.shape
    rows = span // STEPS
    chunk = lambda step: rows_at(step * rows, rows)
    swap = lambda i, src, dst: remote(src, dst, *(pair_sems.at[i, end] for end in BOTH), place.twin)
    pairs = lambda step: [swap(2 * step + i, src.at[chunk(step)], dst.at[chunk(step)]) for i, (src, dst) in enumerate(((dk2_in, dk_got), (dv2_in, dv_got)))]
    for step in range(STEPS):
        for copy in pairs(step):
            copy.start()
    qw = cols_of(dq_in)
    kw = cols_of(dk_in)
    share = Share(place, share_sems, span)
    loads = Loads(load_sems)
    total = Total(place, lambda step: part_buf.at[step], wide, mid, narrow, d_a, send, recv)

    def partial(step):
        here = chunk(step)
        c, s = cosine[here, :], -sine[here, :]
        for copy in pairs(step):
            copy.wait()
        d_qkv[here, :qw] = rope(dq_in[here, :].astype(F32), c, s).astype(BF16)
        dk_sum = (dk_in[here, :] + dk_got[here, :]).astype(BF16).astype(F32)
        d_qkv[here, qw : qw + kw] = rope(dk_sum, c, s).astype(BF16)
        d_qkv[here, qw + kw :] = (dv_in[here, :] + dv_got[here, :]).astype(BF16)

        def tile(n):
            part_buf[step, :, n] = dot_nt(d_qkv[here, :], w_all[n, :])

        col_loop(width, BIG_TILE, tile)
        total.begin(step)

    rows_back = lambda step: dict(x=(x_in.at[chunk(step)], xs), dr=(dr_in.at[chunk(step)], drs))

    clear(gain_a_out)

    def dx_share(step, part):
        start = part * part_rows
        return 1 + 2 * step + part, dxs.at[rows_at(start, part_rows)], dx_all, step * rows + start

    part_rows = rows // 2

    def grad_x(step):
        for part in BOTH:

            def grad(start):
                start = part * part_rows + start
                at = rows_at(start, ROW_BLOCK)
                normed, inverse = norm_block(xs[at, :].astype(F32))
                d_act = d_a[rows_at(step * rows + start, ROW_BLOCK), :].astype(F32)
                gain_a_out[()] += over_column(d_act * normed)
                dxs[at, :] = drs[at, :] + norm_back(d_act, as_row(gain), normed, inverse)

            pl.when(step >= 1)(lambda: share.sent(*dx_share(step - 1, part)))
            each(part_rows, ROW_BLOCK, grad)
            share.begin(*dx_share(step, part))

    _, _, narrow_cols = left.shape
    _, _, wide_cols = right.shape
    lefts, rights = Ring(left, left_sems, True), Ring(right, right_sems, True)
    sides, per_core = width // wide_cols, width // narrow_cols // 2
    whole = (grad_gate, grad_up, grad_down, grad_out)
    ffn_blocks = (len(whole) - 1) * sides
    ffn_tiles = ffn_blocks * per_core
    tiles = ffn_tiles + 1 + per_core
    block_of = lambda t: jnp.where(t < ffn_tiles, lax.div(t, per_core), jnp.minimum(t - ffn_tiles, 1) + ffn_blocks)
    row_of = lambda t: place.cp * per_core + jnp.where(t < ffn_tiles, lax.rem(t, per_core), jnp.maximum(t - ffn_tiles - 1, 0))
    at_left = lambda t: rows_at(row_of(t) * narrow_cols, narrow_cols, TILE)
    at_right = lambda j: rows_at(jnp.where(j < ffn_blocks, lax.rem(j, sides), place.cp) * wide_cols, wide_cols, TILE)
    kind_of = lambda j: jnp.where(j < ffn_blocks, lax.div(j, sides), len(whole) - 1 + j - ffn_blocks)
    left_start = lambda t: lefts.start(t, kind_of(block_of(t)), [ref.at[:, at_left(t)] for ref in (b_all, b_all, hidden_all)] + [att_all, act_all.at[:, at_left(t)]])
    right_start = lambda j: rights.start(j, kind_of(j), [ref.at[:, at_right(j)] for ref in (dgate_all, dup_all, dy_all, drb_all)] + [d_all])

    def to_twin(t, src, dst):
        return remote(src, dst, result_sems.at[lefts.slot(t), 1], result_arrivals.at[t], place.twin)

    def stored(t):
        done = result.at[lefts.slot(t)]
        pltpu.make_async_copy(done, done, result_sems.at[lefts.slot(t), 0]).wait()
        to_twin(t, done, done).wait_send()

    def store(t):
        slot = lefts.slot(t)
        j = block_of(t)

        def put(cols, dst):
            src = result.at[slot, :, cols]
            pltpu.make_async_copy(src, dst, result_sems.at[slot, 0]).start()
            to_twin(t, src, dst).start()

        everything = pl.ds(0, wide_cols)
        for k, ref in enumerate(whole):
            at = at_left(t) if ref is not grad_out else pl.ds(0, narrow_cols)
            pl.when(kind_of(j) == k)(lambda: put(everything, ref.at[at, at_right(j)]))

        @pl.when(j == ffn_blocks + 1)
        def _():
            put(pl.ds(0, qw), grad_q.at[at_left(t)])
            put(pl.ds(qw, kw), grad_k.at[at_left(t)])
            put(pl.ds(qw + kw, kw), grad_v.at[at_left(t)])

    def tile_step(t, carry):
        j = block_of(t)
        pl.when(t + 1 < tiles)(lambda: left_start(t + 1))

        @pl.when(jnp.where(t < ffn_tiles, lax.rem(t, per_core) == 0, t <= ffn_tiles + 1))
        def _():
            pl.when(j < ffn_blocks)(lambda: right_start(j + 1))
            rights.wait(j, d_all)

        lefts.wait(t, att_all)
        pl.when(t >= 2)(lambda: stored(t))
        slot = lefts.slot(t)
        result[slot] = lax.dot_general(left[slot], right[rights.slot(j)], CONTRACT_FIRST, preferred_element_type=F32)
        store(t)
        return carry

    left_start(jnp.int32(0))
    right_start(jnp.int32(0))
    weights = loads.start(**join_columns((wq_in, wk_in, wv_in), w_all))
    loads.start(**rows_back(0))
    weights()
    steps(partial)
    d_here, d_there = share.pair(0, d_qkv, d_all, 0)
    d_here.start()
    d_there.start()

    stages = (total.fold_wide, total.fold_narrow, total.widen)
    waits = len(stages) * STEPS
    portion = ffn_tiles // STEPS
    tiles_until = lambda p: jnp.where(p < STEPS, portion * (p + 1), jnp.where(p < 2 * STEPS - 1, ffn_tiles, jnp.where(p < waits - 1, ffn_tiles + 1, tiles)))

    def wait_step(p, carry):
        @pl.when(p == waits - 1)
        def _():
            d_here.wait()
            d_there.wait_recv()
            right_start(jnp.int32(ffn_blocks + 1))

        lax.fori_loop(jnp.where(p == 0, 0, tiles_until(p - 1)), tiles_until(p), tile_step, 0)
        for k, stage in enumerate(stages):
            pl.when(lax.div(p, STEPS) == k)(lambda: stage(lax.rem(p, STEPS)))
        return carry

    lax.fori_loop(0, waits, wait_step, 0)
    def last_stage(step):
        loads.wait(**rows_back(step))
        total.finish(step)
        grad_x(step)

        @pl.when(step + 1 < STEPS)
        def _():
            loads.start(**rows_back(step + 1))

    steps(last_stage)
    gains = ((gain_a_out, gain_a_out), (dgain_b, gain_b_out))
    swaps = [swap(2 * STEPS + i, mine, gain_got.at[i]) for i, (mine, _) in enumerate(gains)]
    for copy in swaps:
        copy.start()
    for copy in swaps:
        copy.wait()
    for i, (mine, out) in enumerate(gains):
        out[()] = mine[()] + gain_got[i]
    for part in BOTH:
        share.sent(*dx_share(STEPS - 1, part))
    d_there.wait_send()
    for t in range(tiles - 2, tiles):
        stored(t)
    done = result.at[0]
    for t in range(tiles):
        to_twin(t, done, done).wait_recv()

    def close(step):
        total.sent(step, range(4))
        for part in BOTH:
            share.got(*dx_share(step, part))

    steps(close)


def leave(dq, dk, dv, dk2, dv2, cosine, sine, wq, wk, wv, x, d_resid, gain, dgain_b, *products):
    span, width = x.shape
    rows = span // STEPS
    kw = cols_of(wk)
    qw = cols_of(wq)
    cols = qw + 2 * kw
    ffn = products[1].shape[1]
    buf = lambda r, c, dtype=F32: pltpu.VMEM((r, c), dtype)
    gain_grad = shape(1, width, F32)
    out_shape = [shape(2 * span, cols), shape(2 * span, width, F32), gain_grad, gain_grad]
    out_shape += [shape(*dims, F32) for dims in ((width, ffn), (width, ffn), (ffn, width), (qw, width), wq.shape, wk.shape, wv.shape)]
    twice = lambda r, c, dtype: pltpu.VMEM((2, r, c), dtype)
    scratch = total_scratch(width, F32, rows) + [pltpu.VMEM((STEPS, rows, width), F32), buf(span, width, BF16), buf(span, kw), buf(span, kw), buf(span, cols, BF16), buf(width, cols, BF16)]
    scratch += [buf(rows, width, BF16), buf(rows, width), buf(rows, width), pltpu.VMEM((2, 1, width), F32)]
    scratch += [twice(2 * span, WIDE_TILE, BF16), twice(2 * span, BIG_TILE, BF16), twice(WIDE_TILE, BIG_TILE, F32)]
    ring = DMA((2,))
    scratch += [DMA((2 * STEPS + 2, 2)), DMA((5,)), sems(1 + 2 * STEPS), ring, ring, DMA((2, 2)), DMA((MAX_TILES,))]
    call = remote_call(leave_body, 3, "leave", out_shape, "vvvhhvvhhhhhvvhhhhhhhh", "hhvvhhhhhhh", scratch, 1)
    return call(dq, dk, dv, dk2, dv2, cosine, sine, wq, wk, wv, x, d_resid, gain, dgain_b, *products)


def side(v, bit):
    half = rows_in(v) // 2
    return lax.dynamic_slice_in_dim(v, bit * half, half, 0)


def join(own, other, bit):
    return jnp.where(bit == 0, jnp.concatenate([own, other]), jnp.concatenate([other, own]))


def solution(mesh):
    def device_step(tokens, pos, doc_id, dy, table, w_q, w_k, w_v, w_o, w_gate, w_up, w_down, gain_one, gain_two, inv_freq):
        span = rows_in(tokens)
        rows, width = table.shape
        scale = (2 * rows_in(inv_freq)) ** -0.5
        tp = lax.axis_index("tp")
        cp = lax.axis_index("cp")
        starts = pos
        inv_freq, pos, ids = (v[None, :] for v in (inv_freq, pos, tokens))
        base = tp * rows

        wo_half = side(w_o, cp)
        wo_1 = swap_core(wo_half, 0)
        picked, grad = pick_rows(tokens, table, base)
        x, query, key, value, cosine, sine, keys, d_hidden, key2, value2, act_a_all, dy_all = enter(picked, w_q, w_k, w_v, gain_one, pos, inv_freq, ids, dy, w_down)
        wo_1, wo_half, query = lax.optimization_barrier((wo_1, wo_half, query))
        wo_pieces = (w_o, wo_1, swap_core(wo_half, 1), swap_core(wo_1, 1))
        att, lse, grad = attend(scale, starts, query, key, value, key2, value2, pos, grad)
        keep_x, send_x, keep_y, send_y, act_b_all, hidden_all, d_gate_all, d_up_all, att_all, d_resid_all, d_resid, d_att, d_gain_b = middle(att, wo_pieces, x, w_gate, w_up, w_down, d_hidden, dy, gain_two)[1:]

        x_bit, y_bit = tp % 2, tp // 2
        ways = ((keep_x, swap_x, x_bit, swap_y, y_bit), (keep_y, swap_y, y_bit, swap_x, x_bit))
        y_wide = [swap_x(send_x), swap_y(send_y)]
        d_query, d_key, d_value, d_key2, d_value2, grad = attend_back(scale, starts, query, d_att, lse, key, value, key2, value2, pos, grad)

        d_x_all, gain_1, gain_2, grad_gate, grad_up, grad_down, *grads = leave(d_query, d_key, d_value, d_key2, d_value2, cosine, sine, w_q, w_k, w_v, x, d_resid, gain_one, d_gain_b, act_b_all, d_gate_all, d_up_all, hidden_all, dy_all, att_all, d_resid_all, act_a_all)[1:]
        y_wide, d_x_all = lax.optimization_barrier((y_wide, d_x_all))
        halves = lambda bit_2, keep, wide, flip: side(keep, flipped(bit_2, flip)) + side(wide, flipped(bit_2, flip))
        y_narrow = [swap_2(halves(bit_2, keep, wide, 1)) for (keep, _, _, swap_2, bit_2), wide in zip(ways, y_wide)]
        y_wide, grad_gate = lax.optimization_barrier((y_wide, grad_gate))
        grad_gate, grad_out, *grads = move(grad_gate, *grads)
        y_narrow, grad_gate = lax.optimization_barrier((y_narrow, grad_gate))
        y_own = [(halves(bit_2, keep, wide, 0) + narrow).astype(BF16) for (keep, _, _, _, bit_2), wide, narrow in zip(ways, y_wide, y_narrow)]
        y_pair = [join(own, swap_2(own), bit_2) for (_, _, _, swap_2, bit_2), own in zip(ways, y_own)]
        y_own, grad_down = lax.optimization_barrier((y_own, grad_down))
        (grad_down,) = move(grad_down)
        y_pair, grad_down = lax.optimization_barrier((y_pair, grad_down))
        y_far = [swap_1(pair) for (_, swap_1, _, _, _), pair in zip(ways, y_pair)]
        y_pair, d_x_all = lax.optimization_barrier((y_pair, d_x_all))
        grad_table, grad_up = put_rows(keys, d_x_all, grad, (grad_up,))
        y_rows = [jnp.where(bit_1 == k, pair, far) for (_, _, bit_1, _, _), pair, far in zip(ways, y_pair, y_far) for k in BOTH]
        return (jnp.concatenate(y_rows), grad_table, *grads, grad_out, grad_gate, grad_up, grad_down, gain_1[0], gain_2[0])

    col_spec = P(None, "tp")
    row_spec = P("tp", None)
    tok_spec = P("cp")
    rep_spec = P(None)
    in_specs = (tok_spec, tok_spec, tok_spec, P("cp", None), row_spec, col_spec, col_spec, col_spec, row_spec, col_spec, col_spec, row_spec, rep_spec, rep_spec, rep_spec)
    out_specs = (P("cp", None), row_spec, col_spec, col_spec, col_spec, row_spec, col_spec, col_spec, row_spec, rep_spec, rep_spec)
    return jax.shard_map(device_step, mesh=mesh, in_specs=in_specs, out_specs=out_specs, check_vma=False)
```

```python
import functools

import jax
import jax.numpy as jnp
from jax import lax
from jax.experimental import pallas as pl
from jax.experimental.pallas import tpu as pltpu
from jax.sharding import PartitionSpec as P

NORM_EPS = 1e-5
NEG_BIG = -1e30
F32 = jnp.float32
BF16 = jnp.bfloat16
MIB = 2**20
LOCAL_VMEM = 56 * MIB
REMOTE_VMEM = 63 * MIB
STEPS = 4
LOG2_E = 1.4426950408889634
SUBLANES = 8
BOTH = (0, 1)
ROW_BLOCK = 32
WIDE_TILE = 512
BIG_TILE = 1024
TILE = 256
MESH_ID = pl.DeviceIdType.MESH
NT = (((1,), (1,)), ((), ()))
CONTRACT_FIRST = (((0,), (0,)), ((), ()))
VMEM = pl.BlockSpec(memory_space=pltpu.VMEM)
SMEM = pl.BlockSpec(memory_space=pltpu.SMEM)
HBM = pl.BlockSpec(memory_space=pl.ANY)
DMA = pltpu.SemaphoreType.DMA


X_PAIRS, Y_PAIRS = ([(chip, chip ^ flip) for chip in range(4)] for flip in (1, 2))
C_PAIRS = X_PAIRS[:2]
CORE_PAIRS = tuple([(2 * a + core, 2 * b + core) for core, pairs in enumerate(kinds) for a, b in pairs] for kinds in ((Y_PAIRS, X_PAIRS), (X_PAIRS, Y_PAIRS)))


def swap_x(v):
    return lax.ppermute(v, "tp", X_PAIRS)


def swap_y(v):
    return lax.ppermute(v, "tp", Y_PAIRS)


def swap_c(v):
    return lax.ppermute(v, "cp", C_PAIRS)


def swap_core(v, which):
    return lax.ppermute(v, ("tp", "cp"), CORE_PAIRS[which])


def rows_in(v):
    return v.shape[0]


def cols_of(v):
    return v.shape[1]


def over_row(reduce, v):
    return reduce(v, axis=-1, keepdims=True)


def over_column(v):
    return jnp.sum(v, axis=0, keepdims=True)


def specs(places):
    return [{"v": VMEM, "h": HBM, "s": SMEM}[place] for place in places]


def cost(gflops, mib):
    return pl.CostEstimate(flops=gflops * 10**9, bytes_accessed=mib * MIB, transcendentals=0)


def shape(rows, cols, dtype=BF16):
    return jax.ShapeDtypeStruct((rows, cols), dtype)


def local_call(body, name, out_shape, in_specs, out_specs, scratch, gflops, aliases={}, **grid):
    return pl.pallas_call(
        body,
        out_shape=out_shape,
        in_specs=in_specs,
        out_specs=out_specs,
        scratch_shapes=scratch,
        input_output_aliases=aliases,
        compiler_params=pltpu.CompilerParams(vmem_limit_bytes=LOCAL_VMEM),
        cost_estimate=cost(gflops, 60),
        name=name,
        **grid,
    )


def rows_at(start, size, step=32):
    return pl.ds(pl.multiple_of(start, step), size)


class Ring:
    def __init__(self, buf, sems, inward):
        self.buf, self.sems, self.inward = buf, sems, inward

    def slot(self, count):
        return lax.rem(count, rows_in(self.buf))

    def _copy(self, count, view):
        pair = (view, self.buf.at[self.slot(count)])
        return pltpu.make_async_copy(*(pair if self.inward else pair[::-1]), self.sems.at[self.slot(count)])

    def start(self, count, kind, views):
        for k, view in enumerate(views):
            pl.when(kind == k)(lambda: self._copy(count, view).start())

    def wait(self, count, view):
        self._copy(count, view).wait()


ZERO_ROWS = 24
ZEROS = {"attend": (21, 58), "attend_back": (49, 97)}
ZERO_PICK = 1


def zero_block(out_ref, block, count=1):
    return out_ref.at[pl.ds(pl.multiple_of(block * ZERO_ROWS, ZERO_ROWS), count * ZERO_ROWS)]


def clear(ref, value=0.0):
    ref[()] = jnp.full(ref.shape, value, F32)


def start_zeros(out_ref, zero_ref, sem, first, count):
    def start(i, carry):
        pltpu.make_async_copy(zero_ref, zero_block(out_ref, first + i), sem).start()
        return carry

    lax.fori_loop(0, count, start, 0)


def wait_zeros(out_ref, sem, first, count):
    whole = zero_block(out_ref, first, count)
    pltpu.make_async_copy(whole, whole, sem).wait()


def zero_scratch(width):
    return [pltpu.VMEM((ZERO_ROWS, width), F32), DMA]


def grid_zeros(grad_ref, zero_ref, sem, name):
    head, tile = pl.program_id(0), pl.program_id(1)
    heads, tiles = pl.num_programs(0), pl.num_programs(1)
    half = tiles // 2
    early, late = ZEROS[name]
    whole = half * (early + late)
    before = rows_in(grad_ref) // ZERO_ROWS - heads * whole
    if name == "attend":
        before -= heads * half * sum(ZEROS["attend_back"])
    pl.when((head == 0) & (tile == 0))(functools.partial(clear, zero_ref))
    first = before + head * whole + tile * early + jnp.maximum(tile - half, 0) * (late - early)
    start_zeros(grad_ref, zero_ref, sem, first, early)
    pl.when(tile >= half)(functools.partial(start_zeros, grad_ref, zero_ref, sem, first + early, late - early))
    last = (head == heads - 1) & (tile == tiles - 1)
    return lambda: pl.when(last)(lambda: wait_zeros(grad_ref, sem, before, heads * whole))


GATHER_BATCH = 16
GATHER_SLOTS = 16


def pick_body(group_ref, lane_ref, count_ref, table_ref, out_ref, grad_ref, buf, sems, zero_ref, zero_sem):
    batches = rows_in(out_ref) // GATHER_BATCH
    width = cols_of(out_ref)

    def row_copy(group, slot, j):
        return pltpu.make_async_copy(table_ref.at[group], buf.at[slot, j], sems.at[slot])

    def start(step):
        slot = lax.rem(step, GATHER_SLOTS)
        for j in range(GATHER_BATCH):
            group = group_ref[step * GATHER_BATCH + j]
            pl.when(group >= 0)(lambda: row_copy(group, slot, j).start())

    for step in range(GATHER_SLOTS - 1):
        start(step)
    clear(zero_ref)
    row = lax.broadcasted_iota(jnp.int32, (SUBLANES, width), 0)

    def loop(step, carry):
        slot = lax.rem(step, GATHER_SLOTS)

        @pl.when(step + GATHER_SLOTS - 1 < batches)
        def _():
            start(step + GATHER_SLOTS - 1)

        for i in range(ZERO_PICK):
            pltpu.make_async_copy(zero_ref, zero_block(grad_ref, step * ZERO_PICK + i), zero_sem).start()

        count = count_ref[step]
        some = GATHER_BATCH
        while some:
            pl.when(lax.bitwise_and(count, some) > 0)(lambda: pltpu.make_async_copy(table_ref.at[pl.ds(0, some)], buf.at[slot, pl.ds(0, some)], sems.at[slot]).wait())
            some //= 2
        first = pl.multiple_of(step * GATHER_BATCH, GATHER_BATCH)
        parts = []
        for j in range(GATHER_BATCH):
            lane = lane_ref[first + j]
            goal = j % SUBLANES
            if goal == 0:
                parts.append(jnp.zeros((SUBLANES, width), F32))
            turned = pltpu.roll(buf[slot, j].astype(F32), lax.rem(goal + SUBLANES - lane, SUBLANES), 0)
            parts[-1] = jnp.where(row == jnp.where(lane < SUBLANES, goal, SUBLANES), turned, parts[-1])
        out_ref[pl.ds(first, GATHER_BATCH), :] = jnp.concatenate(parts, axis=0).astype(BF16)
        return carry

    lax.fori_loop(0, batches, loop, 0)
    wait_zeros(grad_ref, zero_sem, 0, batches * ZERO_PICK)


def pick_rows(tokens, table, base):
    span = rows_in(tokens)
    rows, width = table.shape
    local = tokens - base
    owned = (local >= 0) & (local < rows)
    group = jnp.where(owned, local // SUBLANES, -1)
    lane = jnp.where(owned, local % SUBLANES, SUBLANES)
    count = jnp.sum(owned.reshape(-1, GATHER_BATCH).astype(jnp.int32), axis=1)
    scratch = [pltpu.VMEM((GATHER_SLOTS, GATHER_BATCH, SUBLANES, width), BF16), DMA((GATHER_SLOTS,))] + zero_scratch(width)
    return local_call(pick_body, "pick_rows", [shape(span, width), shape(rows, width, F32)], specs("sssh"), specs("vh"), scratch, 20)(group, lane, count, table.reshape(rows // SUBLANES, SUBLANES, width))


SEMS = 32
AHEAD = 4
MOVE_SLOTS = 8
MOVE_ROWS = 128
MAX_TILES = 16


LANES = 128
KEY_BITS = 11


def put_body(keys_ref, all_ref, zero_ref, *refs):
    kinds = len(refs) // 2 - 4
    sources, out_ref, rest = refs[:kinds], refs[kinds], refs[kinds + 1 :]
    targets, (rows_ref, load_sem, sems, moved, read_sems, write_sems, place, sent) = rest[:kinds], rest[kinds:]
    load = pltpu.make_async_copy(all_ref, rows_ref, load_sem)
    load.start()
    tokens = rows_in(rows_ref)
    base = lax.axis_index("tp") * rows_in(out_ref)

    def id_at(pos):
        return lax.shift_right_arithmetic(keys_ref[pos], KEY_BITS)

    def first_at(bound):
        def narrow(_, ends):
            low, high = ends
            middle = lax.div(low + high, 2)
            below = id_at(middle) < bound
            return jnp.where(below, middle + 1, low), jnp.where(below, high, middle)

        return lax.fori_loop(0, KEY_BITS + 1, narrow, (jnp.int32(0), jnp.int32(tokens)))[0]

    low, high = first_at(base), first_at(base + rows_in(out_ref))
    pieces = sources[0].shape[0] // MOVE_ROWS
    moves = kinds * pieces
    lag = MOVE_SLOTS // 2
    steps = moves + MOVE_SLOTS

    reads, writes = Ring(moved, read_sems, True), Ring(moved, write_sems, False)

    def views(arrays, step):
        return [ref.at[rows_at(lax.rem(step, pieces) * MOVE_ROWS, MOVE_ROWS)] for ref in arrays]

    def move(step):
        @pl.when(step >= MOVE_SLOTS)
        def _():
            writes.wait(step, views(targets, step)[0])

        @pl.when(step < moves)
        def _():
            reads.start(step, lax.div(step, pieces), views(sources, step))

        ready = step - lag

        @pl.when((ready >= 0) & (ready < moves))
        def _():
            reads.wait(ready, views(sources, ready)[0])
            writes.start(ready, lax.div(ready, pieces), views(targets, ready))

    def row(pos):
        return pl.ds(pos, 1)

    def wait_slot(slot):
        pltpu.make_async_copy(rows_ref.at[row(0), :], out_ref.at[row(0), :], sems.at[slot]).wait()

    def row_of(pos):
        return row(lax.bitwise_and(keys_ref[pos], tokens - 1))

    def token(pos):
        return rows_ref[row_of(pos), :]

    def one_id(carry):
        pos, count = carry
        row_id = id_at(pos)
        first = row_of(pos)

        def more(carry):
            return id_at(carry[0]) == row_id

        def add(carry):
            start, total = carry
            end = start
            for k in range(AHEAD):
                same = id_at(start + k) == row_id
                total = total + jnp.where(same, token(start + k), 0.0)
                end = end + same.astype(jnp.int32)
            return end, total

        after, total = lax.while_loop(more, add, (pos + 1, token(pos)))

        @pl.when(after > pos + 1)
        def _():
            rows_ref[first, :] = total

        slot = lax.rem(count, SEMS)
        pl.when(count >= SEMS)(lambda: wait_slot(slot))
        pltpu.make_async_copy(rows_ref.at[first, :], out_ref.at[row(row_id - base), :], sems.at[slot]).start()
        return after, count + 1

    place[0] = low
    sent[0] = 0

    def step_body(step, carry):
        move(step)
        pl.when(step == 0)(load.wait)
        limit = low + lax.div((high - low) * (step + 1), steps)
        pos, count = lax.while_loop(lambda c: c[0] < limit, one_id, (place[0], sent[0]))
        place[0] = pos
        sent[0] = count
        return carry

    lax.fori_loop(0, steps, step_body, 0)
    count = sent[0]

    def drain(slot, carry):
        pl.when(slot < count)(lambda: wait_slot(slot))
        return carry

    lax.fori_loop(0, SEMS, drain, 0)


def put_rows(keys, rows, zeros, results):
    slots = DMA((MOVE_SLOTS,))
    counter = pltpu.SMEM((1,), jnp.int32)
    scratch = [pltpu.VMEM(rows.shape, F32), DMA, DMA((SEMS,)), pltpu.VMEM((MOVE_SLOTS, MOVE_ROWS, cols_of(rows)), F32), slots, slots, counter, counter]
    out_shape = [shape(*v.shape, F32) for v in (zeros, *results)]
    return local_call(put_body, "put_rows", out_shape, specs("shh") + [HBM] * len(results), [HBM] * len(out_shape), scratch, 20, {2: 0})(keys, rows, zeros, *results)


def move_body(*refs):
    half = len(refs) // 2
    for src, dst in zip(refs[:half], refs[half:]):
        dst[()] = src[()]


def move(*arrays):
    steps = SUBLANES
    blocks = [pl.BlockSpec((rows_in(v) // steps, cols_of(v)), lambda i: (i, 0)) for v in arrays]
    return local_call(move_body, "move", [shape(*v.shape, F32) for v in arrays], blocks, blocks, [], 20, grid=(steps,))(*arrays)


Q_TILE = 256
K_TILE = 512


def as_column(row):
    return jnp.broadcast_to(row, (LANES, LANES)).T


def stack_heads(v):
    half = cols_of(v) // 2
    return jnp.concatenate([v[:, :half], v[:, half:]], axis=0)


def unstack_heads(v):
    half = rows_in(v) // 2
    return jnp.concatenate([v[:half], v[half:]], axis=1)


def sequence_chunks(cp):
    return [chunk * K_TILE for chunk in (cp, 3 - cp, 1 - cp, 2 + cp)]


class Tile:
    def __init__(self, q_ref, pos_ref, starts_ref):
        tile = pl.program_id(1)
        per_chunk = K_TILE // Q_TILE
        cp = lax.axis_index("cp")
        late = tile >= per_chunk
        self.chunks = sequence_chunks(cp)
        first = jnp.where(late, self.chunks[1], self.chunks[0]) + lax.rem(tile, per_chunk) * Q_TILE
        pos = jnp.concatenate([as_column(pos_ref[:, i : i + LANES])[:, :1] for i in range(0, Q_TILE, LANES)], axis=0)
        high = first + lax.broadcasted_iota(jnp.int32, pos.shape, 0)
        twice = lambda v: jnp.concatenate([v, v], axis=0)
        self.low, self.high = twice(high - pos), twice(high)
        self.q = stack_heads(q_ref[()])
        at = tile * Q_TILE
        ends = at + Q_TILE - 1
        lowest, highest = first - starts_ref[at], first + Q_TILE - 1 - starts_ref[ends]
        causal = (True, late, late | (cp == 1), late & (cp == 0))
        self.needed = [when & (chunk + K_TILE > lowest) for when, chunk in zip(causal, self.chunks)]
        self.free = [(chunk + K_TILE <= first + 1) & (highest <= chunk) for chunk in self.chunks]

    def visit(self, visit):
        for block, when in enumerate(self.needed):
            pl.when(when)(functools.partial(visit, block))

    def visit_scores(self, k_refs, visit):
        for block, (when, free) in enumerate(zip(self.needed, self.free)):
            (k,) = block_refs(block, k_refs)
            scores = lambda: lax.dot_general(self.q, k[()], NT, preferred_element_type=F32)
            pl.when(when & free)(lambda: visit(block, scores()))
            pl.when(when & jnp.logical_not(free))(lambda: visit(block, self.mask(scores(), block)))

    def mask(self, scores, block):
        at = self.chunks[block] + lax.broadcasted_iota(jnp.int32, (1, K_TILE), 1)
        return jnp.where((at >= self.low) & (at <= self.high), scores, NEG_BIG)


def block_refs(block, *pairs):
    rows = pl.ds((block % 2) * K_TILE, K_TILE)
    return [pair[block // 2].at[rows] for pair in pairs]


def attend_body(scale, starts_ref, q_ref, k_ref, v_ref, k2_ref, v2_ref, pos_ref, zeros_in, out_ref, lse_ref, grad_ref, s_ref, m_ref, l_ref, acc_ref, zero_ref, zero_sem):
    end_zeros = grid_zeros(grad_ref, zero_ref, zero_sem, "attend")
    tile = Tile(q_ref, pos_ref, starts_ref)
    power = scale * LOG2_E
    clear(m_ref, NEG_BIG)
    clear(l_ref)
    clear(acc_ref)

    def score(block, s):
        s_ref[block] = s
        m_ref[()] = jnp.maximum(m_ref[()], over_row(jnp.max, s))

    def exponent(block):
        e = jnp.exp2((s_ref[block] - m_ref[()]) * power)
        s_ref[block] = e
        l_ref[()] += over_row(jnp.sum, e)

    tile.visit_scores((k_ref, k2_ref), score)
    tile.visit(exponent)
    inverse = 1.0 / l_ref[()]

    def mix(block):
        (v,) = block_refs(block, (v_ref, v2_ref))
        prob = (s_ref[block] * inverse).astype(BF16)
        acc_ref[()] += jnp.dot(prob, v[()], preferred_element_type=F32)

    tile.visit(mix)
    out_ref[()] = unstack_heads(acc_ref[()].astype(BF16))
    lse_ref[()] = (m_ref[()] * power + jnp.log(l_ref[()]) * LOG2_E).reshape(lse_ref.shape)
    end_zeros()


def attention_specs(span, head_dim):
    tile = pl.BlockSpec((Q_TILE, 2 * head_dim), lambda h, t: (t, h))
    keys = pl.BlockSpec((span, head_dim), lambda h, t: (0, h))
    pos = pl.BlockSpec((1, Q_TILE), lambda h, t: (0, t))
    lse = pl.BlockSpec((1, 1, 2 * Q_TILE, 1), lambda h, t: (h, t, 0, 0))
    return tile, keys, pos, lse


def attention_buffers(heads):
    stacked = heads * Q_TILE
    return lambda c: pltpu.VMEM((stacked, c), F32), lambda dtype: pltpu.VMEM((4, stacked, K_TILE), dtype)


def attention_call(body, name, out_shape, in_specs, out_specs, scratch, gflops):
    aliases = {len(in_specs) - 1: len(out_specs) - 1}
    scratch = scratch + zero_scratch(out_shape[-1].shape[1])
    return local_call(body, name, out_shape, in_specs, out_specs, scratch, gflops, aliases, grid=(2, 4))


def attend(scale, starts, q, k, v, k2, v2, pos, grad):
    span = rows_in(q)
    heads = 2
    head_dim = cols_of(k) // heads
    tile, keys, pos_spec, lse = attention_specs(span, head_dim)
    stacked = heads * Q_TILE
    buf, probs = attention_buffers(heads)
    out_shape = [shape(*q.shape), jax.ShapeDtypeStruct((heads, span // Q_TILE, stacked, 1), F32), shape(*grad.shape, F32)]
    column = buf(1)
    scratch = [probs(F32), column, column, buf(head_dim)]
    call = attention_call(functools.partial(attend_body, scale), "attend", out_shape, [SMEM, tile] + [keys] * 4 + [pos_spec, HBM], [tile, lse, HBM], scratch, 14)
    return call(starts, q, k, v, k2, v2, pos, grad)


def attend_back_body(scale, starts_ref, q_ref, do_ref, lse_ref, k_ref, v_ref, k2_ref, v2_ref, pos_ref, zeros_in, dq_ref, dk_ref, dv_ref, dk2_ref, dv2_ref, grad_ref, p_ref, dp_ref, d_ref, acc_ref, zero_ref, zero_sem):
    end_zeros = grid_zeros(grad_ref, zero_ref, zero_sem, "attend_back")
    tile = Tile(q_ref, pos_ref, starts_ref)
    d_out = stack_heads(do_ref[()])
    lse = lse_ref[()].reshape(rows_in(d_out), 1)
    clear(d_ref)
    clear(acc_ref)

    @pl.when(pl.program_id(1) == 0)
    def _():
        for ref in (dk_ref, dv_ref, dk2_ref, dv2_ref):
            clear(ref)

    def first(block, s):
        (v,) = block_refs(block, (v_ref, v2_ref))
        p = jnp.exp2(s * (scale * LOG2_E) - lse)
        dp = lax.dot_general(d_out, v[()], NT, preferred_element_type=F32).astype(BF16)
        p_ref[block] = p
        dp_ref[block] = dp
        d_ref[()] += over_row(jnp.sum, p * dp.astype(F32))

    def second(block):
        k, dk, dv = block_refs(block, (k_ref, k2_ref), (dk_ref, dk2_ref), (dv_ref, dv2_ref))
        p = p_ref[block]
        ds = (p * (dp_ref[block].astype(F32) - d_ref[()]) * scale).astype(BF16)
        acc_ref[()] += jnp.dot(ds, k[()], preferred_element_type=F32)
        dk[()] += lax.dot_general(ds, tile.q, CONTRACT_FIRST, preferred_element_type=F32)
        dv[()] += lax.dot_general(p.astype(BF16), d_out, CONTRACT_FIRST, preferred_element_type=F32)

    tile.visit_scores((k_ref, k2_ref), first)
    tile.visit(second)
    dq_ref[()] = unstack_heads(acc_ref[()].astype(BF16))
    end_zeros()


def attend_back(scale, starts, q, d_out, lse, k, v, k2, v2, pos, grad):
    span = rows_in(q)
    heads = 2
    head_dim = cols_of(k) // heads
    tile, keys, pos_spec, lse_spec = attention_specs(span, head_dim)
    buf, probs = attention_buffers(heads)
    out_shape = [shape(*q.shape)] + [shape(*k.shape, F32)] * 4 + [shape(*grad.shape, F32)]
    in_specs = [SMEM, tile, tile, lse_spec] + [keys] * 4 + [pos_spec, HBM]
    call = attention_call(functools.partial(attend_back_body, scale), "attend_back", out_shape, in_specs, [tile] + [keys] * 4 + [HBM], [probs(F32), probs(BF16), buf(1), buf(head_dim)], 30)
    return call(starts, q, d_out, lse, k, v, k2, v2, pos, grad)


def remote(src, dst, send, recv, device):
    return pltpu.make_async_remote_copy(src_ref=src, dst_ref=dst, send_sem=send, recv_sem=recv, device_id=device, device_id_type=MESH_ID)


def flipped(bit, flip):
    return bit + flip - 2 * bit * flip


class Place:
    def __init__(self):
        self.tp = lax.axis_index("tp")
        self.cp = lax.axis_index("cp")
        self.x = lax.rem(self.tp, 2)
        self.y = lax.div(self.tp, 2)
        self.over_x = (self.chip(1, 0), self.cp)
        self.over_y = (self.chip(0, 1), self.cp)
        self.twin = (self.tp, 1 - self.cp)

    def chip(self, dx, dy):
        return 2 * flipped(self.y, dy) + flipped(self.x, dx)

    def meet(self):
        barrier = pltpu.get_barrier_semaphore()
        peers = (self.over_x, self.over_y, self.twin)
        for device in peers:
            pl.semaphore_signal(barrier, inc=1, device_id=device, device_id_type=MESH_ID)
        pl.semaphore_wait(barrier, len(peers))


class Total:
    def __init__(self, place, part, wide, mid, narrow, out, send, recv, source=None):
        self.source = source or part
        self.part, self.wide, self.mid, self.narrow, self.out = part, wide, mid, narrow, out
        self.send, self.recv = send, recv
        self.rows = rows_in(out) // STEPS
        self.half, self.quarter, self.eighth = (self.rows // n for n in (2, 4, 8))
        self.kinds = [(place.x, place.y, place.over_x, place.over_y), (place.y, place.x, place.over_y, place.over_x)]

    def _rows(self, step, kind):
        first, second = self.kinds[kind][:2]
        side = step * self.rows + kind * self.half + first * self.quarter
        return rows_at(side, self.quarter), rows_at(side + second * self.eighth, self.eighth)

    def _kept(self, kind, flip=0):
        return rows_at(kind * self.half + flipped(self.kinds[kind][0], flip) * self.quarter, self.quarter)

    def _eighth(self, kind, flip=0):
        return rows_at(flipped(self.kinds[kind][1], flip) * self.eighth, self.eighth)

    def _copy(self, step, kind, stage):
        side, mine = self._rows(step, kind)
        _, _, peer_first, peer_second = self.kinds[kind]
        src, dst, peer = (
            lambda: (self.source(step).at[self._kept(kind, 1)], self.wide.at[step, kind], peer_first),
            lambda: (self.mid.at[step, kind, self._eighth(kind, 1)], self.narrow.at[step, kind], peer_second),
            lambda: (self.out.at[mine], self.out.at[mine], peer_second),
            lambda: (self.out.at[side], self.out.at[side], peer_first),
        )[stage]()
        return remote(src, dst, self.send.at[step, kind, stage], self.recv.at[step, kind, stage], peer)

    def begin(self, step):
        for kind in BOTH:
            self._copy(step, kind, 0).start()

    def fold_wide(self, step):
        for kind in BOTH:
            self._copy(step, kind, 0).wait_recv()
            self.mid[step, kind] = self.part(step)[self._kept(kind), :] + self.wide[step, kind]
            self._copy(step, kind, 1).start()

    def fold_narrow(self, step):
        for kind in BOTH:
            self._copy(step, kind, 1).wait_recv()
            total = self.mid[step, kind, self._eighth(kind), :] + self.narrow[step, kind]
            self.out[self._rows(step, kind)[1], :] = total.astype(BF16)
            self._copy(step, kind, 2).start()

    def widen(self, step):
        for kind in BOTH:
            self._copy(step, kind, 2).wait_recv()
            self._copy(step, kind, 3).start()

    def finish(self, step):
        for kind in BOTH:
            self._copy(step, kind, 3).wait_recv()

    def sent(self, step, stages):
        for kind in BOTH:
            for stage in stages:
                self._copy(step, kind, stage).wait_send()


def sems(*dims):
    return DMA((*dims, 3))


def total_scratch(width, dtype, rows):
    stages = DMA((STEPS, 2, 4))
    part = lambda n: pltpu.VMEM((STEPS, 2, rows // n, width), dtype)
    return [part(4), part(4), part(8), stages, stages]


class Share:
    def __init__(self, place, sems, span):
        self.place, self.sems, self.first = place, sems, place.cp * span

    def pair(self, k, src, dst, start):
        here_sem, send, recv = (self.sems.at[k, i] for i in range(3))
        at = dst.at[rows_at(self.first + start, rows_in(src))]
        return pltpu.make_async_copy(src, at, here_sem), remote(src, at, send, recv, self.place.twin)

    def begin(self, *numbered):
        for copy in self.pair(*numbered):
            copy.start()

    def sent(self, *numbered):
        here, there = self.pair(*numbered)
        here.wait()
        there.wait_send()

    def got(self, k, src, dst, start):
        at = dst.at[rows_at(self.first + start, rows_in(src))]
        remote(src, at, *(self.sems.at[k, i] for i in (1, 2)), self.place.twin).wait_recv()


class Loads:
    def __init__(self, sems, *names):
        self.sems, self.names = sems, list(names)

    def _copies(self, moves):
        self.names += [name for name in moves if name not in self.names]
        return [pltpu.make_async_copy(src, dst, self.sems.at[self.names.index(name)]) for name, (src, dst) in moves.items()]

    def start(self, **moves):
        for copy in self._copies(moves):
            copy.start()
        return lambda: self.wait(**moves)

    def wait(self, **moves):
        for copy in self._copies(moves):
            copy.wait()


def steps(visit):
    def body(step, carry):
        visit(step)
        return carry

    lax.fori_loop(0, STEPS, body, 0)


def rope(v, cosine, sine):
    wide = cols_of(cosine)
    heads = []
    for h in range(cols_of(v) // wide):
        part = v[:, h * wide : (h + 1) * wide]
        turned = jnp.concatenate([part[:, wide // 2 :], part[:, : wide // 2]], axis=1)
        heads.append(part * cosine + turned * sine)
    return jnp.concatenate(heads, axis=1)


def each(count, size, visit):
    def body(i, carry):
        visit(pl.multiple_of(i * size, size))
        return carry

    lax.fori_loop(0, count // size, body, 0)


def col_loop(cols, tile, visit):
    each(cols, tile, lambda start: visit(pl.ds(start, tile)))


def dot_nt(a, b):
    return lax.dot_general(a, b, NT, preferred_element_type=F32)


def dot(a, b):
    return jnp.dot(a, b, preferred_element_type=F32)


def as_row(gain):
    return gain[()].astype(F32)[None, :]


def norm_block(feats):
    inverse = lax.rsqrt(over_row(jnp.mean, feats * feats) + NORM_EPS)
    return feats * inverse, inverse


def norm_back(d_act, gain, normed, inverse):
    d_normed = d_act * gain
    return inverse * (d_normed - normed * over_row(jnp.mean, d_normed * normed))


def remote_call(body, collective_id, name, out_shape, in_places, out_places, scratch, gflops):
    return pl.pallas_call(
        body,
        out_shape=out_shape,
        in_specs=specs(in_places),
        out_specs=specs(out_places),
        scratch_shapes=scratch,
        compiler_params=pltpu.CompilerParams(collective_id=collective_id, has_side_effects=True, vmem_limit_bytes=REMOTE_VMEM),
        cost_estimate=cost(gflops, 60),
        name=name,
    )


def join_columns(parts, whole):
    start, moves = 0, {}
    for i, part in enumerate(parts):
        moves[f"join{i}"] = (part, whole.at[:, pl.ds(start, cols_of(part))])
        start += cols_of(part)
    return moves


def order_ids(cp, ids, ids_got, keys, tall, rank, keys_out):
    span = cols_of(ids)
    chunks = rows_in(keys)
    lane = lax.broadcasted_iota(jnp.int32, (1, LANES), 1)
    for core, src in ((cp, ids), (1 - cp, ids_got)):
        for c in range(span // LANES):
            start = c * LANES
            token = core * span + start + lane
            keys[core * (chunks // 2) + c] = lax.shift_left(src[:, start : start + LANES], KEY_BITS) + token

    def count(a, carry):
        mine = as_column(keys[a])
        tall[a] = mine
        rank[a] = over_row(jnp.sum, sum((keys[b] < mine).astype(F32) for b in range(chunks)))
        return carry

    def place(c, carry):
        goal = (c * LANES + lane).astype(F32)
        keys_out[rows_at(c * LANES, LANES, LANES)] = over_column(sum(jnp.where(rank[a] == goal, tall[a], 0) for a in range(chunks)))[0]
        return carry

    lax.fori_loop(0, chunks, count, 0)
    lax.fori_loop(0, chunks, place, 0)
    keys_out[pl.ds(chunks * LANES, LANES)] = jnp.full((LANES,), jnp.iinfo(jnp.int32).max, jnp.int32)


def enter_body(picked_in, wq_in, wk_in, wv_in, gain, pos, inv_freq, ids, dy_in, wd_in, x_rows, q_out, k_out, v_out, cosine, sine, keys_out, dh_out, k2_out, v2_out, act_all, dy_all, wide, mid, narrow, send, recv, picked, x_out, act, dy, wd, dh, w_all, ids_got, keys, tall, rank, pair_sems, share_sems, load_sems, ids_sems):
    place = Place()
    place.meet()
    span = rows_in(x_out)
    rows = span // STEPS
    chunk = lambda step: rows_at(step * rows, rows)
    total = Total(place, lambda step: picked.at[chunk(step)], wide, mid, narrow, x_out, send, recv, lambda step: picked_in.at[chunk(step)])
    share = Share(place, share_sems, span)
    loads = Loads(load_sems)
    steps(total.begin)
    ids_swap = remote(ids, ids_got, *(ids_sems.at[end] for end in BOTH), place.twin)
    ids_swap.start()
    loaded = loads.start(picked=(picked_in, picked), dy=(dy_in, dy), wd=(wd_in, wd))
    projection = loads.start(**join_columns((wq_in, wk_in, wv_in), w_all))
    kw = cols_of(k_out)
    qw = cols_of(q_out)

    def back(step):
        here = chunk(step)

        def tile(cols):
            dh[here, cols] = dot_nt(dy[here, :], wd[cols, :]).astype(BF16)

        col_loop(rows_in(wd), WIDE_TILE, tile)
        total.fold_wide(step)

    def pairs(step):
        return [remote(src.at[chunk(step)], dst.at[chunk(step)], *(pair_sems.at[step, i, end] for end in BOTH), place.twin) for i, (src, dst) in enumerate(((k_out, k2_out), (v_out, v2_out)))]

    x_kept = lambda step: dict(x=(x_out.at[chunk(step)], x_rows.at[chunk(step)]))
    act_share = lambda step: (1 + step, act.at[chunk(step)], act_all, step * rows)

    def project(step):
        total.finish(step)
        here = chunk(step)
        pl.when(step >= 1)(lambda: loads.wait(**x_kept(step - 1)))
        loads.start(**x_kept(step))

        def norm(start):
            at = rows_at(step * rows + start, ROW_BLOCK)
            normed, _ = norm_block(x_out[at, :].astype(F32))
            act[at, :] = (normed * as_row(gain)).astype(BF16)

        each(rows, ROW_BLOCK, norm)
        share.begin(*act_share(step))
        c, s = cosine[here, :], sine[here, :]
        out = dot(act[here, :], w_all[()])
        q_out[here, :] = rope(out[:, :qw], c, s).astype(BF16)
        k_out[here, :] = rope(out[:, qw : qw + kw], c, s).astype(BF16)
        v_out[here, :] = out[:, qw + kw :].astype(BF16)
        for copy in pairs(step):
            copy.start()

    def angles(start):
        at = pl.ds(start, LANES)
        angle = as_column(pos[:, at])[:, : cols_of(inv_freq)].astype(F32) * inv_freq[()]
        c, s = jnp.cos(angle), jnp.sin(angle)
        cosine[at, :] = jnp.concatenate([c, c], axis=1)
        sine[at, :] = jnp.concatenate([-s, s], axis=1)

    loaded()
    dy_share = (0, dy, dy_all, 0)
    share.begin(*dy_share)
    each(span, LANES, angles)
    steps(back)
    stored = loads.start(dh=(dh, dh_out))
    ids_swap.wait()
    order_ids(place.cp, ids, ids_got, keys, tall, rank, keys_out)
    steps(total.fold_narrow)
    steps(total.widen)
    projection()
    steps(project)

    def close(step):
        total.sent(step, range(4))
        share.sent(*act_share(step))
        share.got(*act_share(step))
        for copy in pairs(step):
            copy.wait()

    steps(close)
    share.sent(*dy_share)
    share.got(*dy_share)
    loads.wait(**x_kept(STEPS - 1))
    stored()


def enter(picked, wq, wk, wv, gain, pos, inv_freq, ids, dy, wd):
    span, width = picked.shape
    key = shape(span, cols_of(wk))
    angles = shape(span, 2 * cols_of(inv_freq), F32)
    all_rows = shape(2 * span, width)
    chunks = 2 * span // LANES
    int_buf = lambda *dims: pltpu.VMEM(dims, jnp.int32)
    big = pltpu.VMEM((span, width), BF16)
    out_shape = [shape(span, width), shape(span, cols_of(wq)), key, key, angles, angles, jax.ShapeDtypeStruct(((chunks + SUBLANES) * LANES,), jnp.int32), shape(span, rows_in(wd)), key, key, all_rows, all_rows]
    scratch = total_scratch(width, BF16, span // STEPS) + [big, big, big, big, pltpu.VMEM(wd.shape, BF16), pltpu.VMEM((span, rows_in(wd)), BF16), pltpu.VMEM((width, cols_of(wq) + 2 * cols_of(wk)), BF16)]
    scratch += [int_buf(1, span), int_buf(chunks, 1, LANES), int_buf(chunks, LANES, LANES), pltpu.VMEM((chunks, LANES, 1), F32)]
    scratch += [DMA((STEPS, 2, 2)), sems(STEPS + 1), DMA((8,)), DMA((2,))]
    call = remote_call(enter_body, 1, "enter", out_shape, "hhhhvvvvhh", "hvvvvvvhhhhh", scratch, 80)
    return call(picked, wq, wk, wv, gain, pos, inv_freq, ids, dy, wd)


def middle_body(att, wo_own, wo_1, wo_2, wo_3, x_in, wg_in, wu_in, wd_in, dh_in, dy_in, gain, h_out, keep_x, send_x, keep_y, send_y, b_all, hidden_all, dgate_all, dup_all, att_all, drb_all, dr_out, datt_out, dgain_out,
                wide, mid, narrow, send, recv, wo, wg, wu, att_full, part_buf, d_b, h, row_in, dh, b, hid, dgt, dup, att_send, att_recv, wo_sems, load_sems, share_sems):
    place = Place()
    span, width = x_in.shape
    rows = span // STEPS
    half = rows // 2
    cols = cols_of(att)
    ffn = cols_of(wg)
    loads = Loads(load_sems, "att", "wo", "wg", "wu", "rows", "dh", "h_out", "h_in", "hid", "dr", "y")
    chunk = lambda step: rows_at(step * rows, rows)
    by_chip = lambda tp: rows_at(tp * cols, cols, 128)

    mine = loads.start(att=(att, att_full.at[:, by_chip(place.tp)]), wo=(wo_own, wo.at[by_chip(place.tp)]))
    place.meet()

    x_tp, y_tp = place.over_x[0], place.over_y[0]

    def att_copy(step, kind, hop):
        at = rows_at(step * rows + kind * half, half)
        first, second = ((place.over_y, place.over_x), (place.over_x, place.over_y))[kind]
        relay = hop == 2
        dst = att_full.at[at, by_chip(first[0] if relay else place.tp)]
        return remote(dst if relay else att.at[at], dst, att_send.at[step, kind, hop], att_recv.at[step, kind, hop], second if hop else first)

    def att_begin(step):
        for hop in BOTH:
            for kind in BOTH:
                att_copy(step, kind, hop).start()

    def att_forward(step):
        for kind in BOTH:
            att_copy(step, kind, 0).wait_recv()
            att_copy(step, kind, 2).start()

    att_begin(0)
    part = rows_in(wo_1)
    arrivals = []
    near = jnp.where(place.cp == 0, y_tp, x_tp)
    chips = (near, x_tp + y_tp - near, place.chip(1, 1))
    for i, (src, chip) in enumerate(zip((wo_1, wo_2, wo_3), chips)):
        at = wo.at[rows_at((2 * chip + place.cp) * part, part, 128)]
        here_sem, send_sem, recv_sem = (wo_sems.at[i, end] for end in range(3))
        for copy in (pltpu.make_async_copy(src, at, here_sem), remote(src, at, send_sem, recv_sem, place.twin)):
            copy.start()
            arrivals.append(copy)
    att_begin(1)
    weights = loads.start(wg=(wg_in, wg), wu=(wu_in, wu))

    share = Share(place, share_sems, span)
    att_share = (0, att, att_all, 0)
    share.begin(*att_share)
    total = Total(place, lambda step: part_buf.at[step], wide, mid, narrow, d_b, send, recv)

    def numbered(i, src, dst, step):
        return 1 + len(shares) * step + i, src, dst, step * rows

    shares = ((b, b_all), (hid, hidden_all), (dgt, dgate_all), (dup, dup_all))
    forward_shares = list(enumerate(shares))
    fetched = lambda step: dict(rows=(x_in.at[chunk(step)], row_in), dh=(dh_in.at[chunk(step)], dh))
    h_kept = lambda step: dict(h_out=(h, h_out.at[chunk(step)]))

    def close(step):
        loads.wait(**h_kept(step))
        for i, pair in forward_shares:
            share.sent(*numbered(i, *pair, step))

    def forward(step):
        pl.when(step >= 1)(lambda: close(step - 1))
        loads.wait(**fetched(step))
        for kind in BOTH:
            for hop in (1, 2):
                att_copy(step, kind, hop).wait_recv()

        def residual(c):
            h[:, c] = row_in[:, c].astype(F32) + dot(att_full[chunk(step), :], wo[:, c])

        col_loop(width, BIG_TILE, residual)
        loads.start(**h_kept(step))

        def norm(start):
            at = pl.ds(start, ROW_BLOCK)
            normed, _ = norm_block(h[at, :])
            b[at, :] = (normed * as_row(gain)).astype(BF16)

        each(rows, ROW_BLOCK, norm)
        share.begin(*numbered(0, b, b_all, step))
        pl.when(step == 0)(weights)

        def hidden(c):
            gate = dot(b[()], wg[:, c])
            up = dot(b[()], wu[:, c])
            sig = 1.0 / (1.0 + jnp.exp(-gate))
            d_hid = dh[:, c].astype(F32)
            act = gate * sig
            hid[:, c] = (act * up).astype(BF16)
            dgt[:, c] = (d_hid * up * sig * (1.0 + gate * (1.0 - sig))).astype(BF16)
            dup[:, c] = (d_hid * act).astype(BF16)

        col_loop(ffn, WIDE_TILE, hidden)
        for i, pair in forward_shares[1:]:
            share.begin(*numbered(i, *pair, step))
        pl.when(step == 0)(lambda: att_forward(2))

        @pl.when(step + 1 < STEPS)
        def _():
            loads.start(**fetched(step + 1))

        def back(c):
            part_buf[step, :, c] = dot_nt(dgt[()], wg[c, :]) + dot_nt(dup[()], wu[c, :])

        col_loop(width, WIDE_TILE, back)
        total.begin(step)
        pl.when(step == 0)(lambda: att_forward(3))
        pl.when(step >= 2)(lambda: total.fold_wide(step - 2))

    loads.start(**fetched(0))
    att_forward(0)
    for step in range(2, STEPS):
        att_begin(step)
    mine()
    for copy in arrivals:
        copy.wait()
    att_forward(1)
    steps(forward)
    clear(dgain_out)
    close(STEPS - 1)
    wd = wg
    weights = loads.start(wg=(wd_in, wd))
    d_r, y_buf = part_buf.at[0], part_buf.at[1]

    h_back = lambda step: dict(h_in=(h_out.at[chunk(step)], h))
    hidden_back = lambda step: dict(hid=(hidden_all.at[rows_at(place.cp * span + step * rows, rows)], hid))
    dy_back = lambda step: dict(rows=(dy_in.at[chunk(step)], row_in))
    y_kept = dict(y=(y_buf, keep_x))
    for step in BOTH:
        total.sent(step, (0,))
    loads.start(**h_back(0), **hidden_back(0))

    def output(step):
        pl.when(step < 2)(lambda: total.fold_wide(step + 2))
        loads.wait(**h_back(step), **hidden_back(step))
        pl.when(step == 0)(weights)
        pl.when(step >= 1)(lambda: loads.wait(**y_kept))
        over_x_first = step < 2
        first = jnp.where(over_x_first, place.x, place.y)
        second = place.x + place.y - first
        kept = first == lax.rem(step, 2)
        row = lax.broadcasted_iota(jnp.int32, (rows, 1), 0)
        owner = kept & (lax.div(row, half) == second)

        def tile(c):
            y_buf[:, c] = dot(hid[()], wd[:, c]) + jnp.where(owner, h[:, c], 0.0)

        col_loop(width, BIG_TILE, tile)
        for side_first, keep, send_to in ((over_x_first, keep_x, send_x), (jnp.logical_not(over_x_first), keep_y, send_y)):
            for chosen, dst in ((kept, keep), (jnp.logical_not(kept), send_to)):

                @pl.when(side_first & chosen)
                def _():
                    loads.start(y=(y_buf, dst))

        @pl.when(step + 1 < STEPS)
        def _():
            loads.start(**h_back(step + 1), **hidden_back(step + 1))

        total.fold_narrow(step)
        pl.when(step >= 2)(lambda: total.widen(step - 2))

    steps(output)
    loads.start(**h_back(0), **dy_back(0))
    kept_rows = lambda step: dict(dr=(d_r, dr_out.at[chunk(step)]))

    def resid_share(step, part):
        return 1 + len(shares) * STEPS + 2 * step + part, b.at[rows_at(part * half, half)], drb_all, step * rows + part * half

    def resid_sent(step):
        loads.wait(**kept_rows(step))
        for part in BOTH:
            share.sent(*resid_share(step, part))

    def resid(step):
        pl.when(step < 2)(lambda: total.widen(step + 2))
        total.finish(step)
        loads.wait(**h_back(step), **dy_back(step))
        pl.when(step >= 1)(lambda: resid_sent(step - 1))

        for part in BOTH:

            def grad(start):
                start = part * half + start
                at = rows_at(start, ROW_BLOCK)
                normed, inverse = norm_block(h[at, :])
                d_act = d_b[rows_at(step * rows + start, ROW_BLOCK), :].astype(F32)
                dgain_out[()] += over_column(d_act * normed)
                out = row_in[at, :].astype(F32) + norm_back(d_act, as_row(gain), normed, inverse)
                d_r[at, :] = out
                b[at, :] = out.astype(BF16)

            each(half, ROW_BLOCK, grad)
            share.begin(*resid_share(step, part))

        @pl.when(step + 1 < STEPS)
        def _():
            loads.start(**h_back(step + 1), **dy_back(step + 1))

        loads.start(**kept_rows(step))
        datt_out[chunk(step), :] = dot_nt(b[()], wo[by_chip(place.tp), :]).astype(BF16)

    steps(resid)
    loads.wait(**y_kept)
    resid_sent(STEPS - 1)
    share.sent(*att_share)
    share.got(*att_share)

    def finish(step):
        total.sent(step, range(1, 4))
        pl.when(step >= 2)(lambda: total.sent(step, (0,)))
        for kind in BOTH:
            for hop in range(3):
                att_copy(step, kind, hop).wait_send()
        for i, pair in forward_shares:
            share.got(*numbered(i, *pair, step))
        for part in BOTH:
            share.got(*resid_share(step, part))

    steps(finish)


def middle(att, wo_pieces, x, wg, wu, wd, d_hidden, dy, gain):
    span, width = x.shape
    rows = span // STEPS
    ffn = cols_of(wg)
    cols = cols_of(att)
    full = shape(span, width, F32)
    both = shape(2 * span, ffn)
    out_shape = [full] + [shape(rows, width, F32)] * 4 + [shape(2 * span, width), both, both, both, shape(2 * span, cols), shape(2 * span, width), full, shape(span, cols), shape(1, width, F32)]
    buf = lambda r, c, dtype=BF16: pltpu.VMEM((r, c), dtype)
    scratch = total_scratch(width, F32, rows)
    scratch += [buf(width, width), buf(width, ffn), buf(width, ffn), buf(span, width), pltpu.VMEM((STEPS, rows, width), F32), buf(span, width), buf(rows, width, F32)]
    scratch += [buf(rows, c) for c in (width, ffn, width, ffn, ffn, ffn)]
    scratch += [sems(STEPS, 2), sems(STEPS, 2), sems(3), DMA((11,)), sems(1 + 6 * STEPS)]
    call = remote_call(middle_body, 2, "middle", out_shape, "vhhhhhhhhhhv", "hhhhhhhhhhhhvv", scratch, 120)
    return call(att, *wo_pieces, x, wg, wu, wd, d_hidden, dy, gain)


def leave_body(dq_in, dk_in, dv_in, dk2_in, dv2_in, cosine, sine, wq_in, wk_in, wv_in, x_in, dr_in, gain, dgain_b, b_all, dgate_all, dup_all, hidden_all, dy_all, att_all, drb_all, act_all, d_all, dx_all, gain_a_out, gain_b_out, grad_gate, grad_up, grad_down, grad_out, grad_q, grad_k, grad_v,
               wide, mid, narrow, send, recv, part_buf, d_a, dk_got, dv_got, d_qkv, w_all, xs, drs, dxs, gain_got, left, right, result, pair_sems, load_sems, share_sems, left_sems, right_sems, result_sems, result_arrivals):
    place = Place()
    place.meet()
    span, width = x_in.shape
    rows = span // STEPS
    chunk = lambda step: rows_at(step * rows, rows)
    swap = lambda i, src, dst: remote(src, dst, *(pair_sems.at[i, end] for end in BOTH), place.twin)
    pairs = lambda step: [swap(2 * step + i, src.at[chunk(step)], dst.at[chunk(step)]) for i, (src, dst) in enumerate(((dk2_in, dk_got), (dv2_in, dv_got)))]
    for step in range(STEPS):
        for copy in pairs(step):
            copy.start()
    qw = cols_of(dq_in)
    kw = cols_of(dk_in)
    share = Share(place, share_sems, span)
    loads = Loads(load_sems)
    total = Total(place, lambda step: part_buf.at[step], wide, mid, narrow, d_a, send, recv)

    def partial(step):
        here = chunk(step)
        c, s = cosine[here, :], -sine[here, :]
        for copy in pairs(step):
            copy.wait()
        d_qkv[here, :qw] = rope(dq_in[here, :].astype(F32), c, s).astype(BF16)
        dk_sum = (dk_in[here, :] + dk_got[here, :]).astype(BF16).astype(F32)
        d_qkv[here, qw : qw + kw] = rope(dk_sum, c, s).astype(BF16)
        d_qkv[here, qw + kw :] = (dv_in[here, :] + dv_got[here, :]).astype(BF16)

        def tile(n):
            part_buf[step, :, n] = dot_nt(d_qkv[here, :], w_all[n, :])

        col_loop(width, BIG_TILE, tile)
        total.begin(step)

    rows_back = lambda step: dict(x=(x_in.at[chunk(step)], xs), dr=(dr_in.at[chunk(step)], drs))

    clear(gain_a_out)

    def dx_share(step, part):
        start = part * part_rows
        return 1 + 2 * step + part, dxs.at[rows_at(start, part_rows)], dx_all, step * rows + start

    part_rows = rows // 2

    def grad_x(step):
        for part in BOTH:

            def grad(start):
                start = part * part_rows + start
                at = rows_at(start, ROW_BLOCK)
                normed, inverse = norm_block(xs[at, :].astype(F32))
                d_act = d_a[rows_at(step * rows + start, ROW_BLOCK), :].astype(F32)
                gain_a_out[()] += over_column(d_act * normed)
                dxs[at, :] = drs[at, :] + norm_back(d_act, as_row(gain), normed, inverse)

            pl.when(step >= 1)(lambda: share.sent(*dx_share(step - 1, part)))
            each(part_rows, ROW_BLOCK, grad)
            share.begin(*dx_share(step, part))

    _, _, narrow_cols = left.shape
    _, _, wide_cols = right.shape
    lefts, rights = Ring(left, left_sems, True), Ring(right, right_sems, True)
    sides, per_core = width // wide_cols, width // narrow_cols // 2
    whole = (grad_gate, grad_up, grad_down, grad_out)
    ffn_blocks = (len(whole) - 1) * sides
    ffn_tiles = ffn_blocks * per_core
    tiles = ffn_tiles + 1 + per_core
    block_of = lambda t: jnp.where(t < ffn_tiles, lax.div(t, per_core), jnp.minimum(t - ffn_tiles, 1) + ffn_blocks)
    row_of = lambda t: place.cp * per_core + jnp.where(t < ffn_tiles, lax.rem(t, per_core), jnp.maximum(t - ffn_tiles - 1, 0))
    at_left = lambda t: rows_at(row_of(t) * narrow_cols, narrow_cols, TILE)
    at_right = lambda j: rows_at(jnp.where(j < ffn_blocks, lax.rem(j, sides), place.cp) * wide_cols, wide_cols, TILE)
    kind_of = lambda j: jnp.where(j < ffn_blocks, lax.div(j, sides), len(whole) - 1 + j - ffn_blocks)
    left_start = lambda t: lefts.start(t, kind_of(block_of(t)), [ref.at[:, at_left(t)] for ref in (b_all, b_all, hidden_all)] + [att_all, act_all.at[:, at_left(t)]])
    right_start = lambda j: rights.start(j, kind_of(j), [ref.at[:, at_right(j)] for ref in (dgate_all, dup_all, dy_all, drb_all)] + [d_all])

    def to_twin(t, src, dst):
        return remote(src, dst, result_sems.at[lefts.slot(t), 1], result_arrivals.at[t], place.twin)

    def stored(t):
        done = result.at[lefts.slot(t)]
        pltpu.make_async_copy(done, done, result_sems.at[lefts.slot(t), 0]).wait()
        to_twin(t, done, done).wait_send()

    def store(t):
        slot = lefts.slot(t)
        j = block_of(t)

        def put(cols, dst):
            src = result.at[slot, :, cols]
            pltpu.make_async_copy(src, dst, result_sems.at[slot, 0]).start()
            to_twin(t, src, dst).start()

        everything = pl.ds(0, wide_cols)
        for k, ref in enumerate(whole):
            at = at_left(t) if ref is not grad_out else pl.ds(0, narrow_cols)
            pl.when(kind_of(j) == k)(lambda: put(everything, ref.at[at, at_right(j)]))

        @pl.when(j == ffn_blocks + 1)
        def _():
            put(pl.ds(0, qw), grad_q.at[at_left(t)])
            put(pl.ds(qw, kw), grad_k.at[at_left(t)])
            put(pl.ds(qw + kw, kw), grad_v.at[at_left(t)])

    def tile_step(t, carry):
        j = block_of(t)
        pl.when(t + 1 < tiles)(lambda: left_start(t + 1))

        @pl.when(jnp.where(t < ffn_tiles, lax.rem(t, per_core) == 0, t <= ffn_tiles + 1))
        def _():
            pl.when(j < ffn_blocks)(lambda: right_start(j + 1))
            rights.wait(j, d_all)

        lefts.wait(t, att_all)
        pl.when(t >= 2)(lambda: stored(t))
        slot = lefts.slot(t)
        result[slot] = lax.dot_general(left[slot], right[rights.slot(j)], CONTRACT_FIRST, preferred_element_type=F32)
        store(t)
        return carry

    left_start(jnp.int32(0))
    right_start(jnp.int32(0))
    weights = loads.start(**join_columns((wq_in, wk_in, wv_in), w_all))
    loads.start(**rows_back(0))
    weights()
    steps(partial)
    d_here, d_there = share.pair(0, d_qkv, d_all, 0)
    d_here.start()
    d_there.start()

    stages = (total.fold_wide, total.fold_narrow, total.widen)
    waits = len(stages) * STEPS
    portion = ffn_tiles // STEPS
    tiles_until = lambda p: jnp.where(p < STEPS, portion * (p + 1), jnp.where(p < 2 * STEPS - 1, ffn_tiles, jnp.where(p < waits - 1, ffn_tiles + 1, tiles)))

    def wait_step(p, carry):
        @pl.when(p == waits - 1)
        def _():
            d_here.wait()
            d_there.wait_recv()
            right_start(jnp.int32(ffn_blocks + 1))

        lax.fori_loop(jnp.where(p == 0, 0, tiles_until(p - 1)), tiles_until(p), tile_step, 0)
        for k, stage in enumerate(stages):
            pl.when(lax.div(p, STEPS) == k)(lambda: stage(lax.rem(p, STEPS)))
        return carry

    lax.fori_loop(0, waits, wait_step, 0)
    def last_stage(step):
        loads.wait(**rows_back(step))
        total.finish(step)
        grad_x(step)

        @pl.when(step + 1 < STEPS)
        def _():
            loads.start(**rows_back(step + 1))

    steps(last_stage)
    gains = ((gain_a_out, gain_a_out), (dgain_b, gain_b_out))
    swaps = [swap(2 * STEPS + i, mine, gain_got.at[i]) for i, (mine, _) in enumerate(gains)]
    for copy in swaps:
        copy.start()
    for copy in swaps:
        copy.wait()
    for i, (mine, out) in enumerate(gains):
        out[()] = mine[()] + gain_got[i]
    for part in BOTH:
        share.sent(*dx_share(STEPS - 1, part))
    d_there.wait_send()
    for t in range(tiles - 2, tiles):
        stored(t)
    done = result.at[0]
    for t in range(tiles):
        to_twin(t, done, done).wait_recv()

    def close(step):
        total.sent(step, range(4))
        for part in BOTH:
            share.got(*dx_share(step, part))

    steps(close)


def leave(dq, dk, dv, dk2, dv2, cosine, sine, wq, wk, wv, x, d_resid, gain, dgain_b, *products):
    span, width = x.shape
    rows = span // STEPS
    kw = cols_of(wk)
    qw = cols_of(wq)
    cols = qw + 2 * kw
    ffn = products[1].shape[1]
    buf = lambda r, c, dtype=F32: pltpu.VMEM((r, c), dtype)
    gain_grad = shape(1, width, F32)
    out_shape = [shape(2 * span, cols), shape(2 * span, width, F32), gain_grad, gain_grad]
    out_shape += [shape(*dims, F32) for dims in ((width, ffn), (width, ffn), (ffn, width), (qw, width), wq.shape, wk.shape, wv.shape)]
    twice = lambda r, c, dtype: pltpu.VMEM((2, r, c), dtype)
    scratch = total_scratch(width, F32, rows) + [pltpu.VMEM((STEPS, rows, width), F32), buf(span, width, BF16), buf(span, kw), buf(span, kw), buf(span, cols, BF16), buf(width, cols, BF16)]
    scratch += [buf(rows, width, BF16), buf(rows, width), buf(rows, width), pltpu.VMEM((2, 1, width), F32)]
    scratch += [twice(2 * span, WIDE_TILE, BF16), twice(2 * span, BIG_TILE, BF16), twice(WIDE_TILE, BIG_TILE, F32)]
    ring = DMA((2,))
    scratch += [DMA((2 * STEPS + 2, 2)), DMA((5,)), sems(1 + 2 * STEPS), ring, ring, DMA((2, 2)), DMA((MAX_TILES,))]
    call = remote_call(leave_body, 3, "leave", out_shape, "vvvhhvvhhhhhvvhhhhhhhh", "hhvvhhhhhhh", scratch, 1)
    return call(dq, dk, dv, dk2, dv2, cosine, sine, wq, wk, wv, x, d_resid, gain, dgain_b, *products)


def side(v, bit):
    half = rows_in(v) // 2
    return lax.dynamic_slice_in_dim(v, bit * half, half, 0)


def join(own, other, bit):
    return jnp.where(bit == 0, jnp.concatenate([own, other]), jnp.concatenate([other, own]))


def solution(mesh):
    def device_step(tokens, pos, doc_id, dy, table, w_q, w_k, w_v, w_o, w_gate, w_up, w_down, gain_one, gain_two, inv_freq):
        span = rows_in(tokens)
        rows, width = table.shape
        scale = (2 * rows_in(inv_freq)) ** -0.5
        tp = lax.axis_index("tp")
        cp = lax.axis_index("cp")
        starts = pos
        inv_freq, pos, ids = (v[None, :] for v in (inv_freq, pos, tokens))
        base = tp * rows

        wo_half = side(w_o, cp)
        wo_1 = swap_core(wo_half, 0)
        picked, grad = pick_rows(tokens, table, base)
        x, query, key, value, cosine, sine, keys, d_hidden, key2, value2, act_a_all, dy_all = enter(picked, w_q, w_k, w_v, gain_one, pos, inv_freq, ids, dy, w_down)
        wo_1, wo_half, query = lax.optimization_barrier((wo_1, wo_half, query))
        wo_pieces = (w_o, wo_1, swap_core(wo_half, 1), swap_core(wo_1, 1))
        att, lse, grad = attend(scale, starts, query, key, value, key2, value2, pos, grad)
        keep_x, send_x, keep_y, send_y, act_b_all, hidden_all, d_gate_all, d_up_all, att_all, d_resid_all, d_resid, d_att, d_gain_b = middle(att, wo_pieces, x, w_gate, w_up, w_down, d_hidden, dy, gain_two)[1:]

        x_bit, y_bit = tp % 2, tp // 2
        ways = ((keep_x, swap_x, x_bit, swap_y, y_bit), (keep_y, swap_y, y_bit, swap_x, x_bit))
        y_wide = [swap_x(send_x), swap_y(send_y)]
        d_query, d_key, d_value, d_key2, d_value2, grad = attend_back(scale, starts, query, d_att, lse, key, value, key2, value2, pos, grad)

        d_x_all, gain_1, gain_2, grad_gate, grad_up, grad_down, *grads = leave(d_query, d_key, d_value, d_key2, d_value2, cosine, sine, w_q, w_k, w_v, x, d_resid, gain_one, d_gain_b, act_b_all, d_gate_all, d_up_all, hidden_all, dy_all, att_all, d_resid_all, act_a_all)[1:]
        y_wide, d_x_all = lax.optimization_barrier((y_wide, d_x_all))
        halves = lambda bit_2, keep, wide, flip: side(keep, flipped(bit_2, flip)) + side(wide, flipped(bit_2, flip))
        y_narrow = [swap_2(halves(bit_2, keep, wide, 1)) for (keep, _, _, swap_2, bit_2), wide in zip(ways, y_wide)]
        y_wide, grad_gate = lax.optimization_barrier((y_wide, grad_gate))
        grad_gate, grad_out, *grads = move(grad_gate, *grads)
        y_narrow, grad_gate = lax.optimization_barrier((y_narrow, grad_gate))
        y_own = [(halves(bit_2, keep, wide, 0) + narrow).astype(BF16) for (keep, _, _, _, bit_2), wide, narrow in zip(ways, y_wide, y_narrow)]
        y_pair = [join(own, swap_2(own), bit_2) for (_, _, _, swap_2, bit_2), own in zip(ways, y_own)]
        y_own, grad_down = lax.optimization_barrier((y_own, grad_down))
        (grad_down,) = move(grad_down)
        y_pair, grad_down = lax.optimization_barrier((y_pair, grad_down))
        y_far = [swap_1(pair) for (_, swap_1, _, _, _), pair in zip(ways, y_pair)]
        y_pair, d_x_all = lax.optimization_barrier((y_pair, d_x_all))
        grad_table, grad_up = put_rows(keys, d_x_all, grad, (grad_up,))
        y_rows = [jnp.where(bit_1 == k, pair, far) for (_, _, bit_1, _, _), pair, far in zip(ways, y_pair, y_far) for k in BOTH]
        return (jnp.concatenate(y_rows), grad_table, *grads, grad_out, grad_gate, grad_up, grad_down, gain_1[0], gain_2[0])

    col_spec = P(None, "tp")
    row_spec = P("tp", None)
    tok_spec = P("cp")
    rep_spec = P(None)
    in_specs = (tok_spec, tok_spec, tok_spec, P("cp", None), row_spec, col_spec, col_spec, col_spec, row_spec, col_spec, col_spec, row_spec, rep_spec, rep_spec, rep_spec)
    out_specs = (P("cp", None), row_spec, col_spec, col_spec, col_spec, row_spec, col_spec, col_spec, row_spec, rep_spec, rep_spec)
    return jax.shard_map(device_step, mesh=mesh, in_specs=in_specs, out_specs=out_specs, check_vma=False)
```

```python
import functools

import jax
import jax.numpy as jnp
from jax import lax
from jax.experimental import pallas as pl
from jax.experimental.pallas import tpu as pltpu
from jax.sharding import PartitionSpec as P

NORM_EPS = 1e-5
NEG_BIG = -1e30
F32 = jnp.float32
BF16 = jnp.bfloat16
MIB = 2**20
LOCAL_VMEM = 56 * MIB
REMOTE_VMEM = 63 * MIB
STEPS = 4
LOG2_E = 1.4426950408889634
SUBLANES = 8
BOTH = (0, 1)
ROW_BLOCK = 32
WIDE_TILE = 512
BIG_TILE = 1024
TILE = 256
MESH_ID = pl.DeviceIdType.MESH
NT = (((1,), (1,)), ((), ()))
CONTRACT_FIRST = (((0,), (0,)), ((), ()))
VMEM = pl.BlockSpec(memory_space=pltpu.VMEM)
SMEM = pl.BlockSpec(memory_space=pltpu.SMEM)
HBM = pl.BlockSpec(memory_space=pl.ANY)
DMA = pltpu.SemaphoreType.DMA


X_PAIRS, Y_PAIRS = ([(chip, chip ^ flip) for chip in range(4)] for flip in (1, 2))
C_PAIRS = X_PAIRS[:2]
CORE_PAIRS = tuple([(2 * a + core, 2 * b + core) for core, pairs in enumerate(kinds) for a, b in pairs] for kinds in ((Y_PAIRS, X_PAIRS), (X_PAIRS, Y_PAIRS)))


def swap_x(v):
    return lax.ppermute(v, "tp", X_PAIRS)


def swap_y(v):
    return lax.ppermute(v, "tp", Y_PAIRS)


def swap_c(v):
    return lax.ppermute(v, "cp", C_PAIRS)


def swap_core(v, which):
    return lax.ppermute(v, ("tp", "cp"), CORE_PAIRS[which])


def rows_in(v):
    return v.shape[0]


def cols_of(v):
    return v.shape[1]


def over_row(reduce, v):
    return reduce(v, axis=-1, keepdims=True)


def over_column(v):
    return jnp.sum(v, axis=0, keepdims=True)


def specs(places):
    return [{"v": VMEM, "h": HBM, "s": SMEM}[place] for place in places]


def cost(gflops, mib):
    return pl.CostEstimate(flops=gflops * 10**9, bytes_accessed=mib * MIB, transcendentals=0)


def shape(rows, cols, dtype=BF16):
    return jax.ShapeDtypeStruct((rows, cols), dtype)


def local_call(body, name, out_shape, in_specs, out_specs, scratch, gflops, aliases={}, **grid):
    return pl.pallas_call(
        body,
        out_shape=out_shape,
        in_specs=in_specs,
        out_specs=out_specs,
        scratch_shapes=scratch,
        input_output_aliases=aliases,
        compiler_params=pltpu.CompilerParams(vmem_limit_bytes=LOCAL_VMEM),
        cost_estimate=cost(gflops, 60),
        name=name,
        **grid,
    )


def rows_at(start, size, step=32):
    return pl.ds(pl.multiple_of(start, step), size)


class Ring:
    def __init__(self, buf, sems, inward):
        self.buf, self.sems, self.inward = buf, sems, inward

    def slot(self, count):
        return lax.rem(count, rows_in(self.buf))

    def _copy(self, count, view):
        pair = (view, self.buf.at[self.slot(count)])
        return pltpu.make_async_copy(*(pair if self.inward else pair[::-1]), self.sems.at[self.slot(count)])

    def start(self, count, kind, views):
        for k, view in enumerate(views):
            pl.when(kind == k)(lambda: self._copy(count, view).start())

    def wait(self, count, view):
        self._copy(count, view).wait()


ZERO_ROWS = 24
ZEROS = {"attend": (21, 58), "attend_back": (49, 97)}
ZERO_PICK = 1


def zero_block(out_ref, block, count=1):
    return out_ref.at[pl.ds(pl.multiple_of(block * ZERO_ROWS, ZERO_ROWS), count * ZERO_ROWS)]


def clear(ref, value=0.0):
    ref[()] = jnp.full(ref.shape, value, F32)


def start_zeros(out_ref, zero_ref, sem, first, count):
    def start(i, carry):
        pltpu.make_async_copy(zero_ref, zero_block(out_ref, first + i), sem).start()
        return carry

    lax.fori_loop(0, count, start, 0)


def wait_zeros(out_ref, sem, first, count):
    whole = zero_block(out_ref, first, count)
    pltpu.make_async_copy(whole, whole, sem).wait()


def zero_scratch(width):
    return [pltpu.VMEM((ZERO_ROWS, width), F32), DMA]


def grid_zeros(grad_ref, zero_ref, sem, name):
    head, tile = pl.program_id(0), pl.program_id(1)
    heads, tiles = pl.num_programs(0), pl.num_programs(1)
    half = tiles // 2
    early, late = ZEROS[name]
    whole = half * (early + late)
    before = rows_in(grad_ref) // ZERO_ROWS - heads * whole
    if name == "attend":
        before -= heads * half * sum(ZEROS["attend_back"])
    pl.when((head == 0) & (tile == 0))(functools.partial(clear, zero_ref))
    first = before + head * whole + tile * early + jnp.maximum(tile - half, 0) * (late - early)
    start_zeros(grad_ref, zero_ref, sem, first, early)
    pl.when(tile >= half)(functools.partial(start_zeros, grad_ref, zero_ref, sem, first + early, late - early))
    last = (head == heads - 1) & (tile == tiles - 1)
    return lambda: pl.when(last)(lambda: wait_zeros(grad_ref, sem, before, heads * whole))


GATHER_BATCH = 16
GATHER_SLOTS = 16


def pick_body(group_ref, lane_ref, count_ref, table_ref, out_ref, grad_ref, buf, sems, zero_ref, zero_sem):
    batches = rows_in(out_ref) // GATHER_BATCH
    width = cols_of(out_ref)

    def row_copy(group, slot, j):
        return pltpu.make_async_copy(table_ref.at[group], buf.at[slot, j], sems.at[slot])

    def start(step):
        slot = lax.rem(step, GATHER_SLOTS)
        for j in range(GATHER_BATCH):
            group = group_ref[step * GATHER_BATCH + j]
            pl.when(group >= 0)(lambda: row_copy(group, slot, j).start())

    for step in range(GATHER_SLOTS - 1):
        start(step)
    clear(zero_ref)
    row = lax.broadcasted_iota(jnp.int32, (SUBLANES, width), 0)

    def loop(step, carry):
        slot = lax.rem(step, GATHER_SLOTS)

        @pl.when(step + GATHER_SLOTS - 1 < batches)
        def _():
            start(step + GATHER_SLOTS - 1)

        for i in range(ZERO_PICK):
            pltpu.make_async_copy(zero_ref, zero_block(grad_ref, step * ZERO_PICK + i), zero_sem).start()

        count = count_ref[step]
        some = GATHER_BATCH
        while some:
            pl.when(lax.bitwise_and(count, some) > 0)(lambda: pltpu.make_async_copy(table_ref.at[pl.ds(0, some)], buf.at[slot, pl.ds(0, some)], sems.at[slot]).wait())
            some //= 2
        first = pl.multiple_of(step * GATHER_BATCH, GATHER_BATCH)
        parts = []
        for j in range(GATHER_BATCH):
            lane = lane_ref[first + j]
            goal = j % SUBLANES
            if goal == 0:
                parts.append(jnp.zeros((SUBLANES, width), F32))
            turned = pltpu.roll(buf[slot, j].astype(F32), lax.rem(goal + SUBLANES - lane, SUBLANES), 0)
            parts[-1] = jnp.where(row == jnp.where(lane < SUBLANES, goal, SUBLANES), turned, parts[-1])
        out_ref[pl.ds(first, GATHER_BATCH), :] = jnp.concatenate(parts, axis=0).astype(BF16)
        return carry

    lax.fori_loop(0, batches, loop, 0)
    wait_zeros(grad_ref, zero_sem, 0, batches * ZERO_PICK)


def pick_rows(tokens, table, base):
    span = rows_in(tokens)
    rows, width = table.shape
    local = tokens - base
    owned = (local >= 0) & (local < rows)
    group = jnp.where(owned, local // SUBLANES, -1)
    lane = jnp.where(owned, local % SUBLANES, SUBLANES)
    count = jnp.sum(owned.reshape(-1, GATHER_BATCH).astype(jnp.int32), axis=1)
    scratch = [pltpu.VMEM((GATHER_SLOTS, GATHER_BATCH, SUBLANES, width), BF16), DMA((GATHER_SLOTS,))] + zero_scratch(width)
    return local_call(pick_body, "pick_rows", [shape(span, width), shape(rows, width, F32)], specs("sssh"), specs("vh"), scratch, 20)(group, lane, count, table.reshape(rows // SUBLANES, SUBLANES, width))


SEMS = 32
AHEAD = 4
MOVE_SLOTS = 8
MOVE_ROWS = 128
MAX_TILES = 16


LANES = 128
KEY_BITS = 11


def put_body(keys_ref, all_ref, zero_ref, *refs):
    kinds = len(refs) // 2 - 4
    sources, out_ref, rest = refs[:kinds], refs[kinds], refs[kinds + 1 :]
    targets, (rows_ref, load_sem, sems, moved, read_sems, write_sems, place, sent) = rest[:kinds], rest[kinds:]
    load = pltpu.make_async_copy(all_ref, rows_ref, load_sem)
    load.start()
    tokens = rows_in(rows_ref)
    base = lax.axis_index("tp") * rows_in(out_ref)

    def id_at(pos):
        return lax.shift_right_arithmetic(keys_ref[pos], KEY_BITS)

    def first_at(bound):
        def narrow(_, ends):
            low, high = ends
            middle = lax.div(low + high, 2)
            below = id_at(middle) < bound
            return jnp.where(below, middle + 1, low), jnp.where(below, high, middle)

        return lax.fori_loop(0, KEY_BITS + 1, narrow, (jnp.int32(0), jnp.int32(tokens)))[0]

    low, high = first_at(base), first_at(base + rows_in(out_ref))
    pieces = sources[0].shape[0] // MOVE_ROWS
    moves = kinds * pieces
    lag = MOVE_SLOTS // 2
    steps = moves + MOVE_SLOTS

    reads, writes = Ring(moved, read_sems, True), Ring(moved, write_sems, False)

    def views(arrays, step):
        return [ref.at[rows_at(lax.rem(step, pieces) * MOVE_ROWS, MOVE_ROWS)] for ref in arrays]

    def move(step):
        @pl.when(step >= MOVE_SLOTS)
        def _():
            writes.wait(step, views(targets, step)[0])

        @pl.when(step < moves)
        def _():
            reads.start(step, lax.div(step, pieces), views(sources, step))

        ready = step - lag

        @pl.when((ready >= 0) & (ready < moves))
        def _():
            reads.wait(ready, views(sources, ready)[0])
            writes.start(ready, lax.div(ready, pieces), views(targets, ready))

    def row(pos):
        return pl.ds(pos, 1)

    def wait_slot(slot):
        pltpu.make_async_copy(rows_ref.at[row(0), :], out_ref.at[row(0), :], sems.at[slot]).wait()

    def row_of(pos):
        return row(lax.bitwise_and(keys_ref[pos], tokens - 1))

    def token(pos):
        return rows_ref[row_of(pos), :]

    def one_id(carry):
        pos, count = carry
        row_id = id_at(pos)
        first = row_of(pos)

        def more(carry):
            return id_at(carry[0]) == row_id

        def add(carry):
            start, total = carry
            end = start
            for k in range(AHEAD):
                same = id_at(start + k) == row_id
                total = total + jnp.where(same, token(start + k), 0.0)
                end = end + same.astype(jnp.int32)
            return end, total

        after, total = lax.while_loop(more, add, (pos + 1, token(pos)))

        @pl.when(after > pos + 1)
        def _():
            rows_ref[first, :] = total

        slot = lax.rem(count, SEMS)
        pl.when(count >= SEMS)(lambda: wait_slot(slot))
        pltpu.make_async_copy(rows_ref.at[first, :], out_ref.at[row(row_id - base), :], sems.at[slot]).start()
        return after, count + 1

    place[0] = low
    sent[0] = 0

    def step_body(step, carry):
        move(step)
        pl.when(step == 0)(load.wait)
        limit = low + lax.div((high - low) * (step + 1), steps)
        pos, count = lax.while_loop(lambda c: c[0] < limit, one_id, (place[0], sent[0]))
        place[0] = pos
        sent[0] = count
        return carry

    lax.fori_loop(0, steps, step_body, 0)
    count = sent[0]

    def drain(slot, carry):
        pl.when(slot < count)(lambda: wait_slot(slot))
        return carry

    lax.fori_loop(0, SEMS, drain, 0)


def put_rows(keys, rows, zeros, results):
    slots = DMA((MOVE_SLOTS,))
    counter = pltpu.SMEM((1,), jnp.int32)
    scratch = [pltpu.VMEM(rows.shape, F32), DMA, DMA((SEMS,)), pltpu.VMEM((MOVE_SLOTS, MOVE_ROWS, cols_of(rows)), F32), slots, slots, counter, counter]
    out_shape = [shape(*v.shape, F32) for v in (zeros, *results)]
    return local_call(put_body, "put_rows", out_shape, specs("shh") + [HBM] * len(results), [HBM] * len(out_shape), scratch, 20, {2: 0})(keys, rows, zeros, *results)


def move_body(*refs):
    half = len(refs) // 2
    for src, dst in zip(refs[:half], refs[half:]):
        dst[()] = src[()]


def move(*arrays):
    steps = SUBLANES // 2
    blocks = [pl.BlockSpec((rows_in(v) // steps, cols_of(v)), lambda i: (i, 0)) for v in arrays]
    return local_call(move_body, "move", [shape(*v.shape, F32) for v in arrays], blocks, blocks, [], 20, grid=(steps,))(*arrays)


Q_TILE = 256
K_TILE = 512


def as_column(row):
    return jnp.broadcast_to(row, (LANES, LANES)).T


def stack_heads(v):
    half = cols_of(v) // 2
    return jnp.concatenate([v[:, :half], v[:, half:]], axis=0)


def unstack_heads(v):
    half = rows_in(v) // 2
    return jnp.concatenate([v[:half], v[half:]], axis=1)


def sequence_chunks(cp):
    return [chunk * K_TILE for chunk in (cp, 3 - cp, 1 - cp, 2 + cp)]


class Tile:
    def __init__(self, q_ref, pos_ref, starts_ref):
        tile = pl.program_id(1)
        per_chunk = K_TILE // Q_TILE
        cp = lax.axis_index("cp")
        late = tile >= per_chunk
        self.chunks = sequence_chunks(cp)
        first = jnp.where(late, self.chunks[1], self.chunks[0]) + lax.rem(tile, per_chunk) * Q_TILE
        pos = jnp.concatenate([as_column(pos_ref[:, i : i + LANES])[:, :1] for i in range(0, Q_TILE, LANES)], axis=0)
        high = first + lax.broadcasted_iota(jnp.int32, pos.shape, 0)
        twice = lambda v: jnp.concatenate([v, v], axis=0)
        self.low, self.high = twice(high - pos), twice(high)
        self.q = stack_heads(q_ref[()])
        at = tile * Q_TILE
        ends = at + Q_TILE - 1
        lowest, highest = first - starts_ref[at], first + Q_TILE - 1 - starts_ref[ends]
        causal = (True, late, late | (cp == 1), late & (cp == 0))
        self.needed = [when & (chunk + K_TILE > lowest) for when, chunk in zip(causal, self.chunks)]
        self.free = [(chunk + K_TILE <= first + 1) & (highest <= chunk) for chunk in self.chunks]

    def visit(self, visit):
        for block, when in enumerate(self.needed):
            pl.when(when)(functools.partial(visit, block))

    def visit_scores(self, k_refs, visit):
        for block, (when, free) in enumerate(zip(self.needed, self.free)):
            (k,) = block_refs(block, k_refs)
            scores = lambda: lax.dot_general(self.q, k[()], NT, preferred_element_type=F32)
            pl.when(when & free)(lambda: visit(block, scores()))
            pl.when(when & jnp.logical_not(free))(lambda: visit(block, self.mask(scores(), block)))

    def mask(self, scores, block):
        at = self.chunks[block] + lax.broadcasted_iota(jnp.int32, (1, K_TILE), 1)
        return jnp.where((at >= self.low) & (at <= self.high), scores, NEG_BIG)


def block_refs(block, *pairs):
    rows = pl.ds((block % 2) * K_TILE, K_TILE)
    return [pair[block // 2].at[rows] for pair in pairs]


def attend_body(scale, starts_ref, q_ref, k_ref, v_ref, k2_ref, v2_ref, pos_ref, zeros_in, out_ref, lse_ref, grad_ref, s_ref, m_ref, l_ref, acc_ref, zero_ref, zero_sem):
    end_zeros = grid_zeros(grad_ref, zero_ref, zero_sem, "attend")
    tile = Tile(q_ref, pos_ref, starts_ref)
    power = scale * LOG2_E
    clear(m_ref, NEG_BIG)
    clear(l_ref)
    clear(acc_ref)

    def score(block, s):
        s_ref[block] = s
        m_ref[()] = jnp.maximum(m_ref[()], over_row(jnp.max, s))

    def exponent(block):
        e = jnp.exp2((s_ref[block] - m_ref[()]) * power)
        s_ref[block] = e
        l_ref[()] += over_row(jnp.sum, e)

    tile.visit_scores((k_ref, k2_ref), score)
    tile.visit(exponent)
    inverse = 1.0 / l_ref[()]

    def mix(block):
        (v,) = block_refs(block, (v_ref, v2_ref))
        prob = (s_ref[block] * inverse).astype(BF16)
        acc_ref[()] += jnp.dot(prob, v[()], preferred_element_type=F32)

    tile.visit(mix)
    out_ref[()] = unstack_heads(acc_ref[()].astype(BF16))
    lse_ref[()] = (m_ref[()] * power + jnp.log(l_ref[()]) * LOG2_E).reshape(lse_ref.shape)
    end_zeros()


def attention_specs(span, head_dim):
    tile = pl.BlockSpec((Q_TILE, 2 * head_dim), lambda h, t: (t, h))
    keys = pl.BlockSpec((span, head_dim), lambda h, t: (0, h))
    pos = pl.BlockSpec((1, Q_TILE), lambda h, t: (0, t))
    lse = pl.BlockSpec((1, 1, 2 * Q_TILE, 1), lambda h, t: (h, t, 0, 0))
    return tile, keys, pos, lse


def attention_buffers(heads):
    stacked = heads * Q_TILE
    return lambda c: pltpu.VMEM((stacked, c), F32), lambda dtype: pltpu.VMEM((4, stacked, K_TILE), dtype)


def attention_call(body, name, out_shape, in_specs, out_specs, scratch, gflops):
    aliases = {len(in_specs) - 1: len(out_specs) - 1}
    scratch = scratch + zero_scratch(out_shape[-1].shape[1])
    return local_call(body, name, out_shape, in_specs, out_specs, scratch, gflops, aliases, grid=(2, 4))


def attend(scale, starts, q, k, v, k2, v2, pos, grad):
    span = rows_in(q)
    heads = 2
    head_dim = cols_of(k) // heads
    tile, keys, pos_spec, lse = attention_specs(span, head_dim)
    stacked = heads * Q_TILE
    buf, probs = attention_buffers(heads)
    out_shape = [shape(*q.shape), jax.ShapeDtypeStruct((heads, span // Q_TILE, stacked, 1), F32), shape(*grad.shape, F32)]
    column = buf(1)
    scratch = [probs(F32), column, column, buf(head_dim)]
    call = attention_call(functools.partial(attend_body, scale), "attend", out_shape, [SMEM, tile] + [keys] * 4 + [pos_spec, HBM], [tile, lse, HBM], scratch, 14)
    return call(starts, q, k, v, k2, v2, pos, grad)


def attend_back_body(scale, starts_ref, q_ref, do_ref, lse_ref, k_ref, v_ref, k2_ref, v2_ref, pos_ref, zeros_in, dq_ref, dk_ref, dv_ref, dk2_ref, dv2_ref, grad_ref, p_ref, dp_ref, d_ref, acc_ref, zero_ref, zero_sem):
    end_zeros = grid_zeros(grad_ref, zero_ref, zero_sem, "attend_back")
    tile = Tile(q_ref, pos_ref, starts_ref)
    d_out = stack_heads(do_ref[()])
    lse = lse_ref[()].reshape(rows_in(d_out), 1)
    clear(d_ref)
    clear(acc_ref)

    @pl.when(pl.program_id(1) == 0)
    def _():
        for ref in (dk_ref, dv_ref, dk2_ref, dv2_ref):
            clear(ref)

    def first(block, s):
        (v,) = block_refs(block, (v_ref, v2_ref))
        p = jnp.exp2(s * (scale * LOG2_E) - lse)
        dp = lax.dot_general(d_out, v[()], NT, preferred_element_type=F32).astype(BF16)
        p_ref[block] = p
        dp_ref[block] = dp
        d_ref[()] += over_row(jnp.sum, p * dp.astype(F32))

    def second(block):
        k, dk, dv = block_refs(block, (k_ref, k2_ref), (dk_ref, dk2_ref), (dv_ref, dv2_ref))
        p = p_ref[block]
        ds = (p * (dp_ref[block].astype(F32) - d_ref[()]) * scale).astype(BF16)
        acc_ref[()] += jnp.dot(ds, k[()], preferred_element_type=F32)
        dk[()] += lax.dot_general(ds, tile.q, CONTRACT_FIRST, preferred_element_type=F32)
        dv[()] += lax.dot_general(p.astype(BF16), d_out, CONTRACT_FIRST, preferred_element_type=F32)

    tile.visit_scores((k_ref, k2_ref), first)
    tile.visit(second)
    dq_ref[()] = unstack_heads(acc_ref[()].astype(BF16))
    end_zeros()


def attend_back(scale, starts, q, d_out, lse, k, v, k2, v2, pos, grad):
    span = rows_in(q)
    heads = 2
    head_dim = cols_of(k) // heads
    tile, keys, pos_spec, lse_spec = attention_specs(span, head_dim)
    buf, probs = attention_buffers(heads)
    out_shape = [shape(*q.shape)] + [shape(*k.shape, F32)] * 4 + [shape(*grad.shape, F32)]
    in_specs = [SMEM, tile, tile, lse_spec] + [keys] * 4 + [pos_spec, HBM]
    call = attention_call(functools.partial(attend_back_body, scale), "attend_back", out_shape, in_specs, [tile] + [keys] * 4 + [HBM], [probs(F32), probs(BF16), buf(1), buf(head_dim)], 30)
    return call(starts, q, d_out, lse, k, v, k2, v2, pos, grad)


def remote(src, dst, send, recv, device):
    return pltpu.make_async_remote_copy(src_ref=src, dst_ref=dst, send_sem=send, recv_sem=recv, device_id=device, device_id_type=MESH_ID)


def flipped(bit, flip):
    return bit + flip - 2 * bit * flip


class Place:
    def __init__(self):
        self.tp = lax.axis_index("tp")
        self.cp = lax.axis_index("cp")
        self.x = lax.rem(self.tp, 2)
        self.y = lax.div(self.tp, 2)
        self.over_x = (self.chip(1, 0), self.cp)
        self.over_y = (self.chip(0, 1), self.cp)
        self.twin = (self.tp, 1 - self.cp)

    def chip(self, dx, dy):
        return 2 * flipped(self.y, dy) + flipped(self.x, dx)

    def meet(self):
        barrier = pltpu.get_barrier_semaphore()
        peers = (self.over_x, self.over_y, self.twin)
        for device in peers:
            pl.semaphore_signal(barrier, inc=1, device_id=device, device_id_type=MESH_ID)
        pl.semaphore_wait(barrier, len(peers))


class Total:
    def __init__(self, place, part, wide, mid, narrow, out, send, recv, source=None):
        self.source = source or part
        self.part, self.wide, self.mid, self.narrow, self.out = part, wide, mid, narrow, out
        self.send, self.recv = send, recv
        self.rows = rows_in(out) // STEPS
        self.half, self.quarter, self.eighth = (self.rows // n for n in (2, 4, 8))
        self.kinds = [(place.x, place.y, place.over_x, place.over_y), (place.y, place.x, place.over_y, place.over_x)]

    def _rows(self, step, kind):
        first, second = self.kinds[kind][:2]
        side = step * self.rows + kind * self.half + first * self.quarter
        return rows_at(side, self.quarter), rows_at(side + second * self.eighth, self.eighth)

    def _kept(self, kind, flip=0):
        return rows_at(kind * self.half + flipped(self.kinds[kind][0], flip) * self.quarter, self.quarter)

    def _eighth(self, kind, flip=0):
        return rows_at(flipped(self.kinds[kind][1], flip) * self.eighth, self.eighth)

    def _copy(self, step, kind, stage):
        side, mine = self._rows(step, kind)
        _, _, peer_first, peer_second = self.kinds[kind]
        src, dst, peer = (
            lambda: (self.source(step).at[self._kept(kind, 1)], self.wide.at[step, kind], peer_first),
            lambda: (self.mid.at[step, kind, self._eighth(kind, 1)], self.narrow.at[step, kind], peer_second),
            lambda: (self.out.at[mine], self.out.at[mine], peer_second),
            lambda: (self.out.at[side], self.out.at[side], peer_first),
        )[stage]()
        return remote(src, dst, self.send.at[step, kind, stage], self.recv.at[step, kind, stage], peer)

    def begin(self, step):
        for kind in BOTH:
            self._copy(step, kind, 0).start()

    def fold_wide(self, step):
        for kind in BOTH:
            self._copy(step, kind, 0).wait_recv()
            self.mid[step, kind] = self.part(step)[self._kept(kind), :] + self.wide[step, kind]
            self._copy(step, kind, 1).start()

    def fold_narrow(self, step):
        for kind in BOTH:
            self._copy(step, kind, 1).wait_recv()
            total = self.mid[step, kind, self._eighth(kind), :] + self.narrow[step, kind]
            self.out[self._rows(step, kind)[1], :] = total.astype(BF16)
            self._copy(step, kind, 2).start()

    def widen(self, step):
        for kind in BOTH:
            self._copy(step, kind, 2).wait_recv()
            self._copy(step, kind, 3).start()

    def finish(self, step):
        for kind in BOTH:
            self._copy(step, kind, 3).wait_recv()

    def sent(self, step, stages):
        for kind in BOTH:
            for stage in stages:
                self._copy(step, kind, stage).wait_send()


def sems(*dims):
    return DMA((*dims, 3))


def total_scratch(width, dtype, rows):
    stages = DMA((STEPS, 2, 4))
    part = lambda n: pltpu.VMEM((STEPS, 2, rows // n, width), dtype)
    return [part(4), part(4), part(8), stages, stages]


class Share:
    def __init__(self, place, sems, span):
        self.place, self.sems, self.first = place, sems, place.cp * span

    def pair(self, k, src, dst, start):
        here_sem, send, recv = (self.sems.at[k, i] for i in range(3))
        at = dst.at[rows_at(self.first + start, rows_in(src))]
        return pltpu.make_async_copy(src, at, here_sem), remote(src, at, send, recv, self.place.twin)

    def begin(self, *numbered):
        for copy in self.pair(*numbered):
            copy.start()

    def sent(self, *numbered):
        here, there = self.pair(*numbered)
        here.wait()
        there.wait_send()

    def got(self, k, src, dst, start):
        at = dst.at[rows_at(self.first + start, rows_in(src))]
        remote(src, at, *(self.sems.at[k, i] for i in (1, 2)), self.place.twin).wait_recv()


class Loads:
    def __init__(self, sems, *names):
        self.sems, self.names = sems, list(names)

    def _copies(self, moves):
        self.names += [name for name in moves if name not in self.names]
        return [pltpu.make_async_copy(src, dst, self.sems.at[self.names.index(name)]) for name, (src, dst) in moves.items()]

    def start(self, **moves):
        for copy in self._copies(moves):
            copy.start()
        return lambda: self.wait(**moves)

    def wait(self, **moves):
        for copy in self._copies(moves):
            copy.wait()


def steps(visit):
    def body(step, carry):
        visit(step)
        return carry

    lax.fori_loop(0, STEPS, body, 0)


def rope(v, cosine, sine):
    wide = cols_of(cosine)
    heads = []
    for h in range(cols_of(v) // wide):
        part = v[:, h * wide : (h + 1) * wide]
        turned = jnp.concatenate([part[:, wide // 2 :], part[:, : wide // 2]], axis=1)
        heads.append(part * cosine + turned * sine)
    return jnp.concatenate(heads, axis=1)


def each(count, size, visit):
    def body(i, carry):
        visit(pl.multiple_of(i * size, size))
        return carry

    lax.fori_loop(0, count // size, body, 0)


def col_loop(cols, tile, visit):
    each(cols, tile, lambda start: visit(pl.ds(start, tile)))


def dot_nt(a, b):
    return lax.dot_general(a, b, NT, preferred_element_type=F32)


def dot(a, b):
    return jnp.dot(a, b, preferred_element_type=F32)


def as_row(gain):
    return gain[()].astype(F32)[None, :]


def norm_block(feats):
    inverse = lax.rsqrt(over_row(jnp.mean, feats * feats) + NORM_EPS)
    return feats * inverse, inverse


def norm_back(d_act, gain, normed, inverse):
    d_normed = d_act * gain
    return inverse * (d_normed - normed * over_row(jnp.mean, d_normed * normed))


def remote_call(body, collective_id, name, out_shape, in_places, out_places, scratch, gflops):
    return pl.pallas_call(
        body,
        out_shape=out_shape,
        in_specs=specs(in_places),
        out_specs=specs(out_places),
        scratch_shapes=scratch,
        compiler_params=pltpu.CompilerParams(collective_id=collective_id, has_side_effects=True, vmem_limit_bytes=REMOTE_VMEM),
        cost_estimate=cost(gflops, 60),
        name=name,
    )


def join_columns(parts, whole):
    start, moves = 0, {}
    for i, part in enumerate(parts):
        moves[f"join{i}"] = (part, whole.at[:, pl.ds(start, cols_of(part))])
        start += cols_of(part)
    return moves


def order_ids(cp, ids, ids_got, keys, tall, rank, keys_out):
    span = cols_of(ids)
    chunks = rows_in(keys)
    lane = lax.broadcasted_iota(jnp.int32, (1, LANES), 1)
    for core, src in ((cp, ids), (1 - cp, ids_got)):
        for c in range(span // LANES):
            start = c * LANES
            token = core * span + start + lane
            keys[core * (chunks // 2) + c] = lax.shift_left(src[:, start : start + LANES], KEY_BITS) + token

    def count(a, carry):
        mine = as_column(keys[a])
        tall[a] = mine
        rank[a] = over_row(jnp.sum, sum((keys[b] < mine).astype(F32) for b in range(chunks)))
        return carry

    def place(c, carry):
        goal = (c * LANES + lane).astype(F32)
        keys_out[rows_at(c * LANES, LANES, LANES)] = over_column(sum(jnp.where(rank[a] == goal, tall[a], 0) for a in range(chunks)))[0]
        return carry

    lax.fori_loop(0, chunks, count, 0)
    lax.fori_loop(0, chunks, place, 0)
    keys_out[pl.ds(chunks * LANES, LANES)] = jnp.full((LANES,), jnp.iinfo(jnp.int32).max, jnp.int32)


def enter_body(picked_in, wq_in, wk_in, wv_in, gain, pos, inv_freq, ids, dy_in, wd_in, x_rows, q_out, k_out, v_out, cosine, sine, keys_out, dh_out, k2_out, v2_out, act_all, dy_all, wide, mid, narrow, send, recv, picked, x_out, act, dy, wd, dh, w_all, ids_got, keys, tall, rank, pair_sems, share_sems, load_sems, ids_sems):
    place = Place()
    place.meet()
    span = rows_in(x_out)
    rows = span // STEPS
    chunk = lambda step: rows_at(step * rows, rows)
    total = Total(place, lambda step: picked.at[chunk(step)], wide, mid, narrow, x_out, send, recv, lambda step: picked_in.at[chunk(step)])
    share = Share(place, share_sems, span)
    loads = Loads(load_sems)
    steps(total.begin)
    ids_swap = remote(ids, ids_got, *(ids_sems.at[end] for end in BOTH), place.twin)
    ids_swap.start()
    loaded = loads.start(picked=(picked_in, picked), dy=(dy_in, dy), wd=(wd_in, wd))
    projection = loads.start(**join_columns((wq_in, wk_in, wv_in), w_all))
    kw = cols_of(k_out)
    qw = cols_of(q_out)

    def back(step):
        here = chunk(step)

        def tile(cols):
            dh[here, cols] = dot_nt(dy[here, :], wd[cols, :]).astype(BF16)

        col_loop(rows_in(wd), WIDE_TILE, tile)
        total.fold_wide(step)

    def pairs(step):
        return [remote(src.at[chunk(step)], dst.at[chunk(step)], *(pair_sems.at[step, i, end] for end in BOTH), place.twin) for i, (src, dst) in enumerate(((k_out, k2_out), (v_out, v2_out)))]

    x_kept = lambda step: dict(x=(x_out.at[chunk(step)], x_rows.at[chunk(step)]))
    act_share = lambda step: (1 + step, act.at[chunk(step)], act_all, step * rows)

    def project(step):
        total.finish(step)
        here = chunk(step)
        pl.when(step >= 1)(lambda: loads.wait(**x_kept(step - 1)))
        loads.start(**x_kept(step))

        def norm(start):
            at = rows_at(step * rows + start, ROW_BLOCK)
            normed, _ = norm_block(x_out[at, :].astype(F32))
            act[at, :] = (normed * as_row(gain)).astype(BF16)

        each(rows, ROW_BLOCK, norm)
        share.begin(*act_share(step))
        c, s = cosine[here, :], sine[here, :]
        out = dot(act[here, :], w_all[()])
        q_out[here, :] = rope(out[:, :qw], c, s).astype(BF16)
        k_out[here, :] = rope(out[:, qw : qw + kw], c, s).astype(BF16)
        v_out[here, :] = out[:, qw + kw :].astype(BF16)
        for copy in pairs(step):
            copy.start()

    def angles(start):
        at = pl.ds(start, LANES)
        angle = as_column(pos[:, at])[:, : cols_of(inv_freq)].astype(F32) * inv_freq[()]
        c, s = jnp.cos(angle), jnp.sin(angle)
        cosine[at, :] = jnp.concatenate([c, c], axis=1)
        sine[at, :] = jnp.concatenate([-s, s], axis=1)

    loaded()
    dy_share = (0, dy, dy_all, 0)
    share.begin(*dy_share)
    each(span, LANES, angles)
    steps(back)
    stored = loads.start(dh=(dh, dh_out))
    ids_swap.wait()
    order_ids(place.cp, ids, ids_got, keys, tall, rank, keys_out)
    steps(total.fold_narrow)
    steps(total.widen)
    projection()
    steps(project)

    def close(step):
        total.sent(step, range(4))
        share.sent(*act_share(step))
        share.got(*act_share(step))
        for copy in pairs(step):
            copy.wait()

    steps(close)
    share.sent(*dy_share)
    share.got(*dy_share)
    loads.wait(**x_kept(STEPS - 1))
    stored()


def enter(picked, wq, wk, wv, gain, pos, inv_freq, ids, dy, wd):
    span, width = picked.shape
    key = shape(span, cols_of(wk))
    angles = shape(span, 2 * cols_of(inv_freq), F32)
    all_rows = shape(2 * span, width)
    chunks = 2 * span // LANES
    int_buf = lambda *dims: pltpu.VMEM(dims, jnp.int32)
    big = pltpu.VMEM((span, width), BF16)
    out_shape = [shape(span, width), shape(span, cols_of(wq)), key, key, angles, angles, jax.ShapeDtypeStruct(((chunks + SUBLANES) * LANES,), jnp.int32), shape(span, rows_in(wd)), key, key, all_rows, all_rows]
    scratch = total_scratch(width, BF16, span // STEPS) + [big, big, big, big, pltpu.VMEM(wd.shape, BF16), pltpu.VMEM((span, rows_in(wd)), BF16), pltpu.VMEM((width, cols_of(wq) + 2 * cols_of(wk)), BF16)]
    scratch += [int_buf(1, span), int_buf(chunks, 1, LANES), int_buf(chunks, LANES, LANES), pltpu.VMEM((chunks, LANES, 1), F32)]
    scratch += [DMA((STEPS, 2, 2)), sems(STEPS + 1), DMA((8,)), DMA((2,))]
    call = remote_call(enter_body, 1, "enter", out_shape, "hhhhvvvvhh", "hvvvvvvhhhhh", scratch, 80)
    return call(picked, wq, wk, wv, gain, pos, inv_freq, ids, dy, wd)


def middle_body(att, wo_own, wo_1, wo_2, wo_3, x_in, wg_in, wu_in, wd_in, dh_in, dy_in, gain, h_out, keep_x, send_x, keep_y, send_y, b_all, hidden_all, dgate_all, dup_all, att_all, drb_all, dr_out, datt_out, dgain_out,
                wide, mid, narrow, send, recv, wo, wg, wu, att_full, part_buf, d_b, h, row_in, dh, b, hid, dgt, dup, att_send, att_recv, wo_sems, load_sems, share_sems):
    place = Place()
    span, width = x_in.shape
    rows = span // STEPS
    half = rows // 2
    cols = cols_of(att)
    ffn = cols_of(wg)
    loads = Loads(load_sems, "att", "wo", "wg", "wu", "rows", "dh", "h_out", "h_in", "hid", "dr", "y")
    chunk = lambda step: rows_at(step * rows, rows)
    by_chip = lambda tp: rows_at(tp * cols, cols, 128)

    mine = loads.start(att=(att, att_full.at[:, by_chip(place.tp)]), wo=(wo_own, wo.at[by_chip(place.tp)]))
    place.meet()

    x_tp, y_tp = place.over_x[0], place.over_y[0]

    def att_copy(step, kind, hop):
        at = rows_at(step * rows + kind * half, half)
        first, second = ((place.over_y, place.over_x), (place.over_x, place.over_y))[kind]
        relay = hop == 2
        dst = att_full.at[at, by_chip(first[0] if relay else place.tp)]
        return remote(dst if relay else att.at[at], dst, att_send.at[step, kind, hop], att_recv.at[step, kind, hop], second if hop else first)

    def att_begin(step):
        for hop in BOTH:
            for kind in BOTH:
                att_copy(step, kind, hop).start()

    def att_forward(step):
        for kind in BOTH:
            att_copy(step, kind, 0).wait_recv()
            att_copy(step, kind, 2).start()

    att_begin(0)
    part = rows_in(wo_1)
    arrivals = []
    near = jnp.where(place.cp == 0, y_tp, x_tp)
    chips = (near, x_tp + y_tp - near, place.chip(1, 1))
    for i, (src, chip) in enumerate(zip((wo_1, wo_2, wo_3), chips)):
        at = wo.at[rows_at((2 * chip + place.cp) * part, part, 128)]
        here_sem, send_sem, recv_sem = (wo_sems.at[i, end] for end in range(3))
        for copy in (pltpu.make_async_copy(src, at, here_sem), remote(src, at, send_sem, recv_sem, place.twin)):
            copy.start()
            arrivals.append(copy)
    att_begin(1)
    weights = loads.start(wg=(wg_in, wg), wu=(wu_in, wu))

    share = Share(place, share_sems, span)
    att_share = (0, att, att_all, 0)
    share.begin(*att_share)
    total = Total(place, lambda step: part_buf.at[step], wide, mid, narrow, d_b, send, recv)

    def numbered(i, src, dst, step):
        return 1 + len(shares) * step + i, src, dst, step * rows

    shares = ((b, b_all), (hid, hidden_all), (dgt, dgate_all), (dup, dup_all))
    forward_shares = list(enumerate(shares))
    fetched = lambda step: dict(rows=(x_in.at[chunk(step)], row_in), dh=(dh_in.at[chunk(step)], dh))
    h_kept = lambda step: dict(h_out=(h, h_out.at[chunk(step)]))

    def close(step):
        loads.wait(**h_kept(step))
        for i, pair in forward_shares:
            share.sent(*numbered(i, *pair, step))

    def forward(step):
        pl.when(step >= 1)(lambda: close(step - 1))
        loads.wait(**fetched(step))
        for kind in BOTH:
            for hop in (1, 2):
                att_copy(step, kind, hop).wait_recv()

        def residual(c):
            h[:, c] = row_in[:, c].astype(F32) + dot(att_full[chunk(step), :], wo[:, c])

        col_loop(width, BIG_TILE, residual)
        loads.start(**h_kept(step))

        def norm(start):
            at = pl.ds(start, ROW_BLOCK)
            normed, _ = norm_block(h[at, :])
            b[at, :] = (normed * as_row(gain)).astype(BF16)

        each(rows, ROW_BLOCK, norm)
        share.begin(*numbered(0, b, b_all, step))
        pl.when(step == 0)(weights)

        def hidden(c):
            gate = dot(b[()], wg[:, c])
            up = dot(b[()], wu[:, c])
            sig = 1.0 / (1.0 + jnp.exp(-gate))
            d_hid = dh[:, c].astype(F32)
            act = gate * sig
            hid[:, c] = (act * up).astype(BF16)
            dgt[:, c] = (d_hid * up * sig * (1.0 + gate * (1.0 - sig))).astype(BF16)
            dup[:, c] = (d_hid * act).astype(BF16)

        col_loop(ffn, WIDE_TILE, hidden)
        for i, pair in forward_shares[1:]:
            share.begin(*numbered(i, *pair, step))
        pl.when(step == 0)(lambda: att_forward(2))

        @pl.when(step + 1 < STEPS)
        def _():
            loads.start(**fetched(step + 1))

        def back(c):
            part_buf[step, :, c] = dot_nt(dgt[()], wg[c, :]) + dot_nt(dup[()], wu[c, :])

        col_loop(width, BIG_TILE, back)
        total.begin(step)
        pl.when(step == 0)(lambda: att_forward(3))
        pl.when(step >= 2)(lambda: total.fold_wide(step - 2))

    loads.start(**fetched(0))
    att_forward(0)
    for step in range(2, STEPS):
        att_begin(step)
    mine()
    for copy in arrivals:
        copy.wait()
    att_forward(1)
    steps(forward)
    clear(dgain_out)
    close(STEPS - 1)
    wd = wg
    weights = loads.start(wg=(wd_in, wd))
    d_r, y_buf = part_buf.at[0], part_buf.at[1]

    h_back = lambda step: dict(h_in=(h_out.at[chunk(step)], h))
    hidden_back = lambda step: dict(hid=(hidden_all.at[rows_at(place.cp * span + step * rows, rows)], hid))
    dy_back = lambda step: dict(rows=(dy_in.at[chunk(step)], row_in))
    y_kept = dict(y=(y_buf, keep_x))
    for step in BOTH:
        total.sent(step, (0,))
    loads.start(**h_back(0), **hidden_back(0))

    def output(step):
        pl.when(step < 2)(lambda: total.fold_wide(step + 2))
        loads.wait(**h_back(step), **hidden_back(step))
        pl.when(step == 0)(weights)
        pl.when(step >= 1)(lambda: loads.wait(**y_kept))
        over_x_first = step < 2
        first = jnp.where(over_x_first, place.x, place.y)
        second = place.x + place.y - first
        kept = first == lax.rem(step, 2)
        row = lax.broadcasted_iota(jnp.int32, (rows, 1), 0)
        owner = kept & (lax.div(row, half) == second)

        def tile(c):
            y_buf[:, c] = dot(hid[()], wd[:, c]) + jnp.where(owner, h[:, c], 0.0)

        col_loop(width, BIG_TILE, tile)
        for side_first, keep, send_to in ((over_x_first, keep_x, send_x), (jnp.logical_not(over_x_first), keep_y, send_y)):
            for chosen, dst in ((kept, keep), (jnp.logical_not(kept), send_to)):

                @pl.when(side_first & chosen)
                def _():
                    loads.start(y=(y_buf, dst))

        @pl.when(step + 1 < STEPS)
        def _():
            loads.start(**h_back(step + 1), **hidden_back(step + 1))

        total.fold_narrow(step)
        pl.when(step >= 2)(lambda: total.widen(step - 2))

    steps(output)
    loads.start(**h_back(0), **dy_back(0))
    kept_rows = lambda step: dict(dr=(d_r, dr_out.at[chunk(step)]))

    def resid_share(step, part):
        return 1 + len(shares) * STEPS + 2 * step + part, b.at[rows_at(part * half, half)], drb_all, step * rows + part * half

    def resid_sent(step):
        loads.wait(**kept_rows(step))
        for part in BOTH:
            share.sent(*resid_share(step, part))

    def resid(step):
        pl.when(step < 2)(lambda: total.widen(step + 2))
        total.finish(step)
        loads.wait(**h_back(step), **dy_back(step))
        pl.when(step >= 1)(lambda: resid_sent(step - 1))

        for part in BOTH:

            def grad(start):
                start = part * half + start
                at = rows_at(start, ROW_BLOCK)
                normed, inverse = norm_block(h[at, :])
                d_act = d_b[rows_at(step * rows + start, ROW_BLOCK), :].astype(F32)
                dgain_out[()] += over_column(d_act * normed)
                out = row_in[at, :].astype(F32) + norm_back(d_act, as_row(gain), normed, inverse)
                d_r[at, :] = out
                b[at, :] = out.astype(BF16)

            each(half, ROW_BLOCK, grad)
            share.begin(*resid_share(step, part))

        @pl.when(step + 1 < STEPS)
        def _():
            loads.start(**h_back(step + 1), **dy_back(step + 1))

        loads.start(**kept_rows(step))
        datt_out[chunk(step), :] = dot_nt(b[()], wo[by_chip(place.tp), :]).astype(BF16)

    steps(resid)
    loads.wait(**y_kept)
    resid_sent(STEPS - 1)
    share.sent(*att_share)
    share.got(*att_share)

    def finish(step):
        total.sent(step, range(1, 4))
        pl.when(step >= 2)(lambda: total.sent(step, (0,)))
        for kind in BOTH:
            for hop in range(3):
                att_copy(step, kind, hop).wait_send()
        for i, pair in forward_shares:
            share.got(*numbered(i, *pair, step))
        for part in BOTH:
            share.got(*resid_share(step, part))

    steps(finish)


def middle(att, wo_pieces, x, wg, wu, wd, d_hidden, dy, gain):
    span, width = x.shape
    rows = span // STEPS
    ffn = cols_of(wg)
    cols = cols_of(att)
    full = shape(span, width, F32)
    both = shape(2 * span, ffn)
    out_shape = [full] + [shape(rows, width, F32)] * 4 + [shape(2 * span, width), both, both, both, shape(2 * span, cols), shape(2 * span, width), full, shape(span, cols), shape(1, width, F32)]
    buf = lambda r, c, dtype=BF16: pltpu.VMEM((r, c), dtype)
    scratch = total_scratch(width, F32, rows)
    scratch += [buf(width, width), buf(width, ffn), buf(width, ffn), buf(span, width), pltpu.VMEM((STEPS, rows, width), F32), buf(span, width), buf(rows, width, F32)]
    scratch += [buf(rows, c) for c in (width, ffn, width, ffn, ffn, ffn)]
    scratch += [sems(STEPS, 2), sems(STEPS, 2), sems(3), DMA((11,)), sems(1 + 6 * STEPS)]
    call = remote_call(middle_body, 2, "middle", out_shape, "vhhhhhhhhhhv", "hhhhhhhhhhhhvv", scratch, 120)
    return call(att, *wo_pieces, x, wg, wu, wd, d_hidden, dy, gain)


def leave_body(dq_in, dk_in, dv_in, dk2_in, dv2_in, cosine, sine, wq_in, wk_in, wv_in, x_in, dr_in, gain, dgain_b, b_all, dgate_all, dup_all, hidden_all, dy_all, att_all, drb_all, act_all, d_all, dx_all, gain_a_out, gain_b_out, grad_gate, grad_up, grad_down, grad_out, grad_q, grad_k, grad_v,
               wide, mid, narrow, send, recv, part_buf, d_a, dk_got, dv_got, d_qkv, w_all, xs, drs, dxs, gain_got, left, right, result, pair_sems, load_sems, share_sems, left_sems, right_sems, result_sems, result_arrivals):
    place = Place()
    place.meet()
    span, width = x_in.shape
    rows = span // STEPS
    chunk = lambda step: rows_at(step * rows, rows)
    swap = lambda i, src, dst: remote(src, dst, *(pair_sems.at[i, end] for end in BOTH), place.twin)
    pairs = lambda step: [swap(2 * step + i, src.at[chunk(step)], dst.at[chunk(step)]) for i, (src, dst) in enumerate(((dk2_in, dk_got), (dv2_in, dv_got)))]
    for step in range(STEPS):
        for copy in pairs(step):
            copy.start()
    qw = cols_of(dq_in)
    kw = cols_of(dk_in)
    share = Share(place, share_sems, span)
    loads = Loads(load_sems)
    total = Total(place, lambda step: part_buf.at[step], wide, mid, narrow, d_a, send, recv)

    def partial(step):
        here = chunk(step)
        c, s = cosine[here, :], -sine[here, :]
        for copy in pairs(step):
            copy.wait()
        d_qkv[here, :qw] = rope(dq_in[here, :].astype(F32), c, s).astype(BF16)
        dk_sum = (dk_in[here, :] + dk_got[here, :]).astype(BF16).astype(F32)
        d_qkv[here, qw : qw + kw] = rope(dk_sum, c, s).astype(BF16)
        d_qkv[here, qw + kw :] = (dv_in[here, :] + dv_got[here, :]).astype(BF16)

        def tile(n):
            part_buf[step, :, n] = dot_nt(d_qkv[here, :], w_all[n, :])

        col_loop(width, BIG_TILE, tile)
        total.begin(step)

    rows_back = lambda step: dict(x=(x_in.at[chunk(step)], xs), dr=(dr_in.at[chunk(step)], drs))

    clear(gain_a_out)

    def dx_share(step, part):
        start = part * part_rows
        return 1 + 2 * step + part, dxs.at[rows_at(start, part_rows)], dx_all, step * rows + start

    part_rows = rows // 2

    def grad_x(step):
        for part in BOTH:

            def grad(start):
                start = part * part_rows + start
                at = rows_at(start, ROW_BLOCK)
                normed, inverse = norm_block(xs[at, :].astype(F32))
                d_act = d_a[rows_at(step * rows + start, ROW_BLOCK), :].astype(F32)
                gain_a_out[()] += over_column(d_act * normed)
                dxs[at, :] = drs[at, :] + norm_back(d_act, as_row(gain), normed, inverse)

            pl.when(step >= 1)(lambda: share.sent(*dx_share(step - 1, part)))
            each(part_rows, ROW_BLOCK, grad)
            share.begin(*dx_share(step, part))

    _, _, narrow_cols = left.shape
    _, _, wide_cols = right.shape
    lefts, rights = Ring(left, left_sems, True), Ring(right, right_sems, True)
    sides, per_core = width // wide_cols, width // narrow_cols // 2
    whole = (grad_gate, grad_up, grad_down, grad_out)
    ffn_blocks = (len(whole) - 1) * sides
    ffn_tiles = ffn_blocks * per_core
    tiles = ffn_tiles + 1 + per_core
    block_of = lambda t: jnp.where(t < ffn_tiles, lax.div(t, per_core), jnp.minimum(t - ffn_tiles, 1) + ffn_blocks)
    row_of = lambda t: place.cp * per_core + jnp.where(t < ffn_tiles, lax.rem(t, per_core), jnp.maximum(t - ffn_tiles - 1, 0))
    at_left = lambda t: rows_at(row_of(t) * narrow_cols, narrow_cols, TILE)
    at_right = lambda j: rows_at(jnp.where(j < ffn_blocks, lax.rem(j, sides), place.cp) * wide_cols, wide_cols, TILE)
    kind_of = lambda j: jnp.where(j < ffn_blocks, lax.div(j, sides), len(whole) - 1 + j - ffn_blocks)
    left_start = lambda t: lefts.start(t, kind_of(block_of(t)), [ref.at[:, at_left(t)] for ref in (b_all, b_all, hidden_all)] + [att_all, act_all.at[:, at_left(t)]])
    right_start = lambda j: rights.start(j, kind_of(j), [ref.at[:, at_right(j)] for ref in (dgate_all, dup_all, dy_all, drb_all)] + [d_all])

    def to_twin(t, src, dst):
        return remote(src, dst, result_sems.at[lefts.slot(t), 1], result_arrivals.at[t], place.twin)

    def stored(t):
        done = result.at[lefts.slot(t)]
        pltpu.make_async_copy(done, done, result_sems.at[lefts.slot(t), 0]).wait()
        to_twin(t, done, done).wait_send()

    def store(t):
        slot = lefts.slot(t)
        j = block_of(t)

        def put(cols, dst):
            src = result.at[slot, :, cols]
            pltpu.make_async_copy(src, dst, result_sems.at[slot, 0]).start()
            to_twin(t, src, dst).start()

        everything = pl.ds(0, wide_cols)
        for k, ref in enumerate(whole):
            at = at_left(t) if ref is not grad_out else pl.ds(0, narrow_cols)
            pl.when(kind_of(j) == k)(lambda: put(everything, ref.at[at, at_right(j)]))

        @pl.when(j == ffn_blocks + 1)
        def _():
            put(pl.ds(0, qw), grad_q.at[at_left(t)])
            put(pl.ds(qw, kw), grad_k.at[at_left(t)])
            put(pl.ds(qw + kw, kw), grad_v.at[at_left(t)])

    def tile_step(t, carry):
        j = block_of(t)
        pl.when(t + 1 < tiles)(lambda: left_start(t + 1))

        @pl.when(jnp.where(t < ffn_tiles, lax.rem(t, per_core) == 0, t <= ffn_tiles + 1))
        def _():
            pl.when(j < ffn_blocks)(lambda: right_start(j + 1))
            rights.wait(j, d_all)

        lefts.wait(t, att_all)
        pl.when(t >= 2)(lambda: stored(t))
        slot = lefts.slot(t)
        result[slot] = lax.dot_general(left[slot], right[rights.slot(j)], CONTRACT_FIRST, preferred_element_type=F32)
        store(t)
        return carry

    left_start(jnp.int32(0))
    right_start(jnp.int32(0))
    weights = loads.start(**join_columns((wq_in, wk_in, wv_in), w_all))
    loads.start(**rows_back(0))
    weights()
    steps(partial)
    d_here, d_there = share.pair(0, d_qkv, d_all, 0)
    d_here.start()
    d_there.start()

    stages = (total.fold_wide, total.fold_narrow, total.widen)
    waits = len(stages) * STEPS
    portion = ffn_tiles // STEPS
    tiles_until = lambda p: jnp.where(p < STEPS, portion * (p + 1), jnp.where(p < 2 * STEPS - 1, ffn_tiles, jnp.where(p < waits - 1, ffn_tiles + 1, tiles)))

    def wait_step(p, carry):
        @pl.when(p == waits - 1)
        def _():
            d_here.wait()
            d_there.wait_recv()
            right_start(jnp.int32(ffn_blocks + 1))

        lax.fori_loop(jnp.where(p == 0, 0, tiles_until(p - 1)), tiles_until(p), tile_step, 0)
        for k, stage in enumerate(stages):
            pl.when(lax.div(p, STEPS) == k)(lambda: stage(lax.rem(p, STEPS)))
        return carry

    lax.fori_loop(0, waits, wait_step, 0)
    def last_stage(step):
        loads.wait(**rows_back(step))
        total.finish(step)
        grad_x(step)

        @pl.when(step + 1 < STEPS)
        def _():
            loads.start(**rows_back(step + 1))

    steps(last_stage)
    gains = ((gain_a_out, gain_a_out), (dgain_b, gain_b_out))
    swaps = [swap(2 * STEPS + i, mine, gain_got.at[i]) for i, (mine, _) in enumerate(gains)]
    for copy in swaps:
        copy.start()
    for copy in swaps:
        copy.wait()
    for i, (mine, out) in enumerate(gains):
        out[()] = mine[()] + gain_got[i]
    for part in BOTH:
        share.sent(*dx_share(STEPS - 1, part))
    d_there.wait_send()
    for t in range(tiles - 2, tiles):
        stored(t)
    done = result.at[0]
    for t in range(tiles):
        to_twin(t, done, done).wait_recv()

    def close(step):
        total.sent(step, range(4))
        for part in BOTH:
            share.got(*dx_share(step, part))

    steps(close)


def leave(dq, dk, dv, dk2, dv2, cosine, sine, wq, wk, wv, x, d_resid, gain, dgain_b, *products):
    span, width = x.shape
    rows = span // STEPS
    kw = cols_of(wk)
    qw = cols_of(wq)
    cols = qw + 2 * kw
    ffn = products[1].shape[1]
    buf = lambda r, c, dtype=F32: pltpu.VMEM((r, c), dtype)
    gain_grad = shape(1, width, F32)
    out_shape = [shape(2 * span, cols), shape(2 * span, width, F32), gain_grad, gain_grad]
    out_shape += [shape(*dims, F32) for dims in ((width, ffn), (width, ffn), (ffn, width), (qw, width), wq.shape, wk.shape, wv.shape)]
    twice = lambda r, c, dtype: pltpu.VMEM((2, r, c), dtype)
    scratch = total_scratch(width, F32, rows) + [pltpu.VMEM((STEPS, rows, width), F32), buf(span, width, BF16), buf(span, kw), buf(span, kw), buf(span, cols, BF16), buf(width, cols, BF16)]
    scratch += [buf(rows, width, BF16), buf(rows, width), buf(rows, width), pltpu.VMEM((2, 1, width), F32)]
    scratch += [twice(2 * span, WIDE_TILE, BF16), twice(2 * span, BIG_TILE, BF16), twice(WIDE_TILE, BIG_TILE, F32)]
    ring = DMA((2,))
    scratch += [DMA((2 * STEPS + 2, 2)), DMA((5,)), sems(1 + 2 * STEPS), ring, ring, DMA((2, 2)), DMA((MAX_TILES,))]
    call = remote_call(leave_body, 3, "leave", out_shape, "vvvhhvvhhhhhvvhhhhhhhh", "hhvvhhhhhhh", scratch, 1)
    return call(dq, dk, dv, dk2, dv2, cosine, sine, wq, wk, wv, x, d_resid, gain, dgain_b, *products)


def side(v, bit):
    half = rows_in(v) // 2
    return lax.dynamic_slice_in_dim(v, bit * half, half, 0)


def join(own, other, bit):
    return jnp.where(bit == 0, jnp.concatenate([own, other]), jnp.concatenate([other, own]))


def solution(mesh):
    def device_step(tokens, pos, doc_id, dy, table, w_q, w_k, w_v, w_o, w_gate, w_up, w_down, gain_one, gain_two, inv_freq):
        span = rows_in(tokens)
        rows, width = table.shape
        scale = (2 * rows_in(inv_freq)) ** -0.5
        tp = lax.axis_index("tp")
        cp = lax.axis_index("cp")
        starts = pos
        inv_freq, pos, ids = (v[None, :] for v in (inv_freq, pos, tokens))
        base = tp * rows

        wo_half = side(w_o, cp)
        wo_1 = swap_core(wo_half, 0)
        picked, grad = pick_rows(tokens, table, base)
        x, query, key, value, cosine, sine, keys, d_hidden, key2, value2, act_a_all, dy_all = enter(picked, w_q, w_k, w_v, gain_one, pos, inv_freq, ids, dy, w_down)
        wo_1, wo_half, query = lax.optimization_barrier((wo_1, wo_half, query))
        wo_pieces = (w_o, wo_1, swap_core(wo_half, 1), swap_core(wo_1, 1))
        att, lse, grad = attend(scale, starts, query, key, value, key2, value2, pos, grad)
        keep_x, send_x, keep_y, send_y, act_b_all, hidden_all, d_gate_all, d_up_all, att_all, d_resid_all, d_resid, d_att, d_gain_b = middle(att, wo_pieces, x, w_gate, w_up, w_down, d_hidden, dy, gain_two)[1:]

        x_bit, y_bit = tp % 2, tp // 2
        ways = ((keep_x, swap_x, x_bit, swap_y, y_bit), (keep_y, swap_y, y_bit, swap_x, x_bit))
        y_wide = [swap_x(send_x), swap_y(send_y)]
        d_query, d_key, d_value, d_key2, d_value2, grad = attend_back(scale, starts, query, d_att, lse, key, value, key2, value2, pos, grad)

        d_x_all, gain_1, gain_2, grad_gate, grad_up, grad_down, *grads = leave(d_query, d_key, d_value, d_key2, d_value2, cosine, sine, w_q, w_k, w_v, x, d_resid, gain_one, d_gain_b, act_b_all, d_gate_all, d_up_all, hidden_all, dy_all, att_all, d_resid_all, act_a_all)[1:]
        y_wide, d_x_all = lax.optimization_barrier((y_wide, d_x_all))
        halves = lambda bit_2, keep, wide, flip: side(keep, flipped(bit_2, flip)) + side(wide, flipped(bit_2, flip))
        y_narrow = [swap_2(halves(bit_2, keep, wide, 1)) for (keep, _, _, swap_2, bit_2), wide in zip(ways, y_wide)]
        y_wide, grad_gate = lax.optimization_barrier((y_wide, grad_gate))
        grad_gate, grad_out, *grads = move(grad_gate, *grads)
        y_narrow, grad_gate = lax.optimization_barrier((y_narrow, grad_gate))
        y_own = [(halves(bit_2, keep, wide, 0) + narrow).astype(BF16) for (keep, _, _, _, bit_2), wide, narrow in zip(ways, y_wide, y_narrow)]
        y_pair = [join(own, swap_2(own), bit_2) for (_, _, _, swap_2, bit_2), own in zip(ways, y_own)]
        y_own, grad_down = lax.optimization_barrier((y_own, grad_down))
        (grad_down,) = move(grad_down)
        y_pair, grad_down = lax.optimization_barrier((y_pair, grad_down))
        y_far = [swap_1(pair) for (_, swap_1, _, _, _), pair in zip(ways, y_pair)]
        y_pair, d_x_all = lax.optimization_barrier((y_pair, d_x_all))
        grad_table, grad_up = put_rows(keys, d_x_all, grad, (grad_up,))
        y_rows = [jnp.where(bit_1 == k, pair, far) for (_, _, bit_1, _, _), pair, far in zip(ways, y_pair, y_far) for k in BOTH]
        return (jnp.concatenate(y_rows), grad_table, *grads, grad_out, grad_gate, grad_up, grad_down, gain_1[0], gain_2[0])

    col_spec = P(None, "tp")
    row_spec = P("tp", None)
    tok_spec = P("cp")
    rep_spec = P(None)
    in_specs = (tok_spec, tok_spec, tok_spec, P("cp", None), row_spec, col_spec, col_spec, col_spec, row_spec, col_spec, col_spec, row_spec, rep_spec, rep_spec, rep_spec)
    out_specs = (P("cp", None), row_spec, col_spec, col_spec, col_spec, row_spec, col_spec, col_spec, row_spec, rep_spec, rep_spec)
    return jax.shard_map(device_step, mesh=mesh, in_specs=in_specs, out_specs=out_specs, check_vma=False)
```
